32 devices in a mesh: ctx: 8 (over y, x, core), fsdp: 4 (over z).
Axes of the slice: x: 2, y: 2, z: 4, core: 2. Of those that a mesh axis runs over, the one named last changes fastest.
Arguments:
- block_input: bfloat16 [4, 2048, 1536], P('fsdp', 'ctx'), may hold values from -6 to 6
- block_table: int32 [4, 16], P('fsdp'), may hold values from 0 to 15, as said below
- output_grad: bfloat16 [4, 2048, 1536], P('fsdp', 'ctx'), may hold values from -6 to 6
- attention_gain: bfloat16 [1536], P('fsdp'), may hold values from 0.099609375 to 1.8984375
- query_weight: bfloat16 [1536, 1536], P('fsdp'), may hold values from -5 to 5
- key_weight: bfloat16 [1536, 768], P('fsdp'), may hold values from -1 to 1
- value_projection: bfloat16 [1536, 768], P('fsdp'), may hold values from -0.15625 to 0.15625
- output_weight: bfloat16 [1536, 1536], P('fsdp'), may hold values from -2.5 to 2.5
- feedforward_gain: bfloat16 [1536], P('fsdp'), may hold values from 0.099609375 to 1.8984375
- gate_weight: bfloat16 [1536, 4096], P('fsdp'), may hold values from -0.15625 to 0.15625
- up_weight: bfloat16 [1536, 4096], P('fsdp'), may hold values from -0.15625 to 0.15625
- down_weight: bfloat16 [4096, 1536], P('fsdp'), may hold values from -0.09375 to 0.09375
Outputs:
- layer_output: bfloat16 [4, 2048, 1536], P('fsdp', 'ctx')
- input_grad: float32 [4, 2048, 1536], P('fsdp', 'ctx')
- attention_gain_grad: float32 [1536], P('fsdp')
- query_weight_grad: float32 [1536, 1536], P('fsdp')
- key_weight_grad: float32 [1536, 768], P('fsdp')
- value_weight_grad: float32 [1536, 768], P('fsdp')
- output_weight_grad: float32 [1536, 1536], P('fsdp')
- feedforward_gain_grad: float32 [1536], P('fsdp')
- gate_weight_grad: float32 [1536, 4096], P('fsdp')
- up_weight_grad: float32 [1536, 4096], P('fsdp')
- down_weight_grad: float32 [4096, 1536], P('fsdp')
The draws below stay inside these ranges and needn't reach their ends.
Inputs may be any that keep to these rules, and one draw needn't show every extreme that they name: `block_table`: in every sequence, the two storage slots 2 c and 2 c + 1 hold the blocks p and 15 - p for some p, in either order, and every block stands in exactly one slot.
All inputs are finite; a program needn't handle non-finite values.
Results may differ from the reference program's by a relative error of at most 0.024.
Values may be sent and summed in bfloat16 or wider, within the bound.
A program may use at most 384 MiB of HBM per device.

```python
import math
import jax
import jax.numpy as jnp
from jax import lax

MODEL_WIDTH = 1536
QUERY_HEADS = 16
KEY_VALUE_HEADS = 8
HEAD_SIZE = 96
FF = 4096
TOK_DEV = 256
SEQS = 4
SEQLEN = 2048
SLOTS = 16


def query_key_pair(key):
    first_key_index = jax.random.fold_in(key, 11)
    key_portion = jnp.clip(jax.random.normal(jax.random.fold_in(first_key_index, 1), (MODEL_WIDTH, KEY_VALUE_HEADS * HEAD_SIZE), jnp.float32), -4.0, 4.0) * MODEL_WIDTH ** (-0.5)
    fresh_part = jnp.clip(jax.random.normal(jax.random.fold_in(first_key_index, 2), (MODEL_WIDTH, QUERY_HEADS * HEAD_SIZE), jnp.float32), -4.0, 4.0) * MODEL_WIDTH ** (-0.5)
    query_part = fresh_part
    return (query_part, key_portion)


def draw_query_weight(key, part):
    return query_key_pair(key)[0].astype(jnp.bfloat16)


def draw_key_weight(key, part):
    return query_key_pair(key)[1].astype(jnp.bfloat16)


def draw_block_table(key, part):
    row_keys = jax.random.split(jax.random.fold_in(key, 5), SEQS)

    def one_row(row_key):
        pair_order = jax.random.permutation(jax.random.fold_in(row_key, 1), SLOTS // 2)
        flips = jax.random.randint(jax.random.fold_in(row_key, 2), (SLOTS // 2,), 0, 2)
        mirror = SLOTS - 1 - pair_order
        lower_slot = jnp.where(flips == 1, mirror, pair_order)
        upper_slot = jnp.where(flips == 1, pair_order, mirror)
        return jnp.stack([lower_slot, upper_slot], axis=1).reshape(SLOTS).astype(jnp.int32)
    return jax.vmap(one_row)(row_keys)


def levels(own_key, shape, cuts, low, largest):
    gain, own = 1.0, jax.random.fold_in(own_key, 6)
    for axis_at, parts in cuts:
        draws = jnp.exp(jax.random.uniform(jax.random.fold_in(own, axis_at), (parts,), jnp.float32, low / len(cuts), largest / len(cuts)))
        gain = gain * jnp.repeat(draws, shape[axis_at] // parts).reshape([-1 if axis == axis_at else 1 for axis in range(len(shape))])
    return gain


def noise(own_key, extent, spread, limit, cuts=(), held_as=jnp.bfloat16):
    entries = jax.random.normal(own_key, extent, jnp.float32) * spread
    if len(cuts) > 0:
        entries = levels(own_key, extent, cuts, -0.22, 0.18) * entries
    return jnp.clip(entries, min=-limit, max=limit).astype(held_as)


def setup_inputs(seed: int = 0) -> dict:
    splits = jax.random.split(jax.random.key(seed), 13)
    return {
        "block_input": noise(splits[0], (SEQS, SEQLEN, MODEL_WIDTH), 1.0, 6.0, ((0, 4), (1, 8))),
        "block_table": draw_block_table(jax.random.fold_in(splits[12], 71), 0),
        "output_grad": noise(splits[2], (SEQS, SEQLEN, MODEL_WIDTH), 1.0, 6.0, ((0, 4), (1, 8))),
        "attention_gain": jnp.clip(1.0 + 0.18 * jax.random.normal(splits[3], (MODEL_WIDTH,), jnp.float32), 0.099609375, 1.8984375).astype(jnp.bfloat16),
        "query_weight": draw_query_weight(jax.random.fold_in(splits[12], 71), 0),
        "key_weight": draw_key_weight(jax.random.fold_in(splits[12], 71), 0),
        "value_projection": noise(splits[6], (MODEL_WIDTH, KEY_VALUE_HEADS * HEAD_SIZE), MODEL_WIDTH ** -0.5, 0.15625, ((0, 4),)),
        "output_weight": noise(splits[7], (QUERY_HEADS * HEAD_SIZE, MODEL_WIDTH), (max(1, QUERY_HEADS * HEAD_SIZE * 8 // SEQLEN)) ** -0.5, 2.5, ((0, 4),)),
        "feedforward_gain": jnp.clip(1.0 + 0.18 * jax.random.normal(splits[8], (MODEL_WIDTH,), jnp.float32), 0.099609375, 1.8984375).astype(jnp.bfloat16),
        "gate_weight": noise(splits[9], (MODEL_WIDTH, FF), MODEL_WIDTH ** -0.5, 0.15625, ((0, 4),)),
        "up_weight": noise(splits[10], (MODEL_WIDTH, FF), MODEL_WIDTH ** -0.5, 0.15625, ((0, 4),)),
        "down_weight": noise(splits[11], (FF, MODEL_WIDTH), FF ** -0.5, 0.09375, ((0, 4),)),
    }


norm_epsilon = 1e-05
rotary_base = 100000.0
score_with_mask = -1e+30

def round_half(value_rows):
    return lax.optimization_barrier(value_rows.astype(jnp.bfloat16))

def rope_tables(positions):
    half_width = HEAD_SIZE // 2
    steps_index = jnp.arange(half_width, dtype=jnp.float32)
    inverse = jnp.exp(steps_index * jnp.float32(-2.0 * math.log(rotary_base) / HEAD_SIZE))
    angles = positions.astype(jnp.float32)[:, None] * inverse[None, :]
    return (jnp.cos(angles), jnp.sin(angles))

def rotate(value_rows, cosine, sine_values, direction):
    count_of_rows = value_rows.shape[0]
    head_count = value_rows.shape[1] // HEAD_SIZE
    half_width = HEAD_SIZE // 2
    shaped = value_rows.reshape(count_of_rows, head_count, HEAD_SIZE)
    first_half = shaped[:, :, :half_width]
    second_half = shaped[:, :, half_width:]
    cos_part = cosine[:, None, :]
    sin_part = sine_values[:, None, :] * direction
    turned = jnp.concatenate([first_half * cos_part - second_half * sin_part, second_half * cos_part + first_half * sin_part], axis=2)
    return turned.reshape(count_of_rows, head_count * HEAD_SIZE)

def norm_scale(value_rows):
    return lax.rsqrt(lax.optimization_barrier(jnp.mean(value_rows * value_rows, axis=-1, keepdims=True)) + norm_epsilon)

def product(matrix, operand):
    return jnp.dot(matrix, operand, preferred_element_type=jnp.float32)

def cross_rows(matrix, operand):
    return lax.dot_general(matrix, operand, (((0,), (0,)), ((), ())), preferred_element_type=jnp.float32)

def back_product(matrix, operand):
    return lax.dot_general(matrix, operand, (((1,), (1,)), ((), ())), preferred_element_type=jnp.float32)

def block_scores(block_of_queries, key_rows, query_positions, key_positions):
    query_rank_four = block_of_queries.astype(jnp.float32).reshape(block_of_queries.shape[0], KEY_VALUE_HEADS, QUERY_HEADS // KEY_VALUE_HEADS, HEAD_SIZE)
    keys_rank_three = key_rows.astype(jnp.float32).reshape(key_rows.shape[0], KEY_VALUE_HEADS, HEAD_SIZE)
    scores = jnp.einsum('rgjd,kgd->gjrk', query_rank_four, keys_rank_three, precision=lax.Precision.HIGHEST) * HEAD_SIZE ** (-0.5)
    allowed = (key_positions[None, :] <= query_positions[:, None])[None, None]
    return (jnp.where(allowed, scores, score_with_mask), allowed, query_rank_four, keys_rank_three)

def attend_forward(query_rows, key_rows, value_rows, positions):
    sequence_length = query_rows.shape[0]
    query_block_pass = TOK_DEV
    values_rank_three = value_rows.astype(jnp.float32).reshape(sequence_length, KEY_VALUE_HEADS, HEAD_SIZE)

    def forward_step(state_now, block_index):
        first_row = block_index * query_block_pass
        block_of_queries = lax.dynamic_slice_in_dim(query_rows, first_row, query_block_pass, 0)
        query_positions = lax.dynamic_slice_in_dim(positions, first_row, query_block_pass, 0)
        masked, allowed, query_rank_four, keys_rank_three = block_scores(block_of_queries, key_rows, query_positions, positions)
        row_peak = lax.optimization_barrier(jnp.max(masked, axis=-1))
        row_total = lax.optimization_barrier(jnp.sum(jnp.where(allowed, jnp.exp(masked - row_peak[..., None]), 0.0), axis=-1))
        log_total = row_peak + jnp.log(row_total)
        weights_half = round_half(jnp.where(allowed, jnp.exp(masked - log_total[..., None]), 0.0))
        output = jnp.einsum('gjrk,kgd->rgjd', weights_half.astype(jnp.float32), values_rank_three, precision=lax.Precision.HIGHEST)
        return (state_now, (round_half(output.reshape(query_block_pass, QUERY_HEADS * HEAD_SIZE)), log_total))
    unused, (outputs, log_totals) = lax.scan(forward_step, None, jnp.arange(sequence_length // query_block_pass, dtype=jnp.int32))
    return (outputs.reshape(sequence_length, QUERY_HEADS * HEAD_SIZE), log_totals)

def attend_backward(query_rows, key_rows, value_rows, positions, attended_rows, log_totals, attended_gradient):
    sequence_length = query_rows.shape[0]
    query_block_pass = TOK_DEV
    query_group_width = QUERY_HEADS // KEY_VALUE_HEADS
    values_rank_three = value_rows.astype(jnp.float32).reshape(sequence_length, KEY_VALUE_HEADS, HEAD_SIZE)

    def backward_step(state_now, block_data):
        block_index, log_total = block_data
        first_row = block_index * query_block_pass
        block_of_queries = lax.dynamic_slice_in_dim(query_rows, first_row, query_block_pass, 0)
        query_positions = lax.dynamic_slice_in_dim(positions, first_row, query_block_pass, 0)
        block_gradient = lax.dynamic_slice_in_dim(attended_gradient, first_row, query_block_pass, 0)
        output_block = lax.dynamic_slice_in_dim(attended_rows, first_row, query_block_pass, 0)
        masked, allowed, query_rank_four, keys_rank_three = block_scores(block_of_queries, key_rows, query_positions, positions)
        weights_half = round_half(jnp.where(allowed, jnp.exp(masked - log_total[..., None]), 0.0)).astype(jnp.float32)
        gradient_rank_four = block_gradient.astype(jnp.float32).reshape(query_block_pass, KEY_VALUE_HEADS, query_group_width, HEAD_SIZE)
        output_rank_four = output_block.astype(jnp.float32).reshape(query_block_pass, KEY_VALUE_HEADS, query_group_width, HEAD_SIZE)
        row_delta = jnp.transpose(lax.optimization_barrier(jnp.sum(gradient_rank_four * output_rank_four, axis=-1)), (1, 2, 0))
        grad_weights = jnp.einsum('rgjd,kgd->gjrk', gradient_rank_four, values_rank_three, precision=lax.Precision.HIGHEST)
        grad_scores = round_half(weights_half * (grad_weights - row_delta[..., None]) * HEAD_SIZE ** (-0.5)).astype(jnp.float32)
        grad_query = jnp.einsum('gjrk,kgd->rgjd', grad_scores, keys_rank_three, precision=lax.Precision.HIGHEST)
        key_gradient_total, value_gradient_total = state_now
        key_portion = round_half(jnp.einsum('gjrk,rgjd->kgd', grad_scores, query_rank_four, precision=lax.Precision.HIGHEST))
        value_part = round_half(jnp.einsum('gjrk,rgjd->kgd', weights_half, gradient_rank_four, precision=lax.Precision.HIGHEST))
        key_gradient_total = key_gradient_total + key_portion.astype(jnp.float32)
        value_gradient_total = value_gradient_total + value_part.astype(jnp.float32)
        return ((key_gradient_total, value_gradient_total), grad_query.reshape(query_block_pass, QUERY_HEADS * HEAD_SIZE))
    empty_gradient_total = jnp.zeros((sequence_length, KEY_VALUE_HEADS, HEAD_SIZE), jnp.float32)
    block_ids = jnp.arange(sequence_length // query_block_pass, dtype=jnp.int32)
    (key_gradient_total, value_gradient_total), query_gradients = lax.scan(backward_step, (empty_gradient_total, empty_gradient_total), (block_ids, log_totals))
    return (query_gradients.reshape(sequence_length, QUERY_HEADS * HEAD_SIZE), key_gradient_total.reshape(sequence_length, KEY_VALUE_HEADS * HEAD_SIZE), value_gradient_total.reshape(sequence_length, KEY_VALUE_HEADS * HEAD_SIZE))

def layer_sequence(block_row, table_row, grad_row, weights):
    attention_gain, query_weight, key_weight, value_projection, output_weight, feedforward_gain, gate_weight, up_weight, down_weight = weights
    sequence_length = block_row.shape[0]
    block_rows = sequence_length // table_row.shape[0]
    offsets = jnp.arange(block_rows, dtype=jnp.int32)
    positions = (table_row[:, None] * block_rows + offsets[None, :]).reshape(sequence_length).astype(jnp.int32)
    cosine, sine_values = rope_tables(positions)
    inputs = block_row.astype(jnp.float32)
    scale_one = norm_scale(inputs)
    normed_one = inputs * scale_one
    gained_one = round_half(normed_one * attention_gain.astype(jnp.float32))
    query_rows = round_half(rotate(product(gained_one, query_weight), cosine, sine_values, 1.0))
    key_rows = round_half(rotate(product(gained_one, key_weight), cosine, sine_values, 1.0))
    value_rows = round_half(product(gained_one, value_projection))
    attended_rows, log_totals = attend_forward(query_rows, key_rows, value_rows, positions)
    residual = inputs + product(attended_rows, output_weight)
    scale_two = norm_scale(residual)
    normed_two = residual * scale_two
    gained_two = round_half(normed_two * feedforward_gain.astype(jnp.float32))
    gate_values = product(gained_two, gate_weight)
    up_values = product(gained_two, up_weight)
    sigmoid_gate = jax.nn.sigmoid(gate_values)
    activated = gate_values * sigmoid_gate
    hidden_act = round_half(activated * up_values)
    layer_output = (residual + product(hidden_act, down_weight)).astype(jnp.bfloat16)
    grad_hidden = back_product(grad_row, down_weight)
    down_term = cross_rows(hidden_act, grad_row)
    grad_gate = round_half(grad_hidden * up_values * sigmoid_gate * (1.0 + gate_values * (1.0 - sigmoid_gate)))
    grad_up = round_half(grad_hidden * activated)
    gate_term = cross_rows(gained_two, grad_gate)
    up_term = cross_rows(gained_two, grad_up)
    grad_normed_two = back_product(grad_gate, gate_weight) + back_product(grad_up, up_weight)
    feedforward_term = lax.optimization_barrier(jnp.sum(grad_normed_two * normed_two, axis=0))
    grad_scaled_two = grad_normed_two * feedforward_gain.astype(jnp.float32)
    grad_residual = grad_row.astype(jnp.float32) + scale_two * (grad_scaled_two - normed_two * lax.optimization_barrier(jnp.mean(grad_scaled_two * normed_two, axis=-1, keepdims=True)))
    grad_attn = round_half(grad_residual)
    output_term = cross_rows(attended_rows, grad_attn)
    attended_gradient = round_half(back_product(grad_attn, output_weight))
    query_raw, key_raw, value_raw = attend_backward(query_rows, key_rows, value_rows, positions, attended_rows, log_totals, attended_gradient)
    query_gradients = round_half(rotate(query_raw, cosine, sine_values, -1.0))
    grad_keys = round_half(rotate(key_raw, cosine, sine_values, -1.0))
    grad_values = round_half(value_raw)
    query_term = cross_rows(gained_one, query_gradients)
    key_term = cross_rows(gained_one, grad_keys)
    value_term = cross_rows(gained_one, grad_values)
    grad_normed_one = back_product(query_gradients, query_weight) + back_product(grad_keys, key_weight) + back_product(grad_values, value_projection)
    attention_term = lax.optimization_barrier(jnp.sum(grad_normed_one * normed_one, axis=0))
    grad_scaled_one = grad_normed_one * attention_gain.astype(jnp.float32)
    input_grad = grad_residual + scale_one * (grad_scaled_one - normed_one * lax.optimization_barrier(jnp.mean(grad_scaled_one * normed_one, axis=-1, keepdims=True)))
    terms = (attention_term, query_term, key_term, value_term, output_term, feedforward_term, gate_term, up_term, down_term)
    return ((layer_output, input_grad), terms)

def reference(block_input, block_table, output_grad, attention_gain, query_weight, key_weight, value_projection, output_weight, feedforward_gain, gate_weight, up_weight, down_weight):
    weights = (attention_gain, query_weight, key_weight, value_projection, output_weight, feedforward_gain, gate_weight, up_weight, down_weight)
    zero_terms = tuple((jnp.zeros(weight_array.shape, jnp.float32) for weight_array in weights))

    def sequence_step(state_now, sequence_data):
        block_row, table_row, grad_row = sequence_data
        outputs, terms = layer_sequence(block_row, table_row, grad_row, weights)
        return (tuple((earlier + latest for earlier, latest in zip(state_now, terms))), outputs)
    totals, (layer_output, input_grad) = lax.scan(sequence_step, zero_terms, (block_input, block_table, output_grad))
    return (layer_output, input_grad, totals[0], totals[1], totals[2], totals[3], totals[4], totals[5], totals[6], totals[7], totals[8])
```

```python
import functools
import math

import jax
import jax.numpy as jnp
from jax import lax
from jax.experimental import pallas as pl
from jax.experimental.pallas import tpu as pltpu
from jax.sharding import PartitionSpec as P

QUERY_HEADS = 16
KEY_VALUE_HEADS = 8
HEAD_SIZE = 96


norm_epsilon = 1e-05
rotary_base = 100000.0
score_with_mask = -1e30


def rope_tables(positions):
    half_width = HEAD_SIZE // 2
    steps_index = jnp.arange(half_width, dtype=jnp.float32)
    inverse = jnp.exp(steps_index * jnp.float32(-2.0 * math.log(rotary_base) / HEAD_SIZE))
    angles = positions.astype(jnp.float32)[:, None] * inverse[None, :]
    return (jnp.cos(angles), jnp.sin(angles))


def rotate(value_rows, cosine, sine_values, direction):
    count_of_rows = value_rows.shape[0]
    head_count = value_rows.shape[1] // HEAD_SIZE
    half_width = HEAD_SIZE // 2
    shaped = value_rows.reshape(count_of_rows, head_count, HEAD_SIZE)
    first_half = shaped[:, :, :half_width]
    second_half = shaped[:, :, half_width:]
    cos_part = cosine[:, None, :]
    sin_part = sine_values[:, None, :] * direction
    turned = jnp.concatenate(
        [
            first_half * cos_part - second_half * sin_part,
            second_half * cos_part + first_half * sin_part,
        ],
        axis=2,
    )
    return turned.reshape(count_of_rows, head_count * HEAD_SIZE)


def norm_scale(value_rows):
    return lax.rsqrt(jnp.mean(value_rows * value_rows, axis=-1, keepdims=True) + norm_epsilon)


def product(matrix, operand):
    return jnp.dot(matrix, operand, preferred_element_type=jnp.float32)


def cross_rows(matrix, operand):
    return lax.dot_general(
        matrix, operand, (((0,), (0,)), ((), ())), preferred_element_type=jnp.float32
    )


def back_product(matrix, operand):
    return lax.dot_general(
        matrix, operand, (((1,), (1,)), ((), ())), preferred_element_type=jnp.float32
    )


def block_scores(query_rank_four, block_of_keys, query_positions, key_positions):
    keys_rank_three = block_of_keys.reshape(block_of_keys.shape[0], KEY_VALUE_HEADS, HEAD_SIZE)
    scores = jnp.einsum(
        "rgjd,kgd->gjrk", query_rank_four, keys_rank_three, preferred_element_type=jnp.float32
    ) * HEAD_SIZE ** (-0.5)
    allowed = (key_positions[None, :] <= query_positions[:, None])[None, None]
    return (jnp.where(allowed, scores, score_with_mask), allowed)


def local(
    block_input,
    block_table,
    output_grad,
    attention_gain,
    query_weight,
    key_weight,
    value_projection,
    output_weight,
    feedforward_gain,
    gate_weight,
    up_weight,
    down_weight,
):
    query_group_width = QUERY_HEADS // KEY_VALUE_HEADS
    score_scale = HEAD_SIZE ** (-0.5)
    inputs = block_input[0].astype(jnp.float32)
    count_of_rows = inputs.shape[0]
    block_rows = count_of_rows // 2
    ctx_index = lax.axis_index("ctx")
    table_row = block_table[0]
    offsets = jnp.arange(block_rows, dtype=jnp.int32)
    query_blocks = lax.dynamic_slice_in_dim(table_row, 2 * ctx_index, 2)
    query_positions = (query_blocks[:, None] * block_rows + offsets[None, :]).reshape(count_of_rows)
    key_positions = (table_row[:, None] * block_rows + offsets[None, :]).reshape(-1)
    cosine, sine_values = rope_tables(query_positions)
    gain_one, query_full, key_full, value_full, out_full = (
        lax.all_gather(attention_gain, "fsdp", axis=0, tiled=True),
        lax.all_gather(query_weight, "fsdp", axis=0, tiled=True),
        lax.all_gather(key_weight, "fsdp", axis=0, tiled=True),
        lax.all_gather(value_projection, "fsdp", axis=0, tiled=True),
        lax.all_gather(output_weight, "fsdp", axis=0, tiled=True),
    )
    scale_one = norm_scale(inputs)
    normed_one = inputs * scale_one
    gained_one = (normed_one * gain_one.astype(jnp.float32)).astype(jnp.bfloat16)
    query_rows = rotate(product(gained_one, query_full), cosine, sine_values, 1.0).astype(
        jnp.bfloat16
    )
    keys_local = rotate(product(gained_one, key_full), cosine, sine_values, 1.0).astype(
        jnp.bfloat16
    )
    values_local = product(gained_one, value_full).astype(jnp.bfloat16)
    keys_all, values_all = (
        lax.all_gather(keys_local, "ctx", axis=0, tiled=True),
        lax.all_gather(values_local, "ctx", axis=0, tiled=True),
    )
    key_total_count = keys_all.shape[0]
    key_block_pass = 1024
    block_count = key_total_count // key_block_pass
    query_rank_four = query_rows.reshape(
        count_of_rows, KEY_VALUE_HEADS, query_group_width, HEAD_SIZE
    )
    key_places = key_positions.reshape(block_count, key_block_pass)

    def split_keys(array_in):
        return array_in.reshape(block_count, key_block_pass, array_in.shape[-1])

    def statistics_step(state_now, block_data):
        running_max, running_sum = state_now
        block_of_keys, key_place = block_data
        masked, allowed = block_scores(query_rank_four, block_of_keys, query_positions, key_place)
        new_max = jnp.maximum(running_max, jnp.max(masked, axis=-1))
        block_sum = jnp.sum(jnp.where(allowed, jnp.exp(masked - new_max[..., None]), 0.0), axis=-1)
        return ((new_max, running_sum * jnp.exp(running_max - new_max) + block_sum), None)

    initial_maximum = jnp.full(
        (KEY_VALUE_HEADS, query_group_width, count_of_rows), score_with_mask, jnp.float32
    )
    initial_sum = jnp.zeros((KEY_VALUE_HEADS, query_group_width, count_of_rows), jnp.float32)
    (final_max, final_sum), unused = lax.scan(
        statistics_step, (initial_maximum, initial_sum), (split_keys(keys_all), key_places)
    )
    log_total = final_max + jnp.log(final_sum)

    def output_step(state_now, block_data):
        block_of_keys, block_of_values, key_place = block_data
        masked, allowed = block_scores(query_rank_four, block_of_keys, query_positions, key_place)
        weights_half = jnp.where(allowed, jnp.exp(masked - log_total[..., None]), 0.0).astype(
            jnp.bfloat16
        )
        values_rank_three = block_of_values.reshape(key_block_pass, KEY_VALUE_HEADS, HEAD_SIZE)
        return (
            state_now
            + jnp.einsum(
                "gjrk,kgd->rgjd",
                weights_half,
                values_rank_three,
                preferred_element_type=jnp.float32,
            ),
            None,
        )

    initial_output = jnp.zeros(
        (count_of_rows, KEY_VALUE_HEADS, query_group_width, HEAD_SIZE), jnp.float32
    )
    summed_out, unused = lax.scan(
        output_step, initial_output, (split_keys(keys_all), split_keys(values_all), key_places)
    )
    attended_rows = summed_out.reshape(count_of_rows, QUERY_HEADS * HEAD_SIZE).astype(jnp.bfloat16)
    residual = inputs + product(attended_rows, out_full)
    scale_two = norm_scale(residual)
    normed_two = residual * scale_two
    gain_two, gate_full, up_full, down_full = (
        lax.all_gather(feedforward_gain, "fsdp", axis=0, tiled=True),
        lax.all_gather(gate_weight, "fsdp", axis=0, tiled=True),
        lax.all_gather(up_weight, "fsdp", axis=0, tiled=True),
        lax.all_gather(down_weight, "fsdp", axis=0, tiled=True),
    )
    gained_two = (normed_two * gain_two.astype(jnp.float32)).astype(jnp.bfloat16)
    gate_values = product(gained_two, gate_full)
    up_values = product(gained_two, up_full)
    sigmoid_gate = jax.nn.sigmoid(gate_values)
    activated = gate_values * sigmoid_gate
    hidden_act = (activated * up_values).astype(jnp.bfloat16)
    layer_output = (residual + product(hidden_act, down_full)).astype(jnp.bfloat16)
    gain_two_again, gate_back, up_back, down_back = (
        lax.all_gather(feedforward_gain, "fsdp", axis=0, tiled=True),
        lax.all_gather(gate_weight, "fsdp", axis=0, tiled=True),
        lax.all_gather(up_weight, "fsdp", axis=0, tiled=True),
        lax.all_gather(down_weight, "fsdp", axis=0, tiled=True),
    )
    grad_rows = output_grad[0]
    grad_hidden = back_product(grad_rows, down_back)
    down_term = cross_rows(hidden_act, grad_rows)
    grad_gate = (
        grad_hidden * up_values * sigmoid_gate * (1.0 + gate_values * (1.0 - sigmoid_gate))
    ).astype(jnp.bfloat16)
    grad_up = (grad_hidden * activated).astype(jnp.bfloat16)
    gate_term = cross_rows(gained_two, grad_gate)
    up_term = cross_rows(gained_two, grad_up)
    grad_normed_two = back_product(grad_gate, gate_back) + back_product(grad_up, up_back)
    feedforward_term = jnp.sum(grad_normed_two * normed_two, axis=0)
    grad_scaled_two = grad_normed_two * gain_two_again.astype(jnp.float32)
    grad_residual = grad_rows.astype(jnp.float32) + scale_two * (
        grad_scaled_two
        - normed_two * jnp.mean(grad_scaled_two * normed_two, axis=-1, keepdims=True)
    )
    gain_one_again, query_back, key_back, value_back, out_back = (
        lax.all_gather(attention_gain, "fsdp", axis=0, tiled=True),
        lax.all_gather(query_weight, "fsdp", axis=0, tiled=True),
        lax.all_gather(key_weight, "fsdp", axis=0, tiled=True),
        lax.all_gather(value_projection, "fsdp", axis=0, tiled=True),
        lax.all_gather(output_weight, "fsdp", axis=0, tiled=True),
    )
    grad_attn = grad_residual.astype(jnp.bfloat16)
    output_term = cross_rows(attended_rows, grad_attn)
    attended_gradient = back_product(grad_attn, out_back).astype(jnp.bfloat16)
    gradient_rank_four = attended_gradient.reshape(
        count_of_rows, KEY_VALUE_HEADS, query_group_width, HEAD_SIZE
    )
    attended_rank_four = attended_rows.reshape(
        count_of_rows, KEY_VALUE_HEADS, query_group_width, HEAD_SIZE
    )
    row_delta = jnp.transpose(
        jnp.sum(
            gradient_rank_four.astype(jnp.float32) * attended_rank_four.astype(jnp.float32), axis=-1
        ),
        (1, 2, 0),
    )
    keys_again, values_again = (
        lax.all_gather(keys_local, "ctx", axis=0, tiled=True),
        lax.all_gather(values_local, "ctx", axis=0, tiled=True),
    )

    def back_step(state_now, block_data):
        block_of_keys, block_of_values, key_place = block_data
        masked, allowed = block_scores(query_rank_four, block_of_keys, query_positions, key_place)
        weights_half = jnp.where(allowed, jnp.exp(masked - log_total[..., None]), 0.0).astype(
            jnp.bfloat16
        )
        values_rank_three = block_of_values.reshape(key_block_pass, KEY_VALUE_HEADS, HEAD_SIZE)
        keys_rank_three = block_of_keys.reshape(key_block_pass, KEY_VALUE_HEADS, HEAD_SIZE)
        grad_weights = jnp.einsum(
            "rgjd,kgd->gjrk",
            gradient_rank_four,
            values_rank_three,
            preferred_element_type=jnp.float32,
        )
        grad_scores = (
            weights_half.astype(jnp.float32) * (grad_weights - row_delta[..., None]) * score_scale
        ).astype(jnp.bfloat16)
        state_now = state_now + jnp.einsum(
            "gjrk,kgd->rgjd", grad_scores, keys_rank_three, preferred_element_type=jnp.float32
        )
        key_gradient = jnp.einsum(
            "gjrk,rgjd->kgd", grad_scores, query_rank_four, preferred_element_type=jnp.float32
        )
        value_gradient = jnp.einsum(
            "gjrk,rgjd->kgd", weights_half, gradient_rank_four, preferred_element_type=jnp.float32
        )
        return (
            state_now,
            (
                key_gradient.reshape(key_block_pass, KEY_VALUE_HEADS * HEAD_SIZE).astype(
                    jnp.bfloat16
                ),
                value_gradient.reshape(key_block_pass, KEY_VALUE_HEADS * HEAD_SIZE).astype(
                    jnp.bfloat16
                ),
            ),
        )

    first_query_index = jnp.zeros(
        (count_of_rows, KEY_VALUE_HEADS, query_group_width, HEAD_SIZE), jnp.float32
    )
    query_sum, (key_gradients, value_gradients) = lax.scan(
        back_step, first_query_index, (split_keys(keys_again), split_keys(values_again), key_places)
    )
    key_gradients = key_gradients.reshape(key_total_count, KEY_VALUE_HEADS * HEAD_SIZE)
    value_gradients = value_gradients.reshape(key_total_count, KEY_VALUE_HEADS * HEAD_SIZE)
    key_sums, value_sums = (
        lax.psum_scatter(key_gradients, "ctx", scatter_dimension=0, tiled=True).astype(jnp.float32),
        lax.psum_scatter(value_gradients, "ctx", scatter_dimension=0, tiled=True).astype(
            jnp.float32
        ),
    )
    query_gradients = rotate(
        query_sum.reshape(count_of_rows, QUERY_HEADS * HEAD_SIZE), cosine, sine_values, -1.0
    ).astype(jnp.bfloat16)
    grad_keys = rotate(key_sums, cosine, sine_values, -1.0).astype(jnp.bfloat16)
    grad_values = value_sums.astype(jnp.bfloat16)
    query_term = cross_rows(gained_one, query_gradients)
    key_term = cross_rows(gained_one, grad_keys)
    value_term = cross_rows(gained_one, grad_values)
    grad_normed_one = (
        back_product(query_gradients, query_back)
        + back_product(grad_keys, key_back)
        + back_product(grad_values, value_back)
    )
    attention_term = jnp.sum(grad_normed_one * normed_one, axis=0)
    grad_scaled_one = grad_normed_one * gain_one_again.astype(jnp.float32)
    input_grad = grad_residual + scale_one * (
        grad_scaled_one
        - normed_one * jnp.mean(grad_scaled_one * normed_one, axis=-1, keepdims=True)
    )
    shares = (
        lax.psum_scatter(
            attention_term.astype(jnp.bfloat16), "fsdp", scatter_dimension=0, tiled=True
        ).astype(jnp.float32),
        lax.psum_scatter(
            query_term.astype(jnp.bfloat16), "fsdp", scatter_dimension=0, tiled=True
        ).astype(jnp.float32),
        lax.psum_scatter(
            key_term.astype(jnp.bfloat16), "fsdp", scatter_dimension=0, tiled=True
        ).astype(jnp.float32),
        lax.psum_scatter(
            value_term.astype(jnp.bfloat16), "fsdp", scatter_dimension=0, tiled=True
        ).astype(jnp.float32),
        lax.psum_scatter(
            output_term.astype(jnp.bfloat16), "fsdp", scatter_dimension=0, tiled=True
        ).astype(jnp.float32),
        lax.psum_scatter(
            feedforward_term.astype(jnp.bfloat16), "fsdp", scatter_dimension=0, tiled=True
        ).astype(jnp.float32),
        lax.psum_scatter(
            gate_term.astype(jnp.bfloat16), "fsdp", scatter_dimension=0, tiled=True
        ).astype(jnp.float32),
        lax.psum_scatter(
            up_term.astype(jnp.bfloat16), "fsdp", scatter_dimension=0, tiled=True
        ).astype(jnp.float32),
        lax.psum_scatter(
            down_term.astype(jnp.bfloat16), "fsdp", scatter_dimension=0, tiled=True
        ).astype(jnp.float32),
    )
    totals = (
        lax.psum(shares[0].astype(jnp.bfloat16), "ctx").astype(jnp.float32),
        lax.psum(shares[1].astype(jnp.bfloat16), "ctx").astype(jnp.float32),
        lax.psum(shares[2].astype(jnp.bfloat16), "ctx").astype(jnp.float32),
        lax.psum(shares[3].astype(jnp.bfloat16), "ctx").astype(jnp.float32),
        lax.psum(shares[4].astype(jnp.bfloat16), "ctx").astype(jnp.float32),
        lax.psum(shares[5].astype(jnp.bfloat16), "ctx").astype(jnp.float32),
        lax.psum(shares[6].astype(jnp.bfloat16), "ctx").astype(jnp.float32),
        lax.psum(shares[7].astype(jnp.bfloat16), "ctx").astype(jnp.float32),
        lax.psum(shares[8].astype(jnp.bfloat16), "ctx").astype(jnp.float32),
    )
    return (
        layer_output[None],
        input_grad[None],
        totals[0],
        totals[1],
        totals[2],
        totals[3],
        totals[4],
        totals[5],
        totals[6],
        totals[7],
        totals[8],
    )


LANES = 128
HALF = HEAD_SIZE // 2
GROUP = QUERY_HEADS // KEY_VALUE_HEADS
score_scale = HEAD_SIZE ** (-0.5)


def pad_head(columns):
    rows, heads = columns.shape[0], columns.shape[1] // HEAD_SIZE
    halves = columns.reshape(rows, heads, 2, HALF)
    return jnp.pad(halves, ((0, 0), (0, 0), (0, 0), (0, LANES // 2 - HALF))).reshape(
        rows, heads * LANES
    )


def unpad_head(columns):
    rows, heads = columns.shape[0], columns.shape[1] // LANES
    halves = columns.reshape(rows, heads, 2, LANES // 2)
    return halves[:, :, :, :HALF].reshape(rows, heads * HEAD_SIZE)


def contract(left, right, left_dim, right_dim):
    return lax.dot_general(
        left, right, (((left_dim,), (right_dim,)), ((), ())), preferred_element_type=jnp.float32
    )


def turn(value, cosine, sine):
    heads = value.shape[1] // LANES
    parts = []
    for head in range(heads):
        part = value[:, head * LANES : (head + 1) * LANES]
        parts.append(part * cosine + pltpu.roll(part, LANES // 2, 1) * sine)
    return parts[0] if heads == 1 else jnp.concatenate(parts, axis=1)


def forward_kernel(block, tile, slot_ref, q_ref, k_ref, v_ref, o_ref, lse_ref, qs, ks, vt, s_ref):
    rows = q_ref.shape[0]
    tiles = rows // tile
    per_tile = tile // block
    width = GROUP * tile

    def place(index, carry):
        source = pl.ds(pl.multiple_of(slot_ref[index] * block, block), block)
        target = pl.ds(pl.multiple_of(index * block, block), block)
        for head in range(GROUP):
            at = pl.multiple_of(
                (index // per_tile) * width + head * tile + (index % per_tile) * block, block
            )
            qs[pl.ds(at, block), :] = q_ref[source, head * LANES : (head + 1) * LANES]
        ks[target, :] = k_ref[source, :]
        vt[:, target] = v_ref[source, :].T
        return carry

    lax.fori_loop(0, rows // block, place, 0)
    key_at = lax.broadcasted_iota(jnp.int32, (tile, width), 0)
    query_at = lax.rem(lax.broadcasted_iota(jnp.int32, (tile, width), 1), tile)
    diagonal = key_at <= query_at

    def one_tile(index, carry):
        queries = qs[pl.ds(pl.multiple_of(index * width, width), width), :]

        def scores_of(step):
            keys = ks[pl.ds(pl.multiple_of(step * tile, tile), tile), :]
            return contract(keys, queries, 1, 1) * score_scale

        last = jnp.where(diagonal, scores_of(index), score_with_mask)
        s_ref[pl.ds(pl.multiple_of(index * tile, tile), tile), :] = last
        peak = jnp.max(last, axis=0, keepdims=True)

        def first_pass(step, peak):
            scores = scores_of(step)
            s_ref[pl.ds(pl.multiple_of(step * tile, tile), tile), :] = scores
            return jnp.maximum(peak, jnp.max(scores, axis=0, keepdims=True))

        peak = lax.fori_loop(0, index, first_pass, peak)

        def second_pass(step, state):
            total, out = state
            at = pl.ds(pl.multiple_of(step * tile, tile), tile)
            probs = jnp.exp(s_ref[at, :] - peak)
            total = total + jnp.sum(probs, axis=0, keepdims=True)
            out = out + contract(vt[:, at], probs.astype(jnp.bfloat16), 1, 0)
            return (total, out)

        total, out = lax.fori_loop(
            0,
            index + 1,
            second_pass,
            (jnp.zeros((1, width), jnp.float32), jnp.zeros((LANES, width), jnp.float32)),
        )
        lse_ref[pl.ds(index, 1), :] = peak + jnp.log(total)
        out = (out * (1.0 / total)).T.astype(jnp.bfloat16)
        for part in range(per_tile):
            target = pl.ds(pl.multiple_of(slot_ref[index * per_tile + part] * block, block), block)
            for head in range(GROUP):
                at = head * tile + part * block
                o_ref[target, head * LANES : (head + 1) * LANES] = out[at : at + block, :]
        return carry

    lax.fori_loop(0, tiles, one_tile, 0)


def backward_kernel(
    block,
    tile,
    slot_ref,
    q_ref,
    k_ref,
    v_ref,
    o_ref,
    g_ref,
    lse_ref,
    dq_ref,
    dk_ref,
    dv_ref,
    qs,
    ks,
    vs,
    kt,
    gs,
    os,
    dk,
    dv,
):
    rows = q_ref.shape[0]
    tiles = rows // tile
    per_tile = tile // block
    width = GROUP * tile

    def place(index, carry):
        source = pl.ds(pl.multiple_of(slot_ref[index] * block, block), block)
        target = pl.ds(pl.multiple_of(index * block, block), block)
        for head in range(GROUP):
            at = pl.multiple_of(
                (index // per_tile) * width + head * tile + (index % per_tile) * block, block
            )
            at = pl.ds(at, block)
            lanes = slice(head * LANES, (head + 1) * LANES)
            qs[at, :] = q_ref[source, lanes]
            gs[at, :] = g_ref[source, lanes]
            os[at, :] = o_ref[source, lanes]
        ks[target, :] = k_ref[source, :]
        vs[target, :] = v_ref[source, :]
        kt[:, target] = k_ref[source, :].T
        return carry

    lax.fori_loop(0, rows // block, place, 0)
    dk[...] = jnp.zeros_like(dk)
    dv[...] = jnp.zeros_like(dv)
    key_at = lax.broadcasted_iota(jnp.int32, (tile, width), 0)
    query_at = lax.rem(lax.broadcasted_iota(jnp.int32, (tile, width), 1), tile)
    diagonal = key_at <= query_at

    def one_tile(index, carry):
        here = pl.ds(pl.multiple_of(index * width, width), width)
        queries = qs[here, :]
        grads = gs[here, :]
        products = grads.astype(jnp.float32) * os[here, :].astype(jnp.float32)
        delta = jnp.sum(products.T, axis=0, keepdims=True)
        lse = lse_ref[pl.ds(index, 1), :]

        def piece(step, masked):
            at = pl.ds(pl.multiple_of(step * tile, tile), tile)
            scores = contract(ks[at, :], queries, 1, 1) * score_scale
            probs = jnp.exp(scores - lse)
            if masked:
                probs = jnp.where(diagonal, probs, 0.0)
            probs = probs.astype(jnp.bfloat16)
            dv[at, :] += contract(probs, grads, 1, 0)
            grad_probs = contract(vs[at, :], grads, 1, 1)
            grad_scores = (probs.astype(jnp.float32) * (grad_probs - delta) * score_scale).astype(
                jnp.bfloat16
            )
            dk[at, :] += contract(grad_scores, queries, 1, 0)
            return contract(kt[:, at], grad_scores, 1, 0)

        dq = piece(index, True)
        dq = lax.fori_loop(0, index, lambda step, total: total + piece(step, False), dq)
        dq = dq.T
        for part in range(per_tile):
            target = pl.ds(pl.multiple_of(slot_ref[index * per_tile + part] * block, block), block)
            for head in range(GROUP):
                at = head * tile + part * block
                dq_ref[target, head * LANES : (head + 1) * LANES] = dq[at : at + block, :]
        return carry

    lax.fori_loop(0, tiles, one_tile, 0)

    def give(index, carry):
        target = pl.ds(pl.multiple_of(slot_ref[index] * block, block), block)
        source = pl.ds(pl.multiple_of(index * block, block), block)
        dk_ref[target, :] = dk[source, :]
        dv_ref[target, :] = dv[source, :]
        return carry

    lax.fori_loop(0, rows // block, give, 0)


def in_vmem(count):
    return [pl.BlockSpec(memory_space=pltpu.VMEM)] * count


def attend(slots, q, k, v):
    rows = q.shape[0]
    block = rows // slots.shape[0]
    tile = 2 * block
    width = GROUP * tile
    return pl.pallas_call(
        functools.partial(forward_kernel, block, tile),
        out_shape=(
            jax.ShapeDtypeStruct(q.shape, jnp.bfloat16),
            jax.ShapeDtypeStruct((rows // tile, width), jnp.float32),
        ),
        in_specs=[pl.BlockSpec(memory_space=pltpu.SMEM)] + in_vmem(3),
        out_specs=tuple(in_vmem(2)),
        scratch_shapes=[
            pltpu.VMEM((GROUP * rows, LANES), jnp.bfloat16),
            pltpu.VMEM((rows, LANES), jnp.bfloat16),
            pltpu.VMEM((LANES, rows), jnp.bfloat16),
            pltpu.VMEM((rows, width), jnp.float32),
        ],
        compiler_params=pltpu.CompilerParams(vmem_limit_bytes=40 << 20),
        cost_estimate=pl.CostEstimate(
            flops=4 * GROUP * rows * rows * LANES // 2,
            bytes_accessed=12 * rows * LANES,
            transcendentals=GROUP * rows * rows // 2,
        ),
        name="attend",
    )(slots, q, k, v)


def attend_back(slots, q, k, v, o, g, lse):
    rows = q.shape[0]
    block = rows // slots.shape[0]
    tile = 2 * block
    return pl.pallas_call(
        functools.partial(backward_kernel, block, tile),
        out_shape=(
            jax.ShapeDtypeStruct(q.shape, jnp.float32),
            jax.ShapeDtypeStruct(k.shape, jnp.float32),
            jax.ShapeDtypeStruct(k.shape, jnp.float32),
        ),
        in_specs=[pl.BlockSpec(memory_space=pltpu.SMEM)] + in_vmem(6),
        out_specs=tuple(in_vmem(3)),
        scratch_shapes=[
            pltpu.VMEM((GROUP * rows, LANES), jnp.bfloat16),
            pltpu.VMEM((rows, LANES), jnp.bfloat16),
            pltpu.VMEM((rows, LANES), jnp.bfloat16),
            pltpu.VMEM((LANES, rows), jnp.bfloat16),
            pltpu.VMEM((GROUP * rows, LANES), jnp.bfloat16),
            pltpu.VMEM((GROUP * rows, LANES), jnp.bfloat16),
            pltpu.VMEM((rows, LANES), jnp.float32),
            pltpu.VMEM((rows, LANES), jnp.float32),
        ],
        compiler_params=pltpu.CompilerParams(vmem_limit_bytes=40 << 20),
        cost_estimate=pl.CostEstimate(
            flops=10 * GROUP * rows * rows * LANES // 2,
            bytes_accessed=24 * rows * LANES,
            transcendentals=GROUP * rows * rows // 2,
        ),
        name="attend_back",
    )(slots, q, k, v, o, g, lse)


def head_local(
    block_input,
    block_table,
    output_grad,
    attention_gain,
    query_weight,
    key_weight,
    value_projection,
    output_weight,
    feedforward_gain,
    gate_weight,
    up_weight,
    down_weight,
):
    me = lax.axis_index("ctx")
    plane = lax.axis_size("ctx")
    line = lax.axis_size("fsdp")
    rows, model = block_input.shape[1:]
    shard = model // line
    hidden = gate_weight.shape[1]
    unit = hidden // (line * plane)
    table_row = block_table[0]
    slot_count = table_row.shape[0]
    block = rows * plane // slot_count
    places = jnp.arange(slot_count, dtype=jnp.int32)
    slots = jnp.sum(jnp.where(table_row[None, :] == places[:, None], places[None, :], 0), axis=1)

    def mine(array, width):
        return lax.dynamic_slice_in_dim(array, me * width, width, 1)

    def gather(array, name, axis=0):
        return lax.all_gather(array, name, axis=axis, tiled=True)

    gains = gather(jnp.stack([attention_gain, feedforward_gain]), "fsdp", 1).astype(jnp.float32)
    query_width = query_weight.shape[1] // plane
    key_width = key_weight.shape[1] // plane
    qkv = gather(
        jnp.concatenate(
            [
                mine(query_weight, query_width),
                mine(key_weight, key_width),
                mine(value_projection, key_width),
            ],
            axis=1,
        ),
        "fsdp",
    )
    qkv_pad = pad_head(qkv)
    out_width = model // plane
    out_part = gather(mine(output_weight, out_width), "fsdp")
    out_full = gather(out_part, "ctx", 1)

    def hidden_part(array):
        split = array.reshape(shard, line, plane, unit)
        return lax.dynamic_index_in_dim(split, me, 2, keepdims=False).reshape(shard, line * unit)

    gate_up = gather(
        jnp.concatenate([hidden_part(gate_weight), hidden_part(up_weight)], axis=1), "fsdp"
    )
    down = gather(lax.dynamic_slice_in_dim(down_weight, me * unit, unit, 0), "fsdp")
    gate, up = gate_up[:, : line * unit], gate_up[:, line * unit :]

    positions = (
        table_row[:, None] * block + jnp.arange(block, dtype=jnp.int32)[None, :]
    ).reshape(-1)
    cos, sin = rope_tables(positions)
    blank = jnp.zeros((rows * plane, LANES // 2 - HALF), jnp.float32)
    cosine = jnp.concatenate([cos, blank, cos, blank], axis=1)
    sine = jnp.concatenate([-sin, blank, sin, blank], axis=1)

    def swap(value):
        heads = value.shape[1] // LANES
        halves = value.reshape(-1, heads, 2, LANES // 2)
        return halves[:, :, ::-1, :].reshape(value.shape)

    def turned(value, direction):
        heads = value.shape[1] // LANES
        return value * jnp.tile(cosine, (1, heads)) + swap(value) * jnp.tile(
            sine * direction, (1, heads)
        )

    inputs = block_input[0].astype(jnp.float32)
    scale_one = norm_scale(inputs)
    normed_one = inputs * scale_one
    gained_one = gather((normed_one * gains[0]).astype(jnp.bfloat16), "ctx")
    raw = product(gained_one, qkv_pad)
    split_one, split_two = GROUP * LANES, (GROUP + 1) * LANES
    q = turned(raw[:, :split_one], 1.0).astype(jnp.bfloat16)
    k = turned(raw[:, split_one:split_two], 1.0).astype(jnp.bfloat16)
    v = raw[:, split_two:].astype(jnp.bfloat16)
    o, lse = attend(slots, q, k, v)

    attended = lax.all_to_all(o, "ctx", 0, 1, tiled=True)
    out_pad = pad_head(out_full.T).T
    residual = inputs + product(attended, out_pad)
    scale_two = norm_scale(residual)
    normed_two = residual * scale_two
    gained_two = gather((normed_two * gains[1]).astype(jnp.bfloat16), "ctx")
    grad_all = gather(output_grad[0], "ctx")

    gate_values = product(gained_two, gate)
    up_values = product(gained_two, up)
    sigmoid_gate = jax.nn.sigmoid(gate_values)
    activated = gate_values * sigmoid_gate
    hidden_act = (activated * up_values).astype(jnp.bfloat16)
    out_sum = lax.psum_scatter(
        product(hidden_act, down).astype(jnp.bfloat16), "ctx", scatter_dimension=0, tiled=True
    )
    layer_output = (residual + out_sum.astype(jnp.float32)).astype(jnp.bfloat16)
    grad_hidden = back_product(grad_all, down)
    down_term = cross_rows(hidden_act, grad_all)
    grad_gate = (
        grad_hidden * up_values * sigmoid_gate * (1.0 + gate_values * (1.0 - sigmoid_gate))
    ).astype(jnp.bfloat16)
    grad_up = (grad_hidden * activated).astype(jnp.bfloat16)
    gate_term = cross_rows(gained_two, grad_gate)
    up_term = cross_rows(gained_two, grad_up)
    grad_normed_two = lax.psum_scatter(
        (back_product(grad_gate, gate) + back_product(grad_up, up)).astype(jnp.bfloat16),
        "ctx",
        scatter_dimension=0,
        tiled=True,
    ).astype(jnp.float32)
    feedforward_term = jnp.sum(grad_normed_two * normed_two, axis=0)
    grad_scaled_two = grad_normed_two * gains[1]
    grad_residual = output_grad[0].astype(jnp.float32) + scale_two * (
        grad_scaled_two
        - normed_two * jnp.mean(grad_scaled_two * normed_two, axis=-1, keepdims=True)
    )
    grad_attn = grad_residual.astype(jnp.bfloat16)
    grad_attended = back_product(grad_attn, out_pad).astype(jnp.bfloat16)
    grad_o = lax.all_to_all(grad_attended, "ctx", 1, 0, tiled=True)
    attended_all = gather(unpad_head(o), "ctx", 1)
    grad_attn_mine = lax.all_to_all(grad_attn, "ctx", 1, 0, tiled=True)
    output_term = cross_rows(attended_all, grad_attn_mine)

    dq, dk, dv = attend_back(slots, q, k, v, o, grad_o, lse)
    grads = jnp.concatenate([turned(dq, -1.0), turned(dk, -1.0), dv], axis=1).astype(jnp.bfloat16)
    qkv_term = unpad_head(cross_rows(gained_one, grads))
    grad_normed_one = lax.psum_scatter(
        back_product(grads, qkv_pad).astype(jnp.bfloat16), "ctx", scatter_dimension=0, tiled=True
    ).astype(jnp.float32)
    attention_term = jnp.sum(grad_normed_one * normed_one, axis=0)
    grad_scaled_one = grad_normed_one * gains[0]
    input_grad = grad_residual + scale_one * (
        grad_scaled_one
        - normed_one * jnp.mean(grad_scaled_one * normed_one, axis=-1, keepdims=True)
    )

    def reduce_line(term):
        return lax.psum_scatter(
            term.astype(jnp.bfloat16), "fsdp", scatter_dimension=0, tiled=True
        )

    gate_up_grad = gather(reduce_line(jnp.concatenate([gate_term, up_term], axis=1)), "ctx")
    down_grad = gather(reduce_line(down_term), "ctx").astype(jnp.float32)
    gate_up_grad = jnp.transpose(
        gate_up_grad.reshape(plane, shard, 2, line, unit), (2, 1, 3, 0, 4)
    ).reshape(2, shard, hidden)
    attention_grad = gather(
        reduce_line(jnp.concatenate([qkv_term, output_term], axis=1)), "ctx"
    ).reshape(plane, shard, -1)

    def columns(first, width):
        part = attention_grad[:, :, first : first + width]
        return jnp.transpose(part, (1, 0, 2)).reshape(shard, plane * width).astype(jnp.float32)

    gain_terms = lax.psum(jnp.stack([attention_term, feedforward_term]), ("ctx", "fsdp"))
    gain_terms = lax.dynamic_slice_in_dim(gain_terms, lax.axis_index("fsdp") * shard, shard, 1)
    return (
        layer_output[None],
        input_grad[None],
        gain_terms[0],
        columns(0, query_width),
        columns(query_width, key_width),
        columns(query_width + key_width, key_width),
        columns(query_width + 2 * key_width, out_width),
        gain_terms[1],
        gate_up_grad[0].astype(jnp.float32),
        gate_up_grad[1].astype(jnp.float32),
        down_grad,
    )


def solution(mesh):
    plan = head_local if mesh.shape["ctx"] == KEY_VALUE_HEADS else local
    return jax.shard_map(
        plan,
        mesh=mesh,
        in_specs=(
            P("fsdp", "ctx", None),
            P("fsdp", None),
            P("fsdp", "ctx", None),
            P("fsdp"),
            P("fsdp", None),
            P("fsdp", None),
            P("fsdp", None),
            P("fsdp", None),
            P("fsdp"),
            P("fsdp", None),
            P("fsdp", None),
            P("fsdp", None),
        ),
        out_specs=(
            P("fsdp", "ctx", None),
            P("fsdp", "ctx", None),
            P("fsdp"),
            P("fsdp", None),
            P("fsdp", None),
            P("fsdp", None),
            P("fsdp", None),
            P("fsdp"),
            P("fsdp", None),
            P("fsdp", None),
            P("fsdp", None),
        ),
        check_vma=False,
    )
```

```python
import functools
import math

import jax
import jax.numpy as jnp
from jax import lax
from jax.experimental import pallas as pl
from jax.experimental.pallas import tpu as pltpu
from jax.sharding import PartitionSpec as P

QUERY_HEADS = 16
KEY_VALUE_HEADS = 8
HEAD_SIZE = 96


norm_epsilon = 1e-05
rotary_base = 100000.0
score_with_mask = -1e30


def rope_tables(positions):
    half_width = HEAD_SIZE // 2
    steps_index = jnp.arange(half_width, dtype=jnp.float32)
    inverse = jnp.exp(steps_index * jnp.float32(-2.0 * math.log(rotary_base) / HEAD_SIZE))
    angles = positions.astype(jnp.float32)[:, None] * inverse[None, :]
    return (jnp.cos(angles), jnp.sin(angles))


def rotate(value_rows, cosine, sine_values, direction):
    count_of_rows = value_rows.shape[0]
    head_count = value_rows.shape[1] // HEAD_SIZE
    half_width = HEAD_SIZE // 2
    shaped = value_rows.reshape(count_of_rows, head_count, HEAD_SIZE)
    first_half = shaped[:, :, :half_width]
    second_half = shaped[:, :, half_width:]
    cos_part = cosine[:, None, :]
    sin_part = sine_values[:, None, :] * direction
    turned = jnp.concatenate(
        [
            first_half * cos_part - second_half * sin_part,
            second_half * cos_part + first_half * sin_part,
        ],
        axis=2,
    )
    return turned.reshape(count_of_rows, head_count * HEAD_SIZE)


def norm_scale(value_rows):
    return lax.rsqrt(jnp.mean(value_rows * value_rows, axis=-1, keepdims=True) + norm_epsilon)


def product(matrix, operand):
    return jnp.dot(matrix, operand, preferred_element_type=jnp.float32)


def cross_rows(matrix, operand):
    return lax.dot_general(
        matrix, operand, (((0,), (0,)), ((), ())), preferred_element_type=jnp.float32
    )


def back_product(matrix, operand):
    return lax.dot_general(
        matrix, operand, (((1,), (1,)), ((), ())), preferred_element_type=jnp.float32
    )


def block_scores(query_rank_four, block_of_keys, query_positions, key_positions):
    keys_rank_three = block_of_keys.reshape(block_of_keys.shape[0], KEY_VALUE_HEADS, HEAD_SIZE)
    scores = jnp.einsum(
        "rgjd,kgd->gjrk", query_rank_four, keys_rank_three, preferred_element_type=jnp.float32
    ) * HEAD_SIZE ** (-0.5)
    allowed = (key_positions[None, :] <= query_positions[:, None])[None, None]
    return (jnp.where(allowed, scores, score_with_mask), allowed)


def local(
    block_input,
    block_table,
    output_grad,
    attention_gain,
    query_weight,
    key_weight,
    value_projection,
    output_weight,
    feedforward_gain,
    gate_weight,
    up_weight,
    down_weight,
):
    query_group_width = QUERY_HEADS // KEY_VALUE_HEADS
    score_scale = HEAD_SIZE ** (-0.5)
    inputs = block_input[0].astype(jnp.float32)
    count_of_rows = inputs.shape[0]
    block_rows = count_of_rows // 2
    ctx_index = lax.axis_index("ctx")
    table_row = block_table[0]
    offsets = jnp.arange(block_rows, dtype=jnp.int32)
    query_blocks = lax.dynamic_slice_in_dim(table_row, 2 * ctx_index, 2)
    query_positions = (query_blocks[:, None] * block_rows + offsets[None, :]).reshape(count_of_rows)
    key_positions = (table_row[:, None] * block_rows + offsets[None, :]).reshape(-1)
    cosine, sine_values = rope_tables(query_positions)
    gain_one, query_full, key_full, value_full, out_full = (
        lax.all_gather(attention_gain, "fsdp", axis=0, tiled=True),
        lax.all_gather(query_weight, "fsdp", axis=0, tiled=True),
        lax.all_gather(key_weight, "fsdp", axis=0, tiled=True),
        lax.all_gather(value_projection, "fsdp", axis=0, tiled=True),
        lax.all_gather(output_weight, "fsdp", axis=0, tiled=True),
    )
    scale_one = norm_scale(inputs)
    normed_one = inputs * scale_one
    gained_one = (normed_one * gain_one.astype(jnp.float32)).astype(jnp.bfloat16)
    query_rows = rotate(product(gained_one, query_full), cosine, sine_values, 1.0).astype(
        jnp.bfloat16
    )
    keys_local = rotate(product(gained_one, key_full), cosine, sine_values, 1.0).astype(
        jnp.bfloat16
    )
    values_local = product(gained_one, value_full).astype(jnp.bfloat16)
    keys_all, values_all = (
        lax.all_gather(keys_local, "ctx", axis=0, tiled=True),
        lax.all_gather(values_local, "ctx", axis=0, tiled=True),
    )
    key_total_count = keys_all.shape[0]
    key_block_pass = 1024
    block_count = key_total_count // key_block_pass
    query_rank_four = query_rows.reshape(
        count_of_rows, KEY_VALUE_HEADS, query_group_width, HEAD_SIZE
    )
    key_places = key_positions.reshape(block_count, key_block_pass)

    def split_keys(array_in):
        return array_in.reshape(block_count, key_block_pass, array_in.shape[-1])

    def statistics_step(state_now, block_data):
        running_max, running_sum = state_now
        block_of_keys, key_place = block_data
        masked, allowed = block_scores(query_rank_four, block_of_keys, query_positions, key_place)
        new_max = jnp.maximum(running_max, jnp.max(masked, axis=-1))
        block_sum = jnp.sum(jnp.where(allowed, jnp.exp(masked - new_max[..., None]), 0.0), axis=-1)
        return ((new_max, running_sum * jnp.exp(running_max - new_max) + block_sum), None)

    initial_maximum = jnp.full(
        (KEY_VALUE_HEADS, query_group_width, count_of_rows), score_with_mask, jnp.float32
    )
    initial_sum = jnp.zeros((KEY_VALUE_HEADS, query_group_width, count_of_rows), jnp.float32)
    (final_max, final_sum), unused = lax.scan(
        statistics_step, (initial_maximum, initial_sum), (split_keys(keys_all), key_places)
    )
    log_total = final_max + jnp.log(final_sum)

    def output_step(state_now, block_data):
        block_of_keys, block_of_values, key_place = block_data
        masked, allowed = block_scores(query_rank_four, block_of_keys, query_positions, key_place)
        weights_half = jnp.where(allowed, jnp.exp(masked - log_total[..., None]), 0.0).astype(
            jnp.bfloat16
        )
        values_rank_three = block_of_values.reshape(key_block_pass, KEY_VALUE_HEADS, HEAD_SIZE)
        return (
            state_now
            + jnp.einsum(
                "gjrk,kgd->rgjd",
                weights_half,
                values_rank_three,
                preferred_element_type=jnp.float32,
            ),
            None,
        )

    initial_output = jnp.zeros(
        (count_of_rows, KEY_VALUE_HEADS, query_group_width, HEAD_SIZE), jnp.float32
    )
    summed_out, unused = lax.scan(
        output_step, initial_output, (split_keys(keys_all), split_keys(values_all), key_places)
    )
    attended_rows = summed_out.reshape(count_of_rows, QUERY_HEADS * HEAD_SIZE).astype(jnp.bfloat16)
    residual = inputs + product(attended_rows, out_full)
    scale_two = norm_scale(residual)
    normed_two = residual * scale_two
    gain_two, gate_full, up_full, down_full = (
        lax.all_gather(feedforward_gain, "fsdp", axis=0, tiled=True),
        lax.all_gather(gate_weight, "fsdp", axis=0, tiled=True),
        lax.all_gather(up_weight, "fsdp", axis=0, tiled=True),
        lax.all_gather(down_weight, "fsdp", axis=0, tiled=True),
    )
    gained_two = (normed_two * gain_two.astype(jnp.float32)).astype(jnp.bfloat16)
    gate_values = product(gained_two, gate_full)
    up_values = product(gained_two, up_full)
    sigmoid_gate = jax.nn.sigmoid(gate_values)
    activated = gate_values * sigmoid_gate
    hidden_act = (activated * up_values).astype(jnp.bfloat16)
    layer_output = (residual + product(hidden_act, down_full)).astype(jnp.bfloat16)
    gain_two_again, gate_back, up_back, down_back = (
        lax.all_gather(feedforward_gain, "fsdp", axis=0, tiled=True),
        lax.all_gather(gate_weight, "fsdp", axis=0, tiled=True),
        lax.all_gather(up_weight, "fsdp", axis=0, tiled=True),
        lax.all_gather(down_weight, "fsdp", axis=0, tiled=True),
    )
    grad_rows = output_grad[0]
    grad_hidden = back_product(grad_rows, down_back)
    down_term = cross_rows(hidden_act, grad_rows)
    grad_gate = (
        grad_hidden * up_values * sigmoid_gate * (1.0 + gate_values * (1.0 - sigmoid_gate))
    ).astype(jnp.bfloat16)
    grad_up = (grad_hidden * activated).astype(jnp.bfloat16)
    gate_term = cross_rows(gained_two, grad_gate)
    up_term = cross_rows(gained_two, grad_up)
    grad_normed_two = back_product(grad_gate, gate_back) + back_product(grad_up, up_back)
    feedforward_term = jnp.sum(grad_normed_two * normed_two, axis=0)
    grad_scaled_two = grad_normed_two * gain_two_again.astype(jnp.float32)
    grad_residual = grad_rows.astype(jnp.float32) + scale_two * (
        grad_scaled_two
        - normed_two * jnp.mean(grad_scaled_two * normed_two, axis=-1, keepdims=True)
    )
    gain_one_again, query_back, key_back, value_back, out_back = (
        lax.all_gather(attention_gain, "fsdp", axis=0, tiled=True),
        lax.all_gather(query_weight, "fsdp", axis=0, tiled=True),
        lax.all_gather(key_weight, "fsdp", axis=0, tiled=True),
        lax.all_gather(value_projection, "fsdp", axis=0, tiled=True),
        lax.all_gather(output_weight, "fsdp", axis=0, tiled=True),
    )
    grad_attn = grad_residual.astype(jnp.bfloat16)
    output_term = cross_rows(attended_rows, grad_attn)
    attended_gradient = back_product(grad_attn, out_back).astype(jnp.bfloat16)
    gradient_rank_four = attended_gradient.reshape(
        count_of_rows, KEY_VALUE_HEADS, query_group_width, HEAD_SIZE
    )
    attended_rank_four = attended_rows.reshape(
        count_of_rows, KEY_VALUE_HEADS, query_group_width, HEAD_SIZE
    )
    row_delta = jnp.transpose(
        jnp.sum(
            gradient_rank_four.astype(jnp.float32) * attended_rank_four.astype(jnp.float32), axis=-1
        ),
        (1, 2, 0),
    )
    keys_again, values_again = (
        lax.all_gather(keys_local, "ctx", axis=0, tiled=True),
        lax.all_gather(values_local, "ctx", axis=0, tiled=True),
    )

    def back_step(state_now, block_data):
        block_of_keys, block_of_values, key_place = block_data
        masked, allowed = block_scores(query_rank_four, block_of_keys, query_positions, key_place)
        weights_half = jnp.where(allowed, jnp.exp(masked - log_total[..., None]), 0.0).astype(
            jnp.bfloat16
        )
        values_rank_three = block_of_values.reshape(key_block_pass, KEY_VALUE_HEADS, HEAD_SIZE)
        keys_rank_three = block_of_keys.reshape(key_block_pass, KEY_VALUE_HEADS, HEAD_SIZE)
        grad_weights = jnp.einsum(
            "rgjd,kgd->gjrk",
            gradient_rank_four,
            values_rank_three,
            preferred_element_type=jnp.float32,
        )
        grad_scores = (
            weights_half.astype(jnp.float32) * (grad_weights - row_delta[..., None]) * score_scale
        ).astype(jnp.bfloat16)
        state_now = state_now + jnp.einsum(
            "gjrk,kgd->rgjd", grad_scores, keys_rank_three, preferred_element_type=jnp.float32
        )
        key_gradient = jnp.einsum(
            "gjrk,rgjd->kgd", grad_scores, query_rank_four, preferred_element_type=jnp.float32
        )
        value_gradient = jnp.einsum(
            "gjrk,rgjd->kgd", weights_half, gradient_rank_four, preferred_element_type=jnp.float32
        )
        return (
            state_now,
            (
                key_gradient.reshape(key_block_pass, KEY_VALUE_HEADS * HEAD_SIZE).astype(
                    jnp.bfloat16
                ),
                value_gradient.reshape(key_block_pass, KEY_VALUE_HEADS * HEAD_SIZE).astype(
                    jnp.bfloat16
                ),
            ),
        )

    first_query_index = jnp.zeros(
        (count_of_rows, KEY_VALUE_HEADS, query_group_width, HEAD_SIZE), jnp.float32
    )
    query_sum, (key_gradients, value_gradients) = lax.scan(
        back_step, first_query_index, (split_keys(keys_again), split_keys(values_again), key_places)
    )
    key_gradients = key_gradients.reshape(key_total_count, KEY_VALUE_HEADS * HEAD_SIZE)
    value_gradients = value_gradients.reshape(key_total_count, KEY_VALUE_HEADS * HEAD_SIZE)
    key_sums, value_sums = (
        lax.psum_scatter(key_gradients, "ctx", scatter_dimension=0, tiled=True).astype(jnp.float32),
        lax.psum_scatter(value_gradients, "ctx", scatter_dimension=0, tiled=True).astype(
            jnp.float32
        ),
    )
    query_gradients = rotate(
        query_sum.reshape(count_of_rows, QUERY_HEADS * HEAD_SIZE), cosine, sine_values, -1.0
    ).astype(jnp.bfloat16)
    grad_keys = rotate(key_sums, cosine, sine_values, -1.0).astype(jnp.bfloat16)
    grad_values = value_sums.astype(jnp.bfloat16)
    query_term = cross_rows(gained_one, query_gradients)
    key_term = cross_rows(gained_one, grad_keys)
    value_term = cross_rows(gained_one, grad_values)
    grad_normed_one = (
        back_product(query_gradients, query_back)
        + back_product(grad_keys, key_back)
        + back_product(grad_values, value_back)
    )
    attention_term = jnp.sum(grad_normed_one * normed_one, axis=0)
    grad_scaled_one = grad_normed_one * gain_one_again.astype(jnp.float32)
    input_grad = grad_residual + scale_one * (
        grad_scaled_one
        - normed_one * jnp.mean(grad_scaled_one * normed_one, axis=-1, keepdims=True)
    )
    shares = (
        lax.psum_scatter(
            attention_term.astype(jnp.bfloat16), "fsdp", scatter_dimension=0, tiled=True
        ).astype(jnp.float32),
        lax.psum_scatter(
            query_term.astype(jnp.bfloat16), "fsdp", scatter_dimension=0, tiled=True
        ).astype(jnp.float32),
        lax.psum_scatter(
            key_term.astype(jnp.bfloat16), "fsdp", scatter_dimension=0, tiled=True
        ).astype(jnp.float32),
        lax.psum_scatter(
            value_term.astype(jnp.bfloat16), "fsdp", scatter_dimension=0, tiled=True
        ).astype(jnp.float32),
        lax.psum_scatter(
            output_term.astype(jnp.bfloat16), "fsdp", scatter_dimension=0, tiled=True
        ).astype(jnp.float32),
        lax.psum_scatter(
            feedforward_term.astype(jnp.bfloat16), "fsdp", scatter_dimension=0, tiled=True
        ).astype(jnp.float32),
        lax.psum_scatter(
            gate_term.astype(jnp.bfloat16), "fsdp", scatter_dimension=0, tiled=True
        ).astype(jnp.float32),
        lax.psum_scatter(
            up_term.astype(jnp.bfloat16), "fsdp", scatter_dimension=0, tiled=True
        ).astype(jnp.float32),
        lax.psum_scatter(
            down_term.astype(jnp.bfloat16), "fsdp", scatter_dimension=0, tiled=True
        ).astype(jnp.float32),
    )
    totals = (
        lax.psum(shares[0].astype(jnp.bfloat16), "ctx").astype(jnp.float32),
        lax.psum(shares[1].astype(jnp.bfloat16), "ctx").astype(jnp.float32),
        lax.psum(shares[2].astype(jnp.bfloat16), "ctx").astype(jnp.float32),
        lax.psum(shares[3].astype(jnp.bfloat16), "ctx").astype(jnp.float32),
        lax.psum(shares[4].astype(jnp.bfloat16), "ctx").astype(jnp.float32),
        lax.psum(shares[5].astype(jnp.bfloat16), "ctx").astype(jnp.float32),
        lax.psum(shares[6].astype(jnp.bfloat16), "ctx").astype(jnp.float32),
        lax.psum(shares[7].astype(jnp.bfloat16), "ctx").astype(jnp.float32),
        lax.psum(shares[8].astype(jnp.bfloat16), "ctx").astype(jnp.float32),
    )
    return (
        layer_output[None],
        input_grad[None],
        totals[0],
        totals[1],
        totals[2],
        totals[3],
        totals[4],
        totals[5],
        totals[6],
        totals[7],
        totals[8],
    )


LANES = 128
HALF = HEAD_SIZE // 2
GROUP = QUERY_HEADS // KEY_VALUE_HEADS
score_scale = HEAD_SIZE ** (-0.5)


def contract(left, right, left_dim, right_dim):
    return lax.dot_general(
        left, right, (((left_dim,), (right_dim,)), ((), ())), preferred_element_type=jnp.float32
    )


def in_vmem(count):
    return [pl.BlockSpec(memory_space=pltpu.VMEM)] * count


def padding(heads):
    column = jnp.arange(heads * HEAD_SIZE, dtype=jnp.int32)
    half_at, rest = column // HALF, column % HALF
    target = half_at * (LANES // 2) + rest
    lanes = jnp.arange(heads * LANES, dtype=jnp.int32)
    return (target[:, None] == lanes[None, :]).astype(jnp.bfloat16)


def turn(part, cosine, sine):
    return part * cosine + pltpu.roll(part, LANES // 2, 1) * sine


def tables(inner_ref, outer_ref, index, per_tile):
    inner_cos, inner_sin = inner_ref[0], inner_ref[1]
    sign = jnp.where(
        lax.broadcasted_iota(jnp.int32, inner_cos.shape, 1) < LANES // 2, -1.0, 1.0
    )
    cosines, sines = [], []
    for part in range(per_tile):
        at = pl.ds(index * per_tile + part, 1)
        outer_cos, outer_sin = outer_ref[0, at, :], outer_ref[1, at, :]
        cosines.append(inner_cos * outer_cos - inner_sin * outer_sin)
        sines.append(sign * (inner_sin * outer_cos + inner_cos * outer_sin))
    return jnp.concatenate(cosines, axis=0), jnp.concatenate(sines, axis=0)


def forward_kernel(
    slot_ref,
    xa_ref,
    xb_ref,
    gain_ref,
    w_ref,
    pad_ref,
    inner_ref,
    outer_ref,
    gained_ref,
    qkv_ref,
    o_ref,
    lse_ref,
    wp,
    qs,
    vt,
    s_ref,
):
    index = pl.program_id(0)
    block = xa_ref.shape[0]
    tile = 2 * block
    width = GROUP * tile
    heads = GROUP + 2

    @pl.when(index == 0)
    def _():
        wp[...] = contract(w_ref[...], pad_ref[...], 1, 0).astype(jnp.bfloat16)

    x = jnp.concatenate([xa_ref[...], xb_ref[...]], axis=0).astype(jnp.float32)
    normed = x * lax.rsqrt(jnp.mean(x * x, axis=-1, keepdims=True) + norm_epsilon)
    gained = (normed * gain_ref[...]).astype(jnp.bfloat16)
    gained_ref[...] = gained
    raw = contract(gained, wp[...], 1, 0)
    cosine, sine = tables(inner_ref, outer_ref, index, 2)
    here = pl.ds(pl.multiple_of(index * tile, tile), tile)
    for head in range(heads):
        lanes = slice(head * LANES, (head + 1) * LANES)
        part = raw[:, lanes]
        if head <= GROUP:
            part = turn(part, cosine, sine)
        part = part.astype(jnp.bfloat16)
        qkv_ref[here, lanes] = part
        if head < GROUP:
            qs[head * tile : (head + 1) * tile, :] = part
        if head == heads - 1:
            vt[:, here] = part.T
    queries = qs[...]
    key_at = lax.broadcasted_iota(jnp.int32, (tile, width), 0)
    query_at = lax.rem(lax.broadcasted_iota(jnp.int32, (tile, width), 1), tile)
    diagonal = key_at <= query_at

    def scores_of(step):
        at = pl.ds(pl.multiple_of(step * tile, tile), tile)
        keys = qkv_ref[at, GROUP * LANES : (GROUP + 1) * LANES]
        return contract(keys, queries, 1, 1) * score_scale

    last = jnp.where(diagonal, scores_of(index), score_with_mask)
    s_ref[here, :] = last
    peak = jnp.max(last, axis=0, keepdims=True)

    def first_pass(step, peak):
        scores = scores_of(step)
        s_ref[pl.ds(pl.multiple_of(step * tile, tile), tile), :] = scores
        return jnp.maximum(peak, jnp.max(scores, axis=0, keepdims=True))

    peak = lax.fori_loop(0, index, first_pass, peak)

    def second_pass(step, state):
        total, out = state
        at = pl.ds(pl.multiple_of(step * tile, tile), tile)
        probs = jnp.exp(s_ref[at, :] - peak)
        total = total + jnp.sum(probs, axis=0, keepdims=True)
        out = out + contract(vt[:, at], probs.astype(jnp.bfloat16), 1, 0)
        return (total, out)

    total, out = lax.fori_loop(
        0,
        index + 1,
        second_pass,
        (jnp.zeros((1, width), jnp.float32), jnp.zeros((LANES, width), jnp.float32)),
    )
    lse_ref[pl.ds(index, 1), :] = peak + jnp.log(total)
    out = (out * (1.0 / total)).T.astype(jnp.bfloat16)
    out = jnp.concatenate([out[head * tile : (head + 1) * tile, :] for head in range(GROUP)], axis=1)
    out = contract(out, pad_ref[: GROUP * HEAD_SIZE, : GROUP * LANES], 1, 1).astype(jnp.bfloat16)
    for part in range(2):
        target = pl.ds(pl.multiple_of(slot_ref[index * 2 + part] * block, block), block)
        o_ref[target, :] = out[part * block : (part + 1) * block, :]


def attend(slots, x, gain, w, pad, inner, outer):
    rows, model = x.shape
    block = rows // slots.shape[0]
    tile = 2 * block
    width = GROUP * tile
    columns = pad.shape[1]
    whole = lambda *shape: pl.BlockSpec(shape, lambda i, s: (0,) * len(shape))
    return pl.pallas_call(
        forward_kernel,
        grid_spec=pltpu.PrefetchScalarGridSpec(
            num_scalar_prefetch=1,
            grid=(rows // tile,),
            in_specs=[
                pl.BlockSpec((block, model), lambda i, s: (s[2 * i], 0)),
                pl.BlockSpec((block, model), lambda i, s: (s[2 * i + 1], 0)),
                whole(1, model),
                whole(*w.shape),
                whole(*pad.shape),
                whole(*inner.shape),
                whole(*outer.shape),
            ],
            out_specs=(
                pl.BlockSpec((tile, model), lambda i, s: (i, 0)),
                whole(rows, columns),
                whole(rows, GROUP * HEAD_SIZE),
                whole(rows // tile, width),
            ),
            scratch_shapes=[
                pltpu.VMEM((model, columns), jnp.bfloat16),
                pltpu.VMEM((width, LANES), jnp.bfloat16),
                pltpu.VMEM((LANES, rows), jnp.bfloat16),
                pltpu.VMEM((rows, width), jnp.float32),
            ],
        ),
        out_shape=(
            jax.ShapeDtypeStruct((rows, model), jnp.bfloat16),
            jax.ShapeDtypeStruct((rows, columns), jnp.bfloat16),
            jax.ShapeDtypeStruct((rows, GROUP * HEAD_SIZE), jnp.bfloat16),
            jax.ShapeDtypeStruct((rows // tile, width), jnp.float32),
        ),
        compiler_params=pltpu.CompilerParams(vmem_limit_bytes=44 << 20),
        cost_estimate=pl.CostEstimate(
            flops=4 * GROUP * rows * rows * LANES // 2 + 2 * rows * model * columns,
            bytes_accessed=4 * rows * model,
            transcendentals=GROUP * rows * rows // 2,
        ),
        name="attend",
    )(slots, x, x, gain, w, pad, inner, outer)


def backward_kernel(
    slot_ref,
    ga_ref,
    gb_ref,
    gained_ref,
    qkv_ref,
    o_ref,
    lse_ref,
    w_ref,
    wo_ref,
    pad_ref,
    inner_ref,
    outer_ref,
    dx_ref,
    dw_ref,
    dwo_ref,
    wp,
    qs,
    gs,
    kt,
    dk,
    dv,
    dw,
    dwo,
):
    step_at = pl.program_id(0)
    tiles = pl.num_programs(0)
    index = tiles - 1 - step_at
    block = ga_ref.shape[0]
    tile = 2 * block
    width = GROUP * tile
    rows = qkv_ref.shape[0]
    first_key, first_value = GROUP * LANES, (GROUP + 1) * LANES

    @pl.when(step_at == 0)
    def _():
        wp[...] = contract(w_ref[...], pad_ref[...], 1, 0).astype(jnp.bfloat16)
        kt[...] = qkv_ref[:, first_key:first_value].T
        dk[...] = jnp.zeros_like(dk)
        dv[...] = jnp.zeros_like(dv)
        dw[...] = jnp.zeros_like(dw)
        dwo[...] = jnp.zeros_like(dwo)

    here = pl.ds(pl.multiple_of(index * tile, tile), tile)
    sources = [
        pl.ds(pl.multiple_of(slot_ref[index * 2 + part] * block, block), block) for part in (0, 1)
    ]
    grad_attn = jnp.concatenate([ga_ref[...], gb_ref[...]], axis=0)
    o = jnp.concatenate([o_ref[source, :] for source in sources], axis=0)
    dwo[...] += contract(o, grad_attn, 0, 0)
    grads = contract(grad_attn, wo_ref[...], 1, 1).astype(jnp.bfloat16)
    products = (grads.astype(jnp.float32) * o.astype(jnp.float32)).T
    grads = contract(grads, pad_ref[: GROUP * HEAD_SIZE, : GROUP * LANES], 1, 0).astype(jnp.bfloat16)
    deltas = []
    for head in range(GROUP):
        lanes = slice(head * LANES, (head + 1) * LANES)
        at = slice(head * tile, (head + 1) * tile)
        qs[at, :] = qkv_ref[here, lanes]
        gs[at, :] = grads[:, lanes]
        features = slice(head * HEAD_SIZE, (head + 1) * HEAD_SIZE)
        deltas.append(jnp.sum(products[features, :], axis=0, keepdims=True))
    delta = jnp.concatenate(deltas, axis=1)
    lse = lse_ref[pl.ds(index, 1), :]
    queries, grads = qs[...], gs[...]
    key_at = lax.broadcasted_iota(jnp.int32, (tile, width), 0)
    query_at = lax.rem(lax.broadcasted_iota(jnp.int32, (tile, width), 1), tile)
    diagonal = key_at <= query_at

    def piece(step, masked):
        at = pl.ds(pl.multiple_of(step * tile, tile), tile)
        scores = contract(qkv_ref[at, first_key:first_value], queries, 1, 1) * score_scale
        probs = jnp.exp(scores - lse)
        if masked:
            probs = jnp.where(diagonal, probs, 0.0)
        probs = probs.astype(jnp.bfloat16)
        dv[at, :] += contract(probs, grads, 1, 0)
        grad_probs = contract(qkv_ref[at, first_value:], grads, 1, 1)
        grad_scores = (probs.astype(jnp.float32) * (grad_probs - delta) * score_scale).astype(
            jnp.bfloat16
        )
        dk[at, :] += contract(grad_scores, queries, 1, 0)
        return contract(kt[:, at], grad_scores, 1, 0)

    dq = piece(index, True)
    dq = lax.fori_loop(0, index, lambda step, total: total + piece(step, False), dq)
    dq = dq.T
    cosine, sine = tables(inner_ref, outer_ref, index, 2)
    parts = [turn(dq[head * tile : (head + 1) * tile, :], cosine, -sine) for head in range(GROUP)]
    parts.append(turn(dk[here, :], cosine, -sine))
    parts.append(dv[here, :])
    dqkv = jnp.concatenate([part.astype(jnp.bfloat16) for part in parts], axis=1)
    dw[...] += contract(dqkv, gained_ref[...], 0, 0)
    dx = contract(dqkv, wp[...], 1, 1).astype(jnp.bfloat16)
    for part in (0, 1):
        dx_ref[sources[part], :] = dx[part * block : (part + 1) * block, :]

    @pl.when(step_at == tiles - 1)
    def _():
        packed = contract(pad_ref[...], dw[...].astype(jnp.bfloat16), 1, 0)
        dw_ref[...] = packed.astype(jnp.bfloat16).T
        pieces, _, across = dwo_ref.shape
        for piece in range(pieces):
            rows_at = slice(piece * HALF, (piece + 1) * HALF)
            for number in range(dwo.shape[1] // across):
                columns = slice(number * across, (number + 1) * across)
                dwo_ref[piece, number * HALF : (number + 1) * HALF, :] = dwo[
                    rows_at, columns
                ].astype(jnp.bfloat16)


def attend_back(slots, grad_attn, gained, qkv, o, lse, w, wo, pad, inner, outer):
    rows, model = gained.shape
    block = rows // slots.shape[0]
    tile = 2 * block
    width = GROUP * tile
    tiles = rows // tile
    columns = pad.shape[1]
    across = w.shape[1]
    wo_pieces = (2 * GROUP, HALF * model // across, across)
    whole = lambda *shape: pl.BlockSpec(shape, lambda i, s: (0,) * len(shape))
    return pl.pallas_call(
        backward_kernel,
        grid_spec=pltpu.PrefetchScalarGridSpec(
            num_scalar_prefetch=1,
            grid=(tiles,),
            in_specs=[
                pl.BlockSpec((block, model), lambda i, s: (s[2 * (tiles - 1 - i)], 0)),
                pl.BlockSpec((block, model), lambda i, s: (s[2 * (tiles - 1 - i) + 1], 0)),
                pl.BlockSpec((tile, model), lambda i, s: (tiles - 1 - i, 0)),
                whole(*qkv.shape),
                whole(*o.shape),
                whole(*lse.shape),
                whole(*w.shape),
                whole(*wo.shape),
                whole(*pad.shape),
                whole(*inner.shape),
                whole(*outer.shape),
            ],
            out_specs=(whole(rows, model), whole(*w.shape), whole(*wo_pieces)),
            scratch_shapes=[
                pltpu.VMEM((model, columns), jnp.bfloat16),
                pltpu.VMEM((width, LANES), jnp.bfloat16),
                pltpu.VMEM((width, LANES), jnp.bfloat16),
                pltpu.VMEM((LANES, rows), jnp.bfloat16),
                pltpu.VMEM((rows, LANES), jnp.float32),
                pltpu.VMEM((rows, LANES), jnp.float32),
                pltpu.VMEM((columns, model), jnp.float32),
                pltpu.VMEM(wo.shape, jnp.float32),
            ],
        ),
        out_shape=(
            jax.ShapeDtypeStruct((rows, model), jnp.bfloat16),
            jax.ShapeDtypeStruct(w.shape, jnp.bfloat16),
            jax.ShapeDtypeStruct(wo_pieces, jnp.bfloat16),
        ),
        compiler_params=pltpu.CompilerParams(vmem_limit_bytes=56 << 20),
        cost_estimate=pl.CostEstimate(
            flops=10 * GROUP * rows * rows * LANES // 2 + 8 * rows * model * columns,
            bytes_accessed=8 * rows * model,
            transcendentals=GROUP * rows * rows // 2,
        ),
        name="attend_back",
    )(slots, grad_attn, grad_attn, gained, qkv, o, lse, w, wo, pad, inner, outer)
MESH_IDS = pl.DeviceIdType.MESH
ACROSS = (1, 2, 4, 6)


def start_barrier(me, line_index=None, line=1):
    barrier = pltpu.get_barrier_semaphore()
    peers = [{"ctx": me ^ bit} for bit in range(1, 8)]
    peers += [{"fsdp": lax.rem(line_index + step, line)} for step in range(1, line)]
    for peer in peers:
        pl.semaphore_signal(barrier, inc=1, device_id=peer, device_id_type=MESH_IDS)
    pl.semaphore_wait(barrier, len(peers))


class Copies:
    def __init__(self, send_sems, recv_sems, base=0):
        self.send_sems, self.recv_sems, self.next, self.sent = send_sems, recv_sems, base, []

    def number(self):
        self.next += 1
        return self.next - 1

    def make(self, number, source, target, peer, landing=None):
        return pltpu.make_async_remote_copy(
            src_ref=source,
            dst_ref=target,
            send_sem=self.send_sems.at[number],
            recv_sem=self.recv_sems.at[number if landing is None else landing],
            device_id=peer,
            device_id_type=MESH_IDS,
        )

    def send(self, number, source, target, peer):
        copy = self.make(number, source, target, peer)
        copy.start()
        self.sent.append(copy)

    def arrived(self, number, target):
        self.make(number, target, target, {"ctx": 0}).wait_recv()

    def finish(self):
        for copy in self.sent:
            copy.wait_send()


GATHER_COPIES = 13


class PlaneGather:
    def __init__(self, copies, me, own_half, part):
        self.copies, self.me, self.own_half, self.part = copies, me, own_half, part
        self.first = copies.next
        copies.next += GATHER_COPIES

    def peer(self, bit):
        return {"ctx": self.me ^ bit}

    def begin(self):
        me, part, own, first = self.me, self.part, self.own_half, self.first
        send = self.copies.send
        send(first + 0, own(1), part(me, 1), self.peer(2))
        send(first + 1, own(0), part(me, 0), self.peer(4))
        send(first + 2, own(0), part(me, 0), self.peer(2))
        send(first + 3, own(1), part(me, 1), self.peer(4))
        send(first + 4, own(0), part(me, 0), self.peer(1))
        send(first + 5, own(1), part(me, 1), self.peer(1))

    def hear(self, number, slot, half, onward=None):
        place = self.part(slot, half)
        self.copies.arrived(self.first + number, place)
        if onward is not None:
            self.copies.send(self.first + onward[0], place, place, self.peer(onward[1]))

    def share(self, number, slot, half):
        place = self.part(slot, half)
        self.copies.send(self.first + number, place, place, self.peer(1))

    def first_hop(self):
        me = self.me
        self.hear(0, me ^ 2, 1, (6, 4))
        self.share(8, me ^ 2, 1)
        self.hear(1, me ^ 4, 0, (7, 2))
        self.share(9, me ^ 4, 0)

    def second_hop(self):
        me = self.me
        self.hear(2, me ^ 2, 0)
        self.share(10, me ^ 2, 0)
        self.hear(3, me ^ 4, 1)
        self.share(11, me ^ 4, 1)

    def third_hop(self):
        me = self.me
        self.hear(6, me ^ 6, 1)
        self.hear(7, me ^ 6, 0)
        self.share(12, me ^ 6, slice(None))

    def last(self):
        me, arrived, part = self.me, self.copies.arrived, self.part
        arrived(self.first + 4, part(me ^ 1, 0))
        arrived(self.first + 5, part(me ^ 1, 1))
        arrived(self.first + 8, part(me ^ 3, 1))
        arrived(self.first + 9, part(me ^ 5, 0))
        arrived(self.first + 10, part(me ^ 3, 0))
        arrived(self.first + 11, part(me ^ 5, 1))
        arrived(self.first + 12, part(me ^ 7, slice(None)))


def run_gathers(gathers):
    for gather in gathers:
        gather.begin()
    for gather in gathers:
        gather.first_hop()
    for gather in gathers:
        gather.second_hop()
    for gather in gathers:
        gather.third_hop()
    for gather in gathers:
        gather.last()


def row_half(ref, rows):
    half = rows // 2

    def own(side):
        return ref.at[pl.ds(side * half, half), :]

    return own


def row_part(ref, rows):
    half = rows // 2

    def part(slot, side):
        if isinstance(side, slice):
            return ref.at[pl.ds(pl.multiple_of(slot * rows, rows), rows), :]
        return ref.at[pl.ds(pl.multiple_of(slot * rows + side * half, half), half), :]

    return part


class LineGather:
    def __init__(self, copies, index, line, place):
        self.copies, self.index, self.line, self.place = copies, index, line, place
        self.first = copies.next
        copies.next += 2 * (line - 1)

    def move(self, step, upward, act):
        index, line = self.index, self.line
        if upward:
            slot, there = index - step, index + 1
            leaves = (slot >= 0) & (there < line)
        else:
            slot, there = index + step, index - 1
            leaves = (slot < line) & (there >= 0)
        number = self.first + step + (0 if upward else line - 1)

        @pl.when(leaves)
        def _():
            place = self.place(jnp.clip(slot, 0, line - 1))
            act(self.copies.make(number, place, place, {"fsdp": jnp.clip(there, 0, line - 1)}))

    def hear(self, step, upward):
        index, line = self.index, self.line
        slot = index - 1 - step if upward else index + 1 + step
        comes = (slot >= 0) & (slot < line)
        number = self.first + step + (0 if upward else line - 1)

        @pl.when(comes)
        def _():
            place = self.place(jnp.clip(slot, 0, line - 1))
            self.copies.make(number, place, place, {"fsdp": 0}).wait_recv()

    def begin(self):
        for upward in (True, False):
            self.move(0, upward, lambda copy: copy.start())

    def hop(self, step):
        for upward in (True, False):
            self.hear(step - 1, upward)
            if step < self.line - 1:
                self.move(step, upward, lambda copy: copy.start())

    def finish(self):
        for step in range(self.line - 1):
            for upward in (True, False):
                self.move(step, upward, lambda copy: copy.wait_send())


def anywhere(count):
    return [pl.BlockSpec(memory_space=pl.ANY)] * count


def local_copies(pairs, sems):
    copies = [
        pltpu.make_async_copy(source, target, sems.at[number])
        for number, (source, target) in enumerate(pairs)
    ]
    for copy in copies:
        copy.start()
    return copies


def remote_params(number):
    return pltpu.CompilerParams(
        collective_id=number, has_side_effects=True, vmem_limit_bytes=48 << 20
    )


def first_kernel(line, x_ref, qkv_ref, wo_ref, gain_ref, xo_ref, qkvo_ref, woo_ref, gaino_ref, send, recv, here):
    me, index = lax.axis_index("ctx"), lax.axis_index("fsdp")
    rows = x_ref.shape[0]
    start_barrier(me, index, line)
    part = row_part(xo_ref, rows)
    local = local_copies(
        [
            (qkv_ref, qkvo_ref.at[index]),
            (wo_ref, woo_ref.at[index]),
            (gain_ref, gaino_ref.at[index]),
            (x_ref, part(me, slice(None))),
        ],
        here,
    )
    copies = Copies(send, recv)
    gather = PlaneGather(copies, me, row_half(x_ref, rows), part)
    lines = [
        LineGather(copies, index, line, lambda slot, ref=ref: ref.at[slot])
        for ref in (qkvo_ref, gaino_ref, woo_ref)
    ]
    gather.begin()
    for copy in local[:3]:
        copy.wait()
    for each in lines:
        each.begin()
    gather.first_hop()
    for step in range(1, line):
        for each in lines:
            each.hop(step)
        if step == 1:
            gather.second_hop()
    gather.third_hop()
    gather.last()
    for each in lines:
        each.finish()
    copies.finish()
    local[3].wait()


def first_exchange(line, x, qkv, wo, gains):
    plane = lax.axis_size("ctx")
    count = GATHER_COPIES + 6 * (line - 1)
    return pl.pallas_call(
        functools.partial(first_kernel, line),
        out_shape=(
            jax.ShapeDtypeStruct((plane * x.shape[0], x.shape[1]), x.dtype),
            *(jax.ShapeDtypeStruct((line, *a.shape), a.dtype) for a in (qkv, wo, gains)),
        ),
        in_specs=anywhere(4),
        out_specs=tuple(anywhere(4)),
        scratch_shapes=[
            pltpu.SemaphoreType.DMA((count,)),
            pltpu.SemaphoreType.DMA((count,)),
            pltpu.SemaphoreType.DMA((4,)),
        ],
        compiler_params=remote_params(1),
        name="first_exchange",
    )(x, qkv, wo, gains)


def second_kernel(line, o_ref, wo_ref, dy_ref, att_ref, woo_ref, dyo_ref, send, recv, here):
    me = lax.axis_index("ctx")
    rows = dy_ref.shape[0]
    start_barrier(me)
    copies = Copies(send, recv)

    def columns(slot):
        return att_ref.at[slot]

    def block(slot):
        return o_ref.at[pl.ds(pl.multiple_of(slot * rows, rows), rows), :]

    numbers = {}
    for bit in (6, 7, 4, 5, 2, 3, 1):
        numbers[bit] = copies.number()
        copies.send(numbers[bit], block(me ^ bit), columns(me), {"ctx": me ^ bit})
    local = local_copies(
        [
            (block(me), columns(me)),
            (wo_ref, woo_ref.at[:, me]),
            (dy_ref, row_part(dyo_ref, rows)(me, slice(None))),
        ],
        here,
    )
    middle = line // 2

    def wo_half(side):
        return wo_ref.at[pl.ds(side * middle, middle)]

    def wo_part(slot, side):
        if isinstance(side, slice):
            return woo_ref.at[:, slot]
        return woo_ref.at[pl.ds(side * middle, middle), slot]

    run_gathers(
        [
            PlaneGather(copies, me, wo_half, wo_part),
            PlaneGather(copies, me, row_half(dy_ref, rows), row_part(dyo_ref, rows)),
        ]
    )
    for bit, number in numbers.items():
        copies.arrived(number, columns(me ^ bit))
    for copy in local:
        copy.wait()
    copies.finish()


def second_exchange(o, wo, dy):
    plane = lax.axis_size("ctx")
    rows = dy.shape[0]
    line, part, model = wo.shape
    count = 2 * GATHER_COPIES + 7
    return pl.pallas_call(
        functools.partial(second_kernel, line),
        out_shape=(
            jax.ShapeDtypeStruct((plane, rows, o.shape[1]), o.dtype),
            jax.ShapeDtypeStruct((line, plane, part, model), wo.dtype),
            jax.ShapeDtypeStruct((plane * rows, model), dy.dtype),
        ),
        in_specs=anywhere(3),
        out_specs=tuple(anywhere(3)),
        scratch_shapes=[
            pltpu.SemaphoreType.DMA((count,)),
            pltpu.SemaphoreType.DMA((count,)),
            pltpu.SemaphoreType.DMA((3,)),
        ],
        compiler_params=remote_params(2),
        name="second_exchange",
    )(o, wo, dy)


def gather_kernel(x_ref, xo_ref, send, recv, here):
    me = lax.axis_index("ctx")
    rows = x_ref.shape[0]
    start_barrier(me)
    part = row_part(xo_ref, rows)
    local = local_copies([(x_ref, part(me, slice(None)))], here)
    copies = Copies(send, recv)
    run_gathers([PlaneGather(copies, me, row_half(x_ref, rows), part)])
    copies.finish()
    local[0].wait()


def plane_gather(x, number):
    plane = lax.axis_size("ctx")
    return pl.pallas_call(
        gather_kernel,
        out_shape=jax.ShapeDtypeStruct((plane * x.shape[0], x.shape[1]), x.dtype),
        in_specs=anywhere(1),
        out_specs=anywhere(1)[0],
        scratch_shapes=[
            pltpu.SemaphoreType.DMA((GATHER_COPIES,)),
            pltpu.SemaphoreType.DMA((GATHER_COPIES,)),
            pltpu.SemaphoreType.DMA((1,)),
        ],
        compiler_params=remote_params(number),
        name=f"plane_gather_{number}",
    )(x)


REDUCE_COPIES = 10


class PlaneReduce:
    def __init__(self, copies, me, block, heard, held, landed):
        self.copies, self.me, self.block = copies, me, block
        self.heard, self.held, self.landed = heard, held, landed
        self.first = copies.next
        copies.next += REDUCE_COPIES
        self.half = heard.shape[1] // 2

    def side(self, ref, slot, half):
        return ref.at[slot, pl.ds(half * self.half, self.half), :]

    def share(self, order):
        partner = self.me ^ 1
        bit = (6, 2, 4, 0)[order]
        self.copies.send(
            self.first + order, self.block(partner ^ bit), self.heard.at[order], {"ctx": partner}
        )

    def combine(self, order, rows, extra=None):
        bit = (6, 2, 4)[order]
        total = self.block(self.me ^ bit)[rows, :].astype(jnp.float32) + self.heard[
            order, rows, :
        ].astype(jnp.float32)
        if extra is not None:
            total = total + extra
        self.held[order, rows, :] = total.astype(self.held.dtype)

    def first_sends(self):
        me, copies, first, half = self.me, self.copies, self.first, self.half
        upper, lower = pl.ds(0, half), pl.ds(half, half)
        x, y = {"ctx": me ^ 2}, {"ctx": me ^ 4}
        held, landed, side = self.held, self.landed, self.side
        arrived = copies.arrived
        arrived(first + 0, self.heard.at[0])
        self.combine(0, pl.ds(0, 2 * half))
        copies.send(first + 4, side(held, 0, 0), side(landed, 0, 0), x)
        copies.send(first + 5, side(held, 0, 1), side(landed, 0, 1), y)
        arrived(first + 1, self.heard.at[1])
        self.combine(1, upper)
        copies.send(first + 6, side(held, 1, 0), side(landed, 1, 0), x)
        arrived(first + 2, self.heard.at[2])
        self.combine(2, lower)
        copies.send(first + 7, side(held, 2, 1), side(landed, 2, 1), y)

    def second_sends(self):
        me, copies, first, half = self.me, self.copies, self.first, self.half
        upper, lower = pl.ds(0, half), pl.ds(half, half)
        x, y = {"ctx": me ^ 2}, {"ctx": me ^ 4}
        held, landed, side = self.held, self.landed, self.side
        arrived = copies.arrived
        arrived(first + 5, side(landed, 0, 1))
        self.combine(1, lower, landed[0, lower, :].astype(jnp.float32))
        copies.send(first + 8, side(held, 1, 1), side(landed, 1, 1), x)
        arrived(first + 4, side(landed, 0, 0))
        self.combine(2, upper, landed[0, upper, :].astype(jnp.float32))
        copies.send(first + 9, side(held, 2, 0), side(landed, 2, 0), y)
        arrived(first + 3, self.heard.at[3])

    def sum_half(self, which):
        first, half = self.first, self.half
        rows = pl.ds(which * half, half)
        self.copies.arrived(first + (6, 8)[which], self.side(self.landed, 1, which))
        self.copies.arrived(first + (9, 7)[which], self.side(self.landed, 2, which))
        return (
            self.block(self.me)[rows, :].astype(jnp.float32)
            + self.heard[3, rows, :].astype(jnp.float32)
            + self.landed[1, rows, :].astype(jnp.float32)
            + self.landed[2, rows, :].astype(jnp.float32)
        )
def feed_kernel(
    line,
    g_ref,
    dy_ref,
    w_ref,
    sum_ref,
    out_ref,
    dw_ref,
    down_ref,
    all_g,
    hid,
    hid_t,
    gate_t,
    up_t,
    part,
    heard,
    held,
    landed,
    stage,
    send,
    recv,
    here,
):
    me = lax.axis_index("ctx")
    rows = g_ref.shape[0]
    width, model = down_ref.shape
    blocks = model // width
    unit = width // line
    start_barrier(me)
    copies = Copies(send, recv)
    gather = PlaneGather(copies, me, row_half(g_ref, rows), row_part(all_g, rows))
    gather.begin()

    def at(slot):
        return pl.ds(pl.multiple_of(slot * rows, rows), rows)

    all_g[at(me), :] = g_ref[...]
    gate_ref, up_ref = w_ref.at[:, :width], w_ref.at[:, width : 2 * width]
    for z in range(line):
        for number in range(blocks):
            source = pl.ds((z * blocks + number) * unit, unit)
            down_ref[pl.ds(z * unit, unit), number * width : (number + 1) * width] = w_ref[
                source, 2 * width :
            ]

    def block(slot):
        return part.at[at(slot), :]

    reduce = PlaneReduce(copies, me, block, heard, held, landed)

    def chunk(order):
        place = at(me ^ order)
        g = all_g[place, :]
        dy = dy_ref[place, :]
        gate_values = contract(g, gate_ref[...], 1, 0)
        up_values = contract(g, up_ref[...], 1, 0)
        sigmoid_gate = 1.0 / (1.0 + jnp.exp(-gate_values))
        activated = gate_values * sigmoid_gate
        hidden_act = (activated * up_values).astype(jnp.bfloat16)
        hid[place, :] = hidden_act
        hid_t[:, place] = hidden_act.T
        grad_hidden = contract(dy, down_ref[...], 1, 1)
        grad_gate = (
            grad_hidden * up_values * sigmoid_gate * (1.0 + gate_values * (1.0 - sigmoid_gate))
        ).astype(jnp.bfloat16)
        grad_up = (grad_hidden * activated).astype(jnp.bfloat16)
        gate_t[:, place] = grad_gate.T
        up_t[:, place] = grad_up.T
        part[place, :] = (
            contract(grad_gate, gate_ref[...], 1, 1) + contract(grad_up, up_ref[...], 1, 1)
        ).astype(jnp.bfloat16)

    def step(order, carry):
        for number, slot, sides, when in (
            (4, 1, 0, 1),
            (5, 1, 1, 1),
            (8, 3, 1, 3),
            (10, 3, 0, 3),
            (9, 5, 0, 5),
            (11, 5, 1, 5),
            (12, 7, slice(None), 7),
        ):

            @pl.when(order == when)
            def _(number=number, slot=slot, sides=sides):
                copies.arrived(gather.first + number, gather.part(me ^ slot, sides))

        chunk(order)
        return carry

    lax.fori_loop(0, 2, step, 0)
    gather.first_hop()
    gather.second_hop()
    reduce.share(3)
    lax.fori_loop(2, 6, step, 0)
    gather.third_hop()
    reduce.share(1)
    reduce.share(2)
    lax.fori_loop(6, 8, step, 0)
    reduce.share(0)

    chunks = dy_ref.shape[0] // rows

    def give(number, carry):
        slot = lax.rem(number, 2)
        copy = pltpu.make_async_copy(stage.at[slot], out_ref.at[at(number), :], here.at[slot])

        @pl.when(number >= 2)
        def _():
            copy.wait()

        stage[slot] = contract(hid[at(number), :], down_ref[...], 1, 0).astype(jnp.bfloat16)
        copy.start()
        return carry

    def weights(number, carry):
        columns = pl.ds(pl.multiple_of(number * width, width), width)
        total = contract(hid_t[...], dy_ref[:, columns], 1, 0).astype(jnp.bfloat16)
        for z in range(line):
            target = pl.ds(pl.multiple_of((z * blocks + number) * unit, unit), unit)
            dw_ref[target, 2 * width :] = total[z * unit : (z + 1) * unit, :]
        for side, left in enumerate((gate_t, up_t)):
            total = contract(left[...], all_g[:, columns], 1, 0).astype(jnp.bfloat16)
            dw_ref[columns, side * width : (side + 1) * width] = total.T
        return carry

    lax.fori_loop(0, 2, give, 0)
    reduce.first_sends()
    lax.fori_loop(2, chunks, give, 0)
    reduce.second_sends()
    lax.fori_loop(0, blocks, weights, 0)
    half = rows // 2
    for which in (1, 0):
        sum_ref[pl.ds(which * half, half), :] = reduce.sum_half(which)
    for slot in (0, 1):
        pltpu.make_async_copy(stage.at[slot], out_ref.at[at(slot), :], here.at[slot]).wait()
    copies.finish()


def feed(g, dy, w):
    plane, line = lax.axis_size("ctx"), lax.axis_size("fsdp")
    rows, model = g.shape
    tokens = plane * rows
    width = w.shape[1] // 3
    count = GATHER_COPIES + REDUCE_COPIES
    half_type = jnp.bfloat16
    return pl.pallas_call(
        functools.partial(feed_kernel, line),
        out_shape=(
            jax.ShapeDtypeStruct((rows, model), jnp.float32),
            jax.ShapeDtypeStruct((tokens, model), half_type),
            jax.ShapeDtypeStruct(w.shape, half_type),
        ),
        in_specs=in_vmem(3),
        out_specs=(*in_vmem(1), *anywhere(1), *in_vmem(1)),
        scratch_shapes=[
            pltpu.VMEM((width, model), half_type),
            pltpu.VMEM((tokens, model), half_type),
            pltpu.VMEM((tokens, width), half_type),
            pltpu.VMEM((width, tokens), half_type),
            pltpu.VMEM((width, tokens), half_type),
            pltpu.VMEM((width, tokens), half_type),
            pltpu.VMEM((tokens, model), half_type),
            pltpu.VMEM((4, rows, model), half_type),
            pltpu.VMEM((3, rows, model), half_type),
            pltpu.VMEM((3, rows, model), half_type),
            pltpu.VMEM((2, rows, model), half_type),
            pltpu.SemaphoreType.DMA((count,)),
            pltpu.SemaphoreType.DMA((count,)),
            pltpu.SemaphoreType.DMA((2,)),
        ],
        compiler_params=pltpu.CompilerParams(
            collective_id=3, has_side_effects=True, vmem_limit_bytes=60 << 20
        ),
        name="feed",
    )(g, dy, w)


def gradients_kernel(line, shapes, *refs):
    count = len(shapes)
    pieces, terms_ref = refs[:count], refs[count]
    wholes, total_ref = refs[count + 1 : 2 * count + 1], refs[2 * count + 1]
    heard, plane_sum, across, send, recv, here = refs[2 * count + 2 :]
    me, index = lax.axis_index("ctx"), lax.axis_index("fsdp")
    start_barrier(me, index, line)
    copies = Copies(send, recv)
    gathers, pairs = [], []
    for piece, whole in zip(pieces, wholes):
        rows = piece.shape[0]
        part = row_part(whole, rows)
        gathers.append(PlaneGather(copies, me, row_half(piece, rows), part))
        pairs.append((piece, part(me, slice(None))))
    first = copies.next
    copies.next += 7 + line - 1
    for bit in range(1, 8):
        copies.send(first + bit - 1, terms_ref, heard.at[bit], {"ctx": me ^ bit})
    for gather in gathers:
        gather.begin()
    local = local_copies(pairs, here)
    total = terms_ref[...]
    for bit in range(1, 8):
        copies.arrived(first + bit - 1, heard.at[bit])
        total = total + heard[bit]
    plane_sum[...] = total
    for step in range(1, line):
        peer = {"fsdp": lax.rem(index + step, line)}
        copies.send(first + 6 + step, plane_sum, across.at[step], peer)
    for gather in gathers:
        gather.first_hop()
    for gather in gathers:
        gather.second_hop()
    for step in range(1, line):
        copies.arrived(first + 6 + step, across.at[step])
        total = total + across[step]
    total_ref[...] = total
    for gather in gathers:
        gather.third_hop()
    for gather in gathers:
        gather.last()
    for copy in local:
        copy.wait()
    copies.finish()


def gather_gradients(pieces, terms, number):
    plane, line = lax.axis_size("ctx"), lax.axis_size("fsdp")
    count = len(pieces)
    copies = GATHER_COPIES * count + 7 + line - 1
    shapes = tuple(piece.shape for piece in pieces)
    return pl.pallas_call(
        functools.partial(gradients_kernel, line, shapes),
        out_shape=(
            *(
                jax.ShapeDtypeStruct((plane * piece.shape[0], piece.shape[1]), piece.dtype)
                for piece in pieces
            ),
            jax.ShapeDtypeStruct(terms.shape, terms.dtype),
        ),
        in_specs=anywhere(count) + in_vmem(1),
        out_specs=(*anywhere(count), *in_vmem(1)),
        scratch_shapes=[
            pltpu.VMEM((plane, *terms.shape), terms.dtype),
            pltpu.VMEM(terms.shape, terms.dtype),
            pltpu.VMEM((line, *terms.shape), terms.dtype),
            pltpu.SemaphoreType.DMA((copies,)),
            pltpu.SemaphoreType.DMA((copies,)),
            pltpu.SemaphoreType.DMA((count,)),
        ],
        compiler_params=remote_params(number),
        name=f"gather_gradients_{number}",
    )(*pieces, terms)


def spread_kernel(gate_in, up_in, down_in, gate_ref, up_ref, down_ref):
    plane, shard, unit = gate_in.shape
    for source, target in ((gate_in, gate_ref), (up_in, up_ref)):
        for slot in range(plane):
            target[:, slot * unit : (slot + 1) * unit] = source[slot].astype(jnp.float32)
    step = pl.program_id(0)
    width = down_in.shape[2]
    blocks = shard // unit
    for slot in range(down_in.shape[0]):
        for number in range(blocks):
            down_ref[slot * unit : (slot + 1) * unit, number * width : (number + 1) * width] = (
                down_in[slot, number * unit : (number + 1) * unit, :].astype(jnp.float32)
            )


def spread_feed(pieces, shard, line, unit):
    plane = lax.axis_size("ctx")
    width = line * unit
    model = line * shard
    pieces = pieces.reshape(plane, shard, 3 * width)
    each = plane // line
    return pl.pallas_call(
        spread_kernel,
        grid=(line,),
        in_specs=[
            pl.BlockSpec((plane, shard, unit), lambda z: (0, 0, z)),
            pl.BlockSpec((plane, shard, unit), lambda z: (0, 0, line + z)),
            pl.BlockSpec((each, shard, width), lambda z: (z, 0, 2)),
        ],
        out_specs=(
            pl.BlockSpec((shard, plane * unit), lambda z: (0, z)),
            pl.BlockSpec((shard, plane * unit), lambda z: (0, z)),
            pl.BlockSpec((each * unit, model), lambda z: (z, 0)),
        ),
        out_shape=(
            jax.ShapeDtypeStruct((shard, plane * width), jnp.float32),
            jax.ShapeDtypeStruct((shard, plane * width), jnp.float32),
            jax.ShapeDtypeStruct((plane * unit, model), jnp.float32),
        ),
        compiler_params=pltpu.CompilerParams(vmem_limit_bytes=40 << 20),
        name="spread_feed",
    )(pieces, pieces, pieces)


def spread_attention_kernel(in_ref, q_ref, k_ref, v_ref, wo_ref):
    plane, _, across = in_ref.shape
    shard = q_ref.shape[0]
    key_width = k_ref.shape[1] // plane
    query_width = q_ref.shape[1] // plane
    first = 0
    for target, width in ((q_ref, query_width), (k_ref, key_width), (v_ref, key_width)):
        target[...] = jnp.concatenate(
            [
                in_ref[slot, :shard, first : first + width].astype(jnp.float32)
                for slot in range(plane)
            ],
            axis=1,
        )
        first += width
    for slot in range(plane):
        for number in range(wo_ref.shape[1] // across):
            source = slice(shard + number * HALF, shard + (number + 1) * HALF)
            wo_ref[slot * HALF : (slot + 1) * HALF, number * across : (number + 1) * across] = (
                in_ref[slot, source, :].astype(jnp.float32)
            )


def spread_attention(pieces, shard, model, query_width, key_width):
    plane = lax.axis_size("ctx")
    pieces = pieces.reshape(plane, -1, pieces.shape[1])
    f32 = jnp.float32
    return pl.pallas_call(
        spread_attention_kernel,
        in_specs=in_vmem(1),
        out_specs=tuple(in_vmem(4)),
        out_shape=(
            jax.ShapeDtypeStruct((shard, plane * query_width), f32),
            jax.ShapeDtypeStruct((shard, plane * key_width), f32),
            jax.ShapeDtypeStruct((shard, plane * key_width), f32),
            jax.ShapeDtypeStruct((plane * HALF, model), f32),
        ),
        compiler_params=pltpu.CompilerParams(vmem_limit_bytes=40 << 20),
        name="spread_attention",
    )(pieces)


def last_sums_kernel(
    dx_ref, out_ref, dqkv_ref, wo_ref, dx_sum, out_sum, grads_ref, heard, held, landed, send, recv, here
):
    me = lax.axis_index("ctx")
    rows = dx_sum.shape[0]
    start_barrier(me)
    copies = Copies(send, recv)

    def at(slot):
        return pl.ds(pl.multiple_of(slot * rows, rows), rows)

    pieces, wo_rows = wo_ref.shape[:2]
    line, grad_rows = grads_ref.shape[:2]
    shard = grad_rows - wo_rows
    to_first = pieces * lax.rem(me, 2)
    line_slot = lax.div(me, 2)
    wo_first = copies.next
    copies.next += pieces

    def wo_place(slot):
        return grads_ref.at[slot, pl.ds(shard, wo_rows), :]

    def wo_copy(piece):
        return copies.make(
            wo_first + piece,
            wo_ref.at[piece],
            wo_place(line_slot),
            {"ctx": to_first + piece},
            wo_first + line_slot,
        )

    for piece in range(pieces):

        @pl.when(to_first + piece != me)
        def _(piece=piece):
            wo_copy(piece).start()

        @pl.when(to_first + piece == me)
        def _(piece=piece):
            wo_place(line_slot)[...] = wo_ref[piece]

    reduces = []
    for number, ref in enumerate((dx_ref, out_ref)):
        reduces.append(
            PlaneReduce(
                copies,
                me,
                lambda slot, ref=ref: ref.at[at(slot), :],
                heard.at[number],
                held.at[number],
                landed.at[number],
            )
        )
    for reduce in reduces:
        for order in range(4):
            reduce.share(order)
    for slot in range(line):
        grads_ref[slot, :shard, :] = dqkv_ref[slot * shard : (slot + 1) * shard, :]
    for reduce in reduces:
        reduce.first_sends()
    for reduce in reduces:
        reduce.second_sends()
    half = rows // 2
    for which in (1, 0):
        for reduce, target in zip(reduces, (dx_sum, out_sum)):
            target[pl.ds(which * half, half), :] = reduce.sum_half(which)
    for slot in range(line):

        @pl.when(2 * slot + lax.div(me, pieces) != me)
        def _(slot=slot):
            copies.make(
                wo_first, wo_ref.at[0], wo_place(slot), {"ctx": 0}, wo_first + slot
            ).wait_recv()

    for piece in range(pieces):

        @pl.when(to_first + piece != me)
        def _(piece=piece):
            wo_copy(piece).wait_send()

    copies.finish()


def last_sums(dx, out, dqkv, wo, line):
    plane = lax.axis_size("ctx")
    rows, model = dx.shape[0] // plane, dx.shape[1]
    count = 2 * REDUCE_COPIES + wo.shape[0]
    across = dqkv.shape[1]
    return pl.pallas_call(
        last_sums_kernel,
        out_shape=(
            jax.ShapeDtypeStruct((rows, model), jnp.float32),
            jax.ShapeDtypeStruct((rows, model), jnp.float32),
            jax.ShapeDtypeStruct((line, dqkv.shape[0] // line + wo.shape[1], across), dqkv.dtype),
        ),
        in_specs=in_vmem(4),
        out_specs=tuple(in_vmem(3)),
        scratch_shapes=[
            pltpu.VMEM((2, 4, rows, model), dx.dtype),
            pltpu.VMEM((2, 3, rows, model), dx.dtype),
            pltpu.VMEM((2, 3, rows, model), dx.dtype),
            pltpu.SemaphoreType.DMA((count,)),
            pltpu.SemaphoreType.DMA((count,)),
            pltpu.SemaphoreType.DMA((1,)),
        ],
        compiler_params=remote_params(7),
        name="last_sums",
    )(dx, out, dqkv, wo)
def head_local(
    block_input,
    block_table,
    output_grad,
    attention_gain,
    query_weight,
    key_weight,
    value_projection,
    output_weight,
    feedforward_gain,
    gate_weight,
    up_weight,
    down_weight,
):
    me = lax.axis_index("ctx")
    plane = lax.axis_size("ctx")
    line = lax.axis_size("fsdp")
    rows, model = block_input.shape[1:]
    shard = model // line
    hidden = gate_weight.shape[1]
    unit = hidden // (line * plane)
    table_row = block_table[0]
    slot_count = table_row.shape[0]
    block = rows * plane // slot_count
    places = jnp.arange(slot_count, dtype=jnp.int32)
    slots = jnp.sum(jnp.where(table_row[None, :] == places[:, None], places[None, :], 0), axis=1)

    def mine(array, width):
        return lax.dynamic_slice_in_dim(array, me * width, width, 1)

    query_width = query_weight.shape[1] // plane
    key_width = key_weight.shape[1] // plane
    qkv_mine = jnp.concatenate(
        [
            mine(query_weight, query_width),
            mine(key_weight, key_width),
            mine(value_projection, key_width),
        ],
        axis=1,
    )
    wo_mine = lax.dynamic_slice_in_dim(output_weight, me * HALF, HALF, 0)
    gains_mine = jnp.stack([attention_gain, feedforward_gain])
    x_all, qkv_w, wo_line, gains = first_exchange(
        line, block_input[0], qkv_mine, wo_mine, gains_mine
    )

    feed_width = line * unit
    blocks = [
        lax.dynamic_slice_in_dim(array, (z * plane + me) * unit, unit, 1)
        for array in (gate_weight, up_weight)
        for z in range(line)
    ]
    down_mine = lax.dynamic_slice_in_dim(down_weight, me * unit, unit, 0)
    down_mine = jnp.concatenate(
        [down_mine[:, at : at + feed_width] for at in range(0, model, feed_width)], axis=0
    )
    feed_mine = jnp.concatenate([*blocks, down_mine], axis=1)
    feed_mine, x_all = lax.optimization_barrier((feed_mine, x_all))
    feed_w = lax.all_gather(feed_mine, "fsdp", axis=0, tiled=True)

    steps_index = jnp.arange(HALF, dtype=jnp.float32)
    inverse = jnp.exp(steps_index * jnp.float32(-2.0 * math.log(rotary_base) / HEAD_SIZE))

    def table_of(positions):
        angles = positions.astype(jnp.float32)[:, None] * inverse[None, :]
        both = jnp.stack([jnp.cos(angles), jnp.sin(angles)])
        both = jnp.pad(both, ((0, 0), (0, 0), (0, LANES // 2 - HALF)))
        return jnp.concatenate([both, both], axis=2)

    inner = table_of(jnp.arange(block, dtype=jnp.int32))
    outer = table_of(places * block)
    pad = padding(GROUP + 2)

    gains = jnp.transpose(gains, (1, 0, 2)).reshape(2, model).astype(jnp.float32)
    qkv_w = qkv_w.reshape(model, -1)
    gained_one, qkv, o, lse = attend(slots, x_all, gains[:1], qkv_w, pad, inner, outer)

    attended, wo_full, grad_all = second_exchange(o, wo_line, output_grad[0])
    attended = jnp.transpose(attended, (1, 0, 2)).reshape(rows, -1)
    wo_full = wo_full.reshape(-1, model)
    inputs = block_input[0].astype(jnp.float32)
    residual = inputs + product(attended, wo_full)
    scale_two = norm_scale(residual)
    normed_two = residual * scale_two
    grad_normed_two, out_parts, feed_grads = feed(
        (normed_two * gains[1]).astype(jnp.bfloat16), grad_all, feed_w
    )
    feed_grads = lax.psum_scatter(feed_grads, "fsdp", scatter_dimension=0, tiled=True)
    feedforward_term = jnp.sum(grad_normed_two * normed_two, axis=0)
    grad_scaled_two = grad_normed_two * gains[1]
    grad_residual = output_grad[0].astype(jnp.float32) + scale_two * (
        grad_scaled_two
        - normed_two * jnp.mean(grad_scaled_two * normed_two, axis=-1, keepdims=True)
    )
    grad_attn = plane_gather(grad_residual.astype(jnp.bfloat16), 6)
    own = GROUP * HEAD_SIZE
    wo_mine = lax.dynamic_slice_in_dim(wo_full, me * own, own, 0)
    dx, qkv_term, wo_term = attend_back(
        slots, grad_attn, gained_one, qkv, o, lse, qkv_w, wo_mine, pad, inner, outer
    )
    grad_normed_one, out_sum, attention_grads = last_sums(dx, out_parts, qkv_term, wo_term, line)
    attention_grads = lax.psum_scatter(
        attention_grads.reshape(-1, attention_grads.shape[2]),
        "fsdp",
        scatter_dimension=0,
        tiled=True,
    )
    layer_output = (residual + out_sum).astype(jnp.bfloat16)
    scale_one = norm_scale(inputs)
    normed_one = inputs * scale_one
    attention_term = jnp.sum(grad_normed_one * normed_one, axis=0)
    grad_scaled_one = grad_normed_one * gains[0]
    input_grad = grad_residual + scale_one * (
        grad_scaled_one
        - normed_one * jnp.mean(grad_scaled_one * normed_one, axis=-1, keepdims=True)
    )
    feed_pieces, gain_terms = gather_gradients(
        [feed_grads], jnp.stack([attention_term, feedforward_term]), 8
    )
    gate_grad, up_grad, down_grad = spread_feed(feed_pieces, shard, line, unit)
    attention_pieces = plane_gather(attention_grads, 9)
    query_grad, key_grad, value_grad, out_grad = spread_attention(
        attention_pieces, shard, model, query_width, key_width
    )
    gain_terms = lax.dynamic_slice_in_dim(gain_terms, lax.axis_index("fsdp") * shard, shard, 1)
    return (
        layer_output[None],
        input_grad[None],
        gain_terms[0],
        query_grad,
        key_grad,
        value_grad,
        out_grad,
        gain_terms[1],
        gate_grad,
        up_grad,
        down_grad,
    )


def solution(mesh):
    plane, line = mesh.shape["ctx"], mesh.shape["fsdp"]
    fits = plane == KEY_VALUE_HEADS == 8 and plane * line * HALF == QUERY_HEADS * HEAD_SIZE
    plan = head_local if fits else local
    return jax.shard_map(
        plan,
        mesh=mesh,
        in_specs=(
            P("fsdp", "ctx", None),
            P("fsdp", None),
            P("fsdp", "ctx", None),
            P("fsdp"),
            P("fsdp", None),
            P("fsdp", None),
            P("fsdp", None),
            P("fsdp", None),
            P("fsdp"),
            P("fsdp", None),
            P("fsdp", None),
            P("fsdp", None),
        ),
        out_specs=(
            P("fsdp", "ctx", None),
            P("fsdp", "ctx", None),
            P("fsdp"),
            P("fsdp", None),
            P("fsdp", None),
            P("fsdp", None),
            P("fsdp", None),
            P("fsdp"),
            P("fsdp", None),
            P("fsdp", None),
            P("fsdp", None),
        ),
        check_vma=False,
    )
```

```python
import functools
import math

import jax
import jax.numpy as jnp
from jax import lax
from jax.experimental import pallas as pl
from jax.experimental.pallas import tpu as pltpu
from jax.sharding import PartitionSpec as P


QUERY_HEADS = 16
KEY_VALUE_HEADS = 8
HEAD_SIZE = 96


norm_epsilon = 1e-05
rotary_base = 100000.0
score_with_mask = -1e30


def rope_tables(positions):
    half_width = HEAD_SIZE // 2
    steps_index = jnp.arange(half_width, dtype=jnp.float32)
    inverse = jnp.exp(steps_index * jnp.float32(-2.0 * math.log(rotary_base) / HEAD_SIZE))
    angles = positions.astype(jnp.float32)[:, None] * inverse[None, :]
    return (jnp.cos(angles), jnp.sin(angles))


def rotate(value_rows, cosine, sine_values, direction):
    count_of_rows = value_rows.shape[0]
    head_count = value_rows.shape[1] // HEAD_SIZE
    half_width = HEAD_SIZE // 2
    shaped = value_rows.reshape(count_of_rows, head_count, HEAD_SIZE)
    first_half = shaped[:, :, :half_width]
    second_half = shaped[:, :, half_width:]
    cos_part = cosine[:, None, :]
    sin_part = sine_values[:, None, :] * direction
    turned = jnp.concatenate(
        [
            first_half * cos_part - second_half * sin_part,
            second_half * cos_part + first_half * sin_part,
        ],
        axis=2,
    )
    return turned.reshape(count_of_rows, head_count * HEAD_SIZE)


def norm_scale(value_rows):
    return lax.rsqrt(jnp.mean(value_rows * value_rows, axis=-1, keepdims=True) + norm_epsilon)


def product(matrix, operand):
    return jnp.dot(matrix, operand, preferred_element_type=jnp.float32)


def cross_rows(matrix, operand):
    return lax.dot_general(
        matrix, operand, (((0,), (0,)), ((), ())), preferred_element_type=jnp.float32
    )


def back_product(matrix, operand):
    return lax.dot_general(
        matrix, operand, (((1,), (1,)), ((), ())), preferred_element_type=jnp.float32
    )


def block_scores(query_rank_four, block_of_keys, query_positions, key_positions):
    keys_rank_three = block_of_keys.reshape(block_of_keys.shape[0], KEY_VALUE_HEADS, HEAD_SIZE)
    scores = jnp.einsum(
        "rgjd,kgd->gjrk", query_rank_four, keys_rank_three, preferred_element_type=jnp.float32
    ) * HEAD_SIZE ** (-0.5)
    allowed = (key_positions[None, :] <= query_positions[:, None])[None, None]
    return (jnp.where(allowed, scores, score_with_mask), allowed)


def local(
    block_input,
    block_table,
    output_grad,
    attention_gain,
    query_weight,
    key_weight,
    value_projection,
    output_weight,
    feedforward_gain,
    gate_weight,
    up_weight,
    down_weight,
):
    query_group_width = QUERY_HEADS // KEY_VALUE_HEADS
    score_scale = HEAD_SIZE ** (-0.5)
    inputs = block_input[0].astype(jnp.float32)
    count_of_rows = inputs.shape[0]
    block_rows = count_of_rows // 2
    ctx_index = lax.axis_index("ctx")
    table_row = block_table[0]
    offsets = jnp.arange(block_rows, dtype=jnp.int32)
    query_blocks = lax.dynamic_slice_in_dim(table_row, 2 * ctx_index, 2)
    query_positions = (query_blocks[:, None] * block_rows + offsets[None, :]).reshape(count_of_rows)
    key_positions = (table_row[:, None] * block_rows + offsets[None, :]).reshape(-1)
    cosine, sine_values = rope_tables(query_positions)
    gain_one, query_full, key_full, value_full, out_full = (
        lax.all_gather(attention_gain, "fsdp", axis=0, tiled=True),
        lax.all_gather(query_weight, "fsdp", axis=0, tiled=True),
        lax.all_gather(key_weight, "fsdp", axis=0, tiled=True),
        lax.all_gather(value_projection, "fsdp", axis=0, tiled=True),
        lax.all_gather(output_weight, "fsdp", axis=0, tiled=True),
    )
    scale_one = norm_scale(inputs)
    normed_one = inputs * scale_one
    gained_one = (normed_one * gain_one.astype(jnp.float32)).astype(jnp.bfloat16)
    query_rows = rotate(product(gained_one, query_full), cosine, sine_values, 1.0).astype(
        jnp.bfloat16
    )
    keys_local = rotate(product(gained_one, key_full), cosine, sine_values, 1.0).astype(
        jnp.bfloat16
    )
    values_local = product(gained_one, value_full).astype(jnp.bfloat16)
    keys_all, values_all = (
        lax.all_gather(keys_local, "ctx", axis=0, tiled=True),
        lax.all_gather(values_local, "ctx", axis=0, tiled=True),
    )
    key_total_count = keys_all.shape[0]
    key_block_pass = 1024
    block_count = key_total_count // key_block_pass
    query_rank_four = query_rows.reshape(
        count_of_rows, KEY_VALUE_HEADS, query_group_width, HEAD_SIZE
    )
    key_places = key_positions.reshape(block_count, key_block_pass)

    def split_keys(array_in):
        return array_in.reshape(block_count, key_block_pass, array_in.shape[-1])

    def statistics_step(state_now, block_data):
        running_max, running_sum = state_now
        block_of_keys, key_place = block_data
        masked, allowed = block_scores(query_rank_four, block_of_keys, query_positions, key_place)
        new_max = jnp.maximum(running_max, jnp.max(masked, axis=-1))
        block_sum = jnp.sum(jnp.where(allowed, jnp.exp(masked - new_max[..., None]), 0.0), axis=-1)
        return ((new_max, running_sum * jnp.exp(running_max - new_max) + block_sum), None)

    initial_maximum = jnp.full(
        (KEY_VALUE_HEADS, query_group_width, count_of_rows), score_with_mask, jnp.float32
    )
    initial_sum = jnp.zeros((KEY_VALUE_HEADS, query_group_width, count_of_rows), jnp.float32)
    (final_max, final_sum), unused = lax.scan(
        statistics_step, (initial_maximum, initial_sum), (split_keys(keys_all), key_places)
    )
    log_total = final_max + jnp.log(final_sum)

    def output_step(state_now, block_data):
        block_of_keys, block_of_values, key_place = block_data
        masked, allowed = block_scores(query_rank_four, block_of_keys, query_positions, key_place)
        weights_half = jnp.where(allowed, jnp.exp(masked - log_total[..., None]), 0.0).astype(
            jnp.bfloat16
        )
        values_rank_three = block_of_values.reshape(key_block_pass, KEY_VALUE_HEADS, HEAD_SIZE)
        return (
            state_now
            + jnp.einsum(
                "gjrk,kgd->rgjd",
                weights_half,
                values_rank_three,
                preferred_element_type=jnp.float32,
            ),
            None,
        )

    initial_output = jnp.zeros(
        (count_of_rows, KEY_VALUE_HEADS, query_group_width, HEAD_SIZE), jnp.float32
    )
    summed_out, unused = lax.scan(
        output_step, initial_output, (split_keys(keys_all), split_keys(values_all), key_places)
    )
    attended_rows = summed_out.reshape(count_of_rows, QUERY_HEADS * HEAD_SIZE).astype(jnp.bfloat16)
    residual = inputs + product(attended_rows, out_full)
    scale_two = norm_scale(residual)
    normed_two = residual * scale_two
    gain_two, gate_full, up_full, down_full = (
        lax.all_gather(feedforward_gain, "fsdp", axis=0, tiled=True),
        lax.all_gather(gate_weight, "fsdp", axis=0, tiled=True),
        lax.all_gather(up_weight, "fsdp", axis=0, tiled=True),
        lax.all_gather(down_weight, "fsdp", axis=0, tiled=True),
    )
    gained_two = (normed_two * gain_two.astype(jnp.float32)).astype(jnp.bfloat16)
    gate_values = product(gained_two, gate_full)
    up_values = product(gained_two, up_full)
    sigmoid_gate = jax.nn.sigmoid(gate_values)
    activated = gate_values * sigmoid_gate
    hidden_act = (activated * up_values).astype(jnp.bfloat16)
    layer_output = (residual + product(hidden_act, down_full)).astype(jnp.bfloat16)
    gain_two_again, gate_back, up_back, down_back = (
        lax.all_gather(feedforward_gain, "fsdp", axis=0, tiled=True),
        lax.all_gather(gate_weight, "fsdp", axis=0, tiled=True),
        lax.all_gather(up_weight, "fsdp", axis=0, tiled=True),
        lax.all_gather(down_weight, "fsdp", axis=0, tiled=True),
    )
    grad_rows = output_grad[0]
    grad_hidden = back_product(grad_rows, down_back)
    down_term = cross_rows(hidden_act, grad_rows)
    grad_gate = (
        grad_hidden * up_values * sigmoid_gate * (1.0 + gate_values * (1.0 - sigmoid_gate))
    ).astype(jnp.bfloat16)
    grad_up = (grad_hidden * activated).astype(jnp.bfloat16)
    gate_term = cross_rows(gained_two, grad_gate)
    up_term = cross_rows(gained_two, grad_up)
    grad_normed_two = back_product(grad_gate, gate_back) + back_product(grad_up, up_back)
    feedforward_term = jnp.sum(grad_normed_two * normed_two, axis=0)
    grad_scaled_two = grad_normed_two * gain_two_again.astype(jnp.float32)
    grad_residual = grad_rows.astype(jnp.float32) + scale_two * (
        grad_scaled_two
        - normed_two * jnp.mean(grad_scaled_two * normed_two, axis=-1, keepdims=True)
    )
    gain_one_again, query_back, key_back, value_back, out_back = (
        lax.all_gather(attention_gain, "fsdp", axis=0, tiled=True),
        lax.all_gather(query_weight, "fsdp", axis=0, tiled=True),
        lax.all_gather(key_weight, "fsdp", axis=0, tiled=True),
        lax.all_gather(value_projection, "fsdp", axis=0, tiled=True),
        lax.all_gather(output_weight, "fsdp", axis=0, tiled=True),
    )
    grad_attn = grad_residual.astype(jnp.bfloat16)
    output_term = cross_rows(attended_rows, grad_attn)
    attended_gradient = back_product(grad_attn, out_back).astype(jnp.bfloat16)
    gradient_rank_four = attended_gradient.reshape(
        count_of_rows, KEY_VALUE_HEADS, query_group_width, HEAD_SIZE
    )
    attended_rank_four = attended_rows.reshape(
        count_of_rows, KEY_VALUE_HEADS, query_group_width, HEAD_SIZE
    )
    row_delta = jnp.transpose(
        jnp.sum(
            gradient_rank_four.astype(jnp.float32) * attended_rank_four.astype(jnp.float32), axis=-1
        ),
        (1, 2, 0),
    )
    keys_again, values_again = (
        lax.all_gather(keys_local, "ctx", axis=0, tiled=True),
        lax.all_gather(values_local, "ctx", axis=0, tiled=True),
    )

    def back_step(state_now, block_data):
        block_of_keys, block_of_values, key_place = block_data
        masked, allowed = block_scores(query_rank_four, block_of_keys, query_positions, key_place)
        weights_half = jnp.where(allowed, jnp.exp(masked - log_total[..., None]), 0.0).astype(
            jnp.bfloat16
        )
        values_rank_three = block_of_values.reshape(key_block_pass, KEY_VALUE_HEADS, HEAD_SIZE)
        keys_rank_three = block_of_keys.reshape(key_block_pass, KEY_VALUE_HEADS, HEAD_SIZE)
        grad_weights = jnp.einsum(
            "rgjd,kgd->gjrk",
            gradient_rank_four,
            values_rank_three,
            preferred_element_type=jnp.float32,
        )
        grad_scores = (
            weights_half.astype(jnp.float32) * (grad_weights - row_delta[..., None]) * score_scale
        ).astype(jnp.bfloat16)
        state_now = state_now + jnp.einsum(
            "gjrk,kgd->rgjd", grad_scores, keys_rank_three, preferred_element_type=jnp.float32
        )
        key_gradient = jnp.einsum(
            "gjrk,rgjd->kgd", grad_scores, query_rank_four, preferred_element_type=jnp.float32
        )
        value_gradient = jnp.einsum(
            "gjrk,rgjd->kgd", weights_half, gradient_rank_four, preferred_element_type=jnp.float32
        )
        return (
            state_now,
            (
                key_gradient.reshape(key_block_pass, KEY_VALUE_HEADS * HEAD_SIZE).astype(
                    jnp.bfloat16
                ),
                value_gradient.reshape(key_block_pass, KEY_VALUE_HEADS * HEAD_SIZE).astype(
                    jnp.bfloat16
                ),
            ),
        )

    first_query_index = jnp.zeros(
        (count_of_rows, KEY_VALUE_HEADS, query_group_width, HEAD_SIZE), jnp.float32
    )
    query_sum, (key_gradients, value_gradients) = lax.scan(
        back_step, first_query_index, (split_keys(keys_again), split_keys(values_again), key_places)
    )
    key_gradients = key_gradients.reshape(key_total_count, KEY_VALUE_HEADS * HEAD_SIZE)
    value_gradients = value_gradients.reshape(key_total_count, KEY_VALUE_HEADS * HEAD_SIZE)
    key_sums, value_sums = (
        lax.psum_scatter(key_gradients, "ctx", scatter_dimension=0, tiled=True).astype(jnp.float32),
        lax.psum_scatter(value_gradients, "ctx", scatter_dimension=0, tiled=True).astype(
            jnp.float32
        ),
    )
    query_gradients = rotate(
        query_sum.reshape(count_of_rows, QUERY_HEADS * HEAD_SIZE), cosine, sine_values, -1.0
    ).astype(jnp.bfloat16)
    grad_keys = rotate(key_sums, cosine, sine_values, -1.0).astype(jnp.bfloat16)
    grad_values = value_sums.astype(jnp.bfloat16)
    query_term = cross_rows(gained_one, query_gradients)
    key_term = cross_rows(gained_one, grad_keys)
    value_term = cross_rows(gained_one, grad_values)
    grad_normed_one = (
        back_product(query_gradients, query_back)
        + back_product(grad_keys, key_back)
        + back_product(grad_values, value_back)
    )
    attention_term = jnp.sum(grad_normed_one * normed_one, axis=0)
    grad_scaled_one = grad_normed_one * gain_one_again.astype(jnp.float32)
    input_grad = grad_residual + scale_one * (
        grad_scaled_one
        - normed_one * jnp.mean(grad_scaled_one * normed_one, axis=-1, keepdims=True)
    )
    shares = (
        lax.psum_scatter(
            attention_term.astype(jnp.bfloat16), "fsdp", scatter_dimension=0, tiled=True
        ).astype(jnp.float32),
        lax.psum_scatter(
            query_term.astype(jnp.bfloat16), "fsdp", scatter_dimension=0, tiled=True
        ).astype(jnp.float32),
        lax.psum_scatter(
            key_term.astype(jnp.bfloat16), "fsdp", scatter_dimension=0, tiled=True
        ).astype(jnp.float32),
        lax.psum_scatter(
            value_term.astype(jnp.bfloat16), "fsdp", scatter_dimension=0, tiled=True
        ).astype(jnp.float32),
        lax.psum_scatter(
            output_term.astype(jnp.bfloat16), "fsdp", scatter_dimension=0, tiled=True
        ).astype(jnp.float32),
        lax.psum_scatter(
            feedforward_term.astype(jnp.bfloat16), "fsdp", scatter_dimension=0, tiled=True
        ).astype(jnp.float32),
        lax.psum_scatter(
            gate_term.astype(jnp.bfloat16), "fsdp", scatter_dimension=0, tiled=True
        ).astype(jnp.float32),
        lax.psum_scatter(
            up_term.astype(jnp.bfloat16), "fsdp", scatter_dimension=0, tiled=True
        ).astype(jnp.float32),
        lax.psum_scatter(
            down_term.astype(jnp.bfloat16), "fsdp", scatter_dimension=0, tiled=True
        ).astype(jnp.float32),
    )
    totals = (
        lax.psum(shares[0].astype(jnp.bfloat16), "ctx").astype(jnp.float32),
        lax.psum(shares[1].astype(jnp.bfloat16), "ctx").astype(jnp.float32),
        lax.psum(shares[2].astype(jnp.bfloat16), "ctx").astype(jnp.float32),
        lax.psum(shares[3].astype(jnp.bfloat16), "ctx").astype(jnp.float32),
        lax.psum(shares[4].astype(jnp.bfloat16), "ctx").astype(jnp.float32),
        lax.psum(shares[5].astype(jnp.bfloat16), "ctx").astype(jnp.float32),
        lax.psum(shares[6].astype(jnp.bfloat16), "ctx").astype(jnp.float32),
        lax.psum(shares[7].astype(jnp.bfloat16), "ctx").astype(jnp.float32),
        lax.psum(shares[8].astype(jnp.bfloat16), "ctx").astype(jnp.float32),
    )
    return (
        layer_output[None],
        input_grad[None],
        totals[0],
        totals[1],
        totals[2],
        totals[3],
        totals[4],
        totals[5],
        totals[6],
        totals[7],
        totals[8],
    )


LANES = 128
HALF = HEAD_SIZE // 2
GROUP = QUERY_HEADS // KEY_VALUE_HEADS
score_scale = HEAD_SIZE ** (-0.5)
binary_scale = score_scale * math.log2(math.e)


def contract(left, right, left_dim, right_dim):
    return lax.dot_general(
        left, right, (((left_dim,), (right_dim,)), ((), ())), preferred_element_type=jnp.float32
    )


def in_vmem(count):
    return [pl.BlockSpec(memory_space=pltpu.VMEM)] * count


def padding(heads):
    column = jnp.arange(heads * HEAD_SIZE, dtype=jnp.int32)
    half_at, rest = column // HALF, column % HALF
    target = half_at * (LANES // 2) + rest
    lanes = jnp.arange(heads * LANES, dtype=jnp.int32)
    return (target[:, None] == lanes[None, :]).astype(jnp.bfloat16)


def turn(part, cosine, sine):
    return part * cosine + pltpu.roll(part, LANES // 2, 1) * sine


def tables(inner_ref, outer_ref, index, per_tile):
    inner_cos, inner_sin = inner_ref[0], inner_ref[1]
    sign = jnp.where(
        lax.broadcasted_iota(jnp.int32, inner_cos.shape, 1) < LANES // 2, -1.0, 1.0
    )
    cosines, sines = [], []
    for part in range(per_tile):
        at = pl.ds(index * per_tile + part, 1)
        outer_cos, outer_sin = outer_ref[0, at, :], outer_ref[1, at, :]
        cosines.append(inner_cos * outer_cos - inner_sin * outer_sin)
        sines.append(sign * (inner_sin * outer_cos + inner_cos * outer_sin))
    return jnp.concatenate(cosines, axis=0), jnp.concatenate(sines, axis=0)


def forward_kernel(
    slot_ref,
    xa_ref,
    xb_ref,
    gain_ref,
    w_ref,
    pad_ref,
    inner_ref,
    outer_ref,
    gained_ref,
    qkv_ref,
    o_ref,
    lse_ref,
    wp,
    qs,
    vt,
    s_ref,
):
    index = pl.program_id(0)
    block = xa_ref.shape[0]
    tile = 2 * block
    width = GROUP * tile
    heads = GROUP + 2

    @pl.when(index == 0)
    def _():
        wp[...] = contract(w_ref[...], pad_ref[...], 1, 0).astype(jnp.bfloat16)

    x = jnp.concatenate([xa_ref[...], xb_ref[...]], axis=0).astype(jnp.float32)
    normed = x * lax.rsqrt(jnp.mean(x * x, axis=-1, keepdims=True) + norm_epsilon)
    gained = (normed * gain_ref[...]).astype(jnp.bfloat16)
    gained_ref[...] = gained
    raw = contract(gained, wp[...], 1, 0)
    cosine, sine = tables(inner_ref, outer_ref, index, 2)
    here = pl.ds(pl.multiple_of(index * tile, tile), tile)
    for head in range(heads):
        lanes = slice(head * LANES, (head + 1) * LANES)
        part = raw[:, lanes]
        if head <= GROUP:
            part = turn(part, cosine, sine)
        part = part.astype(jnp.bfloat16)
        qkv_ref[here, lanes] = part
        if head < GROUP:
            qs[head * tile : (head + 1) * tile, :] = part
        if head == heads - 1:
            vt[:, here] = part.T
    queries = qs[...]
    key_at = lax.broadcasted_iota(jnp.int32, (tile, width), 0)
    query_at = lax.rem(lax.broadcasted_iota(jnp.int32, (tile, width), 1), tile)
    diagonal = key_at <= query_at

    def scores_of(step):
        at = pl.ds(pl.multiple_of(step * tile, tile), tile)
        keys = qkv_ref[at, GROUP * LANES : (GROUP + 1) * LANES]
        return contract(keys, queries, 1, 1) * binary_scale

    last = jnp.where(diagonal, scores_of(index), score_with_mask)
    s_ref[here, :] = last
    peak = jnp.max(last, axis=0, keepdims=True)

    def in_pairs(one, state):
        state = lax.fori_loop(
            0, lax.div(index, 2), lambda pair, state: one((2 * pair, 2 * pair + 1), state), state
        )
        return lax.fori_loop(0, lax.rem(index, 2), lambda _, state: one((index - 1,), state), state)

    def first_pass(steps, peak):
        found = [scores_of(step) for step in steps]
        for step, scores in zip(steps, found):
            s_ref[pl.ds(pl.multiple_of(step * tile, tile), tile), :] = scores
            peak = jnp.maximum(peak, jnp.max(scores, axis=0, keepdims=True))
        return peak

    peak = in_pairs(first_pass, peak)

    def second_pass(steps, state):
        total, out = state
        for step in steps:
            at = pl.ds(pl.multiple_of(step * tile, tile), tile)
            probs = jnp.exp2(s_ref[at, :] - peak)
            total = total + jnp.sum(probs, axis=0, keepdims=True)
            out = out + contract(vt[:, at], probs.astype(jnp.bfloat16), 1, 0)
        return (total, out)

    total, out = in_pairs(
        second_pass,
        second_pass(
            (index,), (jnp.zeros((1, width), jnp.float32), jnp.zeros((LANES, width), jnp.float32))
        ),
    )
    lse_ref[pl.ds(index, 1), :] = peak + jnp.log2(total)
    out = (out * (1.0 / total)).T.astype(jnp.bfloat16)
    out = jnp.concatenate([out[head * tile : (head + 1) * tile, :] for head in range(GROUP)], axis=1)
    out = contract(out, pad_ref[: GROUP * HEAD_SIZE, : GROUP * LANES], 1, 1).astype(jnp.bfloat16)
    for part in range(2):
        target = pl.ds(pl.multiple_of(slot_ref[index * 2 + part] * block, block), block)
        o_ref[target, :] = out[part * block : (part + 1) * block, :]


def attend(slots, x, gain, w, pad, inner, outer):
    rows, model = x.shape
    block = rows // slots.shape[0]
    tile = 2 * block
    width = GROUP * tile
    columns = pad.shape[1]
    whole = lambda *shape: pl.BlockSpec(shape, lambda i, s: (0,) * len(shape))
    return pl.pallas_call(
        forward_kernel,
        grid_spec=pltpu.PrefetchScalarGridSpec(
            num_scalar_prefetch=1,
            grid=(rows // tile,),
            in_specs=[
                pl.BlockSpec((block, model), lambda i, s: (s[2 * i], 0)),
                pl.BlockSpec((block, model), lambda i, s: (s[2 * i + 1], 0)),
                whole(1, model),
                whole(*w.shape),
                whole(*pad.shape),
                whole(*inner.shape),
                whole(*outer.shape),
            ],
            out_specs=(
                pl.BlockSpec((tile, model), lambda i, s: (i, 0)),
                whole(rows, columns),
                whole(rows, GROUP * HEAD_SIZE),
                whole(rows // tile, width),
            ),
            scratch_shapes=[
                pltpu.VMEM((model, columns), jnp.bfloat16),
                pltpu.VMEM((width, LANES), jnp.bfloat16),
                pltpu.VMEM((LANES, rows), jnp.bfloat16),
                pltpu.VMEM((rows, width), jnp.float32),
            ],
        ),
        out_shape=(
            jax.ShapeDtypeStruct((rows, model), jnp.bfloat16),
            jax.ShapeDtypeStruct((rows, columns), jnp.bfloat16),
            jax.ShapeDtypeStruct((rows, GROUP * HEAD_SIZE), jnp.bfloat16),
            jax.ShapeDtypeStruct((rows // tile, width), jnp.float32),
        ),
        compiler_params=pltpu.CompilerParams(vmem_limit_bytes=44 << 20),
        cost_estimate=pl.CostEstimate(
            flops=4 * GROUP * rows * rows * LANES // 2 + 2 * rows * model * columns,
            bytes_accessed=4 * rows * model,
            transcendentals=GROUP * rows * rows // 2,
        ),
        name="attend",
    )(slots, x, x, gain, w, pad, inner, outer)


def backward_kernel(
    slot_ref,
    gained_ref,
    qkv_ref,
    o_ref,
    do_ref,
    lse_ref,
    w_ref,
    dwo_ref,
    pad_ref,
    inner_ref,
    outer_ref,
    dx_ref,
    grads_ref,
    wp,
    qs,
    gs,
    kt,
    dk,
    dv,
    dw,
):
    step_at = pl.program_id(0)
    tiles = pl.num_programs(0)
    index = tiles - 1 - step_at
    tile = gained_ref.shape[0]
    block = tile // 2
    width = GROUP * tile
    first_key, first_value = GROUP * LANES, (GROUP + 1) * LANES

    @pl.when(step_at == 0)
    def _():
        wp[...] = contract(w_ref[...], pad_ref[...], 1, 0).astype(jnp.bfloat16)
        kt[...] = qkv_ref[:, first_key:first_value].T
        dk[...] = jnp.zeros_like(dk)
        dv[...] = jnp.zeros_like(dv)
        dw[...] = jnp.zeros_like(dw)

    here = pl.ds(pl.multiple_of(index * tile, tile), tile)
    sources = [
        pl.ds(pl.multiple_of(slot_ref[index * 2 + part] * block, block), block) for part in (0, 1)
    ]
    o = jnp.concatenate([o_ref[source, :] for source in sources], axis=0)
    grads = jnp.concatenate([do_ref[source, :] for source in sources], axis=0)
    products = (grads.astype(jnp.float32) * o.astype(jnp.float32)).T
    grads = contract(grads, pad_ref[: GROUP * HEAD_SIZE, : GROUP * LANES], 1, 0).astype(jnp.bfloat16)
    deltas = []
    for head in range(GROUP):
        lanes = slice(head * LANES, (head + 1) * LANES)
        at = slice(head * tile, (head + 1) * tile)
        qs[at, :] = qkv_ref[here, lanes]
        gs[at, :] = grads[:, lanes]
        features = slice(head * HEAD_SIZE, (head + 1) * HEAD_SIZE)
        deltas.append(jnp.sum(products[features, :], axis=0, keepdims=True))
    delta = jnp.concatenate(deltas, axis=1)
    lse = lse_ref[pl.ds(index, 1), :]
    key_at = lax.broadcasted_iota(jnp.int32, (tile, width), 0)
    query_at = lax.rem(lax.broadcasted_iota(jnp.int32, (tile, width), 1), tile)
    diagonal = key_at <= query_at

    def pieces(steps, masked=False):
        queries, grads = qs[...], gs[...]
        places = [pl.ds(pl.multiple_of(step * tile, tile), tile) for step in steps]
        scores = [contract(qkv_ref[at, first_key:first_value], queries, 1, 1) for at in places]
        grad_probs = [contract(qkv_ref[at, first_value:], grads, 1, 1) for at in places]
        total = None
        for at, score, grad_prob in zip(places, scores, grad_probs):
            probs = jnp.exp2(score * binary_scale - lse)
            if masked:
                probs = jnp.where(diagonal, probs, 0.0)
            dv[at, :] += contract(probs.astype(jnp.bfloat16), grads, 1, 0)
            grad_scores = (probs * (grad_prob - delta)).astype(jnp.bfloat16)
            dk[at, :] += contract(grad_scores, queries, 1, 0)
            part = contract(kt[:, at], grad_scores, 1, 0)
            total = part if total is None else total + part
        return total

    dq = pieces((index,), True)
    dq = lax.fori_loop(
        0, lax.div(index, 2), lambda pair, total: total + pieces((2 * pair, 2 * pair + 1)), dq
    )
    dq = lax.fori_loop(0, lax.rem(index, 2), lambda _, total: total + pieces((index - 1,)), dq)
    dq = dq.T * score_scale
    cosine, sine = tables(inner_ref, outer_ref, index, 2)
    parts = [turn(dq[head * tile : (head + 1) * tile, :], cosine, -sine) for head in range(GROUP)]
    parts.append(turn(dk[here, :] * score_scale, cosine, -sine))
    parts.append(dv[here, :])
    dqkv = jnp.concatenate([part.astype(jnp.bfloat16) for part in parts], axis=1)
    dw[...] += contract(dqkv, gained_ref[...], 0, 0)
    dx = contract(dqkv, wp[...], 1, 1).astype(jnp.bfloat16)
    for part in (0, 1):
        dx_ref[sources[part], :] = dx[part * block : (part + 1) * block, :]

    @pl.when(step_at == tiles - 1)
    def _():
        packed = contract(pad_ref[...], dw[...].astype(jnp.bfloat16), 1, 0)
        packed = packed.astype(jnp.bfloat16).T
        line, _ = dwo_ref.shape[:2]
        shard = packed.shape[0] // line
        for slot in range(line):
            grads_ref[slot, :shard, :] = packed[slot * shard : (slot + 1) * shard, :]
            grads_ref[slot, shard:, :] = dwo_ref[slot]


def attend_back(slots, gained, qkv, o, do, lse, w, dwo, pad, inner, outer):
    rows, model = gained.shape
    block = rows // slots.shape[0]
    tile = 2 * block
    width = GROUP * tile
    tiles = rows // tile
    columns = pad.shape[1]
    line, dealt, across = dwo.shape
    grads = (line, model // line + dealt, across)
    whole = lambda *shape: pl.BlockSpec(shape, lambda i, s: (0,) * len(shape))
    return pl.pallas_call(
        backward_kernel,
        grid_spec=pltpu.PrefetchScalarGridSpec(
            num_scalar_prefetch=1,
            grid=(tiles,),
            in_specs=[
                pl.BlockSpec((tile, model), lambda i, s: (tiles - 1 - i, 0)),
                whole(*qkv.shape),
                whole(*o.shape),
                whole(*do.shape),
                whole(*lse.shape),
                whole(*w.shape),
                whole(*dwo.shape),
                whole(*pad.shape),
                whole(*inner.shape),
                whole(*outer.shape),
            ],
            out_specs=(whole(rows, model), whole(*grads)),
            scratch_shapes=[
                pltpu.VMEM((model, columns), jnp.bfloat16),
                pltpu.VMEM((width, LANES), jnp.bfloat16),
                pltpu.VMEM((width, LANES), jnp.bfloat16),
                pltpu.VMEM((LANES, rows), jnp.bfloat16),
                pltpu.VMEM((rows, LANES), jnp.float32),
                pltpu.VMEM((rows, LANES), jnp.float32),
                pltpu.VMEM((columns, model), jnp.float32),
            ],
        ),
        out_shape=(
            jax.ShapeDtypeStruct((rows, model), jnp.bfloat16),
            jax.ShapeDtypeStruct(grads, jnp.bfloat16),
        ),
        compiler_params=pltpu.CompilerParams(vmem_limit_bytes=44 << 20),
        cost_estimate=pl.CostEstimate(
            flops=10 * GROUP * rows * rows * LANES // 2 + 4 * rows * model * columns,
            bytes_accessed=8 * rows * model,
            transcendentals=GROUP * rows * rows // 2,
        ),
        name="attend_back",
    )(slots, gained, qkv, o, do, lse, w, dwo, pad, inner, outer)


MESH_IDS = pl.DeviceIdType.MESH


def start_barrier(me, line_index=None, line=1):
    barrier = pltpu.get_barrier_semaphore()
    peers = [{"ctx": me ^ bit} for bit in range(1, 8)]
    peers += [{"fsdp": lax.rem(line_index + step, line)} for step in range(1, line)]
    for peer in peers:
        pl.semaphore_signal(barrier, inc=1, device_id=peer, device_id_type=MESH_IDS)
    pl.semaphore_wait(barrier, len(peers))


class Copies:
    def __init__(self, send_sems, recv_sems, base=0):
        self.send_sems, self.recv_sems, self.next, self.sent = send_sems, recv_sems, base, []

    def number(self):
        self.next += 1
        return self.next - 1

    def make(self, number, source, target, peer, landing=None):
        return pltpu.make_async_remote_copy(
            src_ref=source,
            dst_ref=target,
            send_sem=self.send_sems.at[number],
            recv_sem=self.recv_sems.at[number if landing is None else landing],
            device_id=peer,
            device_id_type=MESH_IDS,
        )

    def send(self, number, source, target, peer):
        copy = self.make(number, source, target, peer)
        copy.start()
        self.sent.append(copy)

    def arrived(self, number, target):
        self.make(number, target, target, {"ctx": 0}).wait_recv()

    def finish(self):
        for copy in self.sent:
            copy.wait_send()


GATHER_COPIES = 13


class PlaneGather:
    def __init__(self, copies, me, own_half, part):
        self.copies, self.me, self.own_half, self.part = copies, me, own_half, part
        self.first = copies.next
        copies.next += GATHER_COPIES

    def peer(self, bit):
        return {"ctx": self.me ^ bit}

    def begin(self):
        me, part, own, first = self.me, self.part, self.own_half, self.first
        send = self.copies.send
        send(first + 0, own(1), part(me, 1), self.peer(2))
        send(first + 1, own(0), part(me, 0), self.peer(4))
        send(first + 2, own(0), part(me, 0), self.peer(2))
        send(first + 3, own(1), part(me, 1), self.peer(4))
        send(first + 4, own(0), part(me, 0), self.peer(1))
        send(first + 5, own(1), part(me, 1), self.peer(1))

    def hear(self, number, slot, half, onward=None):
        place = self.part(slot, half)
        self.copies.arrived(self.first + number, place)
        if onward is not None:
            self.copies.send(self.first + onward[0], place, place, self.peer(onward[1]))

    def share(self, number, slot, half):
        place = self.part(slot, half)
        self.copies.send(self.first + number, place, place, self.peer(1))

    def first_hop(self):
        me = self.me
        self.hear(0, me ^ 2, 1, (6, 4))
        self.share(8, me ^ 2, 1)
        self.hear(1, me ^ 4, 0, (7, 2))
        self.share(9, me ^ 4, 0)

    def second_hop(self):
        me = self.me
        self.hear(2, me ^ 2, 0)
        self.share(10, me ^ 2, 0)
        self.hear(3, me ^ 4, 1)
        self.share(11, me ^ 4, 1)

    def third_hop(self):
        me = self.me
        self.hear(6, me ^ 6, 1)
        self.hear(7, me ^ 6, 0)
        self.share(12, me ^ 6, slice(None))

    def last(self):
        me, arrived, part = self.me, self.copies.arrived, self.part
        arrived(self.first + 4, part(me ^ 1, 0))
        arrived(self.first + 5, part(me ^ 1, 1))
        arrived(self.first + 8, part(me ^ 3, 1))
        arrived(self.first + 9, part(me ^ 5, 0))
        arrived(self.first + 10, part(me ^ 3, 0))
        arrived(self.first + 11, part(me ^ 5, 1))
        arrived(self.first + 12, part(me ^ 7, slice(None)))


def run_gathers(gathers):
    for gather in gathers:
        gather.begin()
    for gather in gathers:
        gather.first_hop()
    for gather in gathers:
        gather.second_hop()
    for gather in gathers:
        gather.third_hop()
    for gather in gathers:
        gather.last()


def row_half(ref, rows):
    half = rows // 2

    def own(side):
        return ref.at[pl.ds(side * half, half), :]

    return own


def row_part(ref, rows):
    half = rows // 2

    def part(slot, side):
        if isinstance(side, slice):
            return ref.at[pl.ds(pl.multiple_of(slot * rows, rows), rows), :]
        return ref.at[pl.ds(pl.multiple_of(slot * rows + side * half, half), half), :]

    return part


class LineGather:
    def __init__(self, copies, index, line, own, place):
        self.copies, self.index, self.line = copies, index, line
        self.own, self.place = own, place
        self.first = copies.next
        copies.next += 2 * (line - 1)

    def move(self, step, upward, act):
        index, line = self.index, self.line
        if upward:
            slot, there = index - step, index + 1
            leaves = (slot >= 0) & (there < line)
        else:
            slot, there = index + step, index - 1
            leaves = (slot < line) & (there >= 0)
        number = self.first + step + (0 if upward else line - 1)

        @pl.when(leaves)
        def _():
            place = self.place(jnp.clip(slot, 0, line - 1))
            source = self.own if step == 0 else place
            act(self.copies.make(number, source, place, {"fsdp": jnp.clip(there, 0, line - 1)}))

    def hear(self, step, upward):
        index, line = self.index, self.line
        slot = index - 1 - step if upward else index + 1 + step
        comes = (slot >= 0) & (slot < line)
        number = self.first + step + (0 if upward else line - 1)

        @pl.when(comes)
        def _():
            place = self.place(jnp.clip(slot, 0, line - 1))
            self.copies.make(number, place, place, {"fsdp": 0}).wait_recv()

    def begin(self):
        for upward in (True, False):
            self.move(0, upward, lambda copy: copy.start())

    def hop(self, step):
        for upward in (True, False):
            self.hear(step - 1, upward)
            if step < self.line - 1:
                self.move(step, upward, lambda copy: copy.start())

    def finish(self):
        for step in range(self.line - 1):
            for upward in (True, False):
                self.move(step, upward, lambda copy: copy.wait_send())


def anywhere(count):
    return [pl.BlockSpec(memory_space=pl.ANY)] * count


def local_copies(pairs, sems):
    copies = [
        pltpu.make_async_copy(source, target, sems.at[number])
        for number, (source, target) in enumerate(pairs)
    ]
    for copy in copies:
        copy.start()
    return copies


def remote_params(number, mebibytes=48):
    return pltpu.CompilerParams(
        collective_id=number, has_side_effects=True, vmem_limit_bytes=mebibytes << 20
    )


def first_kernel(
    line,
    x_ref,
    qkv_ref,
    wo_ref,
    gain_ref,
    gate_ref,
    up_ref,
    down_ref,
    xo_ref,
    qkvo_ref,
    woo_ref,
    gaino_ref,
    feedo_ref,
    feed,
    send,
    recv,
    here,
):
    me, index = lax.axis_index("ctx"), lax.axis_index("fsdp")
    plane = lax.axis_size("ctx")
    rows = x_ref.shape[0]
    part = row_part(xo_ref, rows)
    wo_rows = woo_ref.shape[1]
    wo_own = wo_ref.at[pl.ds(pl.multiple_of(me * wo_rows, wo_rows), wo_rows), :]
    local = local_copies(
        [
            (qkv_ref, qkvo_ref.at[index]),
            (wo_own, woo_ref.at[index]),
            (gain_ref, gaino_ref.at[index]),
            (x_ref, part(me, slice(None))),
        ],
        here,
    )
    start_barrier(me, index, line)
    copies = Copies(send, recv)
    gather = PlaneGather(copies, me, row_half(x_ref, rows), part)
    lines = [
        LineGather(copies, index, line, own, lambda slot, ref=ref: ref.at[slot])
        for own, ref in ((qkv_ref, qkvo_ref), (gain_ref, gaino_ref), (wo_own, woo_ref))
    ]
    gather.begin()
    for each in lines:
        each.begin()
    width = feed.shape[1] // 3
    unit = width // line
    pairs = []
    for side, ref in enumerate((gate_ref, up_ref)):
        for z in range(line):
            source = pl.ds(pl.multiple_of((z * plane + me) * unit, unit), unit)
            target = pl.ds(side * width + z * unit, unit)
            pairs.append((ref.at[:, source], feed.at[:, target]))
    for number in range(feed.shape[0] // unit):
        pairs.append(
            (
                down_ref.at[
                    pl.ds(pl.multiple_of(me * unit, unit), unit), pl.ds(number * width, width)
                ],
                feed.at[pl.ds(number * unit, unit), pl.ds(2 * width, width)],
            )
        )
    packed = local_copies(pairs, here.at[pl.ds(4, len(pairs))])
    gather.first_hop()
    for step in range(1, line):
        for each in lines:
            each.hop(step)
        if step == 1:
            gather.second_hop()
            for copy in packed:
                copy.wait()
            packed = local_copies([(feed, feedo_ref)], here.at[pl.ds(4 + len(pairs), 1)])
    gather.third_hop()
    gather.last()
    for each in lines:
        each.finish()
    copies.finish()
    for copy in local:
        copy.wait()
    packed[0].wait()


def first_exchange(line, x, qkv, wo, gains, gate, up, down):
    plane = lax.axis_size("ctx")
    count = GATHER_COPIES + 6 * (line - 1)
    model = x.shape[1]
    shard = model // line
    width = gate.shape[1] // plane
    own_rows = wo.shape[0] // plane
    feed = (shard, 3 * width)
    packing = 2 * line + shard * line // width + 1
    return pl.pallas_call(
        functools.partial(first_kernel, line),
        out_shape=(
            jax.ShapeDtypeStruct((plane * x.shape[0], model), x.dtype),
            jax.ShapeDtypeStruct((line, *qkv.shape), qkv.dtype),
            jax.ShapeDtypeStruct((line, own_rows, model), wo.dtype),
            jax.ShapeDtypeStruct((line, *gains.shape), gains.dtype),
            jax.ShapeDtypeStruct(feed, gate.dtype),
        ),
        in_specs=anywhere(7),
        out_specs=tuple(anywhere(5)),
        scratch_shapes=[
            pltpu.VMEM(feed, gate.dtype),
            pltpu.SemaphoreType.DMA((count,)),
            pltpu.SemaphoreType.DMA((count,)),
            pltpu.SemaphoreType.DMA((4 + packing,)),
        ],
        compiler_params=remote_params(1),
        name="first_exchange",
    )(x, qkv, wo, gains, gate, up, down)


def second_kernel(
    line,
    o_ref,
    wo_ref,
    dy_ref,
    x_ref,
    gain_ref,
    dyo_ref,
    own_ref,
    residual_ref,
    normed_ref,
    scale_ref,
    gained_ref,
    att,
    wo,
    send,
    recv,
    here,
):
    me = lax.axis_index("ctx")
    rows = dy_ref.shape[0]
    local = local_copies(
        [
            (o_ref.at[pl.ds(pl.multiple_of(me * rows, rows), rows), :], att.at[me]),
            (wo_ref, wo.at[:, me]),
            (dy_ref, row_part(dyo_ref, rows)(me, slice(None))),
        ],
        here.at[pl.ds(0, 3)],
    )
    start_barrier(me)
    copies = Copies(send, recv)

    def block(slot):
        return o_ref.at[pl.ds(pl.multiple_of(slot * rows, rows), rows), :]

    numbers = {}
    for bit in (6, 7, 4, 5, 2, 3, 1):
        numbers[bit] = copies.number()
        copies.send(numbers[bit], block(me ^ bit), att.at[me], {"ctx": me ^ bit})
    middle = line // 2

    def wo_half(side):
        return wo_ref.at[pl.ds(side * middle, middle)]

    def wo_part(slot, side):
        if isinstance(side, slice):
            return wo.at[:, slot]
        return wo.at[pl.ds(side * middle, middle), slot]

    wo_gather = PlaneGather(copies, me, wo_half, wo_part)
    dy_gather = PlaneGather(copies, me, row_half(dy_ref, rows), row_part(dyo_ref, rows))
    wo_gather.begin()
    wo_gather.first_hop()
    wo_gather.second_hop()
    dy_gather.begin()
    wo_gather.third_hop()
    wo_gather.last()
    for bit, number in numbers.items():
        copies.arrived(number, att.at[me ^ bit])
    local[0].wait()
    local[1].wait()
    per_head = 2 * GROUP
    own = wo.at[lax.div(me, 2), pl.ds(per_head * lax.rem(me, 2), per_head)]
    keep = local_copies([(own, own_ref)], here.at[pl.ds(3, 1)])
    plane = att.shape[0]
    total = x_ref[...].astype(jnp.float32)
    for slot in range(plane):
        first = per_head * (slot % 2)
        weight = jnp.concatenate(
            [wo[slot // 2, first + piece] for piece in range(per_head)], axis=0
        )
        total = total + contract(att[slot], weight, 1, 0)
    residual_ref[...] = total
    scale = lax.rsqrt(jnp.mean(total * total, axis=-1, keepdims=True) + norm_epsilon)
    normed = total * scale
    scale_ref[...] = scale
    normed_ref[...] = normed
    gained_ref[...] = (normed * gain_ref[...]).astype(jnp.bfloat16)
    dy_gather.first_hop()
    dy_gather.second_hop()
    dy_gather.third_hop()
    dy_gather.last()
    local[2].wait()
    keep[0].wait()
    copies.finish()


def second_exchange(o, wo, dy, x, gain):
    plane = lax.axis_size("ctx")
    rows = dy.shape[0]
    line, part, model = wo.shape
    count = 2 * GATHER_COPIES + 7
    f32 = jnp.float32
    return pl.pallas_call(
        functools.partial(second_kernel, line),
        out_shape=(
            jax.ShapeDtypeStruct((plane * rows, model), dy.dtype),
            jax.ShapeDtypeStruct((2 * GROUP, part, model), wo.dtype),
            jax.ShapeDtypeStruct((rows, model), f32),
            jax.ShapeDtypeStruct((rows, model), f32),
            jax.ShapeDtypeStruct((rows, 1), f32),
            jax.ShapeDtypeStruct((rows, model), dy.dtype),
        ),
        in_specs=anywhere(3) + in_vmem(2),
        out_specs=(*anywhere(2), *in_vmem(4)),
        scratch_shapes=[
            pltpu.VMEM((plane, rows, o.shape[1]), o.dtype),
            pltpu.VMEM((line, plane, part, model), wo.dtype),
            pltpu.SemaphoreType.DMA((count,)),
            pltpu.SemaphoreType.DMA((count,)),
            pltpu.SemaphoreType.DMA((4,)),
        ],
        compiler_params=remote_params(2),
        name="second_exchange",
    )(o, wo, dy, x, gain)


def gather_kernel(x_ref, xo_ref, send, recv, here):
    me = lax.axis_index("ctx")
    rows = x_ref.shape[0]
    start_barrier(me)
    part = row_part(xo_ref, rows)
    local = local_copies([(x_ref, part(me, slice(None)))], here)
    copies = Copies(send, recv)
    run_gathers([PlaneGather(copies, me, row_half(x_ref, rows), part)])
    copies.finish()
    local[0].wait()


def plane_gather(x, number):
    plane = lax.axis_size("ctx")
    return pl.pallas_call(
        gather_kernel,
        out_shape=jax.ShapeDtypeStruct((plane * x.shape[0], x.shape[1]), x.dtype),
        in_specs=anywhere(1),
        out_specs=anywhere(1)[0],
        scratch_shapes=[
            pltpu.SemaphoreType.DMA((GATHER_COPIES,)),
            pltpu.SemaphoreType.DMA((GATHER_COPIES,)),
            pltpu.SemaphoreType.DMA((1,)),
        ],
        compiler_params=remote_params(number),
    )(x)


def deal_rows(copies, me, pieces, wo_ref, place, recv_first):
    to_first = pieces * lax.rem(me, 2)
    line_slot = lax.div(me, 2)

    def copy(piece):
        return copies.make(
            recv_first + piece,
            wo_ref.at[piece],
            place(line_slot),
            {"ctx": to_first + piece},
            recv_first + line_slot,
        )

    for piece in range(pieces):

        @pl.when(to_first + piece != me)
        def _(piece=piece):
            copy(piece).start()

        @pl.when(to_first + piece == me)
        def _(piece=piece):
            place(line_slot)[...] = wo_ref[piece]

    def finish(line):
        for slot in range(line):

            @pl.when(2 * slot + lax.div(me, pieces) != me)
            def _(slot=slot):
                copies.make(
                    recv_first, wo_ref.at[0], place(slot), {"ctx": 0}, recv_first + slot
                ).wait_recv()

        for piece in range(pieces):

            @pl.when(to_first + piece != me)
            def _(piece=piece):
                copy(piece).wait_send()

    return finish


def third_kernel(
    sum_ref,
    normed_ref,
    scale_ref,
    gain_ref,
    dy_ref,
    o_ref,
    wo_ref,
    residual_ref,
    term_ref,
    do_ref,
    dwo_ref,
    own,
    all_grads,
    dwo,
    pieces_ref,
    send,
    recv,
):
    me = lax.axis_index("ctx")
    rows = dy_ref.shape[0]
    start_barrier(me)
    copies = Copies(send, recv)
    part = row_part(all_grads, rows)
    gather = PlaneGather(copies, me, row_half(own, rows), part)
    grad_normed, normed = sum_ref[...], normed_ref[...]
    products = grad_normed * normed
    scaled = grad_normed * gain_ref[...]
    mean = jnp.mean(scaled * normed, axis=-1, keepdims=True)
    residual = dy_ref[...].astype(jnp.float32) + scale_ref[...] * (scaled - normed * mean)
    own[...] = residual.astype(jnp.bfloat16)
    gather.begin()
    residual_ref[...] = residual
    term_ref[...] = jnp.sum(products, axis=0, keepdims=True)
    part(me, slice(None))[...] = own[...]
    dwo[...] = jnp.zeros_like(dwo)

    def step(order, carry):
        for number, slot, sides, when in (
            (4, 1, 0, 1),
            (5, 1, 1, 1),
            (8, 3, 1, 3),
            (10, 3, 0, 3),
            (9, 5, 0, 5),
            (11, 5, 1, 5),
            (12, 7, slice(None), 7),
        ):

            @pl.when(order == when)
            def _(number=number, slot=slot, sides=sides):
                copies.arrived(gather.first + number, gather.part(me ^ slot, sides))

        place = pl.ds(pl.multiple_of((me ^ order) * rows, rows), rows)
        grads = all_grads[place, :]
        do_ref[place, :] = contract(grads, wo_ref[...], 1, 1).astype(jnp.bfloat16)
        share = contract(o_ref[place, :], grads, 0, 0)
        dwo[...] += share
        return carry

    lax.fori_loop(0, 2, step, 0)
    gather.first_hop()
    gather.second_hop()
    lax.fori_loop(2, 6, step, 0)
    gather.third_hop()
    lax.fori_loop(6, 8, step, 0)
    line, _, across = dwo_ref.shape
    count = pieces_ref.shape[0]
    for piece in range(count):
        rows_at = slice(piece * HALF, (piece + 1) * HALF)
        for number in range(dwo.shape[1] // across):
            columns = slice(number * across, (number + 1) * across)
            pieces_ref[piece, number * HALF : (number + 1) * HALF, :] = dwo[
                rows_at, columns
            ].astype(jnp.bfloat16)
    first = copies.next
    finish = deal_rows(copies, me, count, pieces_ref, lambda slot: dwo_ref.at[slot], first)
    finish(line)
    copies.finish()


def third_exchange(line, grad_normed, normed, scale, gain, dy, o, wo, across):
    plane = lax.axis_size("ctx")
    rows, model = dy.shape
    pieces = 2 * GROUP
    dealt = (HALF * model // across, across)
    half_type, f32 = jnp.bfloat16, jnp.float32
    count = GATHER_COPIES + pieces
    return pl.pallas_call(
        third_kernel,
        out_shape=(
            jax.ShapeDtypeStruct((rows, model), f32),
            jax.ShapeDtypeStruct((1, model), f32),
            jax.ShapeDtypeStruct(o.shape, half_type),
            jax.ShapeDtypeStruct((line, *dealt), half_type),
        ),
        in_specs=in_vmem(7),
        out_specs=tuple(in_vmem(4)),
        scratch_shapes=[
            pltpu.VMEM((rows, model), half_type),
            pltpu.VMEM((plane * rows, model), half_type),
            pltpu.VMEM(wo.shape, f32),
            pltpu.VMEM((pieces, *dealt), half_type),
            pltpu.SemaphoreType.DMA((count,)),
            pltpu.SemaphoreType.DMA((count,)),
        ],
        compiler_params=remote_params(6),
        name="third_exchange",
    )(grad_normed, normed, scale, gain, dy, o, wo)


REDUCE_COPIES = 10


class PlaneReduce:
    def __init__(self, copies, me, block, heard, held, landed):
        self.copies, self.me, self.block = copies, me, block
        self.heard, self.held, self.landed = heard, held, landed
        self.first = copies.next
        copies.next += REDUCE_COPIES
        self.half = heard.shape[1] // 2
        self.x, self.y = {"ctx": me ^ 2}, {"ctx": me ^ 4}

    def side(self, ref, slot, half):
        return ref.at[slot, pl.ds(half * self.half, self.half), :]

    def share(self, order):
        partner = self.me ^ 1
        bit = (6, 2, 4, 0)[order]
        self.copies.send(
            self.first + order, self.block(partner ^ bit), self.heard.at[order], {"ctx": partner}
        )

    def combine(self, order, rows, extra=None):
        bit = (6, 2, 4)[order]
        total = self.block(self.me ^ bit)[rows, :].astype(jnp.float32) + self.heard[
            order, rows, :
        ].astype(jnp.float32)
        if extra is not None:
            total = total + extra
        self.held[order, rows, :] = total.astype(self.held.dtype)

    def onward(self, number):
        order, half, peer = {
            4: (0, 0, self.x),
            5: (0, 1, self.y),
            6: (1, 0, self.x),
            7: (2, 1, self.y),
            8: (1, 1, self.x),
            9: (2, 0, self.y),
        }[number]
        held, landed = self.side(self.held, order, half), self.side(self.landed, order, half)
        return self.copies.make(self.first + number, held, landed, peer)

    def finish(self):
        for number in range(4, REDUCE_COPIES):
            self.onward(number).wait_send()

    def diagonal_sends(self):
        first, half = self.first, self.half
        self.copies.arrived(first + 0, self.heard.at[0])
        self.combine(0, pl.ds(0, 2 * half))
        self.onward(4).start()
        self.onward(5).start()

    def neighbour_sends(self):
        first, half = self.first, self.half
        self.copies.arrived(first + 1, self.heard.at[1])
        self.combine(1, pl.ds(0, half))
        self.onward(6).start()
        self.copies.arrived(first + 2, self.heard.at[2])
        self.combine(2, pl.ds(half, half))
        self.onward(7).start()

    def first_sends(self):
        self.diagonal_sends()
        self.neighbour_sends()

    def second_sends(self):
        first, half = self.first, self.half
        upper, lower = pl.ds(0, half), pl.ds(half, half)
        landed, side, arrived = self.landed, self.side, self.copies.arrived
        arrived(first + 5, side(landed, 0, 1))
        self.combine(1, lower, landed[0, lower, :].astype(jnp.float32))
        self.onward(8).start()
        arrived(first + 4, side(landed, 0, 0))
        self.combine(2, upper, landed[0, upper, :].astype(jnp.float32))
        self.onward(9).start()
        arrived(first + 3, self.heard.at[3])

    def sum_half(self, which):
        first, half = self.first, self.half
        rows = pl.ds(which * half, half)
        self.copies.arrived(first + (6, 8)[which], self.side(self.landed, 1, which))
        self.copies.arrived(first + (9, 7)[which], self.side(self.landed, 2, which))
        return (
            self.block(self.me)[rows, :].astype(jnp.float32)
            + self.heard[3, rows, :].astype(jnp.float32)
            + self.landed[1, rows, :].astype(jnp.float32)
            + self.landed[2, rows, :].astype(jnp.float32)
        )


def feed_kernel(
    line,
    g_ref,
    dy_ref,
    w_ref,
    sum_ref,
    out_ref,
    dw_ref,
    down_ref,
    all_g,
    hid,
    hid_t,
    gate_t,
    up_t,
    part,
    heard,
    held,
    landed,
    out_mine,
    out_heard,
    send,
    recv,
):
    me = lax.axis_index("ctx")
    rows = g_ref.shape[0]
    width, model = down_ref.shape
    blocks = model // width
    unit = width // line
    start_barrier(me)
    copies = Copies(send, recv)
    gather = PlaneGather(copies, me, row_half(g_ref, rows), row_part(all_g, rows))
    gather.begin()

    def at(slot):
        return pl.ds(pl.multiple_of(slot * rows, rows), rows)

    all_g[at(me), :] = g_ref[...]
    gate_ref, up_ref = w_ref.at[:, :width], w_ref.at[:, width : 2 * width]
    for z in range(line):
        for number in range(blocks):
            source = pl.ds((z * blocks + number) * unit, unit)
            down_ref[pl.ds(z * unit, unit), number * width : (number + 1) * width] = w_ref[
                source, 2 * width :
            ]

    def block(slot):
        return part.at[at(slot), :]

    reduce = PlaneReduce(copies, me, block, heard, held, landed)

    def chunk(order):
        place = at(me ^ order)
        g = all_g[place, :]
        dy = dy_ref[place, :]
        gate_values = contract(g, gate_ref[...], 1, 0)
        up_values = contract(g, up_ref[...], 1, 0)
        sigmoid_gate = 1.0 / (1.0 + jnp.exp(-gate_values))
        activated = gate_values * sigmoid_gate
        hidden_act = (activated * up_values).astype(jnp.bfloat16)
        hid[place, :] = hidden_act
        hid_t[:, place] = hidden_act.T
        grad_hidden = contract(dy, down_ref[...], 1, 1)
        grad_gate = (
            grad_hidden * up_values * sigmoid_gate * (1.0 + gate_values * (1.0 - sigmoid_gate))
        ).astype(jnp.bfloat16)
        grad_up = (grad_hidden * activated).astype(jnp.bfloat16)
        gate_t[:, place] = grad_gate.T
        up_t[:, place] = grad_up.T
        part[place, :] = (
            contract(grad_gate, gate_ref[...], 1, 1) + contract(grad_up, up_ref[...], 1, 1)
        ).astype(jnp.bfloat16)

    def step(order, carry):
        for number, slot, sides, when in (
            (4, 1, 0, 1),
            (5, 1, 1, 1),
            (8, 3, 1, 3),
            (10, 3, 0, 3),
            (9, 5, 0, 5),
            (11, 5, 1, 5),
            (12, 7, slice(None), 7),
        ):

            @pl.when(order == when)
            def _(number=number, slot=slot, sides=sides):
                copies.arrived(gather.first + number, gather.part(me ^ slot, sides))

        chunk(order)
        return carry

    lax.fori_loop(0, 2, step, 0)
    gather.first_hop()
    gather.second_hop()
    reduce.share(3)
    lax.fori_loop(2, 6, step, 0)
    reduce.share(1)
    reduce.share(2)
    gather.third_hop()
    reduce.neighbour_sends()
    lax.fori_loop(6, 8, step, 0)
    reduce.share(0)

    out_first = copies.next
    copies.next += 4

    def bit_of(number):
        return jnp.where(number == 0, 6, jnp.where(number == 3, 0, 2 * number))

    def out_copy(number):
        return copies.make(out_first + number, out_mine.at[number], out_heard.at[number], partner)

    def out_of(slot):
        return contract(hid[at(slot), :], down_ref[...], 1, 0)

    partner = {"ctx": me ^ 1}

    def give(number, carry):
        out_mine[number] = out_of(me ^ 1 ^ bit_of(number)).astype(jnp.bfloat16)
        out_copy(number).start()
        return carry

    def keep(number, carry):
        total = out_of(me ^ bit_of(number))
        out_copy(number).wait_recv()
        out_ref[number] = (total + out_heard[number].astype(jnp.float32)).astype(jnp.bfloat16)
        return carry

    def weights(number, carry):
        columns = pl.ds(pl.multiple_of(number * width, width), width)
        total = contract(hid_t[...], dy_ref[:, columns], 1, 0).astype(jnp.bfloat16)
        for z in range(line):
            target = pl.ds(pl.multiple_of((z * blocks + number) * unit, unit), unit)
            dw_ref[target, 2 * width :] = total[z * unit : (z + 1) * unit, :]
        for side, left in enumerate((gate_t, up_t)):
            total = contract(left[...], all_g[:, columns], 1, 0).astype(jnp.bfloat16)
            dw_ref[columns, side * width : (side + 1) * width] = total.T
        return carry

    lax.fori_loop(0, 1, give, 0)
    reduce.diagonal_sends()
    lax.fori_loop(1, 4, give, 0)
    reduce.second_sends()
    lax.fori_loop(0, 4, keep, 0)
    lax.fori_loop(0, blocks, weights, 0)
    half = rows // 2
    for which in (1, 0):
        sum_ref[pl.ds(which * half, half), :] = reduce.sum_half(which)
    for number in range(4):
        out_copy(number).wait_send()
    reduce.finish()
    copies.finish()


def feed(g, dy, w):
    plane, line = lax.axis_size("ctx"), lax.axis_size("fsdp")
    rows, model = g.shape
    tokens = plane * rows
    width = w.shape[1] // 3
    count = GATHER_COPIES + REDUCE_COPIES + 4
    half_type = jnp.bfloat16
    return pl.pallas_call(
        functools.partial(feed_kernel, line),
        out_shape=(
            jax.ShapeDtypeStruct((rows, model), jnp.float32),
            jax.ShapeDtypeStruct((4, rows, model), half_type),
            jax.ShapeDtypeStruct(w.shape, half_type),
        ),
        in_specs=in_vmem(3),
        out_specs=tuple(in_vmem(3)),
        scratch_shapes=[
            pltpu.VMEM((width, model), half_type),
            pltpu.VMEM((tokens, model), half_type),
            pltpu.VMEM((tokens, width), half_type),
            pltpu.VMEM((width, tokens), half_type),
            pltpu.VMEM((width, tokens), half_type),
            pltpu.VMEM((width, tokens), half_type),
            pltpu.VMEM((tokens, model), half_type),
            pltpu.VMEM((4, rows, model), half_type),
            pltpu.VMEM((3, rows, model), half_type),
            pltpu.VMEM((3, rows, model), half_type),
            pltpu.VMEM((4, rows, model), half_type),
            pltpu.VMEM((4, rows, model), half_type),
            pltpu.SemaphoreType.DMA((count,)),
            pltpu.SemaphoreType.DMA((count,)),
        ],
        compiler_params=pltpu.CompilerParams(
            collective_id=3, has_side_effects=True, vmem_limit_bytes=60 << 20
        ),
        name="feed",
    )(g, dy, w)


def last_kernel(
    line,
    dx_ref,
    residual_ref,
    x_ref,
    gain_ref,
    term_ref,
    piece_ref,
    input_ref,
    whole_ref,
    total_ref,
    heard,
    held,
    landed,
    terms,
    terms_heard,
    plane_sum,
    across,
    send,
    recv,
    here,
):
    me, index = lax.axis_index("ctx"), lax.axis_index("fsdp")
    start_barrier(me, index, line)
    copies = Copies(send, recv)
    rows = residual_ref.shape[0]

    def block(slot):
        return dx_ref.at[pl.ds(pl.multiple_of(slot * rows, rows), rows), :]

    reduce = PlaneReduce(copies, me, block, heard, held, landed)
    piece_rows = piece_ref.shape[0]
    part = row_part(whole_ref, piece_rows)
    gather = PlaneGather(copies, me, row_half(piece_ref, piece_rows), part)
    for order in range(4):
        reduce.share(order)
    local = local_copies([(piece_ref, part(me, slice(None)))], here)
    reduce.first_sends()
    gather.begin()
    reduce.second_sends()
    gather.first_hop()
    gather.second_hop()
    half = rows // 2
    gain = gain_ref[...]
    total = jnp.zeros_like(gain)
    for which in (1, 0):
        at = pl.ds(which * half, half)
        grad = reduce.sum_half(which)
        x = x_ref[at, :].astype(jnp.float32)
        scale = lax.rsqrt(jnp.mean(x * x, axis=-1, keepdims=True) + norm_epsilon)
        normed = x * scale
        total = total + jnp.sum(grad * normed, axis=0, keepdims=True)
        scaled = grad * gain
        mean = jnp.mean(scaled * normed, axis=-1, keepdims=True)
        input_ref[0, at, :] = residual_ref[at, :] + scale * (scaled - normed * mean)
    terms[0:1, :] = total
    terms[1:2, :] = term_ref[...]
    first = copies.next
    copies.next += 7 + line - 1
    for bit in range(1, 8):
        copies.send(first + bit - 1, terms, terms_heard.at[bit], {"ctx": me ^ bit})
    gather.third_hop()
    total = terms[...]
    for bit in range(1, 8):
        copies.arrived(first + bit - 1, terms_heard.at[bit])
        total = total + terms_heard[bit]
    plane_sum[...] = total
    for step in range(1, line):
        peer = {"fsdp": lax.rem(index + step, line)}
        copies.send(first + 6 + step, plane_sum, across.at[step], peer)
    for step in range(1, line):
        copies.arrived(first + 6 + step, across.at[step])
        total = total + across[step]
    total_ref[...] = total
    gather.last()
    local[0].wait()
    reduce.finish()
    copies.finish()


def last_exchange(line, dx, residual, x, gain, term, piece):
    plane = lax.axis_size("ctx")
    rows, model = x.shape
    f32 = jnp.float32
    copies = GATHER_COPIES + REDUCE_COPIES + 7 + line - 1
    return pl.pallas_call(
        functools.partial(last_kernel, line),
        out_shape=(
            jax.ShapeDtypeStruct((1, rows, model), f32),
            jax.ShapeDtypeStruct((plane * piece.shape[0], piece.shape[1]), piece.dtype),
            jax.ShapeDtypeStruct((2, model), f32),
        ),
        in_specs=in_vmem(5) + anywhere(1),
        out_specs=(*in_vmem(1), *anywhere(1), *in_vmem(1)),
        scratch_shapes=[
            pltpu.VMEM((4, rows, model), dx.dtype),
            pltpu.VMEM((3, rows, model), dx.dtype),
            pltpu.VMEM((3, rows, model), dx.dtype),
            pltpu.VMEM((2, model), f32),
            pltpu.VMEM((plane, 2, model), f32),
            pltpu.VMEM((2, model), f32),
            pltpu.VMEM((line, 2, model), f32),
            pltpu.SemaphoreType.DMA((copies,)),
            pltpu.SemaphoreType.DMA((copies,)),
            pltpu.SemaphoreType.DMA((1,)),
        ],
        compiler_params=remote_params(7),
        name="last_exchange",
    )(dx, residual, x, gain, term, piece)


def spread_kernel(gate_in, up_in, down_in, gate_ref, up_ref, down_ref):
    plane, shard, unit = gate_in.shape
    for source, target in ((gate_in, gate_ref), (up_in, up_ref)):
        for slot in range(plane):
            target[:, slot * unit : (slot + 1) * unit] = source[slot].astype(jnp.float32)
    width = down_in.shape[2]
    blocks = shard // unit
    for slot in range(down_in.shape[0]):
        for number in range(blocks):
            down_ref[slot * unit : (slot + 1) * unit, number * width : (number + 1) * width] = (
                down_in[slot, number * unit : (number + 1) * unit, :].astype(jnp.float32)
            )


def spread_feed(pieces, shard, line, unit):
    plane = lax.axis_size("ctx")
    width = line * unit
    model = line * shard
    pieces = pieces.reshape(plane, shard, 3 * width)
    each = plane // line
    return pl.pallas_call(
        spread_kernel,
        grid=(line,),
        in_specs=[
            pl.BlockSpec((plane, shard, unit), lambda z: (0, 0, z)),
            pl.BlockSpec((plane, shard, unit), lambda z: (0, 0, line + z)),
            pl.BlockSpec((each, shard, width), lambda z: (z, 0, 2)),
        ],
        out_specs=(
            pl.BlockSpec((shard, plane * unit), lambda z: (0, z)),
            pl.BlockSpec((shard, plane * unit), lambda z: (0, z)),
            pl.BlockSpec((each * unit, model), lambda z: (z, 0)),
        ),
        out_shape=(
            jax.ShapeDtypeStruct((shard, plane * width), jnp.float32),
            jax.ShapeDtypeStruct((shard, plane * width), jnp.float32),
            jax.ShapeDtypeStruct((plane * unit, model), jnp.float32),
        ),
        compiler_params=pltpu.CompilerParams(vmem_limit_bytes=62 << 20),
        name="spread_feed",
    )(pieces, pieces, pieces)


def spread_attention_kernel(in_ref, q_ref, k_ref, v_ref, wo_ref):
    plane, _, across = in_ref.shape
    shard = q_ref.shape[0]
    key_width = k_ref.shape[1] // plane
    query_width = q_ref.shape[1] // plane
    first = 0
    for target, width in ((q_ref, query_width), (k_ref, key_width), (v_ref, key_width)):
        target[...] = jnp.concatenate(
            [
                in_ref[slot, :shard, first : first + width].astype(jnp.float32)
                for slot in range(plane)
            ],
            axis=1,
        )
        first += width
    for slot in range(plane):
        for number in range(wo_ref.shape[1] // across):
            source = slice(shard + number * HALF, shard + (number + 1) * HALF)
            wo_ref[slot * HALF : (slot + 1) * HALF, number * across : (number + 1) * across] = (
                in_ref[slot, source, :].astype(jnp.float32)
            )


def spread_attention(pieces, shard, model, query_width, key_width):
    plane = lax.axis_size("ctx")
    pieces = pieces.reshape(plane, -1, pieces.shape[1])
    f32 = jnp.float32
    return pl.pallas_call(
        spread_attention_kernel,
        in_specs=in_vmem(1),
        out_specs=tuple(in_vmem(4)),
        out_shape=(
            jax.ShapeDtypeStruct((shard, plane * query_width), f32),
            jax.ShapeDtypeStruct((shard, plane * key_width), f32),
            jax.ShapeDtypeStruct((shard, plane * key_width), f32),
            jax.ShapeDtypeStruct((plane * HALF, model), f32),
        ),
        compiler_params=pltpu.CompilerParams(vmem_limit_bytes=40 << 20),
        name="spread_attention",
    )(pieces)


def head_local(
    block_input,
    block_table,
    output_grad,
    attention_gain,
    query_weight,
    key_weight,
    value_projection,
    output_weight,
    feedforward_gain,
    gate_weight,
    up_weight,
    down_weight,
):
    me = lax.axis_index("ctx")
    plane = lax.axis_size("ctx")
    line = lax.axis_size("fsdp")
    rows, model = block_input.shape[1:]
    shard = model // line
    hidden = gate_weight.shape[1]
    unit = hidden // (line * plane)
    table_row = block_table[0]
    slot_count = table_row.shape[0]
    block = rows * plane // slot_count
    places = jnp.arange(slot_count, dtype=jnp.int32)
    slots = jnp.sum(jnp.where(table_row[None, :] == places[:, None], places[None, :], 0), axis=1)

    def mine(array, width):
        return lax.dynamic_slice_in_dim(array, me * width, width, 1)

    query_width = query_weight.shape[1] // plane
    key_width = key_weight.shape[1] // plane
    qkv_mine = jnp.concatenate(
        [
            mine(query_weight, query_width),
            mine(key_weight, key_width),
            mine(value_projection, key_width),
        ],
        axis=1,
    )
    gains_mine = jnp.stack([attention_gain, feedforward_gain])
    x_all, qkv_w, wo_line, gains, feed_mine = first_exchange(
        line,
        block_input[0],
        qkv_mine,
        output_weight,
        gains_mine,
        gate_weight,
        up_weight,
        down_weight,
    )
    feed_w = lax.all_gather(feed_mine, "fsdp", axis=0, tiled=True)

    steps_index = jnp.arange(HALF, dtype=jnp.float32)
    inverse = jnp.exp(steps_index * jnp.float32(-2.0 * math.log(rotary_base) / HEAD_SIZE))

    def table_of(positions):
        angles = positions.astype(jnp.float32)[:, None] * inverse[None, :]
        both = jnp.stack([jnp.cos(angles), jnp.sin(angles)])
        both = jnp.pad(both, ((0, 0), (0, 0), (0, LANES // 2 - HALF)))
        return jnp.concatenate([both, both], axis=2)

    inner = table_of(jnp.arange(block, dtype=jnp.int32))
    outer = table_of(places * block)
    pad = padding(GROUP + 2)

    gains = jnp.transpose(gains, (1, 0, 2)).reshape(2, model).astype(jnp.float32)
    qkv_w = qkv_w.reshape(model, -1)
    gained_one, qkv, o, lse = attend(slots, x_all, gains[:1], qkv_w, pad, inner, outer)

    grad_all, wo_mine, residual, normed_two, scale_two, gained_two = second_exchange(
        o, wo_line, output_grad[0], block_input[0], gains[1:]
    )
    wo_mine = wo_mine.reshape(-1, model)
    grad_normed_two, out_parts, feed_grads = feed(gained_two, grad_all, feed_w)
    feed_grads = lax.psum_scatter(feed_grads, "fsdp", scatter_dimension=0, tiled=True)
    grad_residual, feedforward_term, grad_o, wo_term = third_exchange(
        line,
        grad_normed_two,
        normed_two,
        scale_two,
        gains[1:],
        output_grad[0],
        o,
        wo_mine,
        qkv_w.shape[1],
    )
    out_parts, grad_o = lax.optimization_barrier((out_parts, grad_o))
    out_sum = out_parts[3].astype(jnp.float32)
    for part, bit in enumerate((6, 2, 4)):
        pairs = [(device, device ^ bit) for device in range(plane)]
        heard = lax.ppermute(out_parts[part], "ctx", pairs)
        out_sum = out_sum + heard.astype(jnp.float32)
    dx, attention_grads = attend_back(
        slots, gained_one, qkv, o, grad_o, lse, qkv_w, wo_term, pad, inner, outer
    )
    attention_grads, feed_grads = lax.optimization_barrier((attention_grads, feed_grads))
    attention_grads = lax.psum_scatter(
        attention_grads.reshape(-1, attention_grads.shape[2]),
        "fsdp",
        scatter_dimension=0,
        tiled=True,
    )
    layer_output = (residual + out_sum).astype(jnp.bfloat16)
    dx, layer_output = lax.optimization_barrier((dx, layer_output))
    input_grad, feed_pieces, gain_terms = last_exchange(
        line, dx, grad_residual, block_input[0], gains[:1], feedforward_term, feed_grads
    )
    gate_grad, up_grad, down_grad = spread_feed(feed_pieces, shard, line, unit)
    attention_pieces = plane_gather(attention_grads, 9)
    query_grad, key_grad, value_grad, out_grad = spread_attention(
        attention_pieces, shard, model, query_width, key_width
    )
    gain_terms = lax.dynamic_slice_in_dim(gain_terms, lax.axis_index("fsdp") * shard, shard, 1)
    return (
        layer_output[None],
        input_grad,
        gain_terms[0],
        query_grad,
        key_grad,
        value_grad,
        out_grad,
        gain_terms[1],
        gate_grad,
        up_grad,
        down_grad,
    )


def solution(mesh):
    plane, line = mesh.shape["ctx"], mesh.shape["fsdp"]
    fits = plane == KEY_VALUE_HEADS == 8 and plane * line * HALF == QUERY_HEADS * HEAD_SIZE
    if fits:
        return placed(mesh, head_local)
    return placed(mesh, local)


def placed(mesh, plan):
    return jax.shard_map(
        plan,
        mesh=mesh,
        in_specs=(
            P("fsdp", "ctx", None),
            P("fsdp", None),
            P("fsdp", "ctx", None),
            P("fsdp"),
            P("fsdp", None),
            P("fsdp", None),
            P("fsdp", None),
            P("fsdp", None),
            P("fsdp"),
            P("fsdp", None),
            P("fsdp", None),
            P("fsdp", None),
        ),
        out_specs=(
            P("fsdp", "ctx", None),
            P("fsdp", "ctx", None),
            P("fsdp"),
            P("fsdp", None),
            P("fsdp", None),
            P("fsdp", None),
            P("fsdp", None),
            P("fsdp"),
            P("fsdp", None),
            P("fsdp", None),
            P("fsdp", None),
        ),
        check_vma=False,
    )
```

```python
import functools
import math

import jax
import jax.numpy as jnp
from jax import lax
from jax.experimental import pallas as pl
from jax.experimental.pallas import tpu as pltpu
from jax.sharding import PartitionSpec as P


QUERY_HEADS = 16
KEY_VALUE_HEADS = 8
HEAD_SIZE = 96


norm_epsilon = 1e-05
rotary_base = 100000.0
score_with_mask = -1e30


def rope_tables(positions):
    half_width = HEAD_SIZE // 2
    steps_index = jnp.arange(half_width, dtype=jnp.float32)
    inverse = jnp.exp(steps_index * jnp.float32(-2.0 * math.log(rotary_base) / HEAD_SIZE))
    angles = positions.astype(jnp.float32)[:, None] * inverse[None, :]
    return (jnp.cos(angles), jnp.sin(angles))


def rotate(value_rows, cosine, sine_values, direction):
    count_of_rows = value_rows.shape[0]
    head_count = value_rows.shape[1] // HEAD_SIZE
    half_width = HEAD_SIZE // 2
    shaped = value_rows.reshape(count_of_rows, head_count, HEAD_SIZE)
    first_half = shaped[:, :, :half_width]
    second_half = shaped[:, :, half_width:]
    cos_part = cosine[:, None, :]
    sin_part = sine_values[:, None, :] * direction
    turned = jnp.concatenate(
        [
            first_half * cos_part - second_half * sin_part,
            second_half * cos_part + first_half * sin_part,
        ],
        axis=2,
    )
    return turned.reshape(count_of_rows, head_count * HEAD_SIZE)


def norm_scale(value_rows):
    return lax.rsqrt(jnp.mean(value_rows * value_rows, axis=-1, keepdims=True) + norm_epsilon)


def product(matrix, operand):
    return jnp.dot(matrix, operand, preferred_element_type=jnp.float32)


def cross_rows(matrix, operand):
    return lax.dot_general(
        matrix, operand, (((0,), (0,)), ((), ())), preferred_element_type=jnp.float32
    )


def back_product(matrix, operand):
    return lax.dot_general(
        matrix, operand, (((1,), (1,)), ((), ())), preferred_element_type=jnp.float32
    )


def block_scores(query_rank_four, block_of_keys, query_positions, key_positions):
    keys_rank_three = block_of_keys.reshape(block_of_keys.shape[0], KEY_VALUE_HEADS, HEAD_SIZE)
    scores = jnp.einsum(
        "rgjd,kgd->gjrk", query_rank_four, keys_rank_three, preferred_element_type=jnp.float32
    ) * HEAD_SIZE ** (-0.5)
    allowed = (key_positions[None, :] <= query_positions[:, None])[None, None]
    return (jnp.where(allowed, scores, score_with_mask), allowed)


def local(
    block_input,
    block_table,
    output_grad,
    attention_gain,
    query_weight,
    key_weight,
    value_projection,
    output_weight,
    feedforward_gain,
    gate_weight,
    up_weight,
    down_weight,
):
    query_group_width = QUERY_HEADS // KEY_VALUE_HEADS
    score_scale = HEAD_SIZE ** (-0.5)
    inputs = block_input[0].astype(jnp.float32)
    count_of_rows = inputs.shape[0]
    block_rows = count_of_rows // 2
    ctx_index = lax.axis_index("ctx")
    table_row = block_table[0]
    offsets = jnp.arange(block_rows, dtype=jnp.int32)
    query_blocks = lax.dynamic_slice_in_dim(table_row, 2 * ctx_index, 2)
    query_positions = (query_blocks[:, None] * block_rows + offsets[None, :]).reshape(count_of_rows)
    key_positions = (table_row[:, None] * block_rows + offsets[None, :]).reshape(-1)
    cosine, sine_values = rope_tables(query_positions)
    gain_one, query_full, key_full, value_full, out_full = (
        lax.all_gather(attention_gain, "fsdp", axis=0, tiled=True),
        lax.all_gather(query_weight, "fsdp", axis=0, tiled=True),
        lax.all_gather(key_weight, "fsdp", axis=0, tiled=True),
        lax.all_gather(value_projection, "fsdp", axis=0, tiled=True),
        lax.all_gather(output_weight, "fsdp", axis=0, tiled=True),
    )
    scale_one = norm_scale(inputs)
    normed_one = inputs * scale_one
    gained_one = (normed_one * gain_one.astype(jnp.float32)).astype(jnp.bfloat16)
    query_rows = rotate(product(gained_one, query_full), cosine, sine_values, 1.0).astype(
        jnp.bfloat16
    )
    keys_local = rotate(product(gained_one, key_full), cosine, sine_values, 1.0).astype(
        jnp.bfloat16
    )
    values_local = product(gained_one, value_full).astype(jnp.bfloat16)
    keys_all, values_all = (
        lax.all_gather(keys_local, "ctx", axis=0, tiled=True),
        lax.all_gather(values_local, "ctx", axis=0, tiled=True),
    )
    key_total_count = keys_all.shape[0]
    key_block_pass = 1024
    block_count = key_total_count // key_block_pass
    query_rank_four = query_rows.reshape(
        count_of_rows, KEY_VALUE_HEADS, query_group_width, HEAD_SIZE
    )
    key_places = key_positions.reshape(block_count, key_block_pass)

    def split_keys(array_in):
        return array_in.reshape(block_count, key_block_pass, array_in.shape[-1])

    def statistics_step(state_now, block_data):
        running_max, running_sum = state_now
        block_of_keys, key_place = block_data
        masked, allowed = block_scores(query_rank_four, block_of_keys, query_positions, key_place)
        new_max = jnp.maximum(running_max, jnp.max(masked, axis=-1))
        block_sum = jnp.sum(jnp.where(allowed, jnp.exp(masked - new_max[..., None]), 0.0), axis=-1)
        return ((new_max, running_sum * jnp.exp(running_max - new_max) + block_sum), None)

    initial_maximum = jnp.full(
        (KEY_VALUE_HEADS, query_group_width, count_of_rows), score_with_mask, jnp.float32
    )
    initial_sum = jnp.zeros((KEY_VALUE_HEADS, query_group_width, count_of_rows), jnp.float32)
    (final_max, final_sum), unused = lax.scan(
        statistics_step, (initial_maximum, initial_sum), (split_keys(keys_all), key_places)
    )
    log_total = final_max + jnp.log(final_sum)

    def output_step(state_now, block_data):
        block_of_keys, block_of_values, key_place = block_data
        masked, allowed = block_scores(query_rank_four, block_of_keys, query_positions, key_place)
        weights_half = jnp.where(allowed, jnp.exp(masked - log_total[..., None]), 0.0).astype(
            jnp.bfloat16
        )
        values_rank_three = block_of_values.reshape(key_block_pass, KEY_VALUE_HEADS, HEAD_SIZE)
        return (
            state_now
            + jnp.einsum(
                "gjrk,kgd->rgjd",
                weights_half,
                values_rank_three,
                preferred_element_type=jnp.float32,
            ),
            None,
        )

    initial_output = jnp.zeros(
        (count_of_rows, KEY_VALUE_HEADS, query_group_width, HEAD_SIZE), jnp.float32
    )
    summed_out, unused = lax.scan(
        output_step, initial_output, (split_keys(keys_all), split_keys(values_all), key_places)
    )
    attended_rows = summed_out.reshape(count_of_rows, QUERY_HEADS * HEAD_SIZE).astype(jnp.bfloat16)
    residual = inputs + product(attended_rows, out_full)
    scale_two = norm_scale(residual)
    normed_two = residual * scale_two
    gain_two, gate_full, up_full, down_full = (
        lax.all_gather(feedforward_gain, "fsdp", axis=0, tiled=True),
        lax.all_gather(gate_weight, "fsdp", axis=0, tiled=True),
        lax.all_gather(up_weight, "fsdp", axis=0, tiled=True),
        lax.all_gather(down_weight, "fsdp", axis=0, tiled=True),
    )
    gained_two = (normed_two * gain_two.astype(jnp.float32)).astype(jnp.bfloat16)
    gate_values = product(gained_two, gate_full)
    up_values = product(gained_two, up_full)
    sigmoid_gate = jax.nn.sigmoid(gate_values)
    activated = gate_values * sigmoid_gate
    hidden_act = (activated * up_values).astype(jnp.bfloat16)
    layer_output = (residual + product(hidden_act, down_full)).astype(jnp.bfloat16)
    gain_two_again, gate_back, up_back, down_back = (
        lax.all_gather(feedforward_gain, "fsdp", axis=0, tiled=True),
        lax.all_gather(gate_weight, "fsdp", axis=0, tiled=True),
        lax.all_gather(up_weight, "fsdp", axis=0, tiled=True),
        lax.all_gather(down_weight, "fsdp", axis=0, tiled=True),
    )
    grad_rows = output_grad[0]
    grad_hidden = back_product(grad_rows, down_back)
    down_term = cross_rows(hidden_act, grad_rows)
    grad_gate = (
        grad_hidden * up_values * sigmoid_gate * (1.0 + gate_values * (1.0 - sigmoid_gate))
    ).astype(jnp.bfloat16)
    grad_up = (grad_hidden * activated).astype(jnp.bfloat16)
    gate_term = cross_rows(gained_two, grad_gate)
    up_term = cross_rows(gained_two, grad_up)
    grad_normed_two = back_product(grad_gate, gate_back) + back_product(grad_up, up_back)
    feedforward_term = jnp.sum(grad_normed_two * normed_two, axis=0)
    grad_scaled_two = grad_normed_two * gain_two_again.astype(jnp.float32)
    grad_residual = grad_rows.astype(jnp.float32) + scale_two * (
        grad_scaled_two
        - normed_two * jnp.mean(grad_scaled_two * normed_two, axis=-1, keepdims=True)
    )
    gain_one_again, query_back, key_back, value_back, out_back = (
        lax.all_gather(attention_gain, "fsdp", axis=0, tiled=True),
        lax.all_gather(query_weight, "fsdp", axis=0, tiled=True),
        lax.all_gather(key_weight, "fsdp", axis=0, tiled=True),
        lax.all_gather(value_projection, "fsdp", axis=0, tiled=True),
        lax.all_gather(output_weight, "fsdp", axis=0, tiled=True),
    )
    grad_attn = grad_residual.astype(jnp.bfloat16)
    output_term = cross_rows(attended_rows, grad_attn)
    attended_gradient = back_product(grad_attn, out_back).astype(jnp.bfloat16)
    gradient_rank_four = attended_gradient.reshape(
        count_of_rows, KEY_VALUE_HEADS, query_group_width, HEAD_SIZE
    )
    attended_rank_four = attended_rows.reshape(
        count_of_rows, KEY_VALUE_HEADS, query_group_width, HEAD_SIZE
    )
    row_delta = jnp.transpose(
        jnp.sum(
            gradient_rank_four.astype(jnp.float32) * attended_rank_four.astype(jnp.float32), axis=-1
        ),
        (1, 2, 0),
    )
    keys_again, values_again = (
        lax.all_gather(keys_local, "ctx", axis=0, tiled=True),
        lax.all_gather(values_local, "ctx", axis=0, tiled=True),
    )

    def back_step(state_now, block_data):
        block_of_keys, block_of_values, key_place = block_data
        masked, allowed = block_scores(query_rank_four, block_of_keys, query_positions, key_place)
        weights_half = jnp.where(allowed, jnp.exp(masked - log_total[..., None]), 0.0).astype(
            jnp.bfloat16
        )
        values_rank_three = block_of_values.reshape(key_block_pass, KEY_VALUE_HEADS, HEAD_SIZE)
        keys_rank_three = block_of_keys.reshape(key_block_pass, KEY_VALUE_HEADS, HEAD_SIZE)
        grad_weights = jnp.einsum(
            "rgjd,kgd->gjrk",
            gradient_rank_four,
            values_rank_three,
            preferred_element_type=jnp.float32,
        )
        grad_scores = (
            weights_half.astype(jnp.float32) * (grad_weights - row_delta[..., None]) * score_scale
        ).astype(jnp.bfloat16)
        state_now = state_now + jnp.einsum(
            "gjrk,kgd->rgjd", grad_scores, keys_rank_three, preferred_element_type=jnp.float32
        )
        key_gradient = jnp.einsum(
            "gjrk,rgjd->kgd", grad_scores, query_rank_four, preferred_element_type=jnp.float32
        )
        value_gradient = jnp.einsum(
            "gjrk,rgjd->kgd", weights_half, gradient_rank_four, preferred_element_type=jnp.float32
        )
        return (
            state_now,
            (
                key_gradient.reshape(key_block_pass, KEY_VALUE_HEADS * HEAD_SIZE).astype(
                    jnp.bfloat16
                ),
                value_gradient.reshape(key_block_pass, KEY_VALUE_HEADS * HEAD_SIZE).astype(
                    jnp.bfloat16
                ),
            ),
        )

    first_query_index = jnp.zeros(
        (count_of_rows, KEY_VALUE_HEADS, query_group_width, HEAD_SIZE), jnp.float32
    )
    query_sum, (key_gradients, value_gradients) = lax.scan(
        back_step, first_query_index, (split_keys(keys_again), split_keys(values_again), key_places)
    )
    key_gradients = key_gradients.reshape(key_total_count, KEY_VALUE_HEADS * HEAD_SIZE)
    value_gradients = value_gradients.reshape(key_total_count, KEY_VALUE_HEADS * HEAD_SIZE)
    key_sums, value_sums = (
        lax.psum_scatter(key_gradients, "ctx", scatter_dimension=0, tiled=True).astype(jnp.float32),
        lax.psum_scatter(value_gradients, "ctx", scatter_dimension=0, tiled=True).astype(
            jnp.float32
        ),
    )
    query_gradients = rotate(
        query_sum.reshape(count_of_rows, QUERY_HEADS * HEAD_SIZE), cosine, sine_values, -1.0
    ).astype(jnp.bfloat16)
    grad_keys = rotate(key_sums, cosine, sine_values, -1.0).astype(jnp.bfloat16)
    grad_values = value_sums.astype(jnp.bfloat16)
    query_term = cross_rows(gained_one, query_gradients)
    key_term = cross_rows(gained_one, grad_keys)
    value_term = cross_rows(gained_one, grad_values)
    grad_normed_one = (
        back_product(query_gradients, query_back)
        + back_product(grad_keys, key_back)
        + back_product(grad_values, value_back)
    )
    attention_term = jnp.sum(grad_normed_one * normed_one, axis=0)
    grad_scaled_one = grad_normed_one * gain_one_again.astype(jnp.float32)
    input_grad = grad_residual + scale_one * (
        grad_scaled_one
        - normed_one * jnp.mean(grad_scaled_one * normed_one, axis=-1, keepdims=True)
    )
    shares = (
        lax.psum_scatter(
            attention_term.astype(jnp.bfloat16), "fsdp", scatter_dimension=0, tiled=True
        ).astype(jnp.float32),
        lax.psum_scatter(
            query_term.astype(jnp.bfloat16), "fsdp", scatter_dimension=0, tiled=True
        ).astype(jnp.float32),
        lax.psum_scatter(
            key_term.astype(jnp.bfloat16), "fsdp", scatter_dimension=0, tiled=True
        ).astype(jnp.float32),
        lax.psum_scatter(
            value_term.astype(jnp.bfloat16), "fsdp", scatter_dimension=0, tiled=True
        ).astype(jnp.float32),
        lax.psum_scatter(
            output_term.astype(jnp.bfloat16), "fsdp", scatter_dimension=0, tiled=True
        ).astype(jnp.float32),
        lax.psum_scatter(
            feedforward_term.astype(jnp.bfloat16), "fsdp", scatter_dimension=0, tiled=True
        ).astype(jnp.float32),
        lax.psum_scatter(
            gate_term.astype(jnp.bfloat16), "fsdp", scatter_dimension=0, tiled=True
        ).astype(jnp.float32),
        lax.psum_scatter(
            up_term.astype(jnp.bfloat16), "fsdp", scatter_dimension=0, tiled=True
        ).astype(jnp.float32),
        lax.psum_scatter(
            down_term.astype(jnp.bfloat16), "fsdp", scatter_dimension=0, tiled=True
        ).astype(jnp.float32),
    )
    totals = (
        lax.psum(shares[0].astype(jnp.bfloat16), "ctx").astype(jnp.float32),
        lax.psum(shares[1].astype(jnp.bfloat16), "ctx").astype(jnp.float32),
        lax.psum(shares[2].astype(jnp.bfloat16), "ctx").astype(jnp.float32),
        lax.psum(shares[3].astype(jnp.bfloat16), "ctx").astype(jnp.float32),
        lax.psum(shares[4].astype(jnp.bfloat16), "ctx").astype(jnp.float32),
        lax.psum(shares[5].astype(jnp.bfloat16), "ctx").astype(jnp.float32),
        lax.psum(shares[6].astype(jnp.bfloat16), "ctx").astype(jnp.float32),
        lax.psum(shares[7].astype(jnp.bfloat16), "ctx").astype(jnp.float32),
        lax.psum(shares[8].astype(jnp.bfloat16), "ctx").astype(jnp.float32),
    )
    return (
        layer_output[None],
        input_grad[None],
        totals[0],
        totals[1],
        totals[2],
        totals[3],
        totals[4],
        totals[5],
        totals[6],
        totals[7],
        totals[8],
    )


LANES = 128
HALF = HEAD_SIZE // 2
GROUP = QUERY_HEADS // KEY_VALUE_HEADS
score_scale = HEAD_SIZE ** (-0.5)
binary_scale = score_scale * math.log2(math.e)


def contract(left, right, left_dim, right_dim):
    return lax.dot_general(
        left, right, (((left_dim,), (right_dim,)), ((), ())), preferred_element_type=jnp.float32
    )


def in_vmem(count):
    return [pl.BlockSpec(memory_space=pltpu.VMEM)] * count


def padding(heads):
    column = jnp.arange(heads * HEAD_SIZE, dtype=jnp.int32)
    half_at, rest = column // HALF, column % HALF
    target = half_at * (LANES // 2) + rest
    lanes = jnp.arange(heads * LANES, dtype=jnp.int32)
    return (target[:, None] == lanes[None, :]).astype(jnp.bfloat16)


def turn(part, cosine, sine):
    return part * cosine + pltpu.roll(part, LANES // 2, 1) * sine


def tables(inner_ref, outer_ref, index, per_tile):
    inner_cos, inner_sin = inner_ref[0], inner_ref[1]
    sign = jnp.where(
        lax.broadcasted_iota(jnp.int32, inner_cos.shape, 1) < LANES // 2, -1.0, 1.0
    )
    cosines, sines = [], []
    for part in range(per_tile):
        at = pl.ds(index * per_tile + part, 1)
        outer_cos, outer_sin = outer_ref[0, at, :], outer_ref[1, at, :]
        cosines.append(inner_cos * outer_cos - inner_sin * outer_sin)
        sines.append(sign * (inner_sin * outer_cos + inner_cos * outer_sin))
    return jnp.concatenate(cosines, axis=0), jnp.concatenate(sines, axis=0)


def forward_kernel(
    slot_ref,
    xa_ref,
    xb_ref,
    gain_ref,
    w_ref,
    pad_ref,
    inner_ref,
    outer_ref,
    qkv_ref,
    o_ref,
    ot_ref,
    lse_ref,
    wp,
    qs,
    vt,
    s_ref,
):
    index = pl.program_id(0)
    block = xa_ref.shape[0]
    tile = 2 * block
    width = GROUP * tile
    heads = GROUP + 2

    @pl.when(index == 0)
    def _():
        wp[...] = contract(w_ref[...], pad_ref[...], 1, 0).astype(jnp.bfloat16)

    x = jnp.concatenate([xa_ref[...], xb_ref[...]], axis=0).astype(jnp.float32)
    normed = x * lax.rsqrt(jnp.mean(x * x, axis=-1, keepdims=True) + norm_epsilon)
    gained = (normed * gain_ref[...]).astype(jnp.bfloat16)
    raw = contract(gained, wp[...], 1, 0)
    cosine, sine = tables(inner_ref, outer_ref, index, 2)
    here = pl.ds(pl.multiple_of(index * tile, tile), tile)
    for head in range(heads):
        lanes = slice(head * LANES, (head + 1) * LANES)
        part = raw[:, lanes]
        if head <= GROUP:
            part = turn(part, cosine, sine)
        part = part.astype(jnp.bfloat16)
        qkv_ref[here, lanes] = part
        if head < GROUP:
            qs[head * tile : (head + 1) * tile, :] = part
        if head == heads - 1:
            vt[:, here] = part.T
    queries = qs[...]
    key_at = lax.broadcasted_iota(jnp.int32, (tile, width), 0)
    query_at = lax.rem(lax.broadcasted_iota(jnp.int32, (tile, width), 1), tile)
    diagonal = key_at <= query_at

    def scores_of(step):
        at = pl.ds(pl.multiple_of(step * tile, tile), tile)
        keys = qkv_ref[at, GROUP * LANES : (GROUP + 1) * LANES]
        return contract(keys, queries, 1, 1) * binary_scale

    last = jnp.where(diagonal, scores_of(index), score_with_mask)
    s_ref[here, :] = last
    peak = jnp.max(last, axis=0, keepdims=True)

    def in_pairs(one, state):
        state = lax.fori_loop(
            0, lax.div(index, 2), lambda pair, state: one((2 * pair, 2 * pair + 1), state), state
        )
        return lax.fori_loop(0, lax.rem(index, 2), lambda _, state: one((index - 1,), state), state)

    def first_pass(steps, peak):
        found = [scores_of(step) for step in steps]
        for step, scores in zip(steps, found):
            s_ref[pl.ds(pl.multiple_of(step * tile, tile), tile), :] = scores
            peak = jnp.maximum(peak, jnp.max(scores, axis=0, keepdims=True))
        return peak

    peak = in_pairs(first_pass, peak)

    def second_pass(steps, state):
        total, out = state
        for step in steps:
            at = pl.ds(pl.multiple_of(step * tile, tile), tile)
            probs = jnp.exp2(s_ref[at, :] - peak)
            total = total + jnp.sum(probs, axis=0, keepdims=True)
            out = out + contract(vt[:, at], probs.astype(jnp.bfloat16), 1, 0)
        return (total, out)

    total, out = in_pairs(
        second_pass,
        second_pass(
            (index,), (jnp.zeros((1, width), jnp.float32), jnp.zeros((LANES, width), jnp.float32))
        ),
    )
    lse_ref[pl.ds(index, 1), :] = peak + jnp.log2(total)
    out = (out * (1.0 / total)).T.astype(jnp.bfloat16)
    out = jnp.concatenate([out[head * tile : (head + 1) * tile, :] for head in range(GROUP)], axis=1)
    out = contract(out, pad_ref[: GROUP * HEAD_SIZE, : GROUP * LANES], 1, 1).astype(jnp.bfloat16)
    for part in range(2):
        target = pl.ds(pl.multiple_of(slot_ref[index * 2 + part] * block, block), block)
        rows_at = slice(part * block, (part + 1) * block)
        o_ref[target, :] = out[rows_at, :]
        ot_ref[:, target] = out[rows_at, :].T


def attend(slots, x, gain, w, pad, inner, outer):
    rows, model = x.shape
    block = rows // slots.shape[0]
    tile = 2 * block
    width = GROUP * tile
    columns = pad.shape[1]
    whole = lambda *shape: pl.BlockSpec(shape, lambda i, s: (0,) * len(shape))
    return pl.pallas_call(
        forward_kernel,
        grid_spec=pltpu.PrefetchScalarGridSpec(
            num_scalar_prefetch=1,
            grid=(rows // tile,),
            in_specs=[
                pl.BlockSpec((block, model), lambda i, s: (s[2 * i], 0)),
                pl.BlockSpec((block, model), lambda i, s: (s[2 * i + 1], 0)),
                whole(1, model),
                whole(*w.shape),
                whole(*pad.shape),
                whole(*inner.shape),
                whole(*outer.shape),
            ],
            out_specs=(
                whole(rows, columns),
                whole(rows, GROUP * HEAD_SIZE),
                whole(GROUP * HEAD_SIZE, rows),
                whole(rows // tile, width),
                whole(model, columns),
            ),
            scratch_shapes=[
                pltpu.VMEM((width, LANES), jnp.bfloat16),
                pltpu.VMEM((LANES, rows), jnp.bfloat16),
                pltpu.VMEM((rows, width), jnp.float32),
            ],
        ),
        out_shape=(
            jax.ShapeDtypeStruct((rows, columns), jnp.bfloat16),
            jax.ShapeDtypeStruct((rows, GROUP * HEAD_SIZE), jnp.bfloat16),
            jax.ShapeDtypeStruct((GROUP * HEAD_SIZE, rows), jnp.bfloat16),
            jax.ShapeDtypeStruct((rows // tile, width), jnp.float32),
            jax.ShapeDtypeStruct((model, columns), jnp.bfloat16),
        ),
        compiler_params=pltpu.CompilerParams(vmem_limit_bytes=44 << 20),
        cost_estimate=pl.CostEstimate(
            flops=4 * GROUP * rows * rows * LANES // 2 + 2 * rows * model * columns,
            bytes_accessed=4 * rows * model,
            transcendentals=GROUP * rows * rows // 2,
        ),
        name="attend",
    )(slots, x, x, gain, w, pad, inner, outer)


def backward_kernel(
    slot_ref,
    qkv_ref,
    o_ref,
    do_ref,
    lse_ref,
    pad_ref,
    inner_ref,
    outer_ref,
    dqkv_ref,
    qs,
    gs,
    kt,
    dk,
    dv,
):
    step_at = pl.program_id(0)
    tiles = pl.num_programs(0)
    index = tiles - 1 - step_at
    block = qkv_ref.shape[0] // slot_ref.shape[0]
    tile = 2 * block
    width = GROUP * tile
    first_key, first_value = GROUP * LANES, (GROUP + 1) * LANES

    @pl.when(step_at == 0)
    def _():
        kt[...] = qkv_ref[:, first_key:first_value].T
        dk[...] = jnp.zeros_like(dk)
        dv[...] = jnp.zeros_like(dv)

    here = pl.ds(pl.multiple_of(index * tile, tile), tile)
    sources = [
        pl.ds(pl.multiple_of(slot_ref[index * 2 + part] * block, block), block) for part in (0, 1)
    ]
    o = jnp.concatenate([o_ref[source, :] for source in sources], axis=0)
    grads = jnp.concatenate([do_ref[source, :] for source in sources], axis=0)
    products = (grads.astype(jnp.float32) * o.astype(jnp.float32)).T
    grads = contract(grads, pad_ref[: GROUP * HEAD_SIZE, : GROUP * LANES], 1, 0).astype(jnp.bfloat16)
    deltas = []
    for head in range(GROUP):
        lanes = slice(head * LANES, (head + 1) * LANES)
        at = slice(head * tile, (head + 1) * tile)
        qs[at, :] = qkv_ref[here, lanes]
        gs[at, :] = grads[:, lanes]
        features = slice(head * HEAD_SIZE, (head + 1) * HEAD_SIZE)
        deltas.append(jnp.sum(products[features, :], axis=0, keepdims=True))
    delta = jnp.concatenate(deltas, axis=1)
    lse = lse_ref[pl.ds(index, 1), :]
    key_at = lax.broadcasted_iota(jnp.int32, (tile, width), 0)
    query_at = lax.rem(lax.broadcasted_iota(jnp.int32, (tile, width), 1), tile)
    diagonal = key_at <= query_at

    def pieces(steps, masked=False):
        queries, grads = qs[...], gs[...]
        places = [pl.ds(pl.multiple_of(step * tile, tile), tile) for step in steps]
        scores = [contract(qkv_ref[at, first_key:first_value], queries, 1, 1) for at in places]
        grad_probs = [contract(qkv_ref[at, first_value:], grads, 1, 1) for at in places]
        total = None
        for at, score, grad_prob in zip(places, scores, grad_probs):
            probs = jnp.exp2(score * binary_scale - lse)
            if masked:
                probs = jnp.where(diagonal, probs, 0.0)
            dv[at, :] += contract(probs.astype(jnp.bfloat16), grads, 1, 0)
            grad_scores = (probs * (grad_prob - delta)).astype(jnp.bfloat16)
            dk[at, :] += contract(grad_scores, queries, 1, 0)
            part = contract(kt[:, at], grad_scores, 1, 0)
            total = part if total is None else total + part
        return total

    dq = pieces((index,), True)
    dq = lax.fori_loop(
        0, lax.div(index, 2), lambda pair, total: total + pieces((2 * pair, 2 * pair + 1)), dq
    )
    dq = lax.fori_loop(0, lax.rem(index, 2), lambda _, total: total + pieces((index - 1,)), dq)
    dq = dq.T * score_scale
    cosine, sine = tables(inner_ref, outer_ref, index, 2)
    parts = [turn(dq[head * tile : (head + 1) * tile, :], cosine, -sine) for head in range(GROUP)]
    parts.append(turn(dk[here, :] * score_scale, cosine, -sine))
    parts.append(dv[here, :])
    dqkv = jnp.concatenate([part.astype(jnp.bfloat16) for part in parts], axis=1)
    for part in (0, 1):
        dqkv_ref[sources[part], :] = dqkv[part * block : (part + 1) * block, :]


def attend_back(slots, qkv, o, do, lse, pad, inner, outer):
    rows, columns = qkv.shape
    block = rows // slots.shape[0]
    tile = 2 * block
    width = GROUP * tile
    tiles = rows // tile
    operands = (qkv, o, do, lse, pad, inner, outer)
    whole = lambda *shape: pl.BlockSpec(shape, lambda i, s: (0,) * len(shape))
    return pl.pallas_call(
        backward_kernel,
        grid_spec=pltpu.PrefetchScalarGridSpec(
            num_scalar_prefetch=1,
            grid=(tiles,),
            in_specs=[whole(*operand.shape) for operand in operands],
            out_specs=whole(rows, columns),
            scratch_shapes=[
                pltpu.VMEM((width, LANES), jnp.bfloat16),
                pltpu.VMEM((width, LANES), jnp.bfloat16),
                pltpu.VMEM((LANES, rows), jnp.bfloat16),
                pltpu.VMEM((rows, LANES), jnp.float32),
                pltpu.VMEM((rows, LANES), jnp.float32),
            ],
        ),
        out_shape=jax.ShapeDtypeStruct((rows, columns), jnp.bfloat16),
        compiler_params=pltpu.CompilerParams(vmem_limit_bytes=40 << 20),
        cost_estimate=pl.CostEstimate(
            flops=10 * GROUP * rows * rows * LANES // 2,
            bytes_accessed=8 * rows * columns,
            transcendentals=GROUP * rows * rows // 2,
        ),
        name="attend_back",
    )(slots, *operands)


MESH_IDS = pl.DeviceIdType.MESH


def start_barrier(me, line_index=None, line=1):
    barrier = pltpu.get_barrier_semaphore()
    peers = [{"ctx": me ^ bit} for bit in range(1, 8)]
    peers += [{"fsdp": lax.rem(line_index + step, line)} for step in range(1, line)]
    for peer in peers:
        pl.semaphore_signal(barrier, inc=1, device_id=peer, device_id_type=MESH_IDS)
    pl.semaphore_wait(barrier, len(peers))


class Copies:
    def __init__(self, send_sems, recv_sems, base=0):
        self.send_sems, self.recv_sems, self.next, self.sent = send_sems, recv_sems, base, []

    def number(self):
        self.next += 1
        return self.next - 1

    def make(self, number, source, target, peer, landing=None):
        return pltpu.make_async_remote_copy(
            src_ref=source,
            dst_ref=target,
            send_sem=self.send_sems.at[number],
            recv_sem=self.recv_sems.at[number if landing is None else landing],
            device_id=peer,
            device_id_type=MESH_IDS,
        )

    def send(self, number, source, target, peer):
        copy = self.make(number, source, target, peer)
        copy.start()
        self.sent.append(copy)

    def arrived(self, number, target):
        self.make(number, target, target, {"ctx": 0}).wait_recv()

    def finish(self):
        for copy in self.sent:
            copy.wait_send()


GATHER_COPIES = 13


class PlaneGather:
    def __init__(self, copies, me, own_half, part):
        self.copies, self.me, self.own_half, self.part = copies, me, own_half, part
        self.first = copies.next
        copies.next += GATHER_COPIES

    def peer(self, bit):
        return {"ctx": self.me ^ bit}

    def begin(self):
        me, part, own, first = self.me, self.part, self.own_half, self.first
        send = self.copies.send
        send(first + 0, own(1), part(me, 1), self.peer(2))
        send(first + 1, own(0), part(me, 0), self.peer(4))
        send(first + 2, own(0), part(me, 0), self.peer(2))
        send(first + 3, own(1), part(me, 1), self.peer(4))
        send(first + 4, own(0), part(me, 0), self.peer(1))
        send(first + 5, own(1), part(me, 1), self.peer(1))

    def hear(self, number, slot, half, onward=None):
        place = self.part(slot, half)
        self.copies.arrived(self.first + number, place)
        if onward is not None:
            self.copies.send(self.first + onward[0], place, place, self.peer(onward[1]))

    def share(self, number, slot, half):
        place = self.part(slot, half)
        self.copies.send(self.first + number, place, place, self.peer(1))

    def first_hop(self):
        me = self.me
        self.hear(0, me ^ 2, 1, (6, 4))
        self.share(8, me ^ 2, 1)
        self.hear(1, me ^ 4, 0, (7, 2))
        self.share(9, me ^ 4, 0)

    def second_hop(self):
        me = self.me
        self.hear(2, me ^ 2, 0)
        self.share(10, me ^ 2, 0)
        self.hear(3, me ^ 4, 1)
        self.share(11, me ^ 4, 1)

    def third_hop(self):
        me = self.me
        self.hear(6, me ^ 6, 1)
        self.hear(7, me ^ 6, 0)
        self.share(12, me ^ 6, slice(None))

    def last(self):
        me, arrived, part = self.me, self.copies.arrived, self.part
        arrived(self.first + 4, part(me ^ 1, 0))
        arrived(self.first + 5, part(me ^ 1, 1))
        arrived(self.first + 8, part(me ^ 3, 1))
        arrived(self.first + 9, part(me ^ 5, 0))
        arrived(self.first + 10, part(me ^ 3, 0))
        arrived(self.first + 11, part(me ^ 5, 1))
        arrived(self.first + 12, part(me ^ 7, slice(None)))


def run_gathers(gathers):
    for gather in gathers:
        gather.begin()
    for gather in gathers:
        gather.first_hop()
    for gather in gathers:
        gather.second_hop()
    for gather in gathers:
        gather.third_hop()
    for gather in gathers:
        gather.last()


def row_half(ref, rows):
    half = rows // 2

    def own(side):
        return ref.at[pl.ds(side * half, half), :]

    return own


def row_part(ref, rows):
    half = rows // 2

    def part(slot, side):
        if isinstance(side, slice):
            return ref.at[pl.ds(pl.multiple_of(slot * rows, rows), rows), :]
        return ref.at[pl.ds(pl.multiple_of(slot * rows + side * half, half), half), :]

    return part


class LineGather:
    def __init__(self, copies, index, line, own, place):
        self.copies, self.index, self.line = copies, index, line
        self.own, self.place = own, place
        self.first = copies.next
        copies.next += 2 * (line - 1)

    def move(self, step, upward, act):
        index, line = self.index, self.line
        if upward:
            slot, there = index - step, index + 1
            leaves = (slot >= 0) & (there < line)
        else:
            slot, there = index + step, index - 1
            leaves = (slot < line) & (there >= 0)
        number = self.first + step + (0 if upward else line - 1)

        @pl.when(leaves)
        def _():
            place = self.place(jnp.clip(slot, 0, line - 1))
            source = self.own if step == 0 else place
            act(self.copies.make(number, source, place, {"fsdp": jnp.clip(there, 0, line - 1)}))

    def hear(self, step, upward):
        index, line = self.index, self.line
        slot = index - 1 - step if upward else index + 1 + step
        comes = (slot >= 0) & (slot < line)
        number = self.first + step + (0 if upward else line - 1)

        @pl.when(comes)
        def _():
            place = self.place(jnp.clip(slot, 0, line - 1))
            self.copies.make(number, place, place, {"fsdp": 0}).wait_recv()

    def begin(self):
        for upward in (True, False):
            self.move(0, upward, lambda copy: copy.start())

    def hop(self, step):
        for upward in (True, False):
            self.hear(step - 1, upward)
            if step < self.line - 1:
                self.move(step, upward, lambda copy: copy.start())

    def finish(self):
        for step in range(self.line - 1):
            for upward in (True, False):
                self.move(step, upward, lambda copy: copy.wait_send())


def anywhere(count):
    return [pl.BlockSpec(memory_space=pl.ANY)] * count


def local_copies(pairs, sems):
    copies = [
        pltpu.make_async_copy(source, target, sems.at[number])
        for number, (source, target) in enumerate(pairs)
    ]
    for copy in copies:
        copy.start()
    return copies


def remote_params(number, mebibytes=48):
    return pltpu.CompilerParams(
        collective_id=number, has_side_effects=True, vmem_limit_bytes=mebibytes << 20
    )


def first_kernel(
    line,
    x_ref,
    qkv_ref,
    wo_ref,
    gain_ref,
    gate_ref,
    up_ref,
    down_ref,
    xo_ref,
    qkvo_ref,
    woo_ref,
    gaino_ref,
    feedo_ref,
    feed,
    send,
    recv,
    here,
):
    me, index = lax.axis_index("ctx"), lax.axis_index("fsdp")
    plane = lax.axis_size("ctx")
    rows = x_ref.shape[0]
    part = row_part(xo_ref, rows)
    wo_rows = woo_ref.shape[1]
    wo_own = wo_ref.at[pl.ds(pl.multiple_of(me * wo_rows, wo_rows), wo_rows), :]
    local = local_copies(
        [
            (qkv_ref, qkvo_ref.at[index]),
            (wo_own, woo_ref.at[index]),
            (gain_ref, gaino_ref.at[index]),
            (x_ref, part(me, slice(None))),
        ],
        here,
    )
    start_barrier(me, index, line)
    copies = Copies(send, recv)
    gather = PlaneGather(copies, me, row_half(x_ref, rows), part)
    lines = [
        LineGather(copies, index, line, own, lambda slot, ref=ref: ref.at[slot])
        for own, ref in ((qkv_ref, qkvo_ref), (gain_ref, gaino_ref), (wo_own, woo_ref))
    ]
    gather.begin()
    for each in lines:
        each.begin()
    width = feed.shape[1] // 3
    unit = width // line
    pairs = []
    for side, ref in enumerate((gate_ref, up_ref)):
        for z in range(line):
            source = pl.ds(pl.multiple_of((z * plane + me) * unit, unit), unit)
            target = pl.ds(side * width + z * unit, unit)
            pairs.append((ref.at[:, source], feed.at[:, target]))
    for number in range(feed.shape[0] // unit):
        pairs.append(
            (
                down_ref.at[
                    pl.ds(pl.multiple_of(me * unit, unit), unit), pl.ds(number * width, width)
                ],
                feed.at[pl.ds(number * unit, unit), pl.ds(2 * width, width)],
            )
        )
    packed = local_copies(pairs, here.at[pl.ds(4, len(pairs))])
    gather.first_hop()
    for step in range(1, line):
        for each in lines:
            each.hop(step)
        if step == 1:
            gather.second_hop()
            for copy in packed:
                copy.wait()
            packed = local_copies([(feed, feedo_ref)], here.at[pl.ds(4 + len(pairs), 1)])
    gather.third_hop()
    gather.last()
    for each in lines:
        each.finish()
    copies.finish()
    for copy in local:
        copy.wait()
    packed[0].wait()


def first_exchange(line, x, qkv, wo, gains, gate, up, down):
    plane = lax.axis_size("ctx")
    count = GATHER_COPIES + 6 * (line - 1)
    model = x.shape[1]
    shard = model // line
    width = gate.shape[1] // plane
    own_rows = wo.shape[0] // plane
    feed = (shard, 3 * width)
    packing = 2 * line + shard * line // width + 1
    return pl.pallas_call(
        functools.partial(first_kernel, line),
        out_shape=(
            jax.ShapeDtypeStruct((plane * x.shape[0], model), x.dtype),
            jax.ShapeDtypeStruct((line, *qkv.shape), qkv.dtype),
            jax.ShapeDtypeStruct((line, own_rows, model), wo.dtype),
            jax.ShapeDtypeStruct((line, *gains.shape), gains.dtype),
            jax.ShapeDtypeStruct(feed, gate.dtype),
        ),
        in_specs=anywhere(7),
        out_specs=tuple(anywhere(5)),
        scratch_shapes=[
            pltpu.VMEM(feed, gate.dtype),
            pltpu.SemaphoreType.DMA((count,)),
            pltpu.SemaphoreType.DMA((count,)),
            pltpu.SemaphoreType.DMA((4 + packing,)),
        ],
        compiler_params=remote_params(1),
        name="first_exchange",
    )(x, qkv, wo, gains, gate, up, down)


def deal_rows(copies, me, pieces, wo_ref, place, recv_first):
    to_first = pieces * lax.rem(me, 2)
    line_slot = lax.div(me, 2)

    def copy(piece):
        return copies.make(
            recv_first + piece,
            wo_ref.at[piece],
            place(line_slot),
            {"ctx": to_first + piece},
            recv_first + line_slot,
        )

    for piece in range(pieces):

        @pl.when(to_first + piece != me)
        def _(piece=piece):
            copy(piece).start()

        @pl.when(to_first + piece == me)
        def _(piece=piece):
            place(line_slot)[...] = wo_ref[piece]

    def finish(line):
        for slot in range(line):

            @pl.when(2 * slot + lax.div(me, pieces) != me)
            def _(slot=slot):
                copies.make(
                    recv_first, wo_ref.at[0], place(slot), {"ctx": 0}, recv_first + slot
                ).wait_recv()

        for piece in range(pieces):

            @pl.when(to_first + piece != me)
            def _(piece=piece):
                copy(piece).wait_send()

    return finish


def second_kernel(
    o_ref,
    wo_ref,
    ot_ref,
    x_ref,
    gain_ref,
    own_ref,
    dealt_ref,
    residual_ref,
    normed_ref,
    scale_ref,
    gained_ref,
    att,
    wo,
    send,
    recv,
    here,
):
    me = lax.axis_index("ctx")
    rows = x_ref.shape[0]
    local = local_copies(
        [
            (o_ref.at[pl.ds(pl.multiple_of(me * rows, rows), rows), :], att.at[me]),
            (wo_ref, wo.at[:, me]),
        ],
        here.at[pl.ds(0, 2)],
    )
    start_barrier(me)
    copies = Copies(send, recv)

    def block(slot):
        return o_ref.at[pl.ds(pl.multiple_of(slot * rows, rows), rows), :]

    numbers = {}
    for bit in (6, 7, 4, 5, 2, 3, 1):
        numbers[bit] = copies.number()
        copies.send(numbers[bit], block(me ^ bit), att.at[me], {"ctx": me ^ bit})
    line = wo_ref.shape[0]
    middle = line // 2

    def wo_half(side):
        return wo_ref.at[pl.ds(side * middle, middle)]

    def wo_part(slot, side):
        if isinstance(side, slice):
            return wo.at[:, slot]
        return wo.at[pl.ds(side * middle, middle), slot]

    wo_gather = PlaneGather(copies, me, wo_half, wo_part)
    wo_gather.begin()
    wo_gather.first_hop()
    wo_gather.second_hop()
    pieces = ot_ref.shape[0]
    first = copies.next
    copies.next += pieces
    finish = deal_rows(copies, me, pieces, ot_ref, lambda slot: dealt_ref.at[slot], first)
    wo_gather.third_hop()
    wo_gather.last()
    for bit, number in numbers.items():
        copies.arrived(number, att.at[me ^ bit])
    for copy in local:
        copy.wait()
    per_head = 2 * GROUP
    own = wo.at[lax.div(me, 2), pl.ds(per_head * lax.rem(me, 2), per_head)]
    keep = local_copies([(own, own_ref)], here.at[pl.ds(2, 1)])
    plane = att.shape[0]
    total = x_ref[...].astype(jnp.float32)
    for slot in range(plane):
        first = per_head * (slot % 2)
        weight = jnp.concatenate(
            [wo[slot // 2, first + piece] for piece in range(per_head)], axis=0
        )
        total = total + contract(att[slot], weight, 1, 0)
    residual_ref[...] = total
    scale = lax.rsqrt(jnp.mean(total * total, axis=-1, keepdims=True) + norm_epsilon)
    normed = total * scale
    scale_ref[...] = scale
    normed_ref[...] = normed
    gained_ref[...] = (normed * gain_ref[...]).astype(jnp.bfloat16)
    finish(line)
    keep[0].wait()
    copies.finish()


def second_exchange(o, wo, ot, x, gain):
    plane = lax.axis_size("ctx")
    rows = x.shape[0]
    line, part, model = wo.shape
    pieces = 2 * GROUP
    ot = ot.reshape(pieces, -1, ot.shape[1])
    count = GATHER_COPIES + 7 + pieces
    f32 = jnp.float32
    return pl.pallas_call(
        second_kernel,
        out_shape=(
            jax.ShapeDtypeStruct((pieces, part, model), wo.dtype),
            jax.ShapeDtypeStruct((line, *ot.shape[1:]), ot.dtype),
            jax.ShapeDtypeStruct((rows, model), f32),
            jax.ShapeDtypeStruct((rows, model), f32),
            jax.ShapeDtypeStruct((rows, 1), f32),
            jax.ShapeDtypeStruct((rows, model), x.dtype),
        ),
        in_specs=anywhere(2) + in_vmem(3),
        out_specs=(*anywhere(1), *in_vmem(5)),
        scratch_shapes=[
            pltpu.VMEM((plane, rows, o.shape[1]), o.dtype),
            pltpu.VMEM((line, plane, part, model), wo.dtype),
            pltpu.SemaphoreType.DMA((count,)),
            pltpu.SemaphoreType.DMA((count,)),
            pltpu.SemaphoreType.DMA((3,)),
        ],
        compiler_params=remote_params(2),
        name="second_exchange",
    )(o, wo, ot, x, gain)


def gather_kernel(x_ref, xo_ref, send, recv, here):
    me = lax.axis_index("ctx")
    rows = x_ref.shape[0]
    start_barrier(me)
    part = row_part(xo_ref, rows)
    local = local_copies([(x_ref, part(me, slice(None)))], here)
    copies = Copies(send, recv)
    run_gathers([PlaneGather(copies, me, row_half(x_ref, rows), part)])
    copies.finish()
    local[0].wait()


def plane_gather(x, number):
    plane = lax.axis_size("ctx")
    return pl.pallas_call(
        gather_kernel,
        out_shape=jax.ShapeDtypeStruct((plane * x.shape[0], x.shape[1]), x.dtype),
        in_specs=anywhere(1),
        out_specs=anywhere(1)[0],
        scratch_shapes=[
            pltpu.SemaphoreType.DMA((GATHER_COPIES,)),
            pltpu.SemaphoreType.DMA((GATHER_COPIES,)),
            pltpu.SemaphoreType.DMA((1,)),
        ],
        compiler_params=remote_params(number),
    )(x)


def third_kernel(
    sum_ref,
    normed_ref,
    scale_ref,
    gain_ref,
    dy_ref,
    ot_ref,
    wo_ref,
    residual_ref,
    term_ref,
    do_ref,
    dwo_ref,
    own,
    all_grads,
    dwo,
    send,
    recv,
):
    me = lax.axis_index("ctx")
    rows = dy_ref.shape[0]
    start_barrier(me)
    copies = Copies(send, recv)
    part = row_part(all_grads, rows)
    gather = PlaneGather(copies, me, row_half(own, rows), part)
    grad_normed, normed = sum_ref[...], normed_ref[...]
    products = grad_normed * normed
    scaled = grad_normed * gain_ref[...]
    mean = jnp.mean(scaled * normed, axis=-1, keepdims=True)
    residual = dy_ref[...].astype(jnp.float32) + scale_ref[...] * (scaled - normed * mean)
    own[...] = residual.astype(jnp.bfloat16)
    gather.begin()
    residual_ref[...] = residual
    term_ref[...] = jnp.sum(products, axis=0, keepdims=True)
    part(me, slice(None))[...] = own[...]
    dwo[...] = jnp.zeros_like(dwo)

    def step(order, carry):
        for number, slot, sides, when in (
            (4, 1, 0, 1),
            (5, 1, 1, 1),
            (8, 3, 1, 3),
            (10, 3, 0, 3),
            (9, 5, 0, 5),
            (11, 5, 1, 5),
            (12, 7, slice(None), 7),
        ):

            @pl.when(order == when)
            def _(number=number, slot=slot, sides=sides):
                copies.arrived(gather.first + number, gather.part(me ^ slot, sides))

        place = pl.ds(pl.multiple_of((me ^ order) * rows, rows), rows)
        grads = all_grads[place, :]
        do_ref[place, :] = contract(grads, wo_ref[...], 1, 1).astype(jnp.bfloat16)
        dwo[...] += contract(ot_ref[:, place], grads, 1, 0)
        return carry

    lax.fori_loop(0, 2, step, 0)
    gather.first_hop()
    gather.second_hop()
    lax.fori_loop(2, 6, step, 0)
    gather.third_hop()
    lax.fori_loop(6, 8, step, 0)
    line, _, across = dwo_ref.shape
    for slot in range(line):
        rows_at = slice(slot * HALF, (slot + 1) * HALF)
        for number in range(dwo.shape[1] // across):
            columns = slice(number * across, (number + 1) * across)
            dwo_ref[slot, number * HALF : (number + 1) * HALF, :] = dwo[rows_at, columns].astype(
                jnp.bfloat16
            )
    copies.finish()


def third_exchange(line, grad_normed, normed, scale, gain, dy, ot, wo, across):
    plane = lax.axis_size("ctx")
    rows, model = dy.shape
    half_type, f32 = jnp.bfloat16, jnp.float32
    return pl.pallas_call(
        third_kernel,
        out_shape=(
            jax.ShapeDtypeStruct((rows, model), f32),
            jax.ShapeDtypeStruct((1, model), f32),
            jax.ShapeDtypeStruct((plane * rows, wo.shape[0]), half_type),
            jax.ShapeDtypeStruct((line, HALF * model // across, across), half_type),
        ),
        in_specs=in_vmem(7),
        out_specs=tuple(in_vmem(4)),
        scratch_shapes=[
            pltpu.VMEM((rows, model), half_type),
            pltpu.VMEM((plane * rows, model), half_type),
            pltpu.VMEM((line * HALF, model), f32),
            pltpu.SemaphoreType.DMA((GATHER_COPIES,)),
            pltpu.SemaphoreType.DMA((GATHER_COPIES,)),
        ],
        compiler_params=remote_params(6),
        name="third_exchange",
    )(grad_normed, normed, scale, gain, dy, ot, wo)


REDUCE_COPIES = 10


class PlaneReduce:
    def __init__(self, copies, me, block, heard, held, landed):
        self.copies, self.me, self.block = copies, me, block
        self.heard, self.held, self.landed = heard, held, landed
        self.first = copies.next
        copies.next += REDUCE_COPIES
        self.half = heard.shape[1] // 2
        self.x, self.y = {"ctx": me ^ 2}, {"ctx": me ^ 4}

    def side(self, ref, slot, half):
        return ref.at[slot, pl.ds(half * self.half, self.half), :]

    def share(self, order):
        partner = self.me ^ 1
        bit = (6, 2, 4, 0)[order]
        self.copies.send(
            self.first + order, self.block(partner ^ bit), self.heard.at[order], {"ctx": partner}
        )

    def combine(self, order, rows, extra=None):
        bit = (6, 2, 4)[order]
        total = self.block(self.me ^ bit)[rows, :].astype(jnp.float32) + self.heard[
            order, rows, :
        ].astype(jnp.float32)
        if extra is not None:
            total = total + extra
        self.held[order, rows, :] = total.astype(self.held.dtype)

    def onward(self, number):
        order, half, peer = {
            4: (0, 0, self.x),
            5: (0, 1, self.y),
            6: (1, 0, self.x),
            7: (2, 1, self.y),
            8: (1, 1, self.x),
            9: (2, 0, self.y),
        }[number]
        held, landed = self.side(self.held, order, half), self.side(self.landed, order, half)
        return self.copies.make(self.first + number, held, landed, peer)

    def finish(self):
        for number in range(4, REDUCE_COPIES):
            self.onward(number).wait_send()

    def diagonal_sends(self):
        first, half = self.first, self.half
        self.copies.arrived(first + 0, self.heard.at[0])
        self.combine(0, pl.ds(0, 2 * half))
        self.onward(4).start()
        self.onward(5).start()

    def neighbour_sends(self):
        first, half = self.first, self.half
        self.copies.arrived(first + 1, self.heard.at[1])
        self.combine(1, pl.ds(0, half))
        self.onward(6).start()
        self.copies.arrived(first + 2, self.heard.at[2])
        self.combine(2, pl.ds(half, half))
        self.onward(7).start()

    def first_sends(self):
        self.diagonal_sends()
        self.neighbour_sends()

    def second_sends(self):
        first, half = self.first, self.half
        upper, lower = pl.ds(0, half), pl.ds(half, half)
        landed, side, arrived = self.landed, self.side, self.copies.arrived
        arrived(first + 5, side(landed, 0, 1))
        self.combine(1, lower, landed[0, lower, :].astype(jnp.float32))
        self.onward(8).start()
        arrived(first + 4, side(landed, 0, 0))
        self.combine(2, upper, landed[0, upper, :].astype(jnp.float32))
        self.onward(9).start()
        arrived(first + 3, self.heard.at[3])

    def sum_half(self, which):
        first, half = self.first, self.half
        rows = pl.ds(which * half, half)
        self.copies.arrived(first + (6, 8)[which], self.side(self.landed, 1, which))
        self.copies.arrived(first + (9, 7)[which], self.side(self.landed, 2, which))
        return (
            self.block(self.me)[rows, :].astype(jnp.float32)
            + self.heard[3, rows, :].astype(jnp.float32)
            + self.landed[1, rows, :].astype(jnp.float32)
            + self.landed[2, rows, :].astype(jnp.float32)
        )


def feed_kernel(
    line,
    g_ref,
    dy0_hbm,
    dy2_hbm,
    dy4_hbm,
    dy6_hbm,
    w_hbm,
    sum_ref,
    out6_hbm,
    out2_hbm,
    out4_hbm,
    out0_hbm,
    dw_hbm,
    w_ref,
    dw_ref,
    down_ref,
    dy_ref,
    all_g,
    hid,
    hid_t,
    gate_t,
    up_t,
    part,
    heard,
    held,
    landed,
    out_mine,
    out_heard,
    send,
    recv,
    here,
):
    me = lax.axis_index("ctx")
    rows = g_ref.shape[0]
    width, model = down_ref.shape
    blocks = model // width
    unit = width // line

    def at(slot):
        return pl.ds(pl.multiple_of(slot * rows, rows), rows)

    heard_grads = (dy0_hbm, dy2_hbm, dy4_hbm, dy6_hbm)
    local = local_copies(
        [(w_hbm, w_ref)]
        + [(ref, dy_ref.at[at(me ^ (2 * number)), :]) for number, ref in enumerate(heard_grads)],
        here.at[pl.ds(0, 5)],
    )
    start_barrier(me)
    copies = Copies(send, recv)
    gather = PlaneGather(copies, me, row_half(g_ref, rows), row_part(all_g, rows))
    gather.begin()
    dy_first = copies.next
    copies.next += 4
    for number, ref in enumerate(heard_grads):
        place = dy_ref.at[at(me ^ (2 * number)), :]
        copies.send(dy_first + number, ref, place, {"ctx": me ^ 1})
    all_g[at(me), :] = g_ref[...]
    for copy in local:
        copy.wait()
    gate_ref, up_ref = w_ref.at[:, :width], w_ref.at[:, width : 2 * width]
    for z in range(line):
        for number in range(blocks):
            source = pl.ds((z * blocks + number) * unit, unit)
            down_ref[pl.ds(z * unit, unit), number * width : (number + 1) * width] = w_ref[
                source, 2 * width :
            ]

    def block(slot):
        return part.at[at(slot), :]

    reduce = PlaneReduce(copies, me, block, heard, held, landed)

    def chunk(order):
        place = at(me ^ order)
        g = all_g[place, :]
        dy = dy_ref[place, :]
        gate_values = contract(g, gate_ref[...], 1, 0)
        up_values = contract(g, up_ref[...], 1, 0)
        sigmoid_gate = 1.0 / (1.0 + jnp.exp(-gate_values))
        activated = gate_values * sigmoid_gate
        hidden_act = (activated * up_values).astype(jnp.bfloat16)
        hid[place, :] = hidden_act
        hid_t[:, place] = hidden_act.T
        grad_hidden = contract(dy, down_ref[...], 1, 1)
        grad_gate = (
            grad_hidden * up_values * sigmoid_gate * (1.0 + gate_values * (1.0 - sigmoid_gate))
        ).astype(jnp.bfloat16)
        grad_up = (grad_hidden * activated).astype(jnp.bfloat16)
        gate_t[:, place] = grad_gate.T
        up_t[:, place] = grad_up.T
        part[place, :] = (
            contract(grad_gate, gate_ref[...], 1, 1) + contract(grad_up, up_ref[...], 1, 1)
        ).astype(jnp.bfloat16)

    def step(order, carry):
        for number in range(4):

            @pl.when(order == 2 * number + 1)
            def _(number=number):
                place = dy_ref.at[at(me ^ (2 * number + 1)), :]
                copies.arrived(dy_first + number, place)

        for number, slot, sides, when in (
            (4, 1, 0, 1),
            (5, 1, 1, 1),
            (8, 3, 1, 3),
            (10, 3, 0, 3),
            (9, 5, 0, 5),
            (11, 5, 1, 5),
            (12, 7, slice(None), 7),
        ):

            @pl.when(order == when)
            def _(number=number, slot=slot, sides=sides):
                copies.arrived(gather.first + number, gather.part(me ^ slot, sides))

        chunk(order)
        return carry

    lax.fori_loop(0, 2, step, 0)
    gather.first_hop()
    gather.second_hop()
    reduce.share(3)
    lax.fori_loop(2, 6, step, 0)
    reduce.share(1)
    reduce.share(2)
    gather.third_hop()
    reduce.neighbour_sends()
    lax.fori_loop(6, 8, step, 0)
    reduce.share(0)

    out_first = copies.next
    copies.next += 4

    def bit_of(number):
        return jnp.where(number == 0, 6, jnp.where(number == 3, 0, 2 * number))

    def out_copy(number):
        return copies.make(out_first + number, out_mine.at[number], out_heard.at[number], partner)

    def out_of(slot):
        return contract(hid[at(slot), :], down_ref[...], 1, 0)

    partner = {"ctx": me ^ 1}

    def give(number, carry):
        out_mine[number] = out_of(me ^ 1 ^ bit_of(number)).astype(jnp.bfloat16)
        out_copy(number).start()
        return carry

    def keep(number, carry):
        total = out_of(me ^ bit_of(number))
        out_copy(number).wait_recv()
        out_heard[number] = (total + out_heard[number].astype(jnp.float32)).astype(jnp.bfloat16)
        return carry

    def weights(number, carry):
        columns = pl.ds(pl.multiple_of(number * width, width), width)
        total = contract(hid_t[...], dy_ref[:, columns], 1, 0).astype(jnp.bfloat16)
        for z in range(line):
            target = pl.ds(pl.multiple_of((z * blocks + number) * unit, unit), unit)
            dw_ref[target, 2 * width :] = total[z * unit : (z + 1) * unit, :]
        for side, left in enumerate((gate_t, up_t)):
            total = contract(left[...], all_g[:, columns], 1, 0).astype(jnp.bfloat16)
            dw_ref[columns, side * width : (side + 1) * width] = total.T
        return carry

    lax.fori_loop(0, 1, give, 0)
    reduce.diagonal_sends()
    lax.fori_loop(1, 4, give, 0)
    reduce.second_sends()
    lax.fori_loop(0, 4, keep, 0)
    outputs = local_copies(
        [
            (out_heard.at[number], ref)
            for number, ref in enumerate((out6_hbm, out2_hbm, out4_hbm, out0_hbm))
        ],
        here.at[pl.ds(0, 4)],
    )
    lax.fori_loop(0, blocks, weights, 0)
    outputs += local_copies([(dw_ref, dw_hbm)], here.at[pl.ds(4, 1)])
    half = rows // 2
    for which in (1, 0):
        sum_ref[pl.ds(which * half, half), :] = reduce.sum_half(which)
    for number in range(4):
        out_copy(number).wait_send()
    for copy in outputs:
        copy.wait()
    reduce.finish()
    copies.finish()


def feed(g, grads, w):
    plane, line = lax.axis_size("ctx"), lax.axis_size("fsdp")
    rows, model = g.shape
    tokens = plane * rows
    width = w.shape[1] // 3
    count = GATHER_COPIES + REDUCE_COPIES + 8
    half_type = jnp.bfloat16
    return pl.pallas_call(
        functools.partial(feed_kernel, line),
        out_shape=(
            jax.ShapeDtypeStruct((rows, model), jnp.float32),
            *[jax.ShapeDtypeStruct((rows, model), half_type)] * 4,
            jax.ShapeDtypeStruct(w.shape, half_type),
        ),
        in_specs=in_vmem(1) + anywhere(5),
        out_specs=(*in_vmem(1), *anywhere(5)),
        scratch_shapes=[
            pltpu.VMEM(w.shape, half_type),
            pltpu.VMEM(w.shape, half_type),
            pltpu.VMEM((width, model), half_type),
            pltpu.VMEM((tokens, model), half_type),
            pltpu.VMEM((tokens, model), half_type),
            pltpu.VMEM((tokens, width), half_type),
            pltpu.VMEM((width, tokens), half_type),
            pltpu.VMEM((width, tokens), half_type),
            pltpu.VMEM((width, tokens), half_type),
            pltpu.VMEM((tokens, model), half_type),
            pltpu.VMEM((4, rows, model), half_type),
            pltpu.VMEM((3, rows, model), half_type),
            pltpu.VMEM((3, rows, model), half_type),
            pltpu.VMEM((4, rows, model), half_type),
            pltpu.VMEM((4, rows, model), half_type),
            pltpu.SemaphoreType.DMA((count,)),
            pltpu.SemaphoreType.DMA((count,)),
            pltpu.SemaphoreType.DMA((5,)),
        ],
        compiler_params=pltpu.CompilerParams(
            collective_id=3, has_side_effects=True, vmem_limit_bytes=60 << 20
        ),
        name="feed",
    )(g, *grads, w)


def input_kernel(
    dqkv_ref,
    wp_ref,
    x_hbm,
    x_ref,
    gain_ref,
    residual_ref,
    dwo_ref,
    pad_ref,
    input_ref,
    grads_ref,
    term_ref,
    all_x,
    part,
    dw,
    heard,
    held,
    landed,
    send,
    recv,
    here,
):
    me = lax.axis_index("ctx")
    rows = residual_ref.shape[0]
    fetch = local_copies([(x_hbm, all_x)], here)
    start_barrier(me)
    copies = Copies(send, recv)

    def at(slot):
        return pl.ds(pl.multiple_of(slot * rows, rows), rows)

    def compute(slot):
        place = at(slot)
        part[place, :] = contract(dqkv_ref[place, :], wp_ref[...], 1, 1).astype(jnp.bfloat16)

    reduce = PlaneReduce(copies, me, lambda slot: part.at[at(slot), :], heard, held, landed)
    compute(me ^ 7)
    reduce.share(0)
    compute(me ^ 6)
    compute(me ^ 3)
    reduce.share(1)
    reduce.diagonal_sends()
    compute(me ^ 2)
    compute(me ^ 5)
    reduce.share(2)
    compute(me ^ 4)
    reduce.neighbour_sends()
    compute(me ^ 1)
    reduce.share(3)
    compute(me)
    gain = gain_ref[...]
    dw[...] = jnp.zeros_like(dw)
    fetch[0].wait()

    def weights(slot, carry):
        place = at(slot)
        x = all_x[place, :].astype(jnp.float32)
        normed = x * lax.rsqrt(jnp.mean(x * x, axis=-1, keepdims=True) + norm_epsilon)
        gained = (normed * gain).astype(jnp.bfloat16)
        dw[...] += contract(dqkv_ref[place, :], gained, 0, 0)
        return carry

    plane = part.shape[0] // rows
    lax.fori_loop(0, plane // 2, weights, 0)
    reduce.second_sends()
    lax.fori_loop(plane // 2, plane, weights, 0)
    packed = contract(pad_ref[...], dw[...].astype(jnp.bfloat16), 1, 0)
    packed = packed.astype(jnp.bfloat16).T
    line = dwo_ref.shape[0]
    shard = packed.shape[0] // line
    for slot in range(line):
        grads_ref[slot, :shard, :] = packed[slot * shard : (slot + 1) * shard, :]
        grads_ref[slot, shard:, :] = dwo_ref[slot]
    half = rows // 2
    total = jnp.zeros_like(gain)
    for which in (1, 0):
        here_rows = pl.ds(which * half, half)
        grad = reduce.sum_half(which)
        x = x_ref[here_rows, :].astype(jnp.float32)
        scale = lax.rsqrt(jnp.mean(x * x, axis=-1, keepdims=True) + norm_epsilon)
        normed = x * scale
        total = total + jnp.sum(grad * normed, axis=0, keepdims=True)
        scaled = grad * gain
        mean = jnp.mean(scaled * normed, axis=-1, keepdims=True)
        input_ref[0, here_rows, :] = residual_ref[here_rows, :] + scale * (scaled - normed * mean)
    term_ref[...] = total
    reduce.finish()
    copies.finish()


def input_exchange(dqkv, wp, all_x, x, gain, residual, dwo, pad):
    rows, model = x.shape
    line, dealt, across = dwo.shape
    f32 = jnp.float32
    return pl.pallas_call(
        input_kernel,
        out_shape=(
            jax.ShapeDtypeStruct((1, rows, model), f32),
            jax.ShapeDtypeStruct((line, model // line + dealt, across), dwo.dtype),
            jax.ShapeDtypeStruct((1, model), f32),
        ),
        in_specs=in_vmem(2) + anywhere(1) + in_vmem(5),
        out_specs=tuple(in_vmem(3)),
        scratch_shapes=[
            pltpu.VMEM(all_x.shape, all_x.dtype),
            pltpu.VMEM(all_x.shape, all_x.dtype),
            pltpu.VMEM((dqkv.shape[1], model), f32),
            pltpu.VMEM((4, rows, model), x.dtype),
            pltpu.VMEM((3, rows, model), x.dtype),
            pltpu.VMEM((3, rows, model), x.dtype),
            pltpu.SemaphoreType.DMA((REDUCE_COPIES,)),
            pltpu.SemaphoreType.DMA((REDUCE_COPIES,)),
            pltpu.SemaphoreType.DMA((1,)),
        ],
        compiler_params=remote_params(7),
        name="input_exchange",
    )(dqkv, wp, all_x, x, gain, residual, dwo, pad)


def pieces_kernel(
    line,
    piece_ref,
    term_one_ref,
    term_two_ref,
    residual_ref,
    out0_ref,
    out2_ref,
    out4_ref,
    out6_ref,
    whole_ref,
    total_ref,
    output_ref,
    terms,
    terms_heard,
    plane_sum,
    across,
    send,
    recv,
    here,
):
    me, index = lax.axis_index("ctx"), lax.axis_index("fsdp")
    start_barrier(me, index, line)
    copies = Copies(send, recv)
    rows = piece_ref.shape[0]
    part = row_part(whole_ref, rows)
    gather = PlaneGather(copies, me, row_half(piece_ref, rows), part)
    first = copies.next
    copies.next += 7 + line - 1
    terms[0:1, :] = term_one_ref[...]
    terms[1:2, :] = term_two_ref[...]
    gather.begin()
    local = local_copies([(piece_ref, part(me, slice(None)))], here)
    for bit in range(1, 8):
        copies.send(first + bit - 1, terms, terms_heard.at[bit], {"ctx": me ^ bit})
    total = residual_ref[...]
    for ref in (out0_ref, out2_ref, out4_ref, out6_ref):
        total = total + ref[...].astype(jnp.float32)
    output_ref[0] = total.astype(output_ref.dtype)
    gather.first_hop()
    gather.second_hop()
    total = terms[...]
    for bit in range(1, 8):
        copies.arrived(first + bit - 1, terms_heard.at[bit])
        total = total + terms_heard[bit]
    plane_sum[...] = total
    for step in range(1, line):
        peer = {"fsdp": lax.rem(index + step, line)}
        copies.send(first + 6 + step, plane_sum, across.at[step], peer)
    gather.third_hop()
    for step in range(1, line):
        copies.arrived(first + 6 + step, across.at[step])
        total = total + across[step]
    total_ref[...] = total
    gather.last()
    local[0].wait()
    copies.finish()


def pieces_exchange(line, piece, term_one, term_two, residual, outs):
    plane = lax.axis_size("ctx")
    rows, model = residual.shape
    f32 = jnp.float32
    copies = GATHER_COPIES + 7 + line - 1
    return pl.pallas_call(
        functools.partial(pieces_kernel, line),
        out_shape=(
            jax.ShapeDtypeStruct((plane * piece.shape[0], piece.shape[1]), piece.dtype),
            jax.ShapeDtypeStruct((2, model), f32),
            jax.ShapeDtypeStruct((1, rows, model), jnp.bfloat16),
        ),
        in_specs=anywhere(1) + in_vmem(7),
        out_specs=(*anywhere(1), *in_vmem(2)),
        scratch_shapes=[
            pltpu.VMEM((2, model), f32),
            pltpu.VMEM((plane, 2, model), f32),
            pltpu.VMEM((2, model), f32),
            pltpu.VMEM((line, 2, model), f32),
            pltpu.SemaphoreType.DMA((copies,)),
            pltpu.SemaphoreType.DMA((copies,)),
            pltpu.SemaphoreType.DMA((1,)),
        ],
        compiler_params=remote_params(8),
        name="pieces_exchange",
    )(piece, term_one, term_two, residual, *outs)


def spread_kernel(gate_in, up_in, down_in, gate_ref, up_ref, down_ref):
    plane, shard, unit = gate_in.shape
    for source, target in ((gate_in, gate_ref), (up_in, up_ref)):
        for slot in range(plane):
            target[:, slot * unit : (slot + 1) * unit] = source[slot].astype(jnp.float32)
    width = down_in.shape[2]
    blocks = shard // unit
    for slot in range(down_in.shape[0]):
        for number in range(blocks):
            down_ref[slot * unit : (slot + 1) * unit, number * width : (number + 1) * width] = (
                down_in[slot, number * unit : (number + 1) * unit, :].astype(jnp.float32)
            )


def spread_feed(pieces, shard, line, unit):
    plane = lax.axis_size("ctx")
    width = line * unit
    model = line * shard
    pieces = pieces.reshape(plane, shard, 3 * width)
    each = plane // line
    return pl.pallas_call(
        spread_kernel,
        grid=(line,),
        in_specs=[
            pl.BlockSpec((plane, shard, unit), lambda z: (0, 0, z)),
            pl.BlockSpec((plane, shard, unit), lambda z: (0, 0, line + z)),
            pl.BlockSpec((each, shard, width), lambda z: (z, 0, 2)),
        ],
        out_specs=(
            pl.BlockSpec((shard, plane * unit), lambda z: (0, z)),
            pl.BlockSpec((shard, plane * unit), lambda z: (0, z)),
            pl.BlockSpec((each * unit, model), lambda z: (z, 0)),
        ),
        out_shape=(
            jax.ShapeDtypeStruct((shard, plane * width), jnp.float32),
            jax.ShapeDtypeStruct((shard, plane * width), jnp.float32),
            jax.ShapeDtypeStruct((plane * unit, model), jnp.float32),
        ),
        compiler_params=pltpu.CompilerParams(vmem_limit_bytes=62 << 20),
        name="spread_feed",
    )(pieces, pieces, pieces)


def spread_attention_kernel(in_ref, q_ref, k_ref, v_ref, wo_ref):
    plane, _, across = in_ref.shape
    shard = q_ref.shape[0]
    key_width = k_ref.shape[1] // plane
    query_width = q_ref.shape[1] // plane
    first = 0
    for target, width in ((q_ref, query_width), (k_ref, key_width), (v_ref, key_width)):
        target[...] = jnp.concatenate(
            [
                in_ref[slot, :shard, first : first + width].astype(jnp.float32)
                for slot in range(plane)
            ],
            axis=1,
        )
        first += width
    for slot in range(plane):
        for number in range(wo_ref.shape[1] // across):
            source = slice(shard + number * HALF, shard + (number + 1) * HALF)
            wo_ref[slot * HALF : (slot + 1) * HALF, number * across : (number + 1) * across] = (
                in_ref[slot, source, :].astype(jnp.float32)
            )


def spread_attention(pieces, shard, model, query_width, key_width):
    plane = lax.axis_size("ctx")
    pieces = pieces.reshape(plane, -1, pieces.shape[1])
    f32 = jnp.float32
    return pl.pallas_call(
        spread_attention_kernel,
        in_specs=in_vmem(1),
        out_specs=tuple(in_vmem(4)),
        out_shape=(
            jax.ShapeDtypeStruct((shard, plane * query_width), f32),
            jax.ShapeDtypeStruct((shard, plane * key_width), f32),
            jax.ShapeDtypeStruct((shard, plane * key_width), f32),
            jax.ShapeDtypeStruct((plane * HALF, model), f32),
        ),
        compiler_params=pltpu.CompilerParams(vmem_limit_bytes=40 << 20),
        name="spread_attention",
    )(pieces)


def head_local(
    block_input,
    block_table,
    output_grad,
    attention_gain,
    query_weight,
    key_weight,
    value_projection,
    output_weight,
    feedforward_gain,
    gate_weight,
    up_weight,
    down_weight,
):
    me = lax.axis_index("ctx")
    plane = lax.axis_size("ctx")
    line = lax.axis_size("fsdp")
    rows, model = block_input.shape[1:]
    shard = model // line
    hidden = gate_weight.shape[1]
    unit = hidden // (line * plane)
    table_row = block_table[0]
    slot_count = table_row.shape[0]
    block = rows * plane // slot_count
    places = jnp.arange(slot_count, dtype=jnp.int32)
    slots = jnp.sum(jnp.where(table_row[None, :] == places[:, None], places[None, :], 0), axis=1)

    def mine(array, width):
        return lax.dynamic_slice_in_dim(array, me * width, width, 1)

    query_width = query_weight.shape[1] // plane
    key_width = key_weight.shape[1] // plane
    qkv_mine = jnp.concatenate(
        [
            mine(query_weight, query_width),
            mine(key_weight, key_width),
            mine(value_projection, key_width),
        ],
        axis=1,
    )
    gains_mine = jnp.stack([attention_gain, feedforward_gain])
    x_all, qkv_w, wo_line, gains, feed_mine = first_exchange(
        line,
        block_input[0],
        qkv_mine,
        output_weight,
        gains_mine,
        gate_weight,
        up_weight,
        down_weight,
    )
    feed_w = lax.all_gather(feed_mine, "fsdp", axis=0, tiled=True)

    steps_index = jnp.arange(HALF, dtype=jnp.float32)
    inverse = jnp.exp(steps_index * jnp.float32(-2.0 * math.log(rotary_base) / HEAD_SIZE))

    def table_of(positions):
        angles = positions.astype(jnp.float32)[:, None] * inverse[None, :]
        both = jnp.stack([jnp.cos(angles), jnp.sin(angles)])
        both = jnp.pad(both, ((0, 0), (0, 0), (0, LANES // 2 - HALF)))
        return jnp.concatenate([both, both], axis=2)

    inner = table_of(jnp.arange(block, dtype=jnp.int32))
    outer = table_of(places * block)
    pad = padding(GROUP + 2)

    gains = jnp.transpose(gains, (1, 0, 2)).reshape(2, model).astype(jnp.float32)
    qkv_w = qkv_w.reshape(model, -1)
    grad_rows, x_all = lax.optimization_barrier((output_grad[0], x_all))
    grad_parts = [grad_rows]
    for bit in (2, 4, 6):
        pairs = [(device, device ^ bit) for device in range(plane)]
        grad_parts.append(lax.ppermute(grad_rows, "ctx", pairs))
    qkv, o, o_columns, lse, qkv_pad = attend(
        slots, x_all, gains[:1], qkv_w, pad, inner, outer
    )
    wo_mine, columns_mine, residual, normed_two, scale_two, gained_two = second_exchange(
        o, wo_line, o_columns, block_input[0], gains[1:]
    )
    grad_normed_two, *out_parts, feed_grads = feed(gained_two, grad_parts, feed_w)
    feed_grads = lax.psum_scatter(feed_grads, "fsdp", scatter_dimension=0, tiled=True)
    grad_residual, feedforward_term, grad_o, wo_term = third_exchange(
        line,
        grad_normed_two,
        normed_two,
        scale_two,
        gains[1:],
        output_grad[0],
        columns_mine.reshape(-1, columns_mine.shape[2]),
        wo_mine.reshape(-1, model),
        qkv_w.shape[1],
    )
    *out_parts, grad_o = lax.optimization_barrier((*out_parts, grad_o))
    outs = [out_parts[3]]
    for part, bit in enumerate((6, 2, 4)):
        pairs = [(device, device ^ bit) for device in range(plane)]
        outs.append(lax.ppermute(out_parts[part], "ctx", pairs))
    grads = attend_back(slots, qkv, o, grad_o, lse, pad, inner, outer)
    input_grad, attention_grads, attention_term = input_exchange(
        grads, qkv_pad, x_all, block_input[0], gains[:1], grad_residual, wo_term, pad
    )
    attention_grads, feed_grads = lax.optimization_barrier((attention_grads, feed_grads))
    attention_grads = lax.psum_scatter(
        attention_grads.reshape(-1, attention_grads.shape[2]),
        "fsdp",
        scatter_dimension=0,
        tiled=True,
    )
    feed_pieces, gain_terms, layer_output = pieces_exchange(
        line, feed_grads, attention_term, feedforward_term, residual, outs
    )
    gate_grad, up_grad, down_grad = spread_feed(feed_pieces, shard, line, unit)
    attention_pieces = plane_gather(attention_grads, 9)
    query_grad, key_grad, value_grad, out_grad = spread_attention(
        attention_pieces, shard, model, query_width, key_width
    )
    gain_terms = lax.dynamic_slice_in_dim(gain_terms, lax.axis_index("fsdp") * shard, shard, 1)
    return (
        layer_output,
        input_grad,
        gain_terms[0],
        query_grad,
        key_grad,
        value_grad,
        out_grad,
        gain_terms[1],
        gate_grad,
        up_grad,
        down_grad,
    )


def solution(mesh):
    plane, line = mesh.shape["ctx"], mesh.shape["fsdp"]
    fits = plane == KEY_VALUE_HEADS == 8 and plane * line * HALF == QUERY_HEADS * HEAD_SIZE
    if fits:
        return placed(mesh, head_local)
    return placed(mesh, local)


def placed(mesh, plan):
    return jax.shard_map(
        plan,
        mesh=mesh,
        in_specs=(
            P("fsdp", "ctx", None),
            P("fsdp", None),
            P("fsdp", "ctx", None),
            P("fsdp"),
            P("fsdp", None),
            P("fsdp", None),
            P("fsdp", None),
            P("fsdp", None),
            P("fsdp"),
            P("fsdp", None),
            P("fsdp", None),
            P("fsdp", None),
        ),
        out_specs=(
            P("fsdp", "ctx", None),
            P("fsdp", "ctx", None),
            P("fsdp"),
            P("fsdp", None),
            P("fsdp", None),
            P("fsdp", None),
            P("fsdp", None),
            P("fsdp"),
            P("fsdp", None),
            P("fsdp", None),
            P("fsdp", None),
        ),
        check_vma=False,
    )
```

```python
import functools
import math

import jax
import jax.numpy as jnp
from jax import lax
from jax.experimental import pallas as pl
from jax.experimental.pallas import tpu as pltpu
from jax.sharding import PartitionSpec as P


QUERY_HEADS = 16
KEY_VALUE_HEADS = 8
HEAD_SIZE = 96


norm_epsilon = 1e-05
rotary_base = 100000.0
score_with_mask = -1e30


def rope_tables(positions):
    half_width = HEAD_SIZE // 2
    steps_index = jnp.arange(half_width, dtype=jnp.float32)
    inverse = jnp.exp(steps_index * jnp.float32(-2.0 * math.log(rotary_base) / HEAD_SIZE))
    angles = positions.astype(jnp.float32)[:, None] * inverse[None, :]
    return (jnp.cos(angles), jnp.sin(angles))


def rotate(value_rows, cosine, sine_values, direction):
    count_of_rows = value_rows.shape[0]
    head_count = value_rows.shape[1] // HEAD_SIZE
    half_width = HEAD_SIZE // 2
    shaped = value_rows.reshape(count_of_rows, head_count, HEAD_SIZE)
    first_half = shaped[:, :, :half_width]
    second_half = shaped[:, :, half_width:]
    cos_part = cosine[:, None, :]
    sin_part = sine_values[:, None, :] * direction
    turned = jnp.concatenate(
        [
            first_half * cos_part - second_half * sin_part,
            second_half * cos_part + first_half * sin_part,
        ],
        axis=2,
    )
    return turned.reshape(count_of_rows, head_count * HEAD_SIZE)


def norm_scale(value_rows):
    return lax.rsqrt(jnp.mean(value_rows * value_rows, axis=-1, keepdims=True) + norm_epsilon)


def product(matrix, operand):
    return jnp.dot(matrix, operand, preferred_element_type=jnp.float32)


def cross_rows(matrix, operand):
    return lax.dot_general(
        matrix, operand, (((0,), (0,)), ((), ())), preferred_element_type=jnp.float32
    )


def back_product(matrix, operand):
    return lax.dot_general(
        matrix, operand, (((1,), (1,)), ((), ())), preferred_element_type=jnp.float32
    )


def block_scores(query_rank_four, block_of_keys, query_positions, key_positions):
    keys_rank_three = block_of_keys.reshape(block_of_keys.shape[0], KEY_VALUE_HEADS, HEAD_SIZE)
    scores = jnp.einsum(
        "rgjd,kgd->gjrk", query_rank_four, keys_rank_three, preferred_element_type=jnp.float32
    ) * HEAD_SIZE ** (-0.5)
    allowed = (key_positions[None, :] <= query_positions[:, None])[None, None]
    return (jnp.where(allowed, scores, score_with_mask), allowed)


def local(
    block_input,
    block_table,
    output_grad,
    attention_gain,
    query_weight,
    key_weight,
    value_projection,
    output_weight,
    feedforward_gain,
    gate_weight,
    up_weight,
    down_weight,
):
    query_group_width = QUERY_HEADS // KEY_VALUE_HEADS
    score_scale = HEAD_SIZE ** (-0.5)
    inputs = block_input[0].astype(jnp.float32)
    count_of_rows = inputs.shape[0]
    block_rows = count_of_rows // 2
    ctx_index = lax.axis_index("ctx")
    table_row = block_table[0]
    offsets = jnp.arange(block_rows, dtype=jnp.int32)
    query_blocks = lax.dynamic_slice_in_dim(table_row, 2 * ctx_index, 2)
    query_positions = (query_blocks[:, None] * block_rows + offsets[None, :]).reshape(count_of_rows)
    key_positions = (table_row[:, None] * block_rows + offsets[None, :]).reshape(-1)
    cosine, sine_values = rope_tables(query_positions)
    gain_one, query_full, key_full, value_full, out_full = (
        lax.all_gather(attention_gain, "fsdp", axis=0, tiled=True),
        lax.all_gather(query_weight, "fsdp", axis=0, tiled=True),
        lax.all_gather(key_weight, "fsdp", axis=0, tiled=True),
        lax.all_gather(value_projection, "fsdp", axis=0, tiled=True),
        lax.all_gather(output_weight, "fsdp", axis=0, tiled=True),
    )
    scale_one = norm_scale(inputs)
    normed_one = inputs * scale_one
    gained_one = (normed_one * gain_one.astype(jnp.float32)).astype(jnp.bfloat16)
    query_rows = rotate(product(gained_one, query_full), cosine, sine_values, 1.0).astype(
        jnp.bfloat16
    )
    keys_local = rotate(product(gained_one, key_full), cosine, sine_values, 1.0).astype(
        jnp.bfloat16
    )
    values_local = product(gained_one, value_full).astype(jnp.bfloat16)
    keys_all, values_all = (
        lax.all_gather(keys_local, "ctx", axis=0, tiled=True),
        lax.all_gather(values_local, "ctx", axis=0, tiled=True),
    )
    key_total_count = keys_all.shape[0]
    key_block_pass = 1024
    block_count = key_total_count // key_block_pass
    query_rank_four = query_rows.reshape(
        count_of_rows, KEY_VALUE_HEADS, query_group_width, HEAD_SIZE
    )
    key_places = key_positions.reshape(block_count, key_block_pass)

    def split_keys(array_in):
        return array_in.reshape(block_count, key_block_pass, array_in.shape[-1])

    def statistics_step(state_now, block_data):
        running_max, running_sum = state_now
        block_of_keys, key_place = block_data
        masked, allowed = block_scores(query_rank_four, block_of_keys, query_positions, key_place)
        new_max = jnp.maximum(running_max, jnp.max(masked, axis=-1))
        block_sum = jnp.sum(jnp.where(allowed, jnp.exp(masked - new_max[..., None]), 0.0), axis=-1)
        return ((new_max, running_sum * jnp.exp(running_max - new_max) + block_sum), None)

    initial_maximum = jnp.full(
        (KEY_VALUE_HEADS, query_group_width, count_of_rows), score_with_mask, jnp.float32
    )
    initial_sum = jnp.zeros((KEY_VALUE_HEADS, query_group_width, count_of_rows), jnp.float32)
    (final_max, final_sum), unused = lax.scan(
        statistics_step, (initial_maximum, initial_sum), (split_keys(keys_all), key_places)
    )
    log_total = final_max + jnp.log(final_sum)

    def output_step(state_now, block_data):
        block_of_keys, block_of_values, key_place = block_data
        masked, allowed = block_scores(query_rank_four, block_of_keys, query_positions, key_place)
        weights_half = jnp.where(allowed, jnp.exp(masked - log_total[..., None]), 0.0).astype(
            jnp.bfloat16
        )
        values_rank_three = block_of_values.reshape(key_block_pass, KEY_VALUE_HEADS, HEAD_SIZE)
        return (
            state_now
            + jnp.einsum(
                "gjrk,kgd->rgjd",
                weights_half,
                values_rank_three,
                preferred_element_type=jnp.float32,
            ),
            None,
        )

    initial_output = jnp.zeros(
        (count_of_rows, KEY_VALUE_HEADS, query_group_width, HEAD_SIZE), jnp.float32
    )
    summed_out, unused = lax.scan(
        output_step, initial_output, (split_keys(keys_all), split_keys(values_all), key_places)
    )
    attended_rows = summed_out.reshape(count_of_rows, QUERY_HEADS * HEAD_SIZE).astype(jnp.bfloat16)
    residual = inputs + product(attended_rows, out_full)
    scale_two = norm_scale(residual)
    normed_two = residual * scale_two
    gain_two, gate_full, up_full, down_full = (
        lax.all_gather(feedforward_gain, "fsdp", axis=0, tiled=True),
        lax.all_gather(gate_weight, "fsdp", axis=0, tiled=True),
        lax.all_gather(up_weight, "fsdp", axis=0, tiled=True),
        lax.all_gather(down_weight, "fsdp", axis=0, tiled=True),
    )
    gained_two = (normed_two * gain_two.astype(jnp.float32)).astype(jnp.bfloat16)
    gate_values = product(gained_two, gate_full)
    up_values = product(gained_two, up_full)
    sigmoid_gate = jax.nn.sigmoid(gate_values)
    activated = gate_values * sigmoid_gate
    hidden_act = (activated * up_values).astype(jnp.bfloat16)
    layer_output = (residual + product(hidden_act, down_full)).astype(jnp.bfloat16)
    gain_two_again, gate_back, up_back, down_back = (
        lax.all_gather(feedforward_gain, "fsdp", axis=0, tiled=True),
        lax.all_gather(gate_weight, "fsdp", axis=0, tiled=True),
        lax.all_gather(up_weight, "fsdp", axis=0, tiled=True),
        lax.all_gather(down_weight, "fsdp", axis=0, tiled=True),
    )
    grad_rows = output_grad[0]
    grad_hidden = back_product(grad_rows, down_back)
    down_term = cross_rows(hidden_act, grad_rows)
    grad_gate = (
        grad_hidden * up_values * sigmoid_gate * (1.0 + gate_values * (1.0 - sigmoid_gate))
    ).astype(jnp.bfloat16)
    grad_up = (grad_hidden * activated).astype(jnp.bfloat16)
    gate_term = cross_rows(gained_two, grad_gate)
    up_term = cross_rows(gained_two, grad_up)
    grad_normed_two = back_product(grad_gate, gate_back) + back_product(grad_up, up_back)
    feedforward_term = jnp.sum(grad_normed_two * normed_two, axis=0)
    grad_scaled_two = grad_normed_two * gain_two_again.astype(jnp.float32)
    grad_residual = grad_rows.astype(jnp.float32) + scale_two * (
        grad_scaled_two
        - normed_two * jnp.mean(grad_scaled_two * normed_two, axis=-1, keepdims=True)
    )
    gain_one_again, query_back, key_back, value_back, out_back = (
        lax.all_gather(attention_gain, "fsdp", axis=0, tiled=True),
        lax.all_gather(query_weight, "fsdp", axis=0, tiled=True),
        lax.all_gather(key_weight, "fsdp", axis=0, tiled=True),
        lax.all_gather(value_projection, "fsdp", axis=0, tiled=True),
        lax.all_gather(output_weight, "fsdp", axis=0, tiled=True),
    )
    grad_attn = grad_residual.astype(jnp.bfloat16)
    output_term = cross_rows(attended_rows, grad_attn)
    attended_gradient = back_product(grad_attn, out_back).astype(jnp.bfloat16)
    gradient_rank_four = attended_gradient.reshape(
        count_of_rows, KEY_VALUE_HEADS, query_group_width, HEAD_SIZE
    )
    attended_rank_four = attended_rows.reshape(
        count_of_rows, KEY_VALUE_HEADS, query_group_width, HEAD_SIZE
    )
    row_delta = jnp.transpose(
        jnp.sum(
            gradient_rank_four.astype(jnp.float32) * attended_rank_four.astype(jnp.float32), axis=-1
        ),
        (1, 2, 0),
    )
    keys_again, values_again = (
        lax.all_gather(keys_local, "ctx", axis=0, tiled=True),
        lax.all_gather(values_local, "ctx", axis=0, tiled=True),
    )

    def back_step(state_now, block_data):
        block_of_keys, block_of_values, key_place = block_data
        masked, allowed = block_scores(query_rank_four, block_of_keys, query_positions, key_place)
        weights_half = jnp.where(allowed, jnp.exp(masked - log_total[..., None]), 0.0).astype(
            jnp.bfloat16
        )
        values_rank_three = block_of_values.reshape(key_block_pass, KEY_VALUE_HEADS, HEAD_SIZE)
        keys_rank_three = block_of_keys.reshape(key_block_pass, KEY_VALUE_HEADS, HEAD_SIZE)
        grad_weights = jnp.einsum(
            "rgjd,kgd->gjrk",
            gradient_rank_four,
            values_rank_three,
            preferred_element_type=jnp.float32,
        )
        grad_scores = (
            weights_half.astype(jnp.float32) * (grad_weights - row_delta[..., None]) * score_scale
        ).astype(jnp.bfloat16)
        state_now = state_now + jnp.einsum(
            "gjrk,kgd->rgjd", grad_scores, keys_rank_three, preferred_element_type=jnp.float32
        )
        key_gradient = jnp.einsum(
            "gjrk,rgjd->kgd", grad_scores, query_rank_four, preferred_element_type=jnp.float32
        )
        value_gradient = jnp.einsum(
            "gjrk,rgjd->kgd", weights_half, gradient_rank_four, preferred_element_type=jnp.float32
        )
        return (
            state_now,
            (
                key_gradient.reshape(key_block_pass, KEY_VALUE_HEADS * HEAD_SIZE).astype(
                    jnp.bfloat16
                ),
                value_gradient.reshape(key_block_pass, KEY_VALUE_HEADS * HEAD_SIZE).astype(
                    jnp.bfloat16
                ),
            ),
        )

    first_query_index = jnp.zeros(
        (count_of_rows, KEY_VALUE_HEADS, query_group_width, HEAD_SIZE), jnp.float32
    )
    query_sum, (key_gradients, value_gradients) = lax.scan(
        back_step, first_query_index, (split_keys(keys_again), split_keys(values_again), key_places)
    )
    key_gradients = key_gradients.reshape(key_total_count, KEY_VALUE_HEADS * HEAD_SIZE)
    value_gradients = value_gradients.reshape(key_total_count, KEY_VALUE_HEADS * HEAD_SIZE)
    key_sums, value_sums = (
        lax.psum_scatter(key_gradients, "ctx", scatter_dimension=0, tiled=True).astype(jnp.float32),
        lax.psum_scatter(value_gradients, "ctx", scatter_dimension=0, tiled=True).astype(
            jnp.float32
        ),
    )
    query_gradients = rotate(
        query_sum.reshape(count_of_rows, QUERY_HEADS * HEAD_SIZE), cosine, sine_values, -1.0
    ).astype(jnp.bfloat16)
    grad_keys = rotate(key_sums, cosine, sine_values, -1.0).astype(jnp.bfloat16)
    grad_values = value_sums.astype(jnp.bfloat16)
    query_term = cross_rows(gained_one, query_gradients)
    key_term = cross_rows(gained_one, grad_keys)
    value_term = cross_rows(gained_one, grad_values)
    grad_normed_one = (
        back_product(query_gradients, query_back)
        + back_product(grad_keys, key_back)
        + back_product(grad_values, value_back)
    )
    attention_term = jnp.sum(grad_normed_one * normed_one, axis=0)
    grad_scaled_one = grad_normed_one * gain_one_again.astype(jnp.float32)
    input_grad = grad_residual + scale_one * (
        grad_scaled_one
        - normed_one * jnp.mean(grad_scaled_one * normed_one, axis=-1, keepdims=True)
    )
    shares = (
        lax.psum_scatter(
            attention_term.astype(jnp.bfloat16), "fsdp", scatter_dimension=0, tiled=True
        ).astype(jnp.float32),
        lax.psum_scatter(
            query_term.astype(jnp.bfloat16), "fsdp", scatter_dimension=0, tiled=True
        ).astype(jnp.float32),
        lax.psum_scatter(
            key_term.astype(jnp.bfloat16), "fsdp", scatter_dimension=0, tiled=True
        ).astype(jnp.float32),
        lax.psum_scatter(
            value_term.astype(jnp.bfloat16), "fsdp", scatter_dimension=0, tiled=True
        ).astype(jnp.float32),
        lax.psum_scatter(
            output_term.astype(jnp.bfloat16), "fsdp", scatter_dimension=0, tiled=True
        ).astype(jnp.float32),
        lax.psum_scatter(
            feedforward_term.astype(jnp.bfloat16), "fsdp", scatter_dimension=0, tiled=True
        ).astype(jnp.float32),
        lax.psum_scatter(
            gate_term.astype(jnp.bfloat16), "fsdp", scatter_dimension=0, tiled=True
        ).astype(jnp.float32),
        lax.psum_scatter(
            up_term.astype(jnp.bfloat16), "fsdp", scatter_dimension=0, tiled=True
        ).astype(jnp.float32),
        lax.psum_scatter(
            down_term.astype(jnp.bfloat16), "fsdp", scatter_dimension=0, tiled=True
        ).astype(jnp.float32),
    )
    totals = (
        lax.psum(shares[0].astype(jnp.bfloat16), "ctx").astype(jnp.float32),
        lax.psum(shares[1].astype(jnp.bfloat16), "ctx").astype(jnp.float32),
        lax.psum(shares[2].astype(jnp.bfloat16), "ctx").astype(jnp.float32),
        lax.psum(shares[3].astype(jnp.bfloat16), "ctx").astype(jnp.float32),
        lax.psum(shares[4].astype(jnp.bfloat16), "ctx").astype(jnp.float32),
        lax.psum(shares[5].astype(jnp.bfloat16), "ctx").astype(jnp.float32),
        lax.psum(shares[6].astype(jnp.bfloat16), "ctx").astype(jnp.float32),
        lax.psum(shares[7].astype(jnp.bfloat16), "ctx").astype(jnp.float32),
        lax.psum(shares[8].astype(jnp.bfloat16), "ctx").astype(jnp.float32),
    )
    return (
        layer_output[None],
        input_grad[None],
        totals[0],
        totals[1],
        totals[2],
        totals[3],
        totals[4],
        totals[5],
        totals[6],
        totals[7],
        totals[8],
    )


LANES = 128
HALF = HEAD_SIZE // 2
GROUP = QUERY_HEADS // KEY_VALUE_HEADS
score_scale = HEAD_SIZE ** (-0.5)
binary_scale = score_scale * math.log2(math.e)


def contract(left, right, left_dim, right_dim):
    return lax.dot_general(
        left, right, (((left_dim,), (right_dim,)), ((), ())), preferred_element_type=jnp.float32
    )


def in_vmem(count):
    return [pl.BlockSpec(memory_space=pltpu.VMEM)] * count


def padding(heads):
    column = jnp.arange(heads * HEAD_SIZE, dtype=jnp.int32)
    half_at, rest = column // HALF, column % HALF
    target = half_at * (LANES // 2) + rest
    lanes = jnp.arange(heads * LANES, dtype=jnp.int32)
    return (target[:, None] == lanes[None, :]).astype(jnp.bfloat16)


def turn(part, cosine, sine):
    return part * cosine + pltpu.roll(part, LANES // 2, 1) * sine


def tables(inner_ref, outer_ref, index, per_tile):
    inner_cos, inner_sin = inner_ref[0], inner_ref[1]
    sign = jnp.where(
        lax.broadcasted_iota(jnp.int32, inner_cos.shape, 1) < LANES // 2, -1.0, 1.0
    )
    cosines, sines = [], []
    for part in range(per_tile):
        at = pl.ds(index * per_tile + part, 1)
        outer_cos, outer_sin = outer_ref[0, at, :], outer_ref[1, at, :]
        cosines.append(inner_cos * outer_cos - inner_sin * outer_sin)
        sines.append(sign * (inner_sin * outer_cos + inner_cos * outer_sin))
    return jnp.concatenate(cosines, axis=0), jnp.concatenate(sines, axis=0)


def forward_kernel(
    slot_ref,
    xa_ref,
    xb_ref,
    gain_ref,
    w_ref,
    pad_ref,
    inner_ref,
    outer_ref,
    qkv_hbm,
    o_ref,
    ot_ref,
    lse_ref,
    wp_hbm,
    qkv_ref,
    wp,
    qs,
    vt,
    s_ref,
    here,
):
    index = pl.program_id(0)
    block = xa_ref.shape[0]
    tile = 2 * block
    width = GROUP * tile
    heads = GROUP + 2

    @pl.when(index == 0)
    def _():
        wp[...] = contract(w_ref[...], pad_ref[...], 1, 0).astype(jnp.bfloat16)
        pltpu.make_async_copy(wp, wp_hbm, here.at[1]).start()

    x = jnp.concatenate([xa_ref[...], xb_ref[...]], axis=0).astype(jnp.float32)
    normed = x * lax.rsqrt(jnp.mean(x * x, axis=-1, keepdims=True) + norm_epsilon)
    gained = (normed * gain_ref[...]).astype(jnp.bfloat16)
    raw = contract(gained, wp[...], 1, 0)
    cosine, sine = tables(inner_ref, outer_ref, index, 2)
    here_rows = pl.ds(pl.multiple_of(index * tile, tile), tile)
    for head in range(heads):
        lanes = slice(head * LANES, (head + 1) * LANES)
        part = raw[:, lanes]
        if head <= GROUP:
            part = turn(part, cosine, sine)
        part = part.astype(jnp.bfloat16)
        qkv_ref[here_rows, lanes] = part
        if head < GROUP:
            qs[head * tile : (head + 1) * tile, :] = part
        if head == heads - 1:
            vt[:, here_rows] = part.T

    def save(number):
        place = pl.ds(pl.multiple_of(number * tile, tile), tile)
        return pltpu.make_async_copy(qkv_ref.at[place, :], qkv_hbm.at[place, :], here.at[0])

    save(index).start()
    queries = qs[...]
    key_at = lax.broadcasted_iota(jnp.int32, (tile, width), 0)
    query_at = lax.rem(lax.broadcasted_iota(jnp.int32, (tile, width), 1), tile)
    diagonal = key_at <= query_at

    def scores_of(step):
        at = pl.ds(pl.multiple_of(step * tile, tile), tile)
        keys = qkv_ref[at, GROUP * LANES : (GROUP + 1) * LANES]
        return contract(keys, queries, 1, 1) * binary_scale

    last = jnp.where(diagonal, scores_of(index), score_with_mask)
    s_ref[here_rows, :] = last
    peak = jnp.max(last, axis=0, keepdims=True)

    def in_pairs(one, state):
        state = lax.fori_loop(
            0, lax.div(index, 2), lambda pair, state: one((2 * pair, 2 * pair + 1), state), state
        )
        return lax.fori_loop(0, lax.rem(index, 2), lambda _, state: one((index - 1,), state), state)

    def first_pass(steps, peak):
        found = [scores_of(step) for step in steps]
        for step, scores in zip(steps, found):
            s_ref[pl.ds(pl.multiple_of(step * tile, tile), tile), :] = scores
            peak = jnp.maximum(peak, jnp.max(scores, axis=0, keepdims=True))
        return peak

    peak = in_pairs(first_pass, peak)

    def second_pass(steps, state):
        total, out = state
        for step in steps:
            at = pl.ds(pl.multiple_of(step * tile, tile), tile)
            probs = jnp.exp2(s_ref[at, :] - peak)
            total = total + jnp.sum(probs, axis=0, keepdims=True)
            out = out + contract(vt[:, at], probs.astype(jnp.bfloat16), 1, 0)
        return (total, out)

    total, out = in_pairs(
        second_pass,
        second_pass(
            (index,), (jnp.zeros((1, width), jnp.float32), jnp.zeros((LANES, width), jnp.float32))
        ),
    )
    lse_ref[pl.ds(index, 1), :] = peak + jnp.log2(total)
    out = (out * (1.0 / total)).T.astype(jnp.bfloat16)
    out = jnp.concatenate([out[head * tile : (head + 1) * tile, :] for head in range(GROUP)], axis=1)
    out = contract(out, pad_ref[: GROUP * HEAD_SIZE, : GROUP * LANES], 1, 1).astype(jnp.bfloat16)
    for part in range(2):
        target = pl.ds(pl.multiple_of(slot_ref[index * 2 + part] * block, block), block)
        rows_at = slice(part * block, (part + 1) * block)
        o_ref[target, :] = out[rows_at, :]
        ot_ref[:, target] = out[rows_at, :].T

    save(index).wait()

    @pl.when(index == pl.num_programs(0) - 1)
    def _():
        pltpu.make_async_copy(wp, wp_hbm, here.at[1]).wait()


def attend(slots, x, gain, w, pad, inner, outer):
    rows, model = x.shape
    block = rows // slots.shape[0]
    tile = 2 * block
    width = GROUP * tile
    columns = pad.shape[1]
    whole = lambda *shape: pl.BlockSpec(shape, lambda i, s: (0,) * len(shape))
    return pl.pallas_call(
        forward_kernel,
        grid_spec=pltpu.PrefetchScalarGridSpec(
            num_scalar_prefetch=1,
            grid=(rows // tile,),
            in_specs=[
                pl.BlockSpec((block, model), lambda i, s: (s[2 * i], 0)),
                pl.BlockSpec((block, model), lambda i, s: (s[2 * i + 1], 0)),
                whole(1, model),
                whole(*w.shape),
                whole(*pad.shape),
                whole(*inner.shape),
                whole(*outer.shape),
            ],
            out_specs=(
                pl.BlockSpec(memory_space=pl.ANY),
                whole(rows, GROUP * HEAD_SIZE),
                whole(GROUP * HEAD_SIZE, rows),
                whole(rows // tile, width),
                pl.BlockSpec(memory_space=pl.ANY),
            ),
            scratch_shapes=[
                pltpu.VMEM((rows, columns), jnp.bfloat16),
                pltpu.VMEM((model, columns), jnp.bfloat16),
                pltpu.VMEM((width, LANES), jnp.bfloat16),
                pltpu.VMEM((LANES, rows), jnp.bfloat16),
                pltpu.VMEM((rows, width), jnp.float32),
                pltpu.SemaphoreType.DMA((2,)),
            ],
        ),
        out_shape=(
            jax.ShapeDtypeStruct((rows, columns), jnp.bfloat16),
            jax.ShapeDtypeStruct((rows, GROUP * HEAD_SIZE), jnp.bfloat16),
            jax.ShapeDtypeStruct((GROUP * HEAD_SIZE, rows), jnp.bfloat16),
            jax.ShapeDtypeStruct((rows // tile, width), jnp.float32),
            jax.ShapeDtypeStruct((model, columns), jnp.bfloat16),
        ),
        compiler_params=pltpu.CompilerParams(vmem_limit_bytes=62 << 20),
        cost_estimate=pl.CostEstimate(
            flops=4 * GROUP * rows * rows * LANES // 2 + 2 * rows * model * columns,
            bytes_accessed=4 * rows * model,
            transcendentals=GROUP * rows * rows // 2,
        ),
        name="attend",
    )(slots, x, x, gain, w, pad, inner, outer)


def backward_kernel(
    slot_ref,
    qkv_ref,
    o_ref,
    do_ref,
    lse_ref,
    pad_ref,
    inner_ref,
    outer_ref,
    dqkv_ref,
    qs,
    gs,
    kt,
    dk,
    dv,
):
    step_at = pl.program_id(0)
    tiles = pl.num_programs(0)
    index = tiles - 1 - step_at
    block = qkv_ref.shape[0] // slot_ref.shape[0]
    tile = 2 * block
    width = GROUP * tile
    first_key, first_value = GROUP * LANES, (GROUP + 1) * LANES

    @pl.when(step_at == 0)
    def _():
        kt[...] = qkv_ref[:, first_key:first_value].T
        dk[...] = jnp.zeros_like(dk)
        dv[...] = jnp.zeros_like(dv)

    here = pl.ds(pl.multiple_of(index * tile, tile), tile)
    sources = [
        pl.ds(pl.multiple_of(slot_ref[index * 2 + part] * block, block), block) for part in (0, 1)
    ]
    o = jnp.concatenate([o_ref[source, :] for source in sources], axis=0)
    grads = jnp.concatenate([do_ref[source, :] for source in sources], axis=0)
    products = (grads.astype(jnp.float32) * o.astype(jnp.float32)).T
    grads = contract(grads, pad_ref[: GROUP * HEAD_SIZE, : GROUP * LANES], 1, 0).astype(jnp.bfloat16)
    deltas = []
    for head in range(GROUP):
        lanes = slice(head * LANES, (head + 1) * LANES)
        at = slice(head * tile, (head + 1) * tile)
        qs[at, :] = qkv_ref[here, lanes]
        gs[at, :] = grads[:, lanes]
        features = slice(head * HEAD_SIZE, (head + 1) * HEAD_SIZE)
        deltas.append(jnp.sum(products[features, :], axis=0, keepdims=True))
    delta = jnp.concatenate(deltas, axis=1)
    lse = lse_ref[pl.ds(index, 1), :]
    key_at = lax.broadcasted_iota(jnp.int32, (tile, width), 0)
    query_at = lax.rem(lax.broadcasted_iota(jnp.int32, (tile, width), 1), tile)
    diagonal = key_at <= query_at

    def pieces(steps, masked=False):
        queries, grads = qs[...], gs[...]
        places = [pl.ds(pl.multiple_of(step * tile, tile), tile) for step in steps]
        scores = [contract(qkv_ref[at, first_key:first_value], queries, 1, 1) for at in places]
        grad_probs = [contract(qkv_ref[at, first_value:], grads, 1, 1) for at in places]
        total = None
        for at, score, grad_prob in zip(places, scores, grad_probs):
            probs = jnp.exp2(score * binary_scale - lse)
            if masked:
                probs = jnp.where(diagonal, probs, 0.0)
            dv[at, :] += contract(probs.astype(jnp.bfloat16), grads, 1, 0)
            grad_scores = (probs * (grad_prob - delta)).astype(jnp.bfloat16)
            dk[at, :] += contract(grad_scores, queries, 1, 0)
            part = contract(kt[:, at], grad_scores, 1, 0)
            total = part if total is None else total + part
        return total

    dq = pieces((index,), True)
    dq = lax.fori_loop(
        0, lax.div(index, 2), lambda pair, total: total + pieces((2 * pair, 2 * pair + 1)), dq
    )
    dq = lax.fori_loop(0, lax.rem(index, 2), lambda _, total: total + pieces((index - 1,)), dq)
    dq = dq.T * score_scale
    cosine, sine = tables(inner_ref, outer_ref, index, 2)
    parts = [turn(dq[head * tile : (head + 1) * tile, :], cosine, -sine) for head in range(GROUP)]
    parts.append(turn(dk[here, :] * score_scale, cosine, -sine))
    parts.append(dv[here, :])
    dqkv = jnp.concatenate([part.astype(jnp.bfloat16) for part in parts], axis=1)
    for part in (0, 1):
        dqkv_ref[sources[part], :] = dqkv[part * block : (part + 1) * block, :]


def attend_back(slots, qkv, o, do, lse, pad, inner, outer):
    rows, columns = qkv.shape
    block = rows // slots.shape[0]
    tile = 2 * block
    width = GROUP * tile
    tiles = rows // tile
    operands = (qkv, o, do, lse, pad, inner, outer)
    whole = lambda *shape: pl.BlockSpec(shape, lambda i, s: (0,) * len(shape))
    return pl.pallas_call(
        backward_kernel,
        grid_spec=pltpu.PrefetchScalarGridSpec(
            num_scalar_prefetch=1,
            grid=(tiles,),
            in_specs=[whole(*operand.shape) for operand in operands],
            out_specs=whole(rows, columns),
            scratch_shapes=[
                pltpu.VMEM((width, LANES), jnp.bfloat16),
                pltpu.VMEM((width, LANES), jnp.bfloat16),
                pltpu.VMEM((LANES, rows), jnp.bfloat16),
                pltpu.VMEM((rows, LANES), jnp.float32),
                pltpu.VMEM((rows, LANES), jnp.float32),
            ],
        ),
        out_shape=jax.ShapeDtypeStruct((rows, columns), jnp.bfloat16),
        compiler_params=pltpu.CompilerParams(vmem_limit_bytes=40 << 20),
        cost_estimate=pl.CostEstimate(
            flops=10 * GROUP * rows * rows * LANES // 2,
            bytes_accessed=8 * rows * columns,
            transcendentals=GROUP * rows * rows // 2,
        ),
        name="attend_back",
    )(slots, *operands)


MESH_IDS = pl.DeviceIdType.MESH


def start_barrier(me, line_index=None, line=1):
    barrier = pltpu.get_barrier_semaphore()
    peers = [{"ctx": me ^ bit} for bit in range(1, 8)]
    peers += [{"fsdp": lax.rem(line_index + step, line)} for step in range(1, line)]
    for peer in peers:
        pl.semaphore_signal(barrier, inc=1, device_id=peer, device_id_type=MESH_IDS)
    pl.semaphore_wait(barrier, len(peers))


class Copies:
    def __init__(self, send_sems, recv_sems, base=0):
        self.send_sems, self.recv_sems, self.next, self.sent = send_sems, recv_sems, base, []

    def number(self):
        self.next += 1
        return self.next - 1

    def make(self, number, source, target, peer, landing=None):
        return pltpu.make_async_remote_copy(
            src_ref=source,
            dst_ref=target,
            send_sem=self.send_sems.at[number],
            recv_sem=self.recv_sems.at[number if landing is None else landing],
            device_id=peer,
            device_id_type=MESH_IDS,
        )

    def send(self, number, source, target, peer):
        copy = self.make(number, source, target, peer)
        copy.start()
        self.sent.append(copy)

    def arrived(self, number, target):
        self.make(number, target, target, {"ctx": 0}).wait_recv()

    def finish(self):
        for copy in self.sent:
            copy.wait_send()


GATHER_COPIES = 14


class PlaneGather:
    def __init__(self, copies, me, own_half, part):
        self.copies, self.me, self.own_half, self.part = copies, me, own_half, part
        self.first = copies.next
        copies.next += GATHER_COPIES

    def copy(self, number):
        bit, half, receiver = (
            (0, 1, 2),
            (0, 0, 4),
            (0, 0, 2),
            (0, 1, 4),
            (0, 0, 1),
            (0, 1, 1),
            (2, 1, 4),
            (4, 0, 2),
            (2, 1, 1),
            (4, 0, 1),
            (2, 0, 1),
            (4, 1, 1),
            (6, 1, 1),
            (6, 0, 1),
        )[number]
        place = self.part(self.me ^ bit, half)
        source = self.own_half(half) if bit == 0 else place
        return self.copies.make(self.first + number, source, place, {"ctx": self.me ^ receiver})

    def send(self, *numbers):
        for number in numbers:
            self.copy(number).start()

    def hear(self, number, bit, half):
        self.copies.arrived(self.first + number, self.part(self.me ^ bit, half))

    def begin(self):
        self.send(0, 1, 2, 3, 4, 5)

    def first_hop(self):
        self.hear(0, 2, 1)
        self.send(6, 8)
        self.hear(1, 4, 0)
        self.send(7, 9)

    def second_hop(self):
        self.hear(2, 2, 0)
        self.send(10)
        self.hear(3, 4, 1)
        self.send(11)

    def third_hop(self):
        self.hear(6, 6, 1)
        self.send(12)
        self.hear(7, 6, 0)
        self.send(13)

    def shared(self, bit):
        for number, half in {1: (4, 0), 3: (8, 1), 5: (9, 0), 7: (12, 1)}[bit], {
            1: (5, 1),
            3: (10, 0),
            5: (11, 1),
            7: (13, 0),
        }[bit]:
            self.hear(number, bit, half)

    def last(self):
        for bit in (1, 3, 5, 7):
            self.shared(bit)

    def finish(self):
        for number in range(GATHER_COPIES):
            self.copy(number).wait_send()


def row_half(ref, rows):
    half = rows // 2

    def own(side):
        return ref.at[pl.ds(side * half, half), :]

    return own


def row_part(ref, rows):
    half = rows // 2

    def part(slot, side):
        if isinstance(side, slice):
            return ref.at[pl.ds(pl.multiple_of(slot * rows, rows), rows), :]
        return ref.at[pl.ds(pl.multiple_of(slot * rows + side * half, half), half), :]

    return part


class LineGather:
    def __init__(self, copies, index, line, own, place):
        self.copies, self.index, self.line = copies, index, line
        self.own, self.place = own, place
        self.first = copies.next
        copies.next += 2 * (line - 1)

    def move(self, step, upward, act):
        index, line = self.index, self.line
        if upward:
            slot, there = index - step, index + 1
            leaves = (slot >= 0) & (there < line)
        else:
            slot, there = index + step, index - 1
            leaves = (slot < line) & (there >= 0)
        number = self.first + step + (0 if upward else line - 1)

        @pl.when(leaves)
        def _():
            place = self.place(jnp.clip(slot, 0, line - 1))
            source = self.own if step == 0 else place
            act(self.copies.make(number, source, place, {"fsdp": jnp.clip(there, 0, line - 1)}))

    def hear(self, step, upward):
        index, line = self.index, self.line
        slot = index - 1 - step if upward else index + 1 + step
        comes = (slot >= 0) & (slot < line)
        number = self.first + step + (0 if upward else line - 1)

        @pl.when(comes)
        def _():
            place = self.place(jnp.clip(slot, 0, line - 1))
            self.copies.make(number, place, place, {"fsdp": 0}).wait_recv()

    def begin(self):
        for upward in (True, False):
            self.move(0, upward, lambda copy: copy.start())

    def hop(self, step):
        for upward in (True, False):
            self.hear(step - 1, upward)
            if step < self.line - 1:
                self.move(step, upward, lambda copy: copy.start())

    def finish(self):
        for step in range(self.line - 1):
            for upward in (True, False):
                self.move(step, upward, lambda copy: copy.wait_send())


def in_hbm(count):
    return [pl.BlockSpec(memory_space=pltpu.HBM)] * count


def anywhere(count):
    return [pl.BlockSpec(memory_space=pl.ANY)] * count


def local_copies(pairs, sems):
    copies = [
        pltpu.make_async_copy(source, target, sems.at[number])
        for number, (source, target) in enumerate(pairs)
    ]
    for copy in copies:
        copy.start()
    return copies


def remote_params(number, mebibytes=62):
    return pltpu.CompilerParams(
        collective_id=number, has_side_effects=True, vmem_limit_bytes=mebibytes << 20
    )


def first_kernel(
    line,
    x_ref,
    qkv_ref,
    wo_ref,
    gain_ref,
    gate_ref,
    up_ref,
    down_ref,
    xo_ref,
    qkvo_ref,
    woo_ref,
    gaino_ref,
    feedo_ref,
    feed,
    own,
    send,
    recv,
    here,
):
    me, index = lax.axis_index("ctx"), lax.axis_index("fsdp")
    plane = lax.axis_size("ctx")
    rows = x_ref.shape[0]
    part = row_part(xo_ref, rows)
    wo_rows = woo_ref.shape[1]
    wo_own = wo_ref.at[pl.ds(pl.multiple_of(me * wo_rows, wo_rows), wo_rows), :]
    local = local_copies(
        [
            (qkv_ref, qkvo_ref.at[index]),
            (wo_own, woo_ref.at[index]),
            (gain_ref, gaino_ref.at[index]),
            (x_ref, own),
        ],
        here.at[pl.ds(0, 4)],
    )
    start_barrier(me, index, line)
    copies = Copies(send, recv)
    gather = PlaneGather(copies, me, row_half(own, rows), part)
    lines = [
        LineGather(copies, index, line, own, lambda slot, ref=ref: ref.at[slot])
        for own, ref in ((qkv_ref, qkvo_ref), (gain_ref, gaino_ref), (wo_own, woo_ref))
    ]
    local.pop().wait()
    gather.begin()
    local += local_copies([(own, part(me, slice(None)))], here.at[pl.ds(3, 1)])
    for each in lines:
        each.begin()
    width = feed.shape[1] // 3
    unit = width // line
    pairs = []
    for side, ref in enumerate((gate_ref, up_ref)):
        for z in range(line):
            source = pl.ds(pl.multiple_of((z * plane + me) * unit, unit), unit)
            target = pl.ds(side * width + z * unit, unit)
            pairs.append((ref.at[:, source], feed.at[:, target]))
    for number in range(feed.shape[0] // unit):
        pairs.append(
            (
                down_ref.at[
                    pl.ds(pl.multiple_of(me * unit, unit), unit), pl.ds(number * width, width)
                ],
                feed.at[pl.ds(number * unit, unit), pl.ds(2 * width, width)],
            )
        )
    packed = local_copies(pairs, here.at[pl.ds(4, len(pairs))])
    gather.first_hop()
    for step in range(1, line):
        for each in lines:
            each.hop(step)
        if step == 1:
            gather.second_hop()
            for copy in packed:
                copy.wait()
            packed = local_copies([(feed, feedo_ref)], here.at[pl.ds(4 + len(pairs), 1)])
    gather.third_hop()
    gather.last()
    gather.finish()
    for each in lines:
        each.finish()
    for copy in local:
        copy.wait()
    packed[0].wait()


def first_exchange(line, x, qkv, wo, gains, gate, up, down):
    plane = lax.axis_size("ctx")
    count = GATHER_COPIES + 6 * (line - 1)
    model = x.shape[1]
    shard = model // line
    width = gate.shape[1] // plane
    own_rows = wo.shape[0] // plane
    feed = (shard, 3 * width)
    packing = 2 * line + shard * line // width + 1
    return pl.pallas_call(
        functools.partial(first_kernel, line),
        out_shape=(
            jax.ShapeDtypeStruct((plane * x.shape[0], model), x.dtype),
            jax.ShapeDtypeStruct((line, *qkv.shape), qkv.dtype),
            jax.ShapeDtypeStruct((line, own_rows, model), wo.dtype),
            jax.ShapeDtypeStruct((line, *gains.shape), gains.dtype),
            jax.ShapeDtypeStruct(feed, gate.dtype),
        ),
        in_specs=in_hbm(1) + anywhere(1) + in_hbm(1) + anywhere(1) + in_hbm(3),
        out_specs=tuple(anywhere(5)),
        scratch_shapes=[
            pltpu.VMEM(feed, gate.dtype),
            pltpu.VMEM(x.shape, x.dtype),
            pltpu.SemaphoreType.DMA((count,)),
            pltpu.SemaphoreType.DMA((count,)),
            pltpu.SemaphoreType.DMA((4 + packing,)),
        ],
        compiler_params=remote_params(1),
        name="first_exchange",
    )(x, qkv, wo, gains, gate, up, down)


def deal_rows(copies, me, pieces, wo_ref, place, recv_first, here):
    to_first = pieces * lax.rem(me, 2)
    line_slot = lax.div(me, 2)

    def copy(piece):
        return copies.make(
            recv_first + piece,
            wo_ref.at[piece],
            place(line_slot),
            {"ctx": to_first + piece},
            recv_first + line_slot,
        )

    for piece in range(pieces):

        @pl.when(to_first + piece != me)
        def _(piece=piece):
            copy(piece).start()

        @pl.when(to_first + piece == me)
        def _(piece=piece):
            pltpu.make_async_copy(wo_ref.at[piece], place(line_slot), here).start()

    def finish(line):
        for slot in range(line):

            @pl.when(2 * slot + lax.div(me, pieces) != me)
            def _(slot=slot):
                copies.make(
                    recv_first, wo_ref.at[0], place(slot), {"ctx": 0}, recv_first + slot
                ).wait_recv()

        for piece in range(pieces):

            @pl.when(to_first + piece != me)
            def _(piece=piece):
                copy(piece).wait_send()

            @pl.when(to_first + piece == me)
            def _(piece=piece):
                pltpu.make_async_copy(wo_ref.at[piece], place(line_slot), here).wait()

    return finish


class NearShares:
    def __init__(self, copies, me, refs, place):
        self.copies, self.me, self.refs, self.place = copies, me, refs, place
        self.first = copies.next
        copies.next += 7

    def copy(self, number):
        me, (own, near_x, near_y) = self.me, self.refs
        half = own.shape[0] // 2
        partner = {"ctx": me ^ 1}
        source, target, peer = (
            lambda: (near_y.at[pl.ds(0, half)], self.place(me ^ 4, 0), {"ctx": me ^ 2}),
            lambda: (near_x.at[pl.ds(half, half)], self.place(me ^ 2, 1), {"ctx": me ^ 4}),
            lambda: (own, self.place(me, None), partner),
            lambda: (near_x, self.place(me ^ 2, None), partner),
            lambda: (near_y, self.place(me ^ 4, None), partner),
            lambda: (self.place(me ^ 6, 0), self.place(me ^ 6, 0), partner),
            lambda: (self.place(me ^ 6, 1), self.place(me ^ 6, 1), partner),
        )[number]()
        return self.copies.make(self.first + number, source, target, peer)

    def begin(self):
        for number in range(5):
            self.copy(number).start()

    def diagonal(self):
        for side in (0, 1):
            self.copies.arrived(self.first + side, self.place(self.me ^ 6, side))
            self.copy(5 + side).start()

    def shared(self, bit):
        if bit == 7:
            for side in (0, 1):
                self.copies.arrived(self.first + 5 + side, self.place(self.me ^ 7, side))
        else:
            self.copies.arrived(self.first + 2 + bit // 2, self.place(self.me ^ bit, None))

    def finish(self):
        for number in range(7):
            self.copy(number).wait_send()


def block_place(ref, rows):
    half = rows // 2

    def place(slot, side):
        if side is None:
            return ref.at[pl.ds(pl.multiple_of(slot * rows, rows), rows), :]
        return ref.at[pl.ds(pl.multiple_of(slot * rows + side * half, half), half), :]

    return place


def second_kernel(
    o_ref,
    wo0_hbm,
    wo2_hbm,
    wo4_hbm,
    dy2_hbm,
    dy4_hbm,
    x_hbm,
    gain_ref,
    own_hbm,
    dy6_hbm,
    residual_hbm,
    normed_hbm,
    scale_ref,
    gained_hbm,
    near_x_hbm,
    near_y_hbm,
    x_ref,
    residual_ref,
    normed_ref,
    gained_ref,
    att,
    wo,
    send,
    recv,
    here,
):
    me = lax.axis_index("ctx")
    rows = x_ref.shape[0]
    half = rows // 2
    middle = wo.shape[0] // 2

    def wo_place(slot, side):
        return wo.at[:, slot] if side is None else wo.at[pl.ds(side * middle, middle), slot]

    own_wo = (wo0_hbm, wo2_hbm, wo4_hbm)
    local = local_copies(
        [
            (o_ref.at[pl.ds(pl.multiple_of(me * rows, rows), rows), :], att.at[me]),
            (x_hbm, x_ref),
        ]
        + [(ref, wo_place(me ^ (2 * number), None)) for number, ref in enumerate(own_wo)],
        here.at[pl.ds(0, 5)],
    )
    start_barrier(me)
    copies = Copies(send, recv)

    def block(slot):
        return o_ref.at[pl.ds(pl.multiple_of(slot * rows, rows), rows), :]

    numbers = {}
    for bit in (6, 7, 4, 5, 2, 3, 1):
        numbers[bit] = copies.number()
        copies.send(numbers[bit], block(me ^ bit), att.at[me], {"ctx": me ^ bit})
    shares = NearShares(copies, me, own_wo, wo_place)
    shares.begin()
    dy_first = copies.next
    copies.next += 2
    upper, lower = pl.ds(0, half), pl.ds(half, half)
    copies.send(dy_first, dy4_hbm.at[upper, :], dy6_hbm.at[upper, :], {"ctx": me ^ 2})
    copies.send(dy_first + 1, dy2_hbm.at[lower, :], dy6_hbm.at[lower, :], {"ctx": me ^ 4})
    shares.diagonal()
    for bit in (1, 3, 5, 7):
        shares.shared(bit)
    for bit, number in numbers.items():
        copies.arrived(number, att.at[me ^ bit])
    for copy in local:
        copy.wait()
    per_head = 2 * GROUP
    own = wo.at[lax.div(me, 2), pl.ds(per_head * lax.rem(me, 2), per_head)]
    keep = local_copies([(own, own_hbm)], here.at[pl.ds(5, 1)])
    plane = att.shape[0]
    near = copies.next
    for side in (0, 1):
        at = pl.ds(side * half, half)
        total = x_ref[at, :].astype(jnp.float32)
        for slot in range(plane):
            first = per_head * (slot % 2)
            weight = jnp.concatenate(
                [wo[slot // 2, first + piece] for piece in range(per_head)], axis=0
            )
            total = total + contract(att[slot, at, :], weight, 1, 0)
        residual_ref[at, :] = total
        scale = lax.rsqrt(jnp.mean(total * total, axis=-1, keepdims=True) + norm_epsilon)
        normed = total * scale
        scale_ref[at, :] = scale
        normed_ref[at, :] = normed
        gained_ref[at, :] = (normed * gain_ref[...]).astype(jnp.bfloat16)
        for number, target, bit in ((0, near_x_hbm, 2), (1, near_y_hbm, 4)):
            copies.send(
                near + 2 * side + number,
                gained_ref.at[at, :],
                target.at[at, :],
                {"ctx": me ^ bit},
            )
    keep += local_copies(
        [(residual_ref, residual_hbm), (normed_ref, normed_hbm), (gained_ref, gained_hbm)],
        here.at[pl.ds(6, 3)],
    )
    for copy in keep:
        copy.wait()
    shares.finish()
    copies.arrived(dy_first, dy6_hbm.at[upper, :])
    copies.arrived(dy_first + 1, dy6_hbm.at[lower, :])
    for side in (0, 1):
        at = pl.ds(side * half, half)
        copies.arrived(near + 2 * side, near_x_hbm.at[at, :])
        copies.arrived(near + 2 * side + 1, near_y_hbm.at[at, :])
    copies.finish()


def second_exchange(o, own_wo, grads, x, gain):
    plane = lax.axis_size("ctx")
    rows = x.shape[0]
    line, part, model = own_wo[0].shape
    count = 7 + 7 + 2 + 4
    f32 = jnp.float32
    return pl.pallas_call(
        second_kernel,
        out_shape=(
            jax.ShapeDtypeStruct((2 * GROUP, part, model), own_wo[0].dtype),
            jax.ShapeDtypeStruct((rows, model), x.dtype),
            jax.ShapeDtypeStruct((rows, model), f32),
            jax.ShapeDtypeStruct((rows, model), f32),
            jax.ShapeDtypeStruct((rows, 1), f32),
            *[jax.ShapeDtypeStruct((rows, model), x.dtype)] * 3,
        ),
        in_specs=in_hbm(7) + in_vmem(1),
        out_specs=(*anywhere(4), *in_vmem(1), *anywhere(3)),
        scratch_shapes=[
            pltpu.VMEM(x.shape, x.dtype),
            pltpu.VMEM(x.shape, f32),
            pltpu.VMEM(x.shape, f32),
            pltpu.VMEM(x.shape, x.dtype),
            pltpu.VMEM((plane, rows, o.shape[1]), o.dtype),
            pltpu.VMEM((line, plane, part, model), x.dtype),
            pltpu.SemaphoreType.DMA((count,)),
            pltpu.SemaphoreType.DMA((count,)),
            pltpu.SemaphoreType.DMA((9,)),
        ],
        compiler_params=remote_params(2),
        name="second_exchange",
    )(o, *own_wo, *grads, x, gain)


def gather_kernel(x_ref, xo_ref, own, send, recv, here):
    me = lax.axis_index("ctx")
    rows = x_ref.shape[0]
    fetch = local_copies([(x_ref, own)], here)
    start_barrier(me)
    fetch[0].wait()
    part = row_part(xo_ref, rows)
    copies = Copies(send, recv)
    gather = PlaneGather(copies, me, row_half(own, rows), part)
    gather.begin()
    local = local_copies([(own, part(me, slice(None)))], here)
    gather.first_hop()
    gather.second_hop()
    gather.third_hop()
    gather.last()
    gather.finish()
    local[0].wait()


def plane_gather(x, number):
    plane = lax.axis_size("ctx")
    return pl.pallas_call(
        gather_kernel,
        out_shape=jax.ShapeDtypeStruct((plane * x.shape[0], x.shape[1]), x.dtype),
        in_specs=in_hbm(1),
        out_specs=anywhere(1)[0],
        scratch_shapes=[
            pltpu.VMEM(x.shape, x.dtype),
            pltpu.SemaphoreType.DMA((GATHER_COPIES,)),
            pltpu.SemaphoreType.DMA((GATHER_COPIES,)),
            pltpu.SemaphoreType.DMA((1,)),
        ],
        compiler_params=remote_params(number, 24),
    )(x)


def third_kernel(
    g0_hbm, g2_hbm, g4_hbm, ot_hbm, wo_hbm, do_ref, dwo_ref, ot_ref, wo_ref, all_grads, dwo, send, recv, here
):
    me = lax.axis_index("ctx")
    rows = g0_hbm.shape[0]
    place = block_place(all_grads, rows)
    own_rows = (g0_hbm, g2_hbm, g4_hbm)
    fetch = local_copies(
        [(ref, place(me ^ (2 * number), None)) for number, ref in enumerate(own_rows)]
        + [(ot_hbm, ot_ref), (wo_hbm, wo_ref)],
        here,
    )
    start_barrier(me)
    copies = Copies(send, recv)
    shares = NearShares(copies, me, own_rows, place)
    shares.begin()
    dwo[...] = jnp.zeros_like(dwo)
    for copy in fetch:
        copy.wait()

    def step(order, carry):
        @pl.when(order == 5)
        def _():
            shares.diagonal()

        for bit in (1, 3, 5, 7):

            @pl.when(order == bit)
            def _(bit=bit):
                shares.shared(bit)

        here_rows = pl.ds(pl.multiple_of((me ^ order) * rows, rows), rows)
        grads = all_grads[here_rows, :]
        do_ref[here_rows, :] = contract(grads, wo_ref[...], 1, 1).astype(jnp.bfloat16)
        dwo[...] += contract(ot_ref[:, here_rows], grads, 1, 0)
        return carry

    lax.fori_loop(0, 8, step, 0)
    line, _, across = dwo_ref.shape
    for slot in range(line):
        rows_at = slice(slot * HALF, (slot + 1) * HALF)
        for number in range(dwo.shape[1] // across):
            columns = slice(number * across, (number + 1) * across)
            dwo_ref[slot, number * HALF : (number + 1) * HALF, :] = dwo[rows_at, columns].astype(
                jnp.bfloat16
            )
    shares.finish()


def third_exchange(line, own_rows, ot, wo, across):
    plane = lax.axis_size("ctx")
    rows, model = own_rows[0].shape
    half_type, f32 = jnp.bfloat16, jnp.float32
    return pl.pallas_call(
        third_kernel,
        out_shape=(
            jax.ShapeDtypeStruct((plane * rows, wo.shape[0]), half_type),
            jax.ShapeDtypeStruct((line, HALF * model // across, across), half_type),
        ),
        in_specs=anywhere(5),
        out_specs=tuple(in_vmem(2)),
        scratch_shapes=[
            pltpu.VMEM(ot.shape, ot.dtype),
            pltpu.VMEM(wo.shape, wo.dtype),
            pltpu.VMEM((plane * rows, model), half_type),
            pltpu.VMEM((line * HALF, model), f32),
            pltpu.SemaphoreType.DMA((7,)),
            pltpu.SemaphoreType.DMA((7,)),
            pltpu.SemaphoreType.DMA((5,)),
        ],
        compiler_params=remote_params(6),
        name="third_exchange",
    )(*own_rows, ot, wo)


REDUCE_COPIES = 10


class PlaneReduce:
    def __init__(self, copies, me, block, heard, held, landed):
        self.copies, self.me, self.block = copies, me, block
        self.heard, self.held, self.landed = heard, held, landed
        self.first = copies.next
        copies.next += REDUCE_COPIES
        self.half = heard.shape[1] // 2
        self.x, self.y = {"ctx": me ^ 2}, {"ctx": me ^ 4}

    def side(self, ref, slot, half):
        return ref.at[slot, pl.ds(half * self.half, self.half), :]

    def share(self, order):
        self.shared(order).start()

    def shared(self, order):
        partner = self.me ^ 1
        source = self.block(partner ^ (6, 2, 4, 0)[order])
        return self.copies.make(
            self.first + order, source, self.heard.at[order], {"ctx": partner}
        )

    def combine(self, order, rows, extra=None):
        bit = (6, 2, 4)[order]
        total = self.block(self.me ^ bit)[rows, :].astype(jnp.float32) + self.heard[
            order, rows, :
        ].astype(jnp.float32)
        if extra is not None:
            total = total + extra
        self.held[order, rows, :] = total.astype(self.held.dtype)

    def onward(self, number):
        order, half, peer = {
            4: (0, 0, self.x),
            5: (0, 1, self.y),
            6: (1, 0, self.x),
            7: (2, 1, self.y),
            8: (1, 1, self.x),
            9: (2, 0, self.y),
        }[number]
        held, landed = self.side(self.held, order, half), self.side(self.landed, order, half)
        return self.copies.make(self.first + number, held, landed, peer)

    def finish(self):
        for order in range(4):
            self.shared(order).wait_send()
        for number in range(4, REDUCE_COPIES):
            self.onward(number).wait_send()

    def diagonal_sends(self):
        first, half = self.first, self.half
        self.copies.arrived(first + 0, self.heard.at[0])
        self.combine(0, pl.ds(0, 2 * half))
        self.onward(4).start()
        self.onward(5).start()

    def neighbour_send(self, order):
        first, half = self.first, self.half
        self.copies.arrived(first + order, self.heard.at[order])
        self.combine(order, pl.ds((order - 1) * half, half))
        self.onward(5 + order).start()

    def neighbour_sends(self):
        self.neighbour_send(1)
        self.neighbour_send(2)

    def second_sends(self):
        first, half = self.first, self.half
        upper, lower = pl.ds(0, half), pl.ds(half, half)
        landed, side, arrived = self.landed, self.side, self.copies.arrived
        arrived(first + 5, side(landed, 0, 1))
        self.combine(1, lower, landed[0, lower, :].astype(jnp.float32))
        self.onward(8).start()
        arrived(first + 4, side(landed, 0, 0))
        self.combine(2, upper, landed[0, upper, :].astype(jnp.float32))
        self.onward(9).start()

    def own_share(self):
        self.copies.arrived(self.first + 3, self.heard.at[3])

    def sum_half(self, which):
        first, half = self.first, self.half
        rows = pl.ds(which * half, half)
        self.copies.arrived(first + (6, 8)[which], self.side(self.landed, 1, which))
        self.copies.arrived(first + (9, 7)[which], self.side(self.landed, 2, which))
        return (
            self.block(self.me)[rows, :].astype(jnp.float32)
            + self.heard[3, rows, :].astype(jnp.float32)
            + self.landed[1, rows, :].astype(jnp.float32)
            + self.landed[2, rows, :].astype(jnp.float32)
        )


def feed_kernel(
    line,
    g0_hbm,
    g2_hbm,
    g4_hbm,
    dy0_hbm,
    dy2_hbm,
    dy4_hbm,
    dy6_hbm,
    w_hbm,
    ot_hbm,
    normed_hbm,
    scale_ref,
    gain_ref,
    residual_ref,
    term_ref,
    own_ref,
    near_x_ref,
    near_y_ref,
    dealt_hbm,
    out6_hbm,
    out2_hbm,
    out4_hbm,
    out0_hbm,
    dw_hbm,
    normed_ref,
    w_ref,
    dw_ref,
    down_ref,
    dy_ref,
    all_g,
    hid,
    hid_t,
    gate_t,
    up_t,
    part,
    heard,
    held,
    landed,
    out_mine,
    out_heard,
    send,
    recv,
    here,
):
    me = lax.axis_index("ctx")
    rows = residual_ref.shape[0]
    half = rows // 2
    width, model = down_ref.shape
    blocks = model // width
    unit = width // line
    partner = {"ctx": me ^ 1}

    def at(slot):
        return pl.ds(pl.multiple_of(slot * rows, rows), rows)

    own_grads = (dy0_hbm, dy2_hbm, dy4_hbm, dy6_hbm)
    own_rows = (g0_hbm, g2_hbm, g4_hbm)
    place = block_place(all_g, rows)
    dy_place = block_place(dy_ref, rows)
    local = local_copies(
        [(w_hbm, w_ref)]
        + [(ref, place(me ^ (2 * number), None)) for number, ref in enumerate(own_rows)]
        + [(ref, dy_place(me ^ (2 * number), None)) for number, ref in enumerate(own_grads)]
        + [(normed_hbm, normed_ref)],
        here.at[pl.ds(0, 9)],
    )
    start_barrier(me)
    copies = Copies(send, recv)
    shares = NearShares(copies, me, own_rows, place)
    shares.begin()
    dy_first = copies.next
    copies.next += 4
    for number, ref in enumerate(own_grads):
        copies.send(dy_first + number, ref, dy_place(me ^ (2 * number), None), partner)
    deal_first = copies.next
    copies.next += ot_hbm.shape[0]
    dealt = deal_rows(
        copies,
        me,
        ot_hbm.shape[0],
        ot_hbm,
        lambda slot: dealt_hbm.at[slot],
        deal_first,
        here.at[9],
    )
    local[0].wait()
    gate_ref, up_ref = w_ref.at[:, :width], w_ref.at[:, width : 2 * width]
    for z in range(line):
        for number in range(blocks):
            source = pl.ds((z * blocks + number) * unit, unit)
            down_ref[pl.ds(z * unit, unit), number * width : (number + 1) * width] = w_ref[
                source, 2 * width :
            ]
    for copy in local[1:]:
        copy.wait()
    gain = gain_ref[...]

    def block(slot):
        return part.at[at(slot), :]

    reduce = PlaneReduce(copies, me, block, heard, held, landed)

    def chunk(order):
        place = at(me ^ order)
        g = all_g[place, :]
        dy = dy_ref[place, :]
        gate_values = contract(g, gate_ref[...], 1, 0)
        up_values = contract(g, up_ref[...], 1, 0)
        sigmoid_gate = 1.0 / (1.0 + jnp.exp(-gate_values))
        activated = gate_values * sigmoid_gate
        hidden_act = (activated * up_values).astype(jnp.bfloat16)
        hid[place, :] = hidden_act
        hid_t[:, place] = hidden_act.T
        grad_hidden = contract(dy, down_ref[...], 1, 1)
        grad_gate = (
            grad_hidden * up_values * sigmoid_gate * (1.0 + gate_values * (1.0 - sigmoid_gate))
        ).astype(jnp.bfloat16)
        grad_up = (grad_hidden * activated).astype(jnp.bfloat16)
        gate_t[:, place] = grad_gate.T
        up_t[:, place] = grad_up.T
        part[place, :] = (
            contract(grad_gate, gate_ref[...], 1, 1) + contract(grad_up, up_ref[...], 1, 1)
        ).astype(jnp.bfloat16)

    def step(number, carry):
        @pl.when(number == 1)
        def _():
            shares.shared(3)
            copies.arrived(dy_first + 1, dy_place(me ^ 3, None))

        @pl.when(number == 2)
        def _():
            reduce.share(1)
            shares.diagonal()

        @pl.when(number == 3)
        def _():
            reduce.neighbour_send(1)
            shares.shared(7)
            copies.arrived(dy_first + 3, dy_place(me ^ 7, None))

        @pl.when(number == 4)
        def _():
            reduce.share(0)
            reduce.diagonal_sends()

        @pl.when(number == 5)
        def _():
            shares.shared(5)
            copies.arrived(dy_first + 2, dy_place(me ^ 5, None))

        @pl.when(number == 6)
        def _():
            reduce.share(2)
            reduce.neighbour_send(2)

        @pl.when(number == 7)
        def _():
            reduce.second_sends()
            shares.shared(1)
            copies.arrived(dy_first, dy_place(me ^ 1, None))

        pair = lax.div(number, 2)
        chunk(
            lax.rem(number, 2)
            + jnp.where(pair == 0, 2, jnp.where(pair == 1, 6, jnp.where(pair == 2, 4, 0)))
        )
        return carry

    lax.fori_loop(0, 8, step, 0)
    reduce.share(3)
    out_first = copies.next
    copies.next += 4

    def bit_of(number):
        return jnp.where(number == 0, 6, jnp.where(number == 3, 0, 2 * number))

    def out_copy(number):
        return copies.make(out_first + number, out_mine.at[number], out_heard.at[number], partner)

    def out_of(slot):
        return contract(hid[at(slot), :], down_ref[...], 1, 0)

    def give(number, carry):
        out_mine[number] = out_of(me ^ 1 ^ bit_of(number)).astype(jnp.bfloat16)
        out_copy(number).start()
        return carry

    def keep(number, carry):
        total = out_of(me ^ bit_of(number))
        out_copy(number).wait_recv()
        out_heard[number] = (total + out_heard[number].astype(jnp.float32)).astype(jnp.bfloat16)
        return carry

    def weights(number, carry):
        columns = pl.ds(pl.multiple_of(number * width, width), width)
        total = contract(hid_t[...], dy_ref[:, columns], 1, 0).astype(jnp.bfloat16)
        for z in range(line):
            target = pl.ds(pl.multiple_of((z * blocks + number) * unit, unit), unit)
            dw_ref[target, 2 * width :] = total[z * unit : (z + 1) * unit, :]
        for side, left in enumerate((gate_t, up_t)):
            total = contract(left[...], all_g[:, columns], 1, 0).astype(jnp.bfloat16)
            dw_ref[columns, side * width : (side + 1) * width] = total.T
        return carry

    reduce.own_share()
    lax.fori_loop(0, 4, give, 0)
    near = copies.next
    copies.next += 4
    total = jnp.zeros_like(gain)
    for which in (1, 0):
        rows_at = pl.ds(which * half, half)
        grad_normed, normed = reduce.sum_half(which), normed_ref[rows_at, :]
        scaled = grad_normed * gain
        mean = jnp.mean(scaled * normed, axis=-1, keepdims=True)
        total = total + jnp.sum(grad_normed * normed, axis=0, keepdims=True)
        dy = dy_ref[pl.ds(pl.multiple_of(me * rows + which * half, half), half), :]
        residual = dy.astype(jnp.float32) + scale_ref[rows_at, :] * (scaled - normed * mean)
        residual_ref[rows_at, :] = residual
        own_ref[rows_at, :] = residual.astype(jnp.bfloat16)
        for number, target, bit in ((0, near_x_ref, 2), (1, near_y_ref, 4)):
            copies.send(
                near + 2 * which + number,
                own_ref.at[rows_at, :],
                target.at[rows_at, :],
                {"ctx": me ^ bit},
            )
    term_ref[...] = total
    lax.fori_loop(0, 4, keep, 0)
    outputs = local_copies(
        [
            (out_heard.at[number], ref)
            for number, ref in enumerate((out6_hbm, out2_hbm, out4_hbm, out0_hbm))
        ],
        here.at[pl.ds(0, 4)],
    )
    lax.fori_loop(0, blocks, weights, 0)
    outputs += local_copies([(dw_ref, dw_hbm)], here.at[pl.ds(4, 1)])
    for number in range(4):
        out_copy(number).wait_send()
    for copy in outputs:
        copy.wait()
    dealt(dealt_hbm.shape[0])
    shares.finish()
    reduce.finish()
    for which in (1, 0):
        rows_at = pl.ds(which * half, half)
        copies.arrived(near + 2 * which, near_x_ref.at[rows_at, :])
        copies.arrived(near + 2 * which + 1, near_y_ref.at[rows_at, :])
    copies.finish()


def feed(own_rows, grads, w, ot, normed, scale, gain):
    plane, line = lax.axis_size("ctx"), lax.axis_size("fsdp")
    rows, model = own_rows[0].shape
    tokens = plane * rows
    width = w.shape[1] // 3
    pieces = 2 * GROUP
    ot = ot.reshape(pieces, -1, ot.shape[1])
    count = 7 + 4 + pieces + REDUCE_COPIES + 4 + 4
    half_type = jnp.bfloat16
    return pl.pallas_call(
        functools.partial(feed_kernel, line),
        out_shape=(
            jax.ShapeDtypeStruct((rows, model), jnp.float32),
            jax.ShapeDtypeStruct((1, model), jnp.float32),
            *[jax.ShapeDtypeStruct((rows, model), half_type)] * 3,
            jax.ShapeDtypeStruct((line, *ot.shape[1:]), ot.dtype),
            *[jax.ShapeDtypeStruct((rows, model), half_type)] * 4,
            jax.ShapeDtypeStruct(w.shape, half_type),
        ),
        in_specs=anywhere(10) + in_vmem(2),
        out_specs=(*in_vmem(3), *anywhere(8)),
        scratch_shapes=[
            pltpu.VMEM((rows, model), jnp.float32),
            pltpu.VMEM(w.shape, half_type),
            pltpu.VMEM(w.shape, half_type),
            pltpu.VMEM((width, model), half_type),
            pltpu.VMEM((tokens, model), half_type),
            pltpu.VMEM((tokens, model), half_type),
            pltpu.VMEM((tokens, width), half_type),
            pltpu.VMEM((width, tokens), half_type),
            pltpu.VMEM((width, tokens), half_type),
            pltpu.VMEM((width, tokens), half_type),
            pltpu.VMEM((tokens, model), half_type),
            pltpu.VMEM((4, rows, model), half_type),
            pltpu.VMEM((3, rows, model), half_type),
            pltpu.VMEM((3, rows, model), half_type),
            pltpu.VMEM((4, rows, model), half_type),
            pltpu.VMEM((4, rows, model), half_type),
            pltpu.SemaphoreType.DMA((count,)),
            pltpu.SemaphoreType.DMA((count,)),
            pltpu.SemaphoreType.DMA((10,)),
        ],
        compiler_params=pltpu.CompilerParams(
            collective_id=3, has_side_effects=True, vmem_limit_bytes=62 << 20
        ),
        name="feed",
    )(*own_rows, *grads, w, ot, normed, scale, gain)


def input_kernel(
    dqkv_ref,
    wp_hbm,
    x_hbm,
    residual_hbm,
    dwo_hbm,
    gain_ref,
    pad_ref,
    input_ref,
    grads_ref,
    term_ref,
    wp_ref,
    all_x,
    residual_ref,
    dwo_ref,
    part,
    dw,
    heard,
    held,
    landed,
    send,
    recv,
    here,
):
    me = lax.axis_index("ctx")
    rows = residual_ref.shape[0]
    fetch = local_copies(
        [(wp_hbm, wp_ref), (x_hbm, all_x), (residual_hbm, residual_ref), (dwo_hbm, dwo_ref)], here
    )
    start_barrier(me)
    copies = Copies(send, recv)

    def at(slot):
        return pl.ds(pl.multiple_of(slot * rows, rows), rows)

    def compute(slot):
        place = at(slot)
        part[place, :] = contract(dqkv_ref[place, :], wp_ref[...], 1, 1).astype(jnp.bfloat16)

    reduce = PlaneReduce(copies, me, lambda slot: part.at[at(slot), :], heard, held, landed)
    fetch[0].wait()
    compute(me ^ 7)
    reduce.share(0)
    compute(me ^ 6)
    compute(me ^ 3)
    reduce.share(1)
    reduce.diagonal_sends()
    compute(me ^ 2)
    compute(me ^ 5)
    reduce.share(2)
    compute(me ^ 4)
    reduce.neighbour_sends()
    compute(me ^ 1)
    reduce.share(3)
    compute(me)
    gain = gain_ref[...]
    dw[...] = jnp.zeros_like(dw)
    for copy in fetch[1:]:
        copy.wait()

    def weights(slot, carry):
        place = at(slot)
        x = all_x[place, :].astype(jnp.float32)
        normed = x * lax.rsqrt(jnp.mean(x * x, axis=-1, keepdims=True) + norm_epsilon)
        gained = (normed * gain).astype(jnp.bfloat16)
        dw[...] += contract(dqkv_ref[place, :], gained, 0, 0)
        return carry

    plane = part.shape[0] // rows
    lax.fori_loop(0, plane // 2, weights, 0)
    reduce.second_sends()
    reduce.own_share()
    lax.fori_loop(plane // 2, plane, weights, 0)
    packed = contract(pad_ref[...], dw[...].astype(jnp.bfloat16), 1, 0)
    packed = packed.astype(jnp.bfloat16).T
    line = dwo_ref.shape[0]
    shard = packed.shape[0] // line
    for slot in range(line):
        grads_ref[slot, :shard, :] = packed[slot * shard : (slot + 1) * shard, :]
        grads_ref[slot, shard:, :] = dwo_ref[slot]
    half = rows // 2
    total = jnp.zeros_like(gain)
    for which in (1, 0):
        here_rows = pl.ds(which * half, half)
        grad = reduce.sum_half(which)
        own_rows = pl.ds(pl.multiple_of(me * rows + which * half, half), half)
        x = all_x[own_rows, :].astype(jnp.float32)
        scale = lax.rsqrt(jnp.mean(x * x, axis=-1, keepdims=True) + norm_epsilon)
        normed = x * scale
        total = total + jnp.sum(grad * normed, axis=0, keepdims=True)
        scaled = grad * gain
        mean = jnp.mean(scaled * normed, axis=-1, keepdims=True)
        input_ref[0, here_rows, :] = residual_ref[here_rows, :] + scale * (scaled - normed * mean)
    term_ref[...] = total
    reduce.finish()
    copies.finish()


def input_exchange(dqkv, wp, x, residual, dwo, gain, pad):
    rows, model = residual.shape
    line, dealt, across = dwo.shape
    f32 = jnp.float32
    return pl.pallas_call(
        input_kernel,
        out_shape=(
            jax.ShapeDtypeStruct((1, rows, model), f32),
            jax.ShapeDtypeStruct((line, model // line + dealt, across), dwo.dtype),
            jax.ShapeDtypeStruct((1, model), f32),
        ),
        in_specs=in_vmem(1) + in_hbm(4) + in_vmem(2),
        out_specs=tuple(in_vmem(3)),
        scratch_shapes=[
            pltpu.VMEM(wp.shape, wp.dtype),
            pltpu.VMEM(x.shape, x.dtype),
            pltpu.VMEM(residual.shape, residual.dtype),
            pltpu.VMEM(dwo.shape, dwo.dtype),
            pltpu.VMEM(x.shape, x.dtype),
            pltpu.VMEM((dqkv.shape[1], model), f32),
            pltpu.VMEM((4, rows, model), x.dtype),
            pltpu.VMEM((3, rows, model), x.dtype),
            pltpu.VMEM((3, rows, model), x.dtype),
            pltpu.SemaphoreType.DMA((REDUCE_COPIES,)),
            pltpu.SemaphoreType.DMA((REDUCE_COPIES,)),
            pltpu.SemaphoreType.DMA((4,)),
        ],
        compiler_params=remote_params(7),
        name="input_exchange",
    )(dqkv, wp, x, residual, dwo, gain, pad)


def pieces_kernel(
    line,
    piece_ref,
    residual_hbm,
    out0_hbm,
    out2_hbm,
    out4_hbm,
    out6_hbm,
    term_one_ref,
    term_two_ref,
    whole_ref,
    total_ref,
    output_ref,
    own,
    residual_ref,
    outs_ref,
    terms,
    terms_heard,
    plane_sum,
    across,
    send,
    recv,
    here,
):
    me, index = lax.axis_index("ctx"), lax.axis_index("fsdp")
    outs = (out0_hbm, out2_hbm, out4_hbm, out6_hbm)
    fetch = local_copies(
        [(piece_ref, own), (residual_hbm, residual_ref)]
        + [(ref, outs_ref.at[number]) for number, ref in enumerate(outs)],
        here.at[pl.ds(0, 6)],
    )
    start_barrier(me, index, line)
    copies = Copies(send, recv)
    rows = piece_ref.shape[0]
    part = row_part(whole_ref, rows)
    gather = PlaneGather(copies, me, row_half(own, rows), part)
    fetch[0].wait()
    first = copies.next
    copies.next += 7 + line - 1
    terms[0:1, :] = term_one_ref[...]
    terms[1:2, :] = term_two_ref[...]
    gather.begin()
    local = local_copies([(own, part(me, slice(None)))], here.at[pl.ds(6, 1)])
    for bit in range(1, 8):
        copies.send(first + bit - 1, terms, terms_heard.at[bit], {"ctx": me ^ bit})
    for copy in fetch[1:]:
        copy.wait()
    total = residual_ref[...]
    for number in range(4):
        total = total + outs_ref[number].astype(jnp.float32)
    output_ref[0] = total.astype(output_ref.dtype)
    gather.first_hop()
    gather.second_hop()
    total = terms[...]
    for bit in range(1, 8):
        copies.arrived(first + bit - 1, terms_heard.at[bit])
        total = total + terms_heard[bit]
    plane_sum[...] = total
    for step in range(1, line):
        peer = {"fsdp": lax.rem(index + step, line)}
        copies.send(first + 6 + step, plane_sum, across.at[step], peer)
    gather.third_hop()
    for step in range(1, line):
        copies.arrived(first + 6 + step, across.at[step])
        total = total + across[step]
    total_ref[...] = total
    gather.last()
    gather.finish()
    local[0].wait()
    copies.finish()


def pieces_exchange(line, piece, term_one, term_two, residual, outs):
    plane = lax.axis_size("ctx")
    rows, model = residual.shape
    f32 = jnp.float32
    copies = GATHER_COPIES + 7 + line - 1
    return pl.pallas_call(
        functools.partial(pieces_kernel, line),
        out_shape=(
            jax.ShapeDtypeStruct((plane * piece.shape[0], piece.shape[1]), piece.dtype),
            jax.ShapeDtypeStruct((2, model), f32),
            jax.ShapeDtypeStruct((1, rows, model), jnp.bfloat16),
        ),
        in_specs=anywhere(6) + in_vmem(2),
        out_specs=(*anywhere(1), *in_vmem(2)),
        scratch_shapes=[
            pltpu.VMEM(piece.shape, piece.dtype),
            pltpu.VMEM((rows, model), f32),
            pltpu.VMEM((4, rows, model), outs[0].dtype),
            pltpu.VMEM((2, model), f32),
            pltpu.VMEM((plane, 2, model), f32),
            pltpu.VMEM((2, model), f32),
            pltpu.VMEM((line, 2, model), f32),
            pltpu.SemaphoreType.DMA((copies,)),
            pltpu.SemaphoreType.DMA((copies,)),
            pltpu.SemaphoreType.DMA((7,)),
        ],
        compiler_params=remote_params(8, 24),
        name="pieces_exchange",
    )(piece, residual, *outs, term_one, term_two)


def spread_kernel(gate_in, up_in, down_in, gate_ref, up_ref, down_ref):
    plane, shard, unit = gate_in.shape
    for source, target in ((gate_in, gate_ref), (up_in, up_ref)):
        for slot in range(plane):
            target[:, slot * unit : (slot + 1) * unit] = source[slot].astype(jnp.float32)
    width = down_in.shape[2]
    blocks = shard // unit
    for slot in range(down_in.shape[0]):
        for number in range(blocks):
            down_ref[slot * unit : (slot + 1) * unit, number * width : (number + 1) * width] = (
                down_in[slot, number * unit : (number + 1) * unit, :].astype(jnp.float32)
            )


def spread_feed(pieces, shard, line, unit):
    plane = lax.axis_size("ctx")
    width = line * unit
    model = line * shard
    pieces = pieces.reshape(plane, shard, 3 * width)
    each = plane // line
    return pl.pallas_call(
        spread_kernel,
        grid=(line,),
        in_specs=[
            pl.BlockSpec((plane, shard, unit), lambda z: (0, 0, z)),
            pl.BlockSpec((plane, shard, unit), lambda z: (0, 0, line + z)),
            pl.BlockSpec((each, shard, width), lambda z: (z, 0, 2)),
        ],
        out_specs=(
            pl.BlockSpec((shard, plane * unit), lambda z: (0, z)),
            pl.BlockSpec((shard, plane * unit), lambda z: (0, z)),
            pl.BlockSpec((each * unit, model), lambda z: (z, 0)),
        ),
        out_shape=(
            jax.ShapeDtypeStruct((shard, plane * width), jnp.float32),
            jax.ShapeDtypeStruct((shard, plane * width), jnp.float32),
            jax.ShapeDtypeStruct((plane * unit, model), jnp.float32),
        ),
        compiler_params=pltpu.CompilerParams(vmem_limit_bytes=36 << 20),
        name="spread_feed",
    )(pieces, pieces, pieces)


def spread_attention_kernel(in_ref, q_ref, k_ref, v_ref, wo_ref):
    plane, _, across = in_ref.shape
    shard = q_ref.shape[0]
    key_width = k_ref.shape[1] // plane
    query_width = q_ref.shape[1] // plane
    first = 0
    for target, width in ((q_ref, query_width), (k_ref, key_width), (v_ref, key_width)):
        target[...] = jnp.concatenate(
            [
                in_ref[slot, :shard, first : first + width].astype(jnp.float32)
                for slot in range(plane)
            ],
            axis=1,
        )
        first += width
    for slot in range(plane):
        for number in range(wo_ref.shape[1] // across):
            source = slice(shard + number * HALF, shard + (number + 1) * HALF)
            wo_ref[slot * HALF : (slot + 1) * HALF, number * across : (number + 1) * across] = (
                in_ref[slot, source, :].astype(jnp.float32)
            )


def spread_attention(pieces, shard, model, query_width, key_width):
    plane = lax.axis_size("ctx")
    pieces = pieces.reshape(plane, -1, pieces.shape[1])
    f32 = jnp.float32
    return pl.pallas_call(
        spread_attention_kernel,
        in_specs=in_vmem(1),
        out_specs=tuple(in_vmem(4)),
        out_shape=(
            jax.ShapeDtypeStruct((shard, plane * query_width), f32),
            jax.ShapeDtypeStruct((shard, plane * key_width), f32),
            jax.ShapeDtypeStruct((shard, plane * key_width), f32),
            jax.ShapeDtypeStruct((plane * HALF, model), f32),
        ),
        compiler_params=pltpu.CompilerParams(vmem_limit_bytes=40 << 20),
        name="spread_attention",
    )(pieces)


def head_local(
    block_input,
    block_table,
    output_grad,
    attention_gain,
    query_weight,
    key_weight,
    value_projection,
    output_weight,
    feedforward_gain,
    gate_weight,
    up_weight,
    down_weight,
):
    me = lax.axis_index("ctx")
    plane = lax.axis_size("ctx")
    line = lax.axis_size("fsdp")
    rows, model = block_input.shape[1:]
    shard = model // line
    hidden = gate_weight.shape[1]
    unit = hidden // (line * plane)
    table_row = block_table[0]
    slot_count = table_row.shape[0]
    block = rows * plane // slot_count
    places = jnp.arange(slot_count, dtype=jnp.int32)
    slots = jnp.sum(jnp.where(table_row[None, :] == places[:, None], places[None, :], 0), axis=1)

    def mine(array, width):
        return lax.dynamic_slice_in_dim(array, me * width, width, 1)

    query_width = query_weight.shape[1] // plane
    key_width = key_weight.shape[1] // plane
    qkv_mine = jnp.concatenate(
        [
            mine(query_weight, query_width),
            mine(key_weight, key_width),
            mine(value_projection, key_width),
        ],
        axis=1,
    )
    gains_mine = jnp.stack([attention_gain, feedforward_gain])
    x_all, qkv_w, wo_line, gains, feed_mine = first_exchange(
        line,
        block_input[0],
        qkv_mine,
        output_weight,
        gains_mine,
        gate_weight,
        up_weight,
        down_weight,
    )
    feed_w = lax.all_gather(feed_mine, "fsdp", axis=0, tiled=True)

    steps_index = jnp.arange(HALF, dtype=jnp.float32)
    inverse = jnp.exp(steps_index * jnp.float32(-2.0 * math.log(rotary_base) / HEAD_SIZE))

    def table_of(positions):
        angles = positions.astype(jnp.float32)[:, None] * inverse[None, :]
        both = jnp.stack([jnp.cos(angles), jnp.sin(angles)])
        both = jnp.pad(both, ((0, 0), (0, 0), (0, LANES // 2 - HALF)))
        return jnp.concatenate([both, both], axis=2)

    inner = table_of(jnp.arange(block, dtype=jnp.int32))
    outer = table_of(places * block)
    pad = padding(GROUP + 2)

    gains = jnp.transpose(gains, (1, 0, 2)).reshape(2, model).astype(jnp.float32)
    qkv_w = qkv_w.reshape(model, -1)
    grad_rows, wo_line, x_all = lax.optimization_barrier((output_grad[0], wo_line, x_all))
    grad_parts, wo_parts = [grad_rows], [wo_line]
    for bit in (2, 4):
        pairs = [(device, device ^ bit) for device in range(plane)]
        grad_parts.append(lax.ppermute(grad_rows, "ctx", pairs))
        wo_parts.append(lax.ppermute(wo_line, "ctx", pairs))
    qkv, o, o_columns, lse, qkv_pad = attend(
        slots, x_all, gains[:1], qkv_w, pad, inner, outer
    )
    wo_mine, far_grads, residual, normed_two, scale_two, *gained_two = second_exchange(
        o, wo_parts, grad_parts[1:], block_input[0], gains[1:]
    )
    grad_residual, feedforward_term, *rest = feed(
        gained_two,
        [*grad_parts, far_grads],
        feed_w,
        o_columns,
        normed_two,
        scale_two,
        gains[1:],
    )
    grad_attn, columns_mine, out_parts, feed_grads = rest[:3], rest[3], rest[4:8], rest[8]
    feed_grads = lax.psum_scatter(feed_grads, "fsdp", scatter_dimension=0, tiled=True)
    grad_o, wo_term = third_exchange(
        line,
        grad_attn,
        columns_mine.reshape(-1, columns_mine.shape[2]),
        wo_mine.reshape(-1, model),
        qkv_w.shape[1],
    )
    *out_parts, grad_o = lax.optimization_barrier((*out_parts, grad_o))
    outs = [out_parts[3]]
    for part, bit in enumerate((6, 2, 4)):
        pairs = [(device, device ^ bit) for device in range(plane)]
        outs.append(lax.ppermute(out_parts[part], "ctx", pairs))
    grads = attend_back(slots, qkv, o, grad_o, lse, pad, inner, outer)
    input_grad, attention_grads, attention_term = input_exchange(
        grads, qkv_pad, x_all, grad_residual, wo_term, gains[:1], pad
    )
    attention_grads, feed_grads = lax.optimization_barrier((attention_grads, feed_grads))
    attention_grads = lax.psum_scatter(
        attention_grads.reshape(-1, attention_grads.shape[2]),
        "fsdp",
        scatter_dimension=0,
        tiled=True,
    )
    feed_pieces, gain_terms, layer_output = pieces_exchange(
        line, feed_grads, attention_term, feedforward_term, residual, outs
    )
    gate_grad, up_grad, down_grad = spread_feed(feed_pieces, shard, line, unit)
    attention_pieces = plane_gather(attention_grads, 9)
    query_grad, key_grad, value_grad, out_grad = spread_attention(
        attention_pieces, shard, model, query_width, key_width
    )
    gain_terms = lax.dynamic_slice_in_dim(gain_terms, lax.axis_index("fsdp") * shard, shard, 1)
    return (
        layer_output,
        input_grad,
        gain_terms[0],
        query_grad,
        key_grad,
        value_grad,
        out_grad,
        gain_terms[1],
        gate_grad,
        up_grad,
        down_grad,
    )


def solution(mesh):
    plane, line = mesh.shape["ctx"], mesh.shape["fsdp"]
    fits = plane == KEY_VALUE_HEADS == 8 and plane * line * HALF == QUERY_HEADS * HEAD_SIZE
    if fits:
        return placed(mesh, head_local)
    return placed(mesh, local)


def placed(mesh, plan):
    return jax.shard_map(
        plan,
        mesh=mesh,
        in_specs=(
            P("fsdp", "ctx", None),
            P("fsdp", None),
            P("fsdp", "ctx", None),
            P("fsdp"),
            P("fsdp", None),
            P("fsdp", None),
            P("fsdp", None),
            P("fsdp", None),
            P("fsdp"),
            P("fsdp", None),
            P("fsdp", None),
            P("fsdp", None),
        ),
        out_specs=(
            P("fsdp", "ctx", None),
            P("fsdp", "ctx", None),
            P("fsdp"),
            P("fsdp", None),
            P("fsdp", None),
            P("fsdp", None),
            P("fsdp", None),
            P("fsdp"),
            P("fsdp", None),
            P("fsdp", None),
            P("fsdp", None),
        ),
        check_vma=False,
    )
```

```python
import functools
import math

import jax
import jax.numpy as jnp
from jax import lax
from jax.experimental import pallas as pl
from jax.experimental.pallas import tpu as pltpu
from jax.sharding import PartitionSpec as P


QUERY_HEADS = 16
KEY_VALUE_HEADS = 8
HEAD_SIZE = 96


norm_epsilon = 1e-05
rotary_base = 100000.0
score_with_mask = -1e30


def rope_tables(positions):
    half_width = HEAD_SIZE // 2
    steps_index = jnp.arange(half_width, dtype=jnp.float32)
    inverse = jnp.exp(steps_index * jnp.float32(-2.0 * math.log(rotary_base) / HEAD_SIZE))
    angles = positions.astype(jnp.float32)[:, None] * inverse[None, :]
    return (jnp.cos(angles), jnp.sin(angles))


def rotate(value_rows, cosine, sine_values, direction):
    count_of_rows = value_rows.shape[0]
    head_count = value_rows.shape[1] // HEAD_SIZE
    half_width = HEAD_SIZE // 2
    shaped = value_rows.reshape(count_of_rows, head_count, HEAD_SIZE)
    first_half = shaped[:, :, :half_width]
    second_half = shaped[:, :, half_width:]
    cos_part = cosine[:, None, :]
    sin_part = sine_values[:, None, :] * direction
    turned = jnp.concatenate(
        [
            first_half * cos_part - second_half * sin_part,
            second_half * cos_part + first_half * sin_part,
        ],
        axis=2,
    )
    return turned.reshape(count_of_rows, head_count * HEAD_SIZE)


def norm_scale(value_rows):
    return lax.rsqrt(jnp.mean(value_rows * value_rows, axis=-1, keepdims=True) + norm_epsilon)


def product(matrix, operand):
    return jnp.dot(matrix, operand, preferred_element_type=jnp.float32)


def cross_rows(matrix, operand):
    return lax.dot_general(
        matrix, operand, (((0,), (0,)), ((), ())), preferred_element_type=jnp.float32
    )


def back_product(matrix, operand):
    return lax.dot_general(
        matrix, operand, (((1,), (1,)), ((), ())), preferred_element_type=jnp.float32
    )


def block_scores(query_rank_four, block_of_keys, query_positions, key_positions):
    keys_rank_three = block_of_keys.reshape(block_of_keys.shape[0], KEY_VALUE_HEADS, HEAD_SIZE)
    scores = jnp.einsum(
        "rgjd,kgd->gjrk", query_rank_four, keys_rank_three, preferred_element_type=jnp.float32
    ) * HEAD_SIZE ** (-0.5)
    allowed = (key_positions[None, :] <= query_positions[:, None])[None, None]
    return (jnp.where(allowed, scores, score_with_mask), allowed)


def local(
    block_input,
    block_table,
    output_grad,
    attention_gain,
    query_weight,
    key_weight,
    value_projection,
    output_weight,
    feedforward_gain,
    gate_weight,
    up_weight,
    down_weight,
):
    query_group_width = QUERY_HEADS // KEY_VALUE_HEADS
    score_scale = HEAD_SIZE ** (-0.5)
    inputs = block_input[0].astype(jnp.float32)
    count_of_rows = inputs.shape[0]
    block_rows = count_of_rows // 2
    ctx_index = lax.axis_index("ctx")
    table_row = block_table[0]
    offsets = jnp.arange(block_rows, dtype=jnp.int32)
    query_blocks = lax.dynamic_slice_in_dim(table_row, 2 * ctx_index, 2)
    query_positions = (query_blocks[:, None] * block_rows + offsets[None, :]).reshape(count_of_rows)
    key_positions = (table_row[:, None] * block_rows + offsets[None, :]).reshape(-1)
    cosine, sine_values = rope_tables(query_positions)
    gain_one, query_full, key_full, value_full, out_full = (
        lax.all_gather(attention_gain, "fsdp", axis=0, tiled=True),
        lax.all_gather(query_weight, "fsdp", axis=0, tiled=True),
        lax.all_gather(key_weight, "fsdp", axis=0, tiled=True),
        lax.all_gather(value_projection, "fsdp", axis=0, tiled=True),
        lax.all_gather(output_weight, "fsdp", axis=0, tiled=True),
    )
    scale_one = norm_scale(inputs)
    normed_one = inputs * scale_one
    gained_one = (normed_one * gain_one.astype(jnp.float32)).astype(jnp.bfloat16)
    query_rows = rotate(product(gained_one, query_full), cosine, sine_values, 1.0).astype(
        jnp.bfloat16
    )
    keys_local = rotate(product(gained_one, key_full), cosine, sine_values, 1.0).astype(
        jnp.bfloat16
    )
    values_local = product(gained_one, value_full).astype(jnp.bfloat16)
    keys_all, values_all = (
        lax.all_gather(keys_local, "ctx", axis=0, tiled=True),
        lax.all_gather(values_local, "ctx", axis=0, tiled=True),
    )
    key_total_count = keys_all.shape[0]
    key_block_pass = 1024
    block_count = key_total_count // key_block_pass
    query_rank_four = query_rows.reshape(
        count_of_rows, KEY_VALUE_HEADS, query_group_width, HEAD_SIZE
    )
    key_places = key_positions.reshape(block_count, key_block_pass)

    def split_keys(array_in):
        return array_in.reshape(block_count, key_block_pass, array_in.shape[-1])

    def statistics_step(state_now, block_data):
        running_max, running_sum = state_now
        block_of_keys, key_place = block_data
        masked, allowed = block_scores(query_rank_four, block_of_keys, query_positions, key_place)
        new_max = jnp.maximum(running_max, jnp.max(masked, axis=-1))
        block_sum = jnp.sum(jnp.where(allowed, jnp.exp(masked - new_max[..., None]), 0.0), axis=-1)
        return ((new_max, running_sum * jnp.exp(running_max - new_max) + block_sum), None)

    initial_maximum = jnp.full(
        (KEY_VALUE_HEADS, query_group_width, count_of_rows), score_with_mask, jnp.float32
    )
    initial_sum = jnp.zeros((KEY_VALUE_HEADS, query_group_width, count_of_rows), jnp.float32)
    (final_max, final_sum), unused = lax.scan(
        statistics_step, (initial_maximum, initial_sum), (split_keys(keys_all), key_places)
    )
    log_total = final_max + jnp.log(final_sum)

    def output_step(state_now, block_data):
        block_of_keys, block_of_values, key_place = block_data
        masked, allowed = block_scores(query_rank_four, block_of_keys, query_positions, key_place)
        weights_half = jnp.where(allowed, jnp.exp(masked - log_total[..., None]), 0.0).astype(
            jnp.bfloat16
        )
        values_rank_three = block_of_values.reshape(key_block_pass, KEY_VALUE_HEADS, HEAD_SIZE)
        return (
            state_now
            + jnp.einsum(
                "gjrk,kgd->rgjd",
                weights_half,
                values_rank_three,
                preferred_element_type=jnp.float32,
            ),
            None,
        )

    initial_output = jnp.zeros(
        (count_of_rows, KEY_VALUE_HEADS, query_group_width, HEAD_SIZE), jnp.float32
    )
    summed_out, unused = lax.scan(
        output_step, initial_output, (split_keys(keys_all), split_keys(values_all), key_places)
    )
    attended_rows = summed_out.reshape(count_of_rows, QUERY_HEADS * HEAD_SIZE).astype(jnp.bfloat16)
    residual = inputs + product(attended_rows, out_full)
    scale_two = norm_scale(residual)
    normed_two = residual * scale_two
    gain_two, gate_full, up_full, down_full = (
        lax.all_gather(feedforward_gain, "fsdp", axis=0, tiled=True),
        lax.all_gather(gate_weight, "fsdp", axis=0, tiled=True),
        lax.all_gather(up_weight, "fsdp", axis=0, tiled=True),
        lax.all_gather(down_weight, "fsdp", axis=0, tiled=True),
    )
    gained_two = (normed_two * gain_two.astype(jnp.float32)).astype(jnp.bfloat16)
    gate_values = product(gained_two, gate_full)
    up_values = product(gained_two, up_full)
    sigmoid_gate = jax.nn.sigmoid(gate_values)
    activated = gate_values * sigmoid_gate
    hidden_act = (activated * up_values).astype(jnp.bfloat16)
    layer_output = (residual + product(hidden_act, down_full)).astype(jnp.bfloat16)
    gain_two_again, gate_back, up_back, down_back = (
        lax.all_gather(feedforward_gain, "fsdp", axis=0, tiled=True),
        lax.all_gather(gate_weight, "fsdp", axis=0, tiled=True),
        lax.all_gather(up_weight, "fsdp", axis=0, tiled=True),
        lax.all_gather(down_weight, "fsdp", axis=0, tiled=True),
    )
    grad_rows = output_grad[0]
    grad_hidden = back_product(grad_rows, down_back)
    down_term = cross_rows(hidden_act, grad_rows)
    grad_gate = (
        grad_hidden * up_values * sigmoid_gate * (1.0 + gate_values * (1.0 - sigmoid_gate))
    ).astype(jnp.bfloat16)
    grad_up = (grad_hidden * activated).astype(jnp.bfloat16)
    gate_term = cross_rows(gained_two, grad_gate)
    up_term = cross_rows(gained_two, grad_up)
    grad_normed_two = back_product(grad_gate, gate_back) + back_product(grad_up, up_back)
    feedforward_term = jnp.sum(grad_normed_two * normed_two, axis=0)
    grad_scaled_two = grad_normed_two * gain_two_again.astype(jnp.float32)
    grad_residual = grad_rows.astype(jnp.float32) + scale_two * (
        grad_scaled_two
        - normed_two * jnp.mean(grad_scaled_two * normed_two, axis=-1, keepdims=True)
    )
    gain_one_again, query_back, key_back, value_back, out_back = (
        lax.all_gather(attention_gain, "fsdp", axis=0, tiled=True),
        lax.all_gather(query_weight, "fsdp", axis=0, tiled=True),
        lax.all_gather(key_weight, "fsdp", axis=0, tiled=True),
        lax.all_gather(value_projection, "fsdp", axis=0, tiled=True),
        lax.all_gather(output_weight, "fsdp", axis=0, tiled=True),
    )
    grad_attn = grad_residual.astype(jnp.bfloat16)
    output_term = cross_rows(attended_rows, grad_attn)
    attended_gradient = back_product(grad_attn, out_back).astype(jnp.bfloat16)
    gradient_rank_four = attended_gradient.reshape(
        count_of_rows, KEY_VALUE_HEADS, query_group_width, HEAD_SIZE
    )
    attended_rank_four = attended_rows.reshape(
        count_of_rows, KEY_VALUE_HEADS, query_group_width, HEAD_SIZE
    )
    row_delta = jnp.transpose(
        jnp.sum(
            gradient_rank_four.astype(jnp.float32) * attended_rank_four.astype(jnp.float32), axis=-1
        ),
        (1, 2, 0),
    )
    keys_again, values_again = (
        lax.all_gather(keys_local, "ctx", axis=0, tiled=True),
        lax.all_gather(values_local, "ctx", axis=0, tiled=True),
    )

    def back_step(state_now, block_data):
        block_of_keys, block_of_values, key_place = block_data
        masked, allowed = block_scores(query_rank_four, block_of_keys, query_positions, key_place)
        weights_half = jnp.where(allowed, jnp.exp(masked - log_total[..., None]), 0.0).astype(
            jnp.bfloat16
        )
        values_rank_three = block_of_values.reshape(key_block_pass, KEY_VALUE_HEADS, HEAD_SIZE)
        keys_rank_three = block_of_keys.reshape(key_block_pass, KEY_VALUE_HEADS, HEAD_SIZE)
        grad_weights = jnp.einsum(
            "rgjd,kgd->gjrk",
            gradient_rank_four,
            values_rank_three,
            preferred_element_type=jnp.float32,
        )
        grad_scores = (
            weights_half.astype(jnp.float32) * (grad_weights - row_delta[..., None]) * score_scale
        ).astype(jnp.bfloat16)
        state_now = state_now + jnp.einsum(
            "gjrk,kgd->rgjd", grad_scores, keys_rank_three, preferred_element_type=jnp.float32
        )
        key_gradient = jnp.einsum(
            "gjrk,rgjd->kgd", grad_scores, query_rank_four, preferred_element_type=jnp.float32
        )
        value_gradient = jnp.einsum(
            "gjrk,rgjd->kgd", weights_half, gradient_rank_four, preferred_element_type=jnp.float32
        )
        return (
            state_now,
            (
                key_gradient.reshape(key_block_pass, KEY_VALUE_HEADS * HEAD_SIZE).astype(
                    jnp.bfloat16
                ),
                value_gradient.reshape(key_block_pass, KEY_VALUE_HEADS * HEAD_SIZE).astype(
                    jnp.bfloat16
                ),
            ),
        )

    first_query_index = jnp.zeros(
        (count_of_rows, KEY_VALUE_HEADS, query_group_width, HEAD_SIZE), jnp.float32
    )
    query_sum, (key_gradients, value_gradients) = lax.scan(
        back_step, first_query_index, (split_keys(keys_again), split_keys(values_again), key_places)
    )
    key_gradients = key_gradients.reshape(key_total_count, KEY_VALUE_HEADS * HEAD_SIZE)
    value_gradients = value_gradients.reshape(key_total_count, KEY_VALUE_HEADS * HEAD_SIZE)
    key_sums, value_sums = (
        lax.psum_scatter(key_gradients, "ctx", scatter_dimension=0, tiled=True).astype(jnp.float32),
        lax.psum_scatter(value_gradients, "ctx", scatter_dimension=0, tiled=True).astype(
            jnp.float32
        ),
    )
    query_gradients = rotate(
        query_sum.reshape(count_of_rows, QUERY_HEADS * HEAD_SIZE), cosine, sine_values, -1.0
    ).astype(jnp.bfloat16)
    grad_keys = rotate(key_sums, cosine, sine_values, -1.0).astype(jnp.bfloat16)
    grad_values = value_sums.astype(jnp.bfloat16)
    query_term = cross_rows(gained_one, query_gradients)
    key_term = cross_rows(gained_one, grad_keys)
    value_term = cross_rows(gained_one, grad_values)
    grad_normed_one = (
        back_product(query_gradients, query_back)
        + back_product(grad_keys, key_back)
        + back_product(grad_values, value_back)
    )
    attention_term = jnp.sum(grad_normed_one * normed_one, axis=0)
    grad_scaled_one = grad_normed_one * gain_one_again.astype(jnp.float32)
    input_grad = grad_residual + scale_one * (
        grad_scaled_one
        - normed_one * jnp.mean(grad_scaled_one * normed_one, axis=-1, keepdims=True)
    )
    shares = (
        lax.psum_scatter(
            attention_term.astype(jnp.bfloat16), "fsdp", scatter_dimension=0, tiled=True
        ).astype(jnp.float32),
        lax.psum_scatter(
            query_term.astype(jnp.bfloat16), "fsdp", scatter_dimension=0, tiled=True
        ).astype(jnp.float32),
        lax.psum_scatter(
            key_term.astype(jnp.bfloat16), "fsdp", scatter_dimension=0, tiled=True
        ).astype(jnp.float32),
        lax.psum_scatter(
            value_term.astype(jnp.bfloat16), "fsdp", scatter_dimension=0, tiled=True
        ).astype(jnp.float32),
        lax.psum_scatter(
            output_term.astype(jnp.bfloat16), "fsdp", scatter_dimension=0, tiled=True
        ).astype(jnp.float32),
        lax.psum_scatter(
            feedforward_term.astype(jnp.bfloat16), "fsdp", scatter_dimension=0, tiled=True
        ).astype(jnp.float32),
        lax.psum_scatter(
            gate_term.astype(jnp.bfloat16), "fsdp", scatter_dimension=0, tiled=True
        ).astype(jnp.float32),
        lax.psum_scatter(
            up_term.astype(jnp.bfloat16), "fsdp", scatter_dimension=0, tiled=True
        ).astype(jnp.float32),
        lax.psum_scatter(
            down_term.astype(jnp.bfloat16), "fsdp", scatter_dimension=0, tiled=True
        ).astype(jnp.float32),
    )
    totals = (
        lax.psum(shares[0].astype(jnp.bfloat16), "ctx").astype(jnp.float32),
        lax.psum(shares[1].astype(jnp.bfloat16), "ctx").astype(jnp.float32),
        lax.psum(shares[2].astype(jnp.bfloat16), "ctx").astype(jnp.float32),
        lax.psum(shares[3].astype(jnp.bfloat16), "ctx").astype(jnp.float32),
        lax.psum(shares[4].astype(jnp.bfloat16), "ctx").astype(jnp.float32),
        lax.psum(shares[5].astype(jnp.bfloat16), "ctx").astype(jnp.float32),
        lax.psum(shares[6].astype(jnp.bfloat16), "ctx").astype(jnp.float32),
        lax.psum(shares[7].astype(jnp.bfloat16), "ctx").astype(jnp.float32),
        lax.psum(shares[8].astype(jnp.bfloat16), "ctx").astype(jnp.float32),
    )
    return (
        layer_output[None],
        input_grad[None],
        totals[0],
        totals[1],
        totals[2],
        totals[3],
        totals[4],
        totals[5],
        totals[6],
        totals[7],
        totals[8],
    )


LANES = 128
HALF = HEAD_SIZE // 2
GROUP = QUERY_HEADS // KEY_VALUE_HEADS
score_scale = HEAD_SIZE ** (-0.5)
binary_scale = score_scale * math.log2(math.e)


def contract(left, right, left_dim, right_dim):
    return lax.dot_general(
        left, right, (((left_dim,), (right_dim,)), ((), ())), preferred_element_type=jnp.float32
    )


def in_vmem(count):
    return [pl.BlockSpec(memory_space=pltpu.VMEM)] * count


def padding(heads):
    column = jnp.arange(heads * HEAD_SIZE, dtype=jnp.int32)
    half_at, rest = column // HALF, column % HALF
    target = half_at * (LANES // 2) + rest
    lanes = jnp.arange(heads * LANES, dtype=jnp.int32)
    return (target[:, None] == lanes[None, :]).astype(jnp.bfloat16)


def turn(part, cosine, sine):
    return part * cosine + pltpu.roll(part, LANES // 2, 1) * sine


def tables(inner_ref, outer_ref, index, per_tile):
    inner_cos, inner_sin = inner_ref[0], inner_ref[1]
    sign = jnp.where(
        lax.broadcasted_iota(jnp.int32, inner_cos.shape, 1) < LANES // 2, -1.0, 1.0
    )
    cosines, sines = [], []
    for part in range(per_tile):
        at = pl.ds(index * per_tile + part, 1)
        outer_cos, outer_sin = outer_ref[0, at, :], outer_ref[1, at, :]
        cosines.append(inner_cos * outer_cos - inner_sin * outer_sin)
        sines.append(sign * (inner_sin * outer_cos + inner_cos * outer_sin))
    return jnp.concatenate(cosines, axis=0), jnp.concatenate(sines, axis=0)


def forward_kernel(
    slot_ref,
    xa_ref,
    xb_ref,
    gain_ref,
    w_ref,
    pad_ref,
    inner_ref,
    outer_ref,
    qkv_hbm,
    o_ref,
    ot_ref,
    lse_ref,
    wp_hbm,
    qkv_ref,
    wp,
    qs,
    vt,
    s_ref,
    here,
):
    index = pl.program_id(0)
    block = xa_ref.shape[0]
    tile = 2 * block
    width = GROUP * tile
    heads = GROUP + 2

    @pl.when(index == 0)
    def _():
        wp[...] = contract(w_ref[...], pad_ref[...], 1, 0).astype(jnp.bfloat16)
        pltpu.make_async_copy(wp, wp_hbm, here.at[1]).start()

    x = jnp.concatenate([xa_ref[...], xb_ref[...]], axis=0).astype(jnp.float32)
    normed = x * lax.rsqrt(jnp.mean(x * x, axis=-1, keepdims=True) + norm_epsilon)
    gained = (normed * gain_ref[...]).astype(jnp.bfloat16)
    raw = contract(gained, wp[...], 1, 0)
    cosine, sine = tables(inner_ref, outer_ref, index, 2)
    here_rows = pl.ds(pl.multiple_of(index * tile, tile), tile)
    for head in range(heads):
        lanes = slice(head * LANES, (head + 1) * LANES)
        part = raw[:, lanes]
        if head <= GROUP:
            part = turn(part, cosine, sine)
        part = part.astype(jnp.bfloat16)
        qkv_ref[here_rows, lanes] = part
        if head < GROUP:
            qs[head * tile : (head + 1) * tile, :] = part
        if head == heads - 1:
            vt[:, here_rows] = part.T

    def save(number):
        place = pl.ds(pl.multiple_of(number * tile, tile), tile)
        return pltpu.make_async_copy(qkv_ref.at[place, :], qkv_hbm.at[place, :], here.at[0])

    save(index).start()
    queries = qs[...]
    key_at = lax.broadcasted_iota(jnp.int32, (tile, width), 0)
    query_at = lax.rem(lax.broadcasted_iota(jnp.int32, (tile, width), 1), tile)
    diagonal = key_at <= query_at

    def scores_of(step):
        at = pl.ds(pl.multiple_of(step * tile, tile), tile)
        keys = qkv_ref[at, GROUP * LANES : (GROUP + 1) * LANES]
        return contract(keys, queries, 1, 1) * binary_scale

    last = jnp.where(diagonal, scores_of(index), score_with_mask)
    s_ref[here_rows, :] = last
    peak = jnp.max(last, axis=0, keepdims=True)

    def in_pairs(one, state):
        state = lax.fori_loop(
            0, lax.div(index, 2), lambda pair, state: one((2 * pair, 2 * pair + 1), state), state
        )
        return lax.fori_loop(0, lax.rem(index, 2), lambda _, state: one((index - 1,), state), state)

    def first_pass(steps, peak):
        found = [scores_of(step) for step in steps]
        for step, scores in zip(steps, found):
            s_ref[pl.ds(pl.multiple_of(step * tile, tile), tile), :] = scores
            peak = jnp.maximum(peak, jnp.max(scores, axis=0, keepdims=True))
        return peak

    peak = in_pairs(first_pass, peak)

    def second_pass(steps, state):
        total, out = state
        for step in steps:
            at = pl.ds(pl.multiple_of(step * tile, tile), tile)
            probs = jnp.exp2(s_ref[at, :] - peak)
            total = total + jnp.sum(probs, axis=0, keepdims=True)
            out = out + contract(vt[:, at], probs.astype(jnp.bfloat16), 1, 0)
        return (total, out)

    total, out = in_pairs(
        second_pass,
        second_pass(
            (index,), (jnp.zeros((1, width), jnp.float32), jnp.zeros((LANES, width), jnp.float32))
        ),
    )
    lse_ref[pl.ds(index, 1), :] = peak + jnp.log2(total)
    out = (out * (1.0 / total)).T.astype(jnp.bfloat16)
    out = jnp.concatenate([out[head * tile : (head + 1) * tile, :] for head in range(GROUP)], axis=1)
    out = contract(out, pad_ref[: GROUP * HEAD_SIZE, : GROUP * LANES], 1, 1).astype(jnp.bfloat16)
    for part in range(2):
        target = pl.ds(pl.multiple_of(slot_ref[index * 2 + part] * block, block), block)
        rows_at = slice(part * block, (part + 1) * block)
        o_ref[target, :] = out[rows_at, :]
        ot_ref[:, target] = out[rows_at, :].T

    save(index).wait()

    @pl.when(index == pl.num_programs(0) - 1)
    def _():
        pltpu.make_async_copy(wp, wp_hbm, here.at[1]).wait()


def attend(slots, x, gain, w, pad, inner, outer):
    rows, model = x.shape
    block = rows // slots.shape[0]
    tile = 2 * block
    width = GROUP * tile
    columns = pad.shape[1]
    whole = lambda *shape: pl.BlockSpec(shape, lambda i, s: (0,) * len(shape))
    return pl.pallas_call(
        forward_kernel,
        grid_spec=pltpu.PrefetchScalarGridSpec(
            num_scalar_prefetch=1,
            grid=(rows // tile,),
            in_specs=[
                pl.BlockSpec((block, model), lambda i, s: (s[2 * i], 0)),
                pl.BlockSpec((block, model), lambda i, s: (s[2 * i + 1], 0)),
                whole(1, model),
                whole(*w.shape),
                whole(*pad.shape),
                whole(*inner.shape),
                whole(*outer.shape),
            ],
            out_specs=(
                pl.BlockSpec(memory_space=pl.ANY),
                whole(rows, GROUP * HEAD_SIZE),
                whole(GROUP * HEAD_SIZE, rows),
                whole(rows // tile, width),
                pl.BlockSpec(memory_space=pl.ANY),
            ),
            scratch_shapes=[
                pltpu.VMEM((rows, columns), jnp.bfloat16),
                pltpu.VMEM((model, columns), jnp.bfloat16),
                pltpu.VMEM((width, LANES), jnp.bfloat16),
                pltpu.VMEM((LANES, rows), jnp.bfloat16),
                pltpu.VMEM((rows, width), jnp.float32),
                pltpu.SemaphoreType.DMA((2,)),
            ],
        ),
        out_shape=(
            jax.ShapeDtypeStruct((rows, columns), jnp.bfloat16),
            jax.ShapeDtypeStruct((rows, GROUP * HEAD_SIZE), jnp.bfloat16),
            jax.ShapeDtypeStruct((GROUP * HEAD_SIZE, rows), jnp.bfloat16),
            jax.ShapeDtypeStruct((rows // tile, width), jnp.float32),
            jax.ShapeDtypeStruct((model, columns), jnp.bfloat16),
        ),
        compiler_params=pltpu.CompilerParams(vmem_limit_bytes=62 << 20),
        cost_estimate=pl.CostEstimate(
            flops=4 * GROUP * rows * rows * LANES // 2 + 2 * rows * model * columns,
            bytes_accessed=4 * rows * model,
            transcendentals=GROUP * rows * rows // 2,
        ),
        name="attend",
    )(slots, x, x, gain, w, pad, inner, outer)


def backward_kernel(
    slot_ref,
    qkv_ref,
    o_ref,
    do_ref,
    lse_ref,
    pad_ref,
    inner_ref,
    outer_ref,
    dqkv_ref,
    qs,
    gs,
    kt,
    dk,
    dv,
):
    step_at = pl.program_id(0)
    tiles = pl.num_programs(0)
    index = tiles - 1 - step_at
    block = qkv_ref.shape[0] // slot_ref.shape[0]
    tile = 2 * block
    width = GROUP * tile
    first_key, first_value = GROUP * LANES, (GROUP + 1) * LANES

    @pl.when(step_at == 0)
    def _():
        kt[...] = qkv_ref[:, first_key:first_value].T
        dk[...] = jnp.zeros_like(dk)
        dv[...] = jnp.zeros_like(dv)

    here = pl.ds(pl.multiple_of(index * tile, tile), tile)
    sources = [
        pl.ds(pl.multiple_of(slot_ref[index * 2 + part] * block, block), block) for part in (0, 1)
    ]
    o = jnp.concatenate([o_ref[source, :] for source in sources], axis=0)
    grads = jnp.concatenate([do_ref[source, :] for source in sources], axis=0)
    products = (grads.astype(jnp.float32) * o.astype(jnp.float32)).T
    grads = contract(grads, pad_ref[: GROUP * HEAD_SIZE, : GROUP * LANES], 1, 0).astype(jnp.bfloat16)
    deltas = []
    for head in range(GROUP):
        lanes = slice(head * LANES, (head + 1) * LANES)
        at = slice(head * tile, (head + 1) * tile)
        qs[at, :] = qkv_ref[here, lanes]
        gs[at, :] = grads[:, lanes]
        features = slice(head * HEAD_SIZE, (head + 1) * HEAD_SIZE)
        deltas.append(jnp.sum(products[features, :], axis=0, keepdims=True))
    delta = jnp.concatenate(deltas, axis=1)
    lse = lse_ref[pl.ds(index, 1), :]
    key_at = lax.broadcasted_iota(jnp.int32, (tile, width), 0)
    query_at = lax.rem(lax.broadcasted_iota(jnp.int32, (tile, width), 1), tile)
    diagonal = key_at <= query_at

    def pieces(steps, masked=False):
        queries, grads = qs[...], gs[...]
        places = [pl.ds(pl.multiple_of(step * tile, tile), tile) for step in steps]
        scores = [contract(qkv_ref[at, first_key:first_value], queries, 1, 1) for at in places]
        grad_probs = [contract(qkv_ref[at, first_value:], grads, 1, 1) for at in places]
        total = None
        for at, score, grad_prob in zip(places, scores, grad_probs):
            probs = jnp.exp2(score * binary_scale - lse)
            if masked:
                probs = jnp.where(diagonal, probs, 0.0)
            dv[at, :] += contract(probs.astype(jnp.bfloat16), grads, 1, 0)
            grad_scores = (probs * (grad_prob - delta)).astype(jnp.bfloat16)
            dk[at, :] += contract(grad_scores, queries, 1, 0)
            part = contract(kt[:, at], grad_scores, 1, 0)
            total = part if total is None else total + part
        return total

    dq = pieces((index,), True)
    dq = lax.fori_loop(
        0, lax.div(index, 2), lambda pair, total: total + pieces((2 * pair, 2 * pair + 1)), dq
    )
    dq = lax.fori_loop(0, lax.rem(index, 2), lambda _, total: total + pieces((index - 1,)), dq)
    dq = dq.T * score_scale
    cosine, sine = tables(inner_ref, outer_ref, index, 2)
    parts = [turn(dq[head * tile : (head + 1) * tile, :], cosine, -sine) for head in range(GROUP)]
    parts.append(turn(dk[here, :] * score_scale, cosine, -sine))
    parts.append(dv[here, :])
    dqkv = jnp.concatenate([part.astype(jnp.bfloat16) for part in parts], axis=1)
    for part in (0, 1):
        dqkv_ref[sources[part], :] = dqkv[part * block : (part + 1) * block, :]


def attend_back(slots, qkv, o, do, lse, pad, inner, outer):
    rows, columns = qkv.shape
    block = rows // slots.shape[0]
    tile = 2 * block
    width = GROUP * tile
    tiles = rows // tile
    operands = (qkv, o, do, lse, pad, inner, outer)
    whole = lambda *shape: pl.BlockSpec(shape, lambda i, s: (0,) * len(shape))
    return pl.pallas_call(
        backward_kernel,
        grid_spec=pltpu.PrefetchScalarGridSpec(
            num_scalar_prefetch=1,
            grid=(tiles,),
            in_specs=[whole(*operand.shape) for operand in operands],
            out_specs=whole(rows, columns),
            scratch_shapes=[
                pltpu.VMEM((width, LANES), jnp.bfloat16),
                pltpu.VMEM((width, LANES), jnp.bfloat16),
                pltpu.VMEM((LANES, rows), jnp.bfloat16),
                pltpu.VMEM((rows, LANES), jnp.float32),
                pltpu.VMEM((rows, LANES), jnp.float32),
            ],
        ),
        out_shape=jax.ShapeDtypeStruct((rows, columns), jnp.bfloat16),
        compiler_params=pltpu.CompilerParams(vmem_limit_bytes=40 << 20),
        cost_estimate=pl.CostEstimate(
            flops=10 * GROUP * rows * rows * LANES // 2,
            bytes_accessed=8 * rows * columns,
            transcendentals=GROUP * rows * rows // 2,
        ),
        name="attend_back",
    )(slots, *operands)


MESH_IDS = pl.DeviceIdType.MESH


NEAR = (1, 2, 4)
ALL = (1, 2, 3, 4, 5, 6, 7)


def start_barrier(me, bits, line_steps=(), line_index=None, line=1):
    barrier = pltpu.get_barrier_semaphore()
    peers = [{"ctx": me ^ bit} for bit in bits]
    peers += [{"fsdp": lax.rem(line_index + step, line)} for step in line_steps]
    for peer in peers:
        pl.semaphore_signal(barrier, inc=1, device_id=peer, device_id_type=MESH_IDS)
    pl.semaphore_wait(barrier, len(peers))


def start_line_barrier(me, index, line):
    barrier = pltpu.get_barrier_semaphore()
    for bit in NEAR:
        pl.semaphore_signal(barrier, inc=1, device_id={"ctx": me ^ bit}, device_id_type=MESH_IDS)
    up, down = index < line - 1, index > 0
    for there, exists in ((index + 1, up), (index - 1, down)):

        @pl.when(exists)
        def _(there=there):
            peer = {"fsdp": jnp.clip(there, 0, line - 1)}
            pl.semaphore_signal(barrier, inc=1, device_id=peer, device_id_type=MESH_IDS)

    pl.semaphore_wait(barrier, len(NEAR) + up.astype(jnp.int32) + down.astype(jnp.int32))


class Copies:
    def __init__(self, send_sems, recv_sems, base=0):
        self.send_sems, self.recv_sems, self.next, self.sent = send_sems, recv_sems, base, []

    def number(self):
        self.next += 1
        return self.next - 1

    def make(self, number, source, target, peer, landing=None):
        return pltpu.make_async_remote_copy(
            src_ref=source,
            dst_ref=target,
            send_sem=self.send_sems.at[number],
            recv_sem=self.recv_sems.at[number if landing is None else landing],
            device_id=peer,
            device_id_type=MESH_IDS,
        )

    def send(self, number, source, target, peer):
        copy = self.make(number, source, target, peer)
        copy.start()
        self.sent.append(copy)

    def arrived(self, number, target):
        self.make(number, target, target, {"ctx": 0}).wait_recv()

    def finish(self):
        for copy in self.sent:
            copy.wait_send()


GATHER_COPIES = 14


class PlaneGather:
    def __init__(self, copies, me, own_half, part):
        self.copies, self.me, self.own_half, self.part = copies, me, own_half, part
        self.first = copies.next
        copies.next += GATHER_COPIES

    def copy(self, number):
        bit, half, receiver = (
            (0, 1, 2),
            (0, 0, 4),
            (0, 0, 2),
            (0, 1, 4),
            (0, 0, 1),
            (0, 1, 1),
            (2, 1, 4),
            (4, 0, 2),
            (2, 1, 1),
            (4, 0, 1),
            (2, 0, 1),
            (4, 1, 1),
            (6, 1, 1),
            (6, 0, 1),
        )[number]
        place = self.part(self.me ^ bit, half)
        source = self.own_half(half) if bit == 0 else place
        return self.copies.make(self.first + number, source, place, {"ctx": self.me ^ receiver})

    def send(self, *numbers):
        for number in numbers:
            self.copy(number).start()

    def hear(self, number, bit, half):
        self.copies.arrived(self.first + number, self.part(self.me ^ bit, half))

    def begin(self):
        self.send(0, 1, 2, 3, 4, 5)

    def first_hop(self):
        self.hear(0, 2, 1)
        self.send(6, 8)
        self.hear(1, 4, 0)
        self.send(7, 9)

    def second_hop(self):
        self.hear(2, 2, 0)
        self.send(10)
        self.hear(3, 4, 1)
        self.send(11)

    def third_hop(self):
        self.hear(6, 6, 1)
        self.send(12)
        self.hear(7, 6, 0)
        self.send(13)

    def shared(self, bit):
        for number, half in {1: (4, 0), 3: (8, 1), 5: (9, 0), 7: (12, 1)}[bit], {
            1: (5, 1),
            3: (10, 0),
            5: (11, 1),
            7: (13, 0),
        }[bit]:
            self.hear(number, bit, half)

    def last(self):
        for bit in (1, 3, 5, 7):
            self.shared(bit)

    def finish(self):
        for number in range(GATHER_COPIES):
            self.copy(number).wait_send()


def row_half(ref, rows):
    half = rows // 2

    def own(side):
        return ref.at[pl.ds(side * half, half), :]

    return own


def row_part(ref, rows):
    half = rows // 2

    def part(slot, side):
        if isinstance(side, slice):
            return ref.at[pl.ds(pl.multiple_of(slot * rows, rows), rows), :]
        return ref.at[pl.ds(pl.multiple_of(slot * rows + side * half, half), half), :]

    return part


class LineGather:
    def __init__(self, copies, index, line, own, place):
        self.copies, self.index, self.line = copies, index, line
        self.own, self.place = own, place
        self.first = copies.next
        copies.next += 2 * (line - 1)

    def move(self, step, upward, act):
        index, line = self.index, self.line
        if upward:
            slot, there = index - step, index + 1
            leaves = (slot >= 0) & (there < line)
        else:
            slot, there = index + step, index - 1
            leaves = (slot < line) & (there >= 0)
        number = self.first + step + (0 if upward else line - 1)

        @pl.when(leaves)
        def _():
            place = self.place(jnp.clip(slot, 0, line - 1))
            source = self.own if step == 0 else place
            act(self.copies.make(number, source, place, {"fsdp": jnp.clip(there, 0, line - 1)}))

    def hear(self, step, upward):
        index, line = self.index, self.line
        slot = index - 1 - step if upward else index + 1 + step
        comes = (slot >= 0) & (slot < line)
        number = self.first + step + (0 if upward else line - 1)

        @pl.when(comes)
        def _():
            place = self.place(jnp.clip(slot, 0, line - 1))
            self.copies.make(number, place, place, {"fsdp": 0}).wait_recv()

    def begin(self):
        for upward in (True, False):
            self.move(0, upward, lambda copy: copy.start())

    def hop(self, step):
        for upward in (True, False):
            self.hear(step - 1, upward)
            if step < self.line - 1:
                self.move(step, upward, lambda copy: copy.start())

    def finish(self):
        for step in range(self.line - 1):
            for upward in (True, False):
                self.move(step, upward, lambda copy: copy.wait_send())


def in_hbm(count):
    return [pl.BlockSpec(memory_space=pltpu.HBM)] * count


def anywhere(count):
    return [pl.BlockSpec(memory_space=pl.ANY)] * count


def local_copies(pairs, sems):
    copies = [
        pltpu.make_async_copy(source, target, sems.at[number])
        for number, (source, target) in enumerate(pairs)
    ]
    for copy in copies:
        copy.start()
    return copies


def remote_params(number, mebibytes=62):
    return pltpu.CompilerParams(
        collective_id=number, has_side_effects=True, vmem_limit_bytes=mebibytes << 20
    )


def first_kernel(
    line,
    x_ref,
    qkv_ref,
    wo_ref,
    gain_ref,
    gate_ref,
    up_ref,
    down_ref,
    xo_ref,
    qkvo_ref,
    woo_ref,
    gaino_ref,
    feedo_ref,
    feed,
    own,
    send,
    recv,
    here,
):
    me, index = lax.axis_index("ctx"), lax.axis_index("fsdp")
    plane = lax.axis_size("ctx")
    rows = x_ref.shape[0]
    part = row_part(xo_ref, rows)
    wo_rows = woo_ref.shape[1]
    wo_own = wo_ref.at[pl.ds(pl.multiple_of(me * wo_rows, wo_rows), wo_rows), :]
    local = local_copies(
        [
            (qkv_ref, qkvo_ref.at[index]),
            (wo_own, woo_ref.at[index]),
            (gain_ref, gaino_ref.at[index]),
            (x_ref, own),
        ],
        here.at[pl.ds(0, 4)],
    )
    start_line_barrier(me, index, line)
    copies = Copies(send, recv)
    gather = PlaneGather(copies, me, row_half(own, rows), part)
    lines = [
        LineGather(copies, index, line, own, lambda slot, ref=ref: ref.at[slot])
        for own, ref in ((qkv_ref, qkvo_ref), (gain_ref, gaino_ref), (wo_own, woo_ref))
    ]
    local.pop().wait()
    gather.begin()
    local += local_copies([(own, part(me, slice(None)))], here.at[pl.ds(3, 1)])
    for each in lines:
        each.begin()
    width = feed.shape[1] // 3
    unit = width // line
    pairs = []
    for side, ref in enumerate((gate_ref, up_ref)):
        for z in range(line):
            source = pl.ds(pl.multiple_of((z * plane + me) * unit, unit), unit)
            target = pl.ds(side * width + z * unit, unit)
            pairs.append((ref.at[:, source], feed.at[:, target]))
    for number in range(feed.shape[0] // unit):
        pairs.append(
            (
                down_ref.at[
                    pl.ds(pl.multiple_of(me * unit, unit), unit), pl.ds(number * width, width)
                ],
                feed.at[pl.ds(number * unit, unit), pl.ds(2 * width, width)],
            )
        )
    packed = local_copies(pairs, here.at[pl.ds(4, len(pairs))])
    gather.first_hop()
    for step in range(1, line):
        for each in lines:
            each.hop(step)
        if step == 1:
            gather.second_hop()
            for copy in packed:
                copy.wait()
            packed = local_copies([(feed, feedo_ref)], here.at[pl.ds(4 + len(pairs), 1)])
    gather.third_hop()
    gather.last()
    gather.finish()
    for each in lines:
        each.finish()
    for copy in local:
        copy.wait()
    packed[0].wait()


def first_exchange(line, x, qkv, wo, gains, gate, up, down):
    plane = lax.axis_size("ctx")
    count = GATHER_COPIES + 6 * (line - 1)
    model = x.shape[1]
    shard = model // line
    width = gate.shape[1] // plane
    own_rows = wo.shape[0] // plane
    feed = (shard, 3 * width)
    packing = 2 * line + shard * line // width + 1
    return pl.pallas_call(
        functools.partial(first_kernel, line),
        out_shape=(
            jax.ShapeDtypeStruct((plane * x.shape[0], model), x.dtype),
            jax.ShapeDtypeStruct((line, *qkv.shape), qkv.dtype),
            jax.ShapeDtypeStruct((line, own_rows, model), wo.dtype),
            jax.ShapeDtypeStruct((line, *gains.shape), gains.dtype),
            jax.ShapeDtypeStruct(feed, gate.dtype),
        ),
        in_specs=in_hbm(1) + anywhere(1) + in_hbm(1) + anywhere(1) + in_hbm(3),
        out_specs=tuple(anywhere(5)),
        scratch_shapes=[
            pltpu.VMEM(feed, gate.dtype),
            pltpu.VMEM(x.shape, x.dtype),
            pltpu.SemaphoreType.DMA((count,)),
            pltpu.SemaphoreType.DMA((count,)),
            pltpu.SemaphoreType.DMA((4 + packing,)),
        ],
        compiler_params=remote_params(1),
        name="first_exchange",
    )(x, qkv, wo, gains, gate, up, down)


def deal_rows(copies, me, pieces, wo_ref, place, recv_first, here):
    to_first = pieces * lax.rem(me, 2)
    line_slot = lax.div(me, 2)

    def copy(piece):
        return copies.make(
            recv_first + piece,
            wo_ref.at[piece],
            place(line_slot),
            {"ctx": to_first + piece},
            recv_first + line_slot,
        )

    for piece in range(pieces):

        @pl.when(to_first + piece != me)
        def _(piece=piece):
            copy(piece).start()

        @pl.when(to_first + piece == me)
        def _(piece=piece):
            pltpu.make_async_copy(wo_ref.at[piece], place(line_slot), here).start()

    def finish(line):
        for slot in range(line):

            @pl.when(2 * slot + lax.div(me, pieces) != me)
            def _(slot=slot):
                copies.make(
                    recv_first, wo_ref.at[0], place(slot), {"ctx": 0}, recv_first + slot
                ).wait_recv()

        for piece in range(pieces):

            @pl.when(to_first + piece != me)
            def _(piece=piece):
                copy(piece).wait_send()

            @pl.when(to_first + piece == me)
            def _(piece=piece):
                pltpu.make_async_copy(wo_ref.at[piece], place(line_slot), here).wait()

    return finish


class NearShares:
    def __init__(self, copies, me, refs, place):
        self.copies, self.me, self.refs, self.place = copies, me, refs, place
        self.first = copies.next
        copies.next += 7

    def copy(self, number):
        me, (own, near_x, near_y) = self.me, self.refs
        half = own.shape[0] // 2
        partner = {"ctx": me ^ 1}
        source, target, peer = (
            lambda: (near_y.at[pl.ds(0, half)], self.place(me ^ 4, 0), {"ctx": me ^ 2}),
            lambda: (near_x.at[pl.ds(half, half)], self.place(me ^ 2, 1), {"ctx": me ^ 4}),
            lambda: (own, self.place(me, None), partner),
            lambda: (near_x, self.place(me ^ 2, None), partner),
            lambda: (near_y, self.place(me ^ 4, None), partner),
            lambda: (self.place(me ^ 6, 0), self.place(me ^ 6, 0), partner),
            lambda: (self.place(me ^ 6, 1), self.place(me ^ 6, 1), partner),
        )[number]()
        return self.copies.make(self.first + number, source, target, peer)

    def begin(self):
        for number in range(5):
            self.copy(number).start()

    def diagonal(self):
        for side in (0, 1):
            self.copies.arrived(self.first + side, self.place(self.me ^ 6, side))
            self.copy(5 + side).start()

    def shared(self, bit):
        if bit == 7:
            for side in (0, 1):
                self.copies.arrived(self.first + 5 + side, self.place(self.me ^ 7, side))
        else:
            self.copies.arrived(self.first + 2 + bit // 2, self.place(self.me ^ bit, None))

    def finish(self):
        for number in range(7):
            self.copy(number).wait_send()


def block_place(ref, rows):
    half = rows // 2

    def place(slot, side):
        if side is None:
            return ref.at[pl.ds(pl.multiple_of(slot * rows, rows), rows), :]
        return ref.at[pl.ds(pl.multiple_of(slot * rows + side * half, half), half), :]

    return place


def second_kernel(
    o_ref,
    wo0_hbm,
    wo2_hbm,
    wo4_hbm,
    dy2_hbm,
    dy4_hbm,
    x_hbm,
    gain_ref,
    own_hbm,
    dy6_hbm,
    residual_hbm,
    normed_hbm,
    scale_ref,
    gained_hbm,
    near_x_hbm,
    near_y_hbm,
    x_ref,
    residual_ref,
    normed_ref,
    gained_ref,
    att,
    wo,
    send,
    recv,
    here,
):
    me = lax.axis_index("ctx")
    rows = x_ref.shape[0]
    half = rows // 2
    middle = wo.shape[0] // 2

    def wo_place(slot, side):
        return wo.at[:, slot] if side is None else wo.at[pl.ds(side * middle, middle), slot]

    own_wo = (wo0_hbm, wo2_hbm, wo4_hbm)
    local = local_copies(
        [
            (o_ref.at[pl.ds(pl.multiple_of(me * rows, rows), rows), :], att.at[me]),
            (x_hbm, x_ref),
        ]
        + [(ref, wo_place(me ^ (2 * number), None)) for number, ref in enumerate(own_wo)],
        here.at[pl.ds(0, 5)],
    )
    start_barrier(me, ALL)
    copies = Copies(send, recv)

    def block(slot):
        return o_ref.at[pl.ds(pl.multiple_of(slot * rows, rows), rows), :]

    numbers = {}
    for bit in (6, 7, 4, 5, 2, 3, 1):
        numbers[bit] = copies.number()
        copies.send(numbers[bit], block(me ^ bit), att.at[me], {"ctx": me ^ bit})
    shares = NearShares(copies, me, own_wo, wo_place)
    shares.begin()
    dy_first = copies.next
    copies.next += 2
    upper, lower = pl.ds(0, half), pl.ds(half, half)
    copies.send(dy_first, dy4_hbm.at[upper, :], dy6_hbm.at[upper, :], {"ctx": me ^ 2})
    copies.send(dy_first + 1, dy2_hbm.at[lower, :], dy6_hbm.at[lower, :], {"ctx": me ^ 4})
    shares.diagonal()
    for bit in (1, 3, 5, 7):
        shares.shared(bit)
    for bit, number in numbers.items():
        copies.arrived(number, att.at[me ^ bit])
    for copy in local:
        copy.wait()
    per_head = 2 * GROUP
    own = wo.at[lax.div(me, 2), pl.ds(per_head * lax.rem(me, 2), per_head)]
    keep = local_copies([(own, own_hbm)], here.at[pl.ds(5, 1)])
    plane = att.shape[0]
    near = copies.next
    for side in (0, 1):
        at = pl.ds(side * half, half)
        total = x_ref[at, :].astype(jnp.float32)
        for slot in range(plane):
            first = per_head * (slot % 2)
            weight = jnp.concatenate(
                [wo[slot // 2, first + piece] for piece in range(per_head)], axis=0
            )
            total = total + contract(att[slot, at, :], weight, 1, 0)
        residual_ref[at, :] = total
        scale = lax.rsqrt(jnp.mean(total * total, axis=-1, keepdims=True) + norm_epsilon)
        normed = total * scale
        scale_ref[at, :] = scale
        normed_ref[at, :] = normed
        gained_ref[at, :] = (normed * gain_ref[...]).astype(jnp.bfloat16)
        for number, target, bit in ((0, near_x_hbm, 2), (1, near_y_hbm, 4)):
            copies.send(
                near + 2 * side + number,
                gained_ref.at[at, :],
                target.at[at, :],
                {"ctx": me ^ bit},
            )
    keep += local_copies(
        [(residual_ref, residual_hbm), (normed_ref, normed_hbm), (gained_ref, gained_hbm)],
        here.at[pl.ds(6, 3)],
    )
    for copy in keep:
        copy.wait()
    shares.finish()
    copies.arrived(dy_first, dy6_hbm.at[upper, :])
    copies.arrived(dy_first + 1, dy6_hbm.at[lower, :])
    for side in (0, 1):
        at = pl.ds(side * half, half)
        copies.arrived(near + 2 * side, near_x_hbm.at[at, :])
        copies.arrived(near + 2 * side + 1, near_y_hbm.at[at, :])
    copies.finish()


def second_exchange(o, own_wo, grads, x, gain):
    plane = lax.axis_size("ctx")
    rows = x.shape[0]
    line, part, model = own_wo[0].shape
    count = 7 + 7 + 2 + 4
    f32 = jnp.float32
    return pl.pallas_call(
        second_kernel,
        out_shape=(
            jax.ShapeDtypeStruct((2 * GROUP, part, model), own_wo[0].dtype),
            jax.ShapeDtypeStruct((rows, model), x.dtype),
            jax.ShapeDtypeStruct((rows, model), f32),
            jax.ShapeDtypeStruct((rows, model), f32),
            jax.ShapeDtypeStruct((rows, 1), f32),
            *[jax.ShapeDtypeStruct((rows, model), x.dtype)] * 3,
        ),
        in_specs=in_hbm(7) + in_vmem(1),
        out_specs=(*anywhere(4), *in_vmem(1), *anywhere(3)),
        scratch_shapes=[
            pltpu.VMEM(x.shape, x.dtype),
            pltpu.VMEM(x.shape, f32),
            pltpu.VMEM(x.shape, f32),
            pltpu.VMEM(x.shape, x.dtype),
            pltpu.VMEM((plane, rows, o.shape[1]), o.dtype),
            pltpu.VMEM((line, plane, part, model), x.dtype),
            pltpu.SemaphoreType.DMA((count,)),
            pltpu.SemaphoreType.DMA((count,)),
            pltpu.SemaphoreType.DMA((9,)),
        ],
        compiler_params=remote_params(2),
        name="second_exchange",
    )(o, *own_wo, *grads, x, gain)


def near_kernel(own_hbm, near_x_hbm, near_y_hbm, whole_ref, send, recv, here):
    me = lax.axis_index("ctx")
    refs = (own_hbm, near_x_hbm, near_y_hbm)
    place = block_place(whole_ref, own_hbm.shape[0])
    local = local_copies(
        [(ref, place(me ^ (2 * number), None)) for number, ref in enumerate(refs)], here
    )
    start_barrier(me, NEAR)
    copies = Copies(send, recv)
    shares = NearShares(copies, me, refs, place)
    shares.begin()
    shares.diagonal()
    for bit in (1, 3, 5, 7):
        shares.shared(bit)
    for copy in local:
        copy.wait()
    shares.finish()


def near_gather(refs, number):
    plane = lax.axis_size("ctx")
    rows, columns = refs[0].shape
    return pl.pallas_call(
        near_kernel,
        out_shape=jax.ShapeDtypeStruct((plane * rows, columns), refs[0].dtype),
        in_specs=anywhere(3),
        out_specs=in_vmem(1)[0],
        scratch_shapes=[
            pltpu.SemaphoreType.DMA((7,)),
            pltpu.SemaphoreType.DMA((7,)),
            pltpu.SemaphoreType.DMA((3,)),
        ],
        compiler_params=remote_params(number, 24),
    )(*refs)


def third_kernel(
    g0_hbm, g2_hbm, g4_hbm, ot_hbm, wo_hbm, do_ref, dwo_ref, ot_ref, wo_ref, all_grads, dwo, send, recv, here
):
    me = lax.axis_index("ctx")
    rows = g0_hbm.shape[0]
    place = block_place(all_grads, rows)
    own_rows = (g0_hbm, g2_hbm, g4_hbm)
    fetch = local_copies(
        [(ref, place(me ^ (2 * number), None)) for number, ref in enumerate(own_rows)]
        + [(ot_hbm, ot_ref), (wo_hbm, wo_ref)],
        here,
    )
    start_barrier(me, NEAR)
    copies = Copies(send, recv)
    shares = NearShares(copies, me, own_rows, place)
    shares.begin()
    dwo[...] = jnp.zeros_like(dwo)
    for copy in fetch:
        copy.wait()

    def step(order, carry):
        @pl.when(order == 5)
        def _():
            shares.diagonal()

        for bit in (1, 3, 5, 7):

            @pl.when(order == bit)
            def _(bit=bit):
                shares.shared(bit)

        here_rows = pl.ds(pl.multiple_of((me ^ order) * rows, rows), rows)
        grads = all_grads[here_rows, :]
        do_ref[here_rows, :] = contract(grads, wo_ref[...], 1, 1).astype(jnp.bfloat16)
        dwo[...] += contract(ot_ref[:, here_rows], grads, 1, 0)
        return carry

    lax.fori_loop(0, 8, step, 0)
    line, _, across = dwo_ref.shape
    for slot in range(line):
        rows_at = slice(slot * HALF, (slot + 1) * HALF)
        for number in range(dwo.shape[1] // across):
            columns = slice(number * across, (number + 1) * across)
            dwo_ref[slot, number * HALF : (number + 1) * HALF, :] = dwo[rows_at, columns].astype(
                jnp.bfloat16
            )
    shares.finish()


def third_exchange(line, own_rows, ot, wo, across):
    plane = lax.axis_size("ctx")
    rows, model = own_rows[0].shape
    half_type, f32 = jnp.bfloat16, jnp.float32
    return pl.pallas_call(
        third_kernel,
        out_shape=(
            jax.ShapeDtypeStruct((plane * rows, wo.shape[0]), half_type),
            jax.ShapeDtypeStruct((line, HALF * model // across, across), half_type),
        ),
        in_specs=anywhere(5),
        out_specs=tuple(in_vmem(2)),
        scratch_shapes=[
            pltpu.VMEM(ot.shape, ot.dtype),
            pltpu.VMEM(wo.shape, wo.dtype),
            pltpu.VMEM((plane * rows, model), half_type),
            pltpu.VMEM((line * HALF, model), f32),
            pltpu.SemaphoreType.DMA((7,)),
            pltpu.SemaphoreType.DMA((7,)),
            pltpu.SemaphoreType.DMA((5,)),
        ],
        compiler_params=remote_params(6),
        name="third_exchange",
    )(*own_rows, ot, wo)


REDUCE_COPIES = 10


class PlaneReduce:
    def __init__(self, copies, me, block, heard, held, landed):
        self.copies, self.me, self.block = copies, me, block
        self.heard, self.held, self.landed = heard, held, landed
        self.first = copies.next
        copies.next += REDUCE_COPIES
        self.half = heard.shape[1] // 2
        self.x, self.y = {"ctx": me ^ 2}, {"ctx": me ^ 4}

    def side(self, ref, slot, half):
        return ref.at[slot, pl.ds(half * self.half, self.half), :]

    def share(self, order):
        self.shared(order).start()

    def shared(self, order):
        partner = self.me ^ 1
        source = self.block(partner ^ (6, 2, 4, 0)[order])
        return self.copies.make(
            self.first + order, source, self.heard.at[order], {"ctx": partner}
        )

    def combine(self, order, rows, extra=None):
        bit = (6, 2, 4)[order]
        total = self.block(self.me ^ bit)[rows, :].astype(jnp.float32) + self.heard[
            order, rows, :
        ].astype(jnp.float32)
        if extra is not None:
            total = total + extra
        self.held[order, rows, :] = total.astype(self.held.dtype)

    def onward(self, number):
        order, half, peer = {
            4: (0, 0, self.x),
            5: (0, 1, self.y),
            6: (1, 0, self.x),
            7: (2, 1, self.y),
            8: (1, 1, self.x),
            9: (2, 0, self.y),
        }[number]
        held, landed = self.side(self.held, order, half), self.side(self.landed, order, half)
        return self.copies.make(self.first + number, held, landed, peer)

    def finish(self):
        for order in range(4):
            self.shared(order).wait_send()
        for number in range(4, REDUCE_COPIES):
            self.onward(number).wait_send()

    def diagonal_sends(self):
        first, half = self.first, self.half
        self.copies.arrived(first + 0, self.heard.at[0])
        self.combine(0, pl.ds(0, 2 * half))
        self.onward(4).start()
        self.onward(5).start()

    def neighbour_send(self, order):
        first, half = self.first, self.half
        self.copies.arrived(first + order, self.heard.at[order])
        self.combine(order, pl.ds((order - 1) * half, half))
        self.onward(5 + order).start()

    def neighbour_sends(self):
        self.neighbour_send(1)
        self.neighbour_send(2)

    def second_sends(self):
        first, half = self.first, self.half
        upper, lower = pl.ds(0, half), pl.ds(half, half)
        landed, side, arrived = self.landed, self.side, self.copies.arrived
        arrived(first + 5, side(landed, 0, 1))
        self.combine(1, lower, landed[0, lower, :].astype(jnp.float32))
        self.onward(8).start()
        arrived(first + 4, side(landed, 0, 0))
        self.combine(2, upper, landed[0, upper, :].astype(jnp.float32))
        self.onward(9).start()

    def own_share(self):
        self.copies.arrived(self.first + 3, self.heard.at[3])

    def sum_half(self, which):
        first, half = self.first, self.half
        rows = pl.ds(which * half, half)
        self.copies.arrived(first + (6, 8)[which], self.side(self.landed, 1, which))
        self.copies.arrived(first + (9, 7)[which], self.side(self.landed, 2, which))
        return (
            self.block(self.me)[rows, :].astype(jnp.float32)
            + self.heard[3, rows, :].astype(jnp.float32)
            + self.landed[1, rows, :].astype(jnp.float32)
            + self.landed[2, rows, :].astype(jnp.float32)
        )


def feed_kernel(
    line,
    g0_hbm,
    g2_hbm,
    g4_hbm,
    dy0_hbm,
    dy2_hbm,
    dy4_hbm,
    dy6_hbm,
    w_hbm,
    ot_hbm,
    normed_hbm,
    scale_ref,
    gain_ref,
    residual_ref,
    term_ref,
    own_ref,
    near_x_ref,
    near_y_ref,
    dealt_hbm,
    out6_hbm,
    out2_hbm,
    out4_hbm,
    out0_hbm,
    dw_hbm,
    normed_ref,
    w_ref,
    dw_ref,
    down_ref,
    dy_ref,
    all_g,
    hid,
    hid_t,
    gate_t,
    up_t,
    part,
    heard,
    held,
    landed,
    out_mine,
    out_heard,
    send,
    recv,
    here,
):
    me = lax.axis_index("ctx")
    rows = residual_ref.shape[0]
    half = rows // 2
    width, model = down_ref.shape
    blocks = model // width
    unit = width // line
    partner = {"ctx": me ^ 1}

    def at(slot):
        return pl.ds(pl.multiple_of(slot * rows, rows), rows)

    own_grads = (dy0_hbm, dy2_hbm, dy4_hbm, dy6_hbm)
    own_rows = (g0_hbm, g2_hbm, g4_hbm)
    place = block_place(all_g, rows)
    dy_place = block_place(dy_ref, rows)
    local = local_copies(
        [(w_hbm, w_ref)]
        + [(ref, place(me ^ (2 * number), None)) for number, ref in enumerate(own_rows)]
        + [(ref, dy_place(me ^ (2 * number), None)) for number, ref in enumerate(own_grads)]
        + [(normed_hbm, normed_ref)],
        here.at[pl.ds(0, 9)],
    )
    start_barrier(me, ALL)
    copies = Copies(send, recv)
    shares = NearShares(copies, me, own_rows, place)
    shares.begin()
    dy_first = copies.next
    copies.next += 4
    for number, ref in enumerate(own_grads):
        copies.send(dy_first + number, ref, dy_place(me ^ (2 * number), None), partner)
    deal_first = copies.next
    copies.next += ot_hbm.shape[0]
    dealt = deal_rows(
        copies,
        me,
        ot_hbm.shape[0],
        ot_hbm,
        lambda slot: dealt_hbm.at[slot],
        deal_first,
        here.at[9],
    )
    local[0].wait()
    gate_ref, up_ref = w_ref.at[:, :width], w_ref.at[:, width : 2 * width]
    for z in range(line):
        for number in range(blocks):
            source = pl.ds((z * blocks + number) * unit, unit)
            down_ref[pl.ds(z * unit, unit), number * width : (number + 1) * width] = w_ref[
                source, 2 * width :
            ]
    for copy in local[1:]:
        copy.wait()
    gain = gain_ref[...]

    def block(slot):
        return part.at[at(slot), :]

    reduce = PlaneReduce(copies, me, block, heard, held, landed)

    def chunk(order):
        place = at(me ^ order)
        g = all_g[place, :]
        dy = dy_ref[place, :]
        gate_values = contract(g, gate_ref[...], 1, 0)
        up_values = contract(g, up_ref[...], 1, 0)
        sigmoid_gate = 1.0 / (1.0 + jnp.exp(-gate_values))
        activated = gate_values * sigmoid_gate
        hidden_act = (activated * up_values).astype(jnp.bfloat16)
        hid[place, :] = hidden_act
        hid_t[:, place] = hidden_act.T
        grad_hidden = contract(dy, down_ref[...], 1, 1)
        grad_gate = (
            grad_hidden * up_values * sigmoid_gate * (1.0 + gate_values * (1.0 - sigmoid_gate))
        ).astype(jnp.bfloat16)
        grad_up = (grad_hidden * activated).astype(jnp.bfloat16)
        gate_t[:, place] = grad_gate.T
        up_t[:, place] = grad_up.T
        part[place, :] = (
            contract(grad_gate, gate_ref[...], 1, 1) + contract(grad_up, up_ref[...], 1, 1)
        ).astype(jnp.bfloat16)

    def step(number, carry):
        @pl.when(number == 1)
        def _():
            shares.shared(3)
            copies.arrived(dy_first + 1, dy_place(me ^ 3, None))

        @pl.when(number == 2)
        def _():
            reduce.share(1)
            shares.diagonal()

        @pl.when(number == 3)
        def _():
            reduce.neighbour_send(1)
            shares.shared(7)
            copies.arrived(dy_first + 3, dy_place(me ^ 7, None))

        @pl.when(number == 4)
        def _():
            reduce.share(0)
            reduce.diagonal_sends()

        @pl.when(number == 5)
        def _():
            shares.shared(5)
            copies.arrived(dy_first + 2, dy_place(me ^ 5, None))

        @pl.when(number == 6)
        def _():
            reduce.share(2)
            reduce.neighbour_send(2)

        @pl.when(number == 7)
        def _():
            reduce.second_sends()
            shares.shared(1)
            copies.arrived(dy_first, dy_place(me ^ 1, None))

        pair = lax.div(number, 2)
        chunk(
            lax.rem(number, 2)
            + jnp.where(pair == 0, 2, jnp.where(pair == 1, 6, jnp.where(pair == 2, 4, 0)))
        )
        return carry

    lax.fori_loop(0, 8, step, 0)
    reduce.share(3)
    out_first = copies.next
    copies.next += 4

    def bit_of(number):
        return jnp.where(number == 0, 6, jnp.where(number == 3, 0, 2 * number))

    def out_copy(number):
        return copies.make(out_first + number, out_mine.at[number], out_heard.at[number], partner)

    def out_of(slot):
        return contract(hid[at(slot), :], down_ref[...], 1, 0)

    def give(number, carry):
        out_mine[number] = out_of(me ^ 1 ^ bit_of(number)).astype(jnp.bfloat16)
        out_copy(number).start()
        return carry

    def keep(number, carry):
        total = out_of(me ^ bit_of(number))
        out_copy(number).wait_recv()
        out_heard[number] = (total + out_heard[number].astype(jnp.float32)).astype(jnp.bfloat16)
        return carry

    def weights(number, carry):
        columns = pl.ds(pl.multiple_of(number * width, width), width)
        total = contract(hid_t[...], dy_ref[:, columns], 1, 0).astype(jnp.bfloat16)
        for z in range(line):
            target = pl.ds(pl.multiple_of((z * blocks + number) * unit, unit), unit)
            dw_ref[target, 2 * width :] = total[z * unit : (z + 1) * unit, :]
        for side, left in enumerate((gate_t, up_t)):
            total = contract(left[...], all_g[:, columns], 1, 0).astype(jnp.bfloat16)
            dw_ref[columns, side * width : (side + 1) * width] = total.T
        return carry

    reduce.own_share()
    lax.fori_loop(0, 4, give, 0)
    near = copies.next
    copies.next += 4
    total = jnp.zeros_like(gain)
    for which in (1, 0):
        rows_at = pl.ds(which * half, half)
        grad_normed, normed = reduce.sum_half(which), normed_ref[rows_at, :]
        scaled = grad_normed * gain
        mean = jnp.mean(scaled * normed, axis=-1, keepdims=True)
        total = total + jnp.sum(grad_normed * normed, axis=0, keepdims=True)
        dy = dy_ref[pl.ds(pl.multiple_of(me * rows + which * half, half), half), :]
        residual = dy.astype(jnp.float32) + scale_ref[rows_at, :] * (scaled - normed * mean)
        residual_ref[rows_at, :] = residual
        own_ref[rows_at, :] = residual.astype(jnp.bfloat16)
        for number, target, bit in ((0, near_x_ref, 2), (1, near_y_ref, 4)):
            copies.send(
                near + 2 * which + number,
                own_ref.at[rows_at, :],
                target.at[rows_at, :],
                {"ctx": me ^ bit},
            )
    term_ref[...] = total
    lax.fori_loop(0, 4, keep, 0)
    outputs = local_copies(
        [
            (out_heard.at[number], ref)
            for number, ref in enumerate((out6_hbm, out2_hbm, out4_hbm, out0_hbm))
        ],
        here.at[pl.ds(0, 4)],
    )
    lax.fori_loop(0, blocks, weights, 0)
    outputs += local_copies([(dw_ref, dw_hbm)], here.at[pl.ds(4, 1)])
    for number in range(4):
        out_copy(number).wait_send()
    for copy in outputs:
        copy.wait()
    dealt(dealt_hbm.shape[0])
    shares.finish()
    reduce.finish()
    for which in (1, 0):
        rows_at = pl.ds(which * half, half)
        copies.arrived(near + 2 * which, near_x_ref.at[rows_at, :])
        copies.arrived(near + 2 * which + 1, near_y_ref.at[rows_at, :])
    copies.finish()


def feed(own_rows, grads, w, ot, normed, scale, gain):
    plane, line = lax.axis_size("ctx"), lax.axis_size("fsdp")
    rows, model = own_rows[0].shape
    tokens = plane * rows
    width = w.shape[1] // 3
    pieces = 2 * GROUP
    ot = ot.reshape(pieces, -1, ot.shape[1])
    count = 7 + 4 + pieces + REDUCE_COPIES + 4 + 4
    half_type = jnp.bfloat16
    return pl.pallas_call(
        functools.partial(feed_kernel, line),
        out_shape=(
            jax.ShapeDtypeStruct((rows, model), jnp.float32),
            jax.ShapeDtypeStruct((1, model), jnp.float32),
            *[jax.ShapeDtypeStruct((rows, model), half_type)] * 3,
            jax.ShapeDtypeStruct((line, *ot.shape[1:]), ot.dtype),
            *[jax.ShapeDtypeStruct((rows, model), half_type)] * 4,
            jax.ShapeDtypeStruct(w.shape, half_type),
        ),
        in_specs=anywhere(10) + in_vmem(2),
        out_specs=(*in_vmem(3), *anywhere(8)),
        scratch_shapes=[
            pltpu.VMEM((rows, model), jnp.float32),
            pltpu.VMEM(w.shape, half_type),
            pltpu.VMEM(w.shape, half_type),
            pltpu.VMEM((width, model), half_type),
            pltpu.VMEM((tokens, model), half_type),
            pltpu.VMEM((tokens, model), half_type),
            pltpu.VMEM((tokens, width), half_type),
            pltpu.VMEM((width, tokens), half_type),
            pltpu.VMEM((width, tokens), half_type),
            pltpu.VMEM((width, tokens), half_type),
            pltpu.VMEM((tokens, model), half_type),
            pltpu.VMEM((4, rows, model), half_type),
            pltpu.VMEM((3, rows, model), half_type),
            pltpu.VMEM((3, rows, model), half_type),
            pltpu.VMEM((4, rows, model), half_type),
            pltpu.VMEM((4, rows, model), half_type),
            pltpu.SemaphoreType.DMA((count,)),
            pltpu.SemaphoreType.DMA((count,)),
            pltpu.SemaphoreType.DMA((10,)),
        ],
        compiler_params=pltpu.CompilerParams(
            collective_id=3, has_side_effects=True, vmem_limit_bytes=62 << 20
        ),
        name="feed",
    )(*own_rows, *grads, w, ot, normed, scale, gain)


def input_kernel(
    dqkv_ref,
    wp_hbm,
    x_hbm,
    residual_hbm,
    dwo_hbm,
    gain_ref,
    pad_ref,
    input_ref,
    grads_ref,
    term_ref,
    wp_ref,
    all_x,
    residual_ref,
    dwo_ref,
    part,
    dw,
    heard,
    held,
    landed,
    send,
    recv,
    here,
):
    me = lax.axis_index("ctx")
    rows = residual_ref.shape[0]
    fetch = local_copies(
        [(wp_hbm, wp_ref), (x_hbm, all_x), (residual_hbm, residual_ref), (dwo_hbm, dwo_ref)], here
    )
    start_barrier(me, NEAR)
    copies = Copies(send, recv)

    def at(slot):
        return pl.ds(pl.multiple_of(slot * rows, rows), rows)

    def compute(slot):
        place = at(slot)
        part[place, :] = contract(dqkv_ref[place, :], wp_ref[...], 1, 1).astype(jnp.bfloat16)

    reduce = PlaneReduce(copies, me, lambda slot: part.at[at(slot), :], heard, held, landed)
    fetch[0].wait()
    compute(me ^ 7)
    reduce.share(0)
    compute(me ^ 6)
    compute(me ^ 3)
    reduce.share(1)
    reduce.diagonal_sends()
    compute(me ^ 2)
    compute(me ^ 5)
    reduce.share(2)
    compute(me ^ 4)
    reduce.neighbour_sends()
    compute(me ^ 1)
    reduce.share(3)
    compute(me)
    gain = gain_ref[...]
    dw[...] = jnp.zeros_like(dw)
    for copy in fetch[1:]:
        copy.wait()

    def weights(slot, carry):
        place = at(slot)
        x = all_x[place, :].astype(jnp.float32)
        normed = x * lax.rsqrt(jnp.mean(x * x, axis=-1, keepdims=True) + norm_epsilon)
        gained = (normed * gain).astype(jnp.bfloat16)
        dw[...] += contract(dqkv_ref[place, :], gained, 0, 0)
        return carry

    plane = part.shape[0] // rows
    lax.fori_loop(0, plane // 2, weights, 0)
    reduce.second_sends()
    reduce.own_share()
    lax.fori_loop(plane // 2, plane, weights, 0)
    packed = contract(pad_ref[...], dw[...].astype(jnp.bfloat16), 1, 0)
    packed = packed.astype(jnp.bfloat16).T
    line = dwo_ref.shape[0]
    shard = packed.shape[0] // line
    for slot in range(line):
        grads_ref[slot, :shard, :] = packed[slot * shard : (slot + 1) * shard, :]
        grads_ref[slot, shard:, :] = dwo_ref[slot]
    half = rows // 2
    total = jnp.zeros_like(gain)
    for which in (1, 0):
        here_rows = pl.ds(which * half, half)
        grad = reduce.sum_half(which)
        own_rows = pl.ds(pl.multiple_of(me * rows + which * half, half), half)
        x = all_x[own_rows, :].astype(jnp.float32)
        scale = lax.rsqrt(jnp.mean(x * x, axis=-1, keepdims=True) + norm_epsilon)
        normed = x * scale
        total = total + jnp.sum(grad * normed, axis=0, keepdims=True)
        scaled = grad * gain
        mean = jnp.mean(scaled * normed, axis=-1, keepdims=True)
        input_ref[0, here_rows, :] = residual_ref[here_rows, :] + scale * (scaled - normed * mean)
    term_ref[...] = total
    reduce.finish()
    copies.finish()


def input_exchange(dqkv, wp, x, residual, dwo, gain, pad):
    rows, model = residual.shape
    line, dealt, across = dwo.shape
    f32 = jnp.float32
    return pl.pallas_call(
        input_kernel,
        out_shape=(
            jax.ShapeDtypeStruct((1, rows, model), f32),
            jax.ShapeDtypeStruct((line, model // line + dealt, across), dwo.dtype),
            jax.ShapeDtypeStruct((1, model), f32),
        ),
        in_specs=in_vmem(1) + in_hbm(4) + in_vmem(2),
        out_specs=tuple(in_vmem(3)),
        scratch_shapes=[
            pltpu.VMEM(wp.shape, wp.dtype),
            pltpu.VMEM(x.shape, x.dtype),
            pltpu.VMEM(residual.shape, residual.dtype),
            pltpu.VMEM(dwo.shape, dwo.dtype),
            pltpu.VMEM(x.shape, x.dtype),
            pltpu.VMEM((dqkv.shape[1], model), f32),
            pltpu.VMEM((4, rows, model), x.dtype),
            pltpu.VMEM((3, rows, model), x.dtype),
            pltpu.VMEM((3, rows, model), x.dtype),
            pltpu.SemaphoreType.DMA((REDUCE_COPIES,)),
            pltpu.SemaphoreType.DMA((REDUCE_COPIES,)),
            pltpu.SemaphoreType.DMA((4,)),
        ],
        compiler_params=remote_params(7),
        name="input_exchange",
    )(dqkv, wp, x, residual, dwo, gain, pad)


def pieces_kernel(
    line,
    piece_ref,
    residual_hbm,
    out0_hbm,
    out2_hbm,
    out4_hbm,
    out6_hbm,
    term_one_ref,
    term_two_ref,
    whole_ref,
    total_ref,
    output_ref,
    own,
    residual_ref,
    outs_ref,
    terms,
    terms_heard,
    plane_sum,
    across,
    send,
    recv,
    here,
):
    me, index = lax.axis_index("ctx"), lax.axis_index("fsdp")
    outs = (out0_hbm, out2_hbm, out4_hbm, out6_hbm)
    fetch = local_copies(
        [(piece_ref, own), (residual_hbm, residual_ref)]
        + [(ref, outs_ref.at[number]) for number, ref in enumerate(outs)],
        here.at[pl.ds(0, 6)],
    )
    start_barrier(me, ALL, range(1, line), index, line)
    copies = Copies(send, recv)
    rows = piece_ref.shape[0]
    part = row_part(whole_ref, rows)
    gather = PlaneGather(copies, me, row_half(own, rows), part)
    first = copies.next
    copies.next += 7 + line - 1
    terms[0:1, :] = term_one_ref[...]
    terms[1:2, :] = term_two_ref[...]
    for bit in range(1, 8):
        copies.send(first + bit - 1, terms, terms_heard.at[bit], {"ctx": me ^ bit})
    fetch[0].wait()
    gather.begin()
    local = local_copies([(own, part(me, slice(None)))], here.at[pl.ds(6, 1)])
    total = terms[...]
    for bit in range(1, 8):
        copies.arrived(first + bit - 1, terms_heard.at[bit])
        total = total + terms_heard[bit]
    plane_sum[...] = total
    for step in range(1, line):
        peer = {"fsdp": lax.rem(index + step, line)}
        copies.send(first + 6 + step, plane_sum, across.at[step], peer)
    for copy in fetch[1:]:
        copy.wait()
    total = residual_ref[...]
    for number in range(4):
        total = total + outs_ref[number].astype(jnp.float32)
    output_ref[0] = total.astype(output_ref.dtype)
    gather.first_hop()
    gather.second_hop()
    total = plane_sum[...]
    for step in range(1, line):
        copies.arrived(first + 6 + step, across.at[step])
        total = total + across[step]
    total_ref[...] = total
    gather.third_hop()
    gather.last()
    gather.finish()
    local[0].wait()
    copies.finish()


def pieces_exchange(line, piece, term_one, term_two, residual, outs):
    plane = lax.axis_size("ctx")
    rows, model = residual.shape
    f32 = jnp.float32
    copies = GATHER_COPIES + 7 + line - 1
    return pl.pallas_call(
        functools.partial(pieces_kernel, line),
        out_shape=(
            jax.ShapeDtypeStruct((plane * piece.shape[0], piece.shape[1]), piece.dtype),
            jax.ShapeDtypeStruct((2, model), f32),
            jax.ShapeDtypeStruct((1, rows, model), jnp.bfloat16),
        ),
        in_specs=anywhere(6) + in_vmem(2),
        out_specs=(*anywhere(1), *in_vmem(2)),
        scratch_shapes=[
            pltpu.VMEM(piece.shape, piece.dtype),
            pltpu.VMEM((rows, model), f32),
            pltpu.VMEM((4, rows, model), outs[0].dtype),
            pltpu.VMEM((2, model), f32),
            pltpu.VMEM((plane, 2, model), f32),
            pltpu.VMEM((2, model), f32),
            pltpu.VMEM((line, 2, model), f32),
            pltpu.SemaphoreType.DMA((copies,)),
            pltpu.SemaphoreType.DMA((copies,)),
            pltpu.SemaphoreType.DMA((7,)),
        ],
        compiler_params=remote_params(8),
        name="pieces_exchange",
    )(piece, residual, *outs, term_one, term_two)


def spread_kernel(gate_in, up_in, down_in, gate_ref, up_ref, down_ref):
    plane, shard, unit = gate_in.shape
    for source, target in ((gate_in, gate_ref), (up_in, up_ref)):
        for slot in range(plane):
            target[:, slot * unit : (slot + 1) * unit] = source[slot].astype(jnp.float32)
    width = down_in.shape[2]
    blocks = shard // unit
    for slot in range(down_in.shape[0]):
        for number in range(blocks):
            down_ref[slot * unit : (slot + 1) * unit, number * width : (number + 1) * width] = (
                down_in[slot, number * unit : (number + 1) * unit, :].astype(jnp.float32)
            )


def spread_feed(pieces, shard, line, unit):
    plane = lax.axis_size("ctx")
    width = line * unit
    model = line * shard
    pieces = pieces.reshape(plane, shard, 3 * width)
    each = plane // line
    return pl.pallas_call(
        spread_kernel,
        grid=(line,),
        in_specs=[
            pl.BlockSpec((plane, shard, unit), lambda z: (0, 0, z)),
            pl.BlockSpec((plane, shard, unit), lambda z: (0, 0, line + z)),
            pl.BlockSpec((each, shard, width), lambda z: (z, 0, 2)),
        ],
        out_specs=(
            pl.BlockSpec((shard, plane * unit), lambda z: (0, z)),
            pl.BlockSpec((shard, plane * unit), lambda z: (0, z)),
            pl.BlockSpec((each * unit, model), lambda z: (z, 0)),
        ),
        out_shape=(
            jax.ShapeDtypeStruct((shard, plane * width), jnp.float32),
            jax.ShapeDtypeStruct((shard, plane * width), jnp.float32),
            jax.ShapeDtypeStruct((plane * unit, model), jnp.float32),
        ),
        compiler_params=pltpu.CompilerParams(vmem_limit_bytes=62 << 20),
        name="spread_feed",
    )(pieces, pieces, pieces)


def spread_attention_kernel(in_ref, q_ref, k_ref, v_ref, wo_ref):
    plane, _, across = in_ref.shape
    shard = q_ref.shape[0]
    key_width = k_ref.shape[1] // plane
    query_width = q_ref.shape[1] // plane
    first = 0
    for target, width in ((q_ref, query_width), (k_ref, key_width), (v_ref, key_width)):
        target[...] = jnp.concatenate(
            [
                in_ref[slot, :shard, first : first + width].astype(jnp.float32)
                for slot in range(plane)
            ],
            axis=1,
        )
        first += width
    for slot in range(plane):
        for number in range(wo_ref.shape[1] // across):
            source = slice(shard + number * HALF, shard + (number + 1) * HALF)
            wo_ref[slot * HALF : (slot + 1) * HALF, number * across : (number + 1) * across] = (
                in_ref[slot, source, :].astype(jnp.float32)
            )


def spread_attention(pieces, shard, model, query_width, key_width):
    plane = lax.axis_size("ctx")
    pieces = pieces.reshape(plane, -1, pieces.shape[1])
    f32 = jnp.float32
    return pl.pallas_call(
        spread_attention_kernel,
        in_specs=in_vmem(1),
        out_specs=tuple(in_vmem(4)),
        out_shape=(
            jax.ShapeDtypeStruct((shard, plane * query_width), f32),
            jax.ShapeDtypeStruct((shard, plane * key_width), f32),
            jax.ShapeDtypeStruct((shard, plane * key_width), f32),
            jax.ShapeDtypeStruct((plane * HALF, model), f32),
        ),
        compiler_params=pltpu.CompilerParams(vmem_limit_bytes=40 << 20),
        name="spread_attention",
    )(pieces)


def head_local(
    block_input,
    block_table,
    output_grad,
    attention_gain,
    query_weight,
    key_weight,
    value_projection,
    output_weight,
    feedforward_gain,
    gate_weight,
    up_weight,
    down_weight,
):
    me = lax.axis_index("ctx")
    plane = lax.axis_size("ctx")
    line = lax.axis_size("fsdp")
    rows, model = block_input.shape[1:]
    shard = model // line
    hidden = gate_weight.shape[1]
    unit = hidden // (line * plane)
    table_row = block_table[0]
    slot_count = table_row.shape[0]
    block = rows * plane // slot_count
    places = jnp.arange(slot_count, dtype=jnp.int32)
    slots = jnp.sum(jnp.where(table_row[None, :] == places[:, None], places[None, :], 0), axis=1)

    def mine(array, width):
        return lax.dynamic_slice_in_dim(array, me * width, width, 1)

    query_width = query_weight.shape[1] // plane
    key_width = key_weight.shape[1] // plane
    qkv_mine = jnp.concatenate(
        [
            mine(query_weight, query_width),
            mine(key_weight, key_width),
            mine(value_projection, key_width),
        ],
        axis=1,
    )
    gains_mine = jnp.stack([attention_gain, feedforward_gain])
    x_all, qkv_w, wo_line, gains, feed_mine = first_exchange(
        line,
        block_input[0],
        qkv_mine,
        output_weight,
        gains_mine,
        gate_weight,
        up_weight,
        down_weight,
    )
    feed_w = lax.all_gather(feed_mine, "fsdp", axis=0, tiled=True)

    steps_index = jnp.arange(HALF, dtype=jnp.float32)
    inverse = jnp.exp(steps_index * jnp.float32(-2.0 * math.log(rotary_base) / HEAD_SIZE))

    def table_of(positions):
        angles = positions.astype(jnp.float32)[:, None] * inverse[None, :]
        both = jnp.stack([jnp.cos(angles), jnp.sin(angles)])
        both = jnp.pad(both, ((0, 0), (0, 0), (0, LANES // 2 - HALF)))
        return jnp.concatenate([both, both], axis=2)

    inner = table_of(jnp.arange(block, dtype=jnp.int32))
    outer = table_of(places * block)
    pad = padding(GROUP + 2)

    gains = jnp.transpose(gains, (1, 0, 2)).reshape(2, model).astype(jnp.float32)
    qkv_w = qkv_w.reshape(model, -1)
    grad_rows, wo_line, x_all = lax.optimization_barrier((output_grad[0], wo_line, x_all))
    grad_parts, wo_parts = [grad_rows], [wo_line]
    for bit in (2, 4):
        pairs = [(device, device ^ bit) for device in range(plane)]
        grad_parts.append(lax.ppermute(grad_rows, "ctx", pairs))
        wo_parts.append(lax.ppermute(wo_line, "ctx", pairs))
    qkv, o, o_columns, lse, qkv_pad = attend(
        slots, x_all, gains[:1], qkv_w, pad, inner, outer
    )
    wo_mine, far_grads, residual, normed_two, scale_two, *gained_two = second_exchange(
        o, wo_parts, grad_parts[1:], block_input[0], gains[1:]
    )
    grad_residual, feedforward_term, *rest = feed(
        gained_two,
        [*grad_parts, far_grads],
        feed_w,
        o_columns,
        normed_two,
        scale_two,
        gains[1:],
    )
    grad_attn, columns_mine, out_parts, feed_grads = rest[:3], rest[3], rest[4:8], rest[8]
    feed_grads = lax.psum_scatter(feed_grads, "fsdp", scatter_dimension=0, tiled=True)
    grad_o, wo_term = third_exchange(
        line,
        grad_attn,
        columns_mine.reshape(-1, columns_mine.shape[2]),
        wo_mine.reshape(-1, model),
        qkv_w.shape[1],
    )
    *out_parts, grad_o = lax.optimization_barrier((*out_parts, grad_o))
    outs = [out_parts[3]]
    for part, bit in enumerate((6, 2, 4)):
        pairs = [(device, device ^ bit) for device in range(plane)]
        outs.append(lax.ppermute(out_parts[part], "ctx", pairs))
    grads = attend_back(slots, qkv, o, grad_o, lse, pad, inner, outer)
    input_grad, attention_grads, attention_term = input_exchange(
        grads, qkv_pad, x_all, grad_residual, wo_term, gains[:1], pad
    )
    attention_grads, feed_grads = lax.optimization_barrier((attention_grads, feed_grads))
    attention_grads = lax.psum_scatter(
        attention_grads.reshape(-1, attention_grads.shape[2]),
        "fsdp",
        scatter_dimension=0,
        tiled=True,
    )
    feed_pieces, gain_terms, layer_output = pieces_exchange(
        line, feed_grads, attention_term, feedforward_term, residual, outs
    )
    attention_grads, gain_terms = lax.optimization_barrier((attention_grads, gain_terms))
    near_grads = []
    for bit in (2, 4):
        pairs = [(device, device ^ bit) for device in range(plane)]
        near_grads.append(lax.ppermute(attention_grads, "ctx", pairs))
    gate_grad, up_grad, down_grad = spread_feed(feed_pieces, shard, line, unit)
    attention_pieces = near_gather([attention_grads, *near_grads], 9)
    query_grad, key_grad, value_grad, out_grad = spread_attention(
        attention_pieces, shard, model, query_width, key_width
    )
    gain_terms = lax.dynamic_slice_in_dim(gain_terms, lax.axis_index("fsdp") * shard, shard, 1)
    return (
        layer_output,
        input_grad,
        gain_terms[0],
        query_grad,
        key_grad,
        value_grad,
        out_grad,
        gain_terms[1],
        gate_grad,
        up_grad,
        down_grad,
    )


def solution(mesh):
    plane, line = mesh.shape["ctx"], mesh.shape["fsdp"]
    fits = plane == KEY_VALUE_HEADS == 8 and plane * line * HALF == QUERY_HEADS * HEAD_SIZE
    if fits:
        return placed(mesh, head_local)
    return placed(mesh, local)


def placed(mesh, plan):
    return jax.shard_map(
        plan,
        mesh=mesh,
        in_specs=(
            P("fsdp", "ctx", None),
            P("fsdp", None),
            P("fsdp", "ctx", None),
            P("fsdp"),
            P("fsdp", None),
            P("fsdp", None),
            P("fsdp", None),
            P("fsdp", None),
            P("fsdp"),
            P("fsdp", None),
            P("fsdp", None),
            P("fsdp", None),
        ),
        out_specs=(
            P("fsdp", "ctx", None),
            P("fsdp", "ctx", None),
            P("fsdp"),
            P("fsdp", None),
            P("fsdp", None),
            P("fsdp", None),
            P("fsdp", None),
            P("fsdp"),
            P("fsdp", None),
            P("fsdp", None),
            P("fsdp", None),
        ),
        check_vma=False,
    )
```

```python
import functools
import math

import jax
import jax.numpy as jnp
import numpy as np
from jax import lax
from jax.experimental import pallas as pl
from jax.experimental.pallas import tpu as pltpu
from jax.sharding import PartitionSpec as P


QUERY_HEADS = 16
KEY_VALUE_HEADS = 8
HEAD_SIZE = 96


norm_epsilon = 1e-05
rotary_base = 100000.0
score_with_mask = -1e30


def rope_tables(positions):
    half_width = HEAD_SIZE // 2
    steps_index = jnp.arange(half_width, dtype=jnp.float32)
    inverse = jnp.exp(steps_index * jnp.float32(-2.0 * math.log(rotary_base) / HEAD_SIZE))
    angles = positions.astype(jnp.float32)[:, None] * inverse[None, :]
    return (jnp.cos(angles), jnp.sin(angles))


def rotate(value_rows, cosine, sine_values, direction):
    count_of_rows = value_rows.shape[0]
    head_count = value_rows.shape[1] // HEAD_SIZE
    half_width = HEAD_SIZE // 2
    shaped = value_rows.reshape(count_of_rows, head_count, HEAD_SIZE)
    first_half = shaped[:, :, :half_width]
    second_half = shaped[:, :, half_width:]
    cos_part = cosine[:, None, :]
    sin_part = sine_values[:, None, :] * direction
    turned = jnp.concatenate(
        [
            first_half * cos_part - second_half * sin_part,
            second_half * cos_part + first_half * sin_part,
        ],
        axis=2,
    )
    return turned.reshape(count_of_rows, head_count * HEAD_SIZE)


def norm_scale(value_rows):
    return lax.rsqrt(jnp.mean(value_rows * value_rows, axis=-1, keepdims=True) + norm_epsilon)


def product(matrix, operand):
    return jnp.dot(matrix, operand, preferred_element_type=jnp.float32)


def cross_rows(matrix, operand):
    return lax.dot_general(
        matrix, operand, (((0,), (0,)), ((), ())), preferred_element_type=jnp.float32
    )


def back_product(matrix, operand):
    return lax.dot_general(
        matrix, operand, (((1,), (1,)), ((), ())), preferred_element_type=jnp.float32
    )


def block_scores(query_rank_four, block_of_keys, query_positions, key_positions):
    keys_rank_three = block_of_keys.reshape(block_of_keys.shape[0], KEY_VALUE_HEADS, HEAD_SIZE)
    scores = jnp.einsum(
        "rgjd,kgd->gjrk", query_rank_four, keys_rank_three, preferred_element_type=jnp.float32
    ) * HEAD_SIZE ** (-0.5)
    allowed = (key_positions[None, :] <= query_positions[:, None])[None, None]
    return (jnp.where(allowed, scores, score_with_mask), allowed)


def local(
    block_input,
    block_table,
    output_grad,
    attention_gain,
    query_weight,
    key_weight,
    value_projection,
    output_weight,
    feedforward_gain,
    gate_weight,
    up_weight,
    down_weight,
):
    query_group_width = QUERY_HEADS // KEY_VALUE_HEADS
    score_scale = HEAD_SIZE ** (-0.5)
    inputs = block_input[0].astype(jnp.float32)
    count_of_rows = inputs.shape[0]
    block_rows = count_of_rows // 2
    ctx_index = lax.axis_index("ctx")
    table_row = block_table[0]
    offsets = jnp.arange(block_rows, dtype=jnp.int32)
    query_blocks = lax.dynamic_slice_in_dim(table_row, 2 * ctx_index, 2)
    query_positions = (query_blocks[:, None] * block_rows + offsets[None, :]).reshape(count_of_rows)
    key_positions = (table_row[:, None] * block_rows + offsets[None, :]).reshape(-1)
    cosine, sine_values = rope_tables(query_positions)
    gain_one, query_full, key_full, value_full, out_full = (
        lax.all_gather(attention_gain, "fsdp", axis=0, tiled=True),
        lax.all_gather(query_weight, "fsdp", axis=0, tiled=True),
        lax.all_gather(key_weight, "fsdp", axis=0, tiled=True),
        lax.all_gather(value_projection, "fsdp", axis=0, tiled=True),
        lax.all_gather(output_weight, "fsdp", axis=0, tiled=True),
    )
    scale_one = norm_scale(inputs)
    normed_one = inputs * scale_one
    gained_one = (normed_one * gain_one.astype(jnp.float32)).astype(jnp.bfloat16)
    query_rows = rotate(product(gained_one, query_full), cosine, sine_values, 1.0).astype(
        jnp.bfloat16
    )
    keys_local = rotate(product(gained_one, key_full), cosine, sine_values, 1.0).astype(
        jnp.bfloat16
    )
    values_local = product(gained_one, value_full).astype(jnp.bfloat16)
    keys_all, values_all = (
        lax.all_gather(keys_local, "ctx", axis=0, tiled=True),
        lax.all_gather(values_local, "ctx", axis=0, tiled=True),
    )
    key_total_count = keys_all.shape[0]
    key_block_pass = 1024
    block_count = key_total_count // key_block_pass
    query_rank_four = query_rows.reshape(
        count_of_rows, KEY_VALUE_HEADS, query_group_width, HEAD_SIZE
    )
    key_places = key_positions.reshape(block_count, key_block_pass)

    def split_keys(array_in):
        return array_in.reshape(block_count, key_block_pass, array_in.shape[-1])

    def statistics_step(state_now, block_data):
        running_max, running_sum = state_now
        block_of_keys, key_place = block_data
        masked, allowed = block_scores(query_rank_four, block_of_keys, query_positions, key_place)
        new_max = jnp.maximum(running_max, jnp.max(masked, axis=-1))
        block_sum = jnp.sum(jnp.where(allowed, jnp.exp(masked - new_max[..., None]), 0.0), axis=-1)
        return ((new_max, running_sum * jnp.exp(running_max - new_max) + block_sum), None)

    initial_maximum = jnp.full(
        (KEY_VALUE_HEADS, query_group_width, count_of_rows), score_with_mask, jnp.float32
    )
    initial_sum = jnp.zeros((KEY_VALUE_HEADS, query_group_width, count_of_rows), jnp.float32)
    (final_max, final_sum), unused = lax.scan(
        statistics_step, (initial_maximum, initial_sum), (split_keys(keys_all), key_places)
    )
    log_total = final_max + jnp.log(final_sum)

    def output_step(state_now, block_data):
        block_of_keys, block_of_values, key_place = block_data
        masked, allowed = block_scores(query_rank_four, block_of_keys, query_positions, key_place)
        weights_half = jnp.where(allowed, jnp.exp(masked - log_total[..., None]), 0.0).astype(
            jnp.bfloat16
        )
        values_rank_three = block_of_values.reshape(key_block_pass, KEY_VALUE_HEADS, HEAD_SIZE)
        return (
            state_now
            + jnp.einsum(
                "gjrk,kgd->rgjd",
                weights_half,
                values_rank_three,
                preferred_element_type=jnp.float32,
            ),
            None,
        )

    initial_output = jnp.zeros(
        (count_of_rows, KEY_VALUE_HEADS, query_group_width, HEAD_SIZE), jnp.float32
    )
    summed_out, unused = lax.scan(
        output_step, initial_output, (split_keys(keys_all), split_keys(values_all), key_places)
    )
    attended_rows = summed_out.reshape(count_of_rows, QUERY_HEADS * HEAD_SIZE).astype(jnp.bfloat16)
    residual = inputs + product(attended_rows, out_full)
    scale_two = norm_scale(residual)
    normed_two = residual * scale_two
    gain_two, gate_full, up_full, down_full = (
        lax.all_gather(feedforward_gain, "fsdp", axis=0, tiled=True),
        lax.all_gather(gate_weight, "fsdp", axis=0, tiled=True),
        lax.all_gather(up_weight, "fsdp", axis=0, tiled=True),
        lax.all_gather(down_weight, "fsdp", axis=0, tiled=True),
    )
    gained_two = (normed_two * gain_two.astype(jnp.float32)).astype(jnp.bfloat16)
    gate_values = product(gained_two, gate_full)
    up_values = product(gained_two, up_full)
    sigmoid_gate = jax.nn.sigmoid(gate_values)
    activated = gate_values * sigmoid_gate
    hidden_act = (activated * up_values).astype(jnp.bfloat16)
    layer_output = (residual + product(hidden_act, down_full)).astype(jnp.bfloat16)
    gain_two_again, gate_back, up_back, down_back = (
        lax.all_gather(feedforward_gain, "fsdp", axis=0, tiled=True),
        lax.all_gather(gate_weight, "fsdp", axis=0, tiled=True),
        lax.all_gather(up_weight, "fsdp", axis=0, tiled=True),
        lax.all_gather(down_weight, "fsdp", axis=0, tiled=True),
    )
    grad_rows = output_grad[0]
    grad_hidden = back_product(grad_rows, down_back)
    down_term = cross_rows(hidden_act, grad_rows)
    grad_gate = (
        grad_hidden * up_values * sigmoid_gate * (1.0 + gate_values * (1.0 - sigmoid_gate))
    ).astype(jnp.bfloat16)
    grad_up = (grad_hidden * activated).astype(jnp.bfloat16)
    gate_term = cross_rows(gained_two, grad_gate)
    up_term = cross_rows(gained_two, grad_up)
    grad_normed_two = back_product(grad_gate, gate_back) + back_product(grad_up, up_back)
    feedforward_term = jnp.sum(grad_normed_two * normed_two, axis=0)
    grad_scaled_two = grad_normed_two * gain_two_again.astype(jnp.float32)
    grad_residual = grad_rows.astype(jnp.float32) + scale_two * (
        grad_scaled_two
        - normed_two * jnp.mean(grad_scaled_two * normed_two, axis=-1, keepdims=True)
    )
    gain_one_again, query_back, key_back, value_back, out_back = (
        lax.all_gather(attention_gain, "fsdp", axis=0, tiled=True),
        lax.all_gather(query_weight, "fsdp", axis=0, tiled=True),
        lax.all_gather(key_weight, "fsdp", axis=0, tiled=True),
        lax.all_gather(value_projection, "fsdp", axis=0, tiled=True),
        lax.all_gather(output_weight, "fsdp", axis=0, tiled=True),
    )
    grad_attn = grad_residual.astype(jnp.bfloat16)
    output_term = cross_rows(attended_rows, grad_attn)
    attended_gradient = back_product(grad_attn, out_back).astype(jnp.bfloat16)
    gradient_rank_four = attended_gradient.reshape(
        count_of_rows, KEY_VALUE_HEADS, query_group_width, HEAD_SIZE
    )
    attended_rank_four = attended_rows.reshape(
        count_of_rows, KEY_VALUE_HEADS, query_group_width, HEAD_SIZE
    )
    row_delta = jnp.transpose(
        jnp.sum(
            gradient_rank_four.astype(jnp.float32) * attended_rank_four.astype(jnp.float32), axis=-1
        ),
        (1, 2, 0),
    )
    keys_again, values_again = (
        lax.all_gather(keys_local, "ctx", axis=0, tiled=True),
        lax.all_gather(values_local, "ctx", axis=0, tiled=True),
    )

    def back_step(state_now, block_data):
        block_of_keys, block_of_values, key_place = block_data
        masked, allowed = block_scores(query_rank_four, block_of_keys, query_positions, key_place)
        weights_half = jnp.where(allowed, jnp.exp(masked - log_total[..., None]), 0.0).astype(
            jnp.bfloat16
        )
        values_rank_three = block_of_values.reshape(key_block_pass, KEY_VALUE_HEADS, HEAD_SIZE)
        keys_rank_three = block_of_keys.reshape(key_block_pass, KEY_VALUE_HEADS, HEAD_SIZE)
        grad_weights = jnp.einsum(
            "rgjd,kgd->gjrk",
            gradient_rank_four,
            values_rank_three,
            preferred_element_type=jnp.float32,
        )
        grad_scores = (
            weights_half.astype(jnp.float32) * (grad_weights - row_delta[..., None]) * score_scale
        ).astype(jnp.bfloat16)
        state_now = state_now + jnp.einsum(
            "gjrk,kgd->rgjd", grad_scores, keys_rank_three, preferred_element_type=jnp.float32
        )
        key_gradient = jnp.einsum(
            "gjrk,rgjd->kgd", grad_scores, query_rank_four, preferred_element_type=jnp.float32
        )
        value_gradient = jnp.einsum(
            "gjrk,rgjd->kgd", weights_half, gradient_rank_four, preferred_element_type=jnp.float32
        )
        return (
            state_now,
            (
                key_gradient.reshape(key_block_pass, KEY_VALUE_HEADS * HEAD_SIZE).astype(
                    jnp.bfloat16
                ),
                value_gradient.reshape(key_block_pass, KEY_VALUE_HEADS * HEAD_SIZE).astype(
                    jnp.bfloat16
                ),
            ),
        )

    first_query_index = jnp.zeros(
        (count_of_rows, KEY_VALUE_HEADS, query_group_width, HEAD_SIZE), jnp.float32
    )
    query_sum, (key_gradients, value_gradients) = lax.scan(
        back_step, first_query_index, (split_keys(keys_again), split_keys(values_again), key_places)
    )
    key_gradients = key_gradients.reshape(key_total_count, KEY_VALUE_HEADS * HEAD_SIZE)
    value_gradients = value_gradients.reshape(key_total_count, KEY_VALUE_HEADS * HEAD_SIZE)
    key_sums, value_sums = (
        lax.psum_scatter(key_gradients, "ctx", scatter_dimension=0, tiled=True).astype(jnp.float32),
        lax.psum_scatter(value_gradients, "ctx", scatter_dimension=0, tiled=True).astype(
            jnp.float32
        ),
    )
    query_gradients = rotate(
        query_sum.reshape(count_of_rows, QUERY_HEADS * HEAD_SIZE), cosine, sine_values, -1.0
    ).astype(jnp.bfloat16)
    grad_keys = rotate(key_sums, cosine, sine_values, -1.0).astype(jnp.bfloat16)
    grad_values = value_sums.astype(jnp.bfloat16)
    query_term = cross_rows(gained_one, query_gradients)
    key_term = cross_rows(gained_one, grad_keys)
    value_term = cross_rows(gained_one, grad_values)
    grad_normed_one = (
        back_product(query_gradients, query_back)
        + back_product(grad_keys, key_back)
        + back_product(grad_values, value_back)
    )
    attention_term = jnp.sum(grad_normed_one * normed_one, axis=0)
    grad_scaled_one = grad_normed_one * gain_one_again.astype(jnp.float32)
    input_grad = grad_residual + scale_one * (
        grad_scaled_one
        - normed_one * jnp.mean(grad_scaled_one * normed_one, axis=-1, keepdims=True)
    )
    shares = (
        lax.psum_scatter(
            attention_term.astype(jnp.bfloat16), "fsdp", scatter_dimension=0, tiled=True
        ).astype(jnp.float32),
        lax.psum_scatter(
            query_term.astype(jnp.bfloat16), "fsdp", scatter_dimension=0, tiled=True
        ).astype(jnp.float32),
        lax.psum_scatter(
            key_term.astype(jnp.bfloat16), "fsdp", scatter_dimension=0, tiled=True
        ).astype(jnp.float32),
        lax.psum_scatter(
            value_term.astype(jnp.bfloat16), "fsdp", scatter_dimension=0, tiled=True
        ).astype(jnp.float32),
        lax.psum_scatter(
            output_term.astype(jnp.bfloat16), "fsdp", scatter_dimension=0, tiled=True
        ).astype(jnp.float32),
        lax.psum_scatter(
            feedforward_term.astype(jnp.bfloat16), "fsdp", scatter_dimension=0, tiled=True
        ).astype(jnp.float32),
        lax.psum_scatter(
            gate_term.astype(jnp.bfloat16), "fsdp", scatter_dimension=0, tiled=True
        ).astype(jnp.float32),
        lax.psum_scatter(
            up_term.astype(jnp.bfloat16), "fsdp", scatter_dimension=0, tiled=True
        ).astype(jnp.float32),
        lax.psum_scatter(
            down_term.astype(jnp.bfloat16), "fsdp", scatter_dimension=0, tiled=True
        ).astype(jnp.float32),
    )
    totals = (
        lax.psum(shares[0].astype(jnp.bfloat16), "ctx").astype(jnp.float32),
        lax.psum(shares[1].astype(jnp.bfloat16), "ctx").astype(jnp.float32),
        lax.psum(shares[2].astype(jnp.bfloat16), "ctx").astype(jnp.float32),
        lax.psum(shares[3].astype(jnp.bfloat16), "ctx").astype(jnp.float32),
        lax.psum(shares[4].astype(jnp.bfloat16), "ctx").astype(jnp.float32),
        lax.psum(shares[5].astype(jnp.bfloat16), "ctx").astype(jnp.float32),
        lax.psum(shares[6].astype(jnp.bfloat16), "ctx").astype(jnp.float32),
        lax.psum(shares[7].astype(jnp.bfloat16), "ctx").astype(jnp.float32),
        lax.psum(shares[8].astype(jnp.bfloat16), "ctx").astype(jnp.float32),
    )
    return (
        layer_output[None],
        input_grad[None],
        totals[0],
        totals[1],
        totals[2],
        totals[3],
        totals[4],
        totals[5],
        totals[6],
        totals[7],
        totals[8],
    )


LANES = 128
HALF = HEAD_SIZE // 2
GROUP = QUERY_HEADS // KEY_VALUE_HEADS
score_scale = HEAD_SIZE ** (-0.5)
binary_scale = score_scale * math.log2(math.e)


def contract(left, right, left_dim, right_dim):
    return lax.dot_general(
        left, right, (((left_dim,), (right_dim,)), ((), ())), preferred_element_type=jnp.float32
    )


def in_vmem(count):
    return [pl.BlockSpec(memory_space=pltpu.VMEM)] * count


def padding(heads):
    column = np.arange(heads * HEAD_SIZE)
    target = column // HALF * (LANES // 2) + column % HALF
    lanes = np.arange(heads * LANES)
    return jnp.asarray((target[:, None] == lanes[None, :]).astype(np.float32), jnp.bfloat16)


def angle_table(positions):
    inverse = rotary_base ** (-2.0 * np.arange(HALF) / HEAD_SIZE)
    angles = positions[:, None] * inverse[None, :]
    both = np.stack([np.cos(angles), np.sin(angles)])
    both = np.pad(both, ((0, 0), (0, 0), (0, LANES // 2 - HALF)))
    return jnp.asarray(np.concatenate([both, both], axis=2), jnp.float32)


def turn(part, cosine, sine):
    return part * cosine + pltpu.roll(part, LANES // 2, 1) * sine


def tables(inner_ref, outer_ref, index, per_tile):
    inner_cos, inner_sin = inner_ref[0], inner_ref[1]
    sign = jnp.where(
        lax.broadcasted_iota(jnp.int32, inner_cos.shape, 1) < LANES // 2, -1.0, 1.0
    )
    cosines, sines = [], []
    for part in range(per_tile):
        at = pl.ds(index * per_tile + part, 1)
        outer_cos, outer_sin = outer_ref[0, at, :], outer_ref[1, at, :]
        cosines.append(inner_cos * outer_cos - inner_sin * outer_sin)
        sines.append(sign * (inner_sin * outer_cos + inner_cos * outer_sin))
    return jnp.concatenate(cosines, axis=0), jnp.concatenate(sines, axis=0)


def forward_kernel(
    slot_ref,
    xa_ref,
    xb_ref,
    gain_ref,
    w_ref,
    pad_ref,
    inner_ref,
    outer_ref,
    qkv_hbm,
    o_ref,
    ot_ref,
    lse_ref,
    wp_hbm,
    qkv_ref,
    wp,
    qs,
    vt,
    s_ref,
    here,
):
    index = pl.program_id(0)
    block = xa_ref.shape[0]
    tile = 2 * block
    width = GROUP * tile
    heads = GROUP + 2

    @pl.when(index == 0)
    def _():
        wp[...] = contract(w_ref[...], pad_ref[...], 1, 0).astype(jnp.bfloat16)
        pltpu.make_async_copy(wp, wp_hbm, here.at[1]).start()

    x = jnp.concatenate([xa_ref[...], xb_ref[...]], axis=0).astype(jnp.float32)
    normed = x * lax.rsqrt(jnp.mean(x * x, axis=-1, keepdims=True) + norm_epsilon)
    gained = (normed * gain_ref[...]).astype(jnp.bfloat16)
    raw = contract(gained, wp[...], 1, 0)
    cosine, sine = tables(inner_ref, outer_ref, index, 2)
    here_rows = pl.ds(pl.multiple_of(index * tile, tile), tile)
    for head in range(heads):
        lanes = slice(head * LANES, (head + 1) * LANES)
        part = raw[:, lanes]
        if head <= GROUP:
            part = turn(part, cosine, sine)
        part = part.astype(jnp.bfloat16)
        qkv_ref[here_rows, lanes] = part
        if head < GROUP:
            qs[head * tile : (head + 1) * tile, :] = part
        if head == heads - 1:
            vt[:, here_rows] = part.T

    def save(number):
        place = pl.ds(pl.multiple_of(number * tile, tile), tile)
        return pltpu.make_async_copy(qkv_ref.at[place, :], qkv_hbm.at[place, :], here.at[0])

    save(index).start()
    queries = qs[...]
    key_at = lax.broadcasted_iota(jnp.int32, (tile, width), 0)
    query_at = lax.rem(lax.broadcasted_iota(jnp.int32, (tile, width), 1), tile)
    diagonal = key_at <= query_at

    def scores_of(step):
        at = pl.ds(pl.multiple_of(step * tile, tile), tile)
        keys = qkv_ref[at, GROUP * LANES : (GROUP + 1) * LANES]
        return contract(keys, queries, 1, 1) * binary_scale

    last = jnp.where(diagonal, scores_of(index), score_with_mask)
    s_ref[here_rows, :] = last
    peak = jnp.max(last, axis=0, keepdims=True)

    def in_pairs(one, state):
        state = lax.fori_loop(
            0, lax.div(index, 2), lambda pair, state: one((2 * pair, 2 * pair + 1), state), state
        )
        return lax.fori_loop(0, lax.rem(index, 2), lambda _, state: one((index - 1,), state), state)

    def first_pass(steps, peak):
        found = [scores_of(step) for step in steps]
        for step, scores in zip(steps, found):
            s_ref[pl.ds(pl.multiple_of(step * tile, tile), tile), :] = scores
            peak = jnp.maximum(peak, jnp.max(scores, axis=0, keepdims=True))
        return peak

    peak = in_pairs(first_pass, peak)

    def second_pass(steps, state):
        total, out = state
        for step in steps:
            at = pl.ds(pl.multiple_of(step * tile, tile), tile)
            probs = jnp.exp2(s_ref[at, :] - peak)
            total = total + jnp.sum(probs, axis=0, keepdims=True)
            out = out + contract(vt[:, at], probs.astype(jnp.bfloat16), 1, 0)
        return (total, out)

    total, out = in_pairs(
        second_pass,
        second_pass(
            (index,), (jnp.zeros((1, width), jnp.float32), jnp.zeros((LANES, width), jnp.float32))
        ),
    )
    lse_ref[pl.ds(index, 1), :] = peak + jnp.log2(total)
    out = (out * (1.0 / total)).T.astype(jnp.bfloat16)
    out = jnp.concatenate([out[head * tile : (head + 1) * tile, :] for head in range(GROUP)], axis=1)
    out = contract(out, pad_ref[: GROUP * HEAD_SIZE, : GROUP * LANES], 1, 1).astype(jnp.bfloat16)
    for part in range(2):
        target = pl.ds(pl.multiple_of(slot_ref[index * 2 + part] * block, block), block)
        rows_at = slice(part * block, (part + 1) * block)
        o_ref[target, :] = out[rows_at, :]
        ot_ref[:, target] = out[rows_at, :].T

    save(index).wait()

    @pl.when(index == pl.num_programs(0) - 1)
    def _():
        pltpu.make_async_copy(wp, wp_hbm, here.at[1]).wait()


def attend(slots, x, gain, w, pad, inner, outer):
    rows, model = x.shape
    block = rows // slots.shape[0]
    tile = 2 * block
    width = GROUP * tile
    columns = pad.shape[1]
    whole = lambda *shape: pl.BlockSpec(shape, lambda i, s: (0,) * len(shape))
    return pl.pallas_call(
        forward_kernel,
        grid_spec=pltpu.PrefetchScalarGridSpec(
            num_scalar_prefetch=1,
            grid=(rows // tile,),
            in_specs=[
                pl.BlockSpec((block, model), lambda i, s: (s[2 * i], 0)),
                pl.BlockSpec((block, model), lambda i, s: (s[2 * i + 1], 0)),
                whole(1, model),
                whole(*w.shape),
                whole(*pad.shape),
                whole(*inner.shape),
                whole(*outer.shape),
            ],
            out_specs=(
                pl.BlockSpec(memory_space=pl.ANY),
                whole(rows, GROUP * HEAD_SIZE),
                whole(GROUP * HEAD_SIZE, rows),
                whole(rows // tile, width),
                pl.BlockSpec(memory_space=pl.ANY),
            ),
            scratch_shapes=[
                pltpu.VMEM((rows, columns), jnp.bfloat16),
                pltpu.VMEM((model, columns), jnp.bfloat16),
                pltpu.VMEM((width, LANES), jnp.bfloat16),
                pltpu.VMEM((LANES, rows), jnp.bfloat16),
                pltpu.VMEM((rows, width), jnp.float32),
                pltpu.SemaphoreType.DMA((2,)),
            ],
        ),
        out_shape=(
            jax.ShapeDtypeStruct((rows, columns), jnp.bfloat16),
            jax.ShapeDtypeStruct((rows, GROUP * HEAD_SIZE), jnp.bfloat16),
            jax.ShapeDtypeStruct((GROUP * HEAD_SIZE, rows), jnp.bfloat16),
            jax.ShapeDtypeStruct((rows // tile, width), jnp.float32),
            jax.ShapeDtypeStruct((model, columns), jnp.bfloat16),
        ),
        compiler_params=pltpu.CompilerParams(vmem_limit_bytes=62 << 20),
        cost_estimate=pl.CostEstimate(
            flops=4 * GROUP * rows * rows * LANES // 2 + 2 * rows * model * columns,
            bytes_accessed=4 * rows * model,
            transcendentals=GROUP * rows * rows // 2,
        ),
        name="attend",
    )(slots, x, x, gain, w, pad, inner, outer)


def backward_kernel(
    slot_ref,
    qkv_ref,
    o_ref,
    do_ref,
    lse_ref,
    pad_ref,
    inner_ref,
    outer_ref,
    dqkv_ref,
    qs,
    gs,
    kt,
    dk,
    dv,
):
    step_at = pl.program_id(0)
    tiles = pl.num_programs(0)
    index = tiles - 1 - step_at
    block = qkv_ref.shape[0] // slot_ref.shape[0]
    tile = 2 * block
    width = GROUP * tile
    first_key, first_value = GROUP * LANES, (GROUP + 1) * LANES

    @pl.when(step_at == 0)
    def _():
        kt[...] = qkv_ref[:, first_key:first_value].T
        dk[...] = jnp.zeros_like(dk)
        dv[...] = jnp.zeros_like(dv)

    here = pl.ds(pl.multiple_of(index * tile, tile), tile)
    sources = [
        pl.ds(pl.multiple_of(slot_ref[index * 2 + part] * block, block), block) for part in (0, 1)
    ]
    o = jnp.concatenate([o_ref[source, :] for source in sources], axis=0)
    grads = jnp.concatenate([do_ref[source, :] for source in sources], axis=0)
    products = (grads.astype(jnp.float32) * o.astype(jnp.float32)).T
    grads = contract(grads, pad_ref[: GROUP * HEAD_SIZE, : GROUP * LANES], 1, 0).astype(jnp.bfloat16)
    deltas = []
    for head in range(GROUP):
        lanes = slice(head * LANES, (head + 1) * LANES)
        at = slice(head * tile, (head + 1) * tile)
        qs[at, :] = qkv_ref[here, lanes]
        gs[at, :] = grads[:, lanes]
        features = slice(head * HEAD_SIZE, (head + 1) * HEAD_SIZE)
        deltas.append(jnp.sum(products[features, :], axis=0, keepdims=True))
    delta = jnp.concatenate(deltas, axis=1)
    lse = lse_ref[pl.ds(index, 1), :]
    key_at = lax.broadcasted_iota(jnp.int32, (tile, width), 0)
    query_at = lax.rem(lax.broadcasted_iota(jnp.int32, (tile, width), 1), tile)
    diagonal = key_at <= query_at

    def pieces(steps, masked=False):
        queries, grads = qs[...], gs[...]
        places = [pl.ds(pl.multiple_of(step * tile, tile), tile) for step in steps]
        scores = [contract(qkv_ref[at, first_key:first_value], queries, 1, 1) for at in places]
        grad_probs = [contract(qkv_ref[at, first_value:], grads, 1, 1) for at in places]
        total = None
        for at, score, grad_prob in zip(places, scores, grad_probs):
            probs = jnp.exp2(score * binary_scale - lse)
            if masked:
                probs = jnp.where(diagonal, probs, 0.0)
            dv[at, :] += contract(probs.astype(jnp.bfloat16), grads, 1, 0)
            grad_scores = (probs * (grad_prob - delta)).astype(jnp.bfloat16)
            dk[at, :] += contract(grad_scores, queries, 1, 0)
            part = contract(kt[:, at], grad_scores, 1, 0)
            total = part if total is None else total + part
        return total

    dq = pieces((index,), True)
    dq = lax.fori_loop(
        0, lax.div(index, 2), lambda pair, total: total + pieces((2 * pair, 2 * pair + 1)), dq
    )
    dq = lax.fori_loop(0, lax.rem(index, 2), lambda _, total: total + pieces((index - 1,)), dq)
    dq = dq.T * score_scale
    cosine, sine = tables(inner_ref, outer_ref, index, 2)
    parts = [turn(dq[head * tile : (head + 1) * tile, :], cosine, -sine) for head in range(GROUP)]
    parts.append(turn(dk[here, :] * score_scale, cosine, -sine))
    parts.append(dv[here, :])
    dqkv = jnp.concatenate([part.astype(jnp.bfloat16) for part in parts], axis=1)
    for part in (0, 1):
        dqkv_ref[sources[part], :] = dqkv[part * block : (part + 1) * block, :]


def attend_back(slots, qkv, o, do, lse, pad, inner, outer):
    rows, columns = qkv.shape
    block = rows // slots.shape[0]
    tile = 2 * block
    width = GROUP * tile
    tiles = rows // tile
    operands = (qkv, o, do, lse, pad, inner, outer)
    whole = lambda *shape: pl.BlockSpec(shape, lambda i, s: (0,) * len(shape))
    return pl.pallas_call(
        backward_kernel,
        grid_spec=pltpu.PrefetchScalarGridSpec(
            num_scalar_prefetch=1,
            grid=(tiles,),
            in_specs=[whole(*operand.shape) for operand in operands],
            out_specs=whole(rows, columns),
            scratch_shapes=[
                pltpu.VMEM((width, LANES), jnp.bfloat16),
                pltpu.VMEM((width, LANES), jnp.bfloat16),
                pltpu.VMEM((LANES, rows), jnp.bfloat16),
                pltpu.VMEM((rows, LANES), jnp.float32),
                pltpu.VMEM((rows, LANES), jnp.float32),
            ],
        ),
        out_shape=jax.ShapeDtypeStruct((rows, columns), jnp.bfloat16),
        compiler_params=pltpu.CompilerParams(vmem_limit_bytes=40 << 20),
        cost_estimate=pl.CostEstimate(
            flops=10 * GROUP * rows * rows * LANES // 2,
            bytes_accessed=8 * rows * columns,
            transcendentals=GROUP * rows * rows // 2,
        ),
        name="attend_back",
    )(slots, *operands)


MESH_IDS = pl.DeviceIdType.MESH


NEAR = (1, 2, 4)
ALL = (1, 2, 3, 4, 5, 6, 7)


def start_barrier(me, bits, line_steps=(), line_index=None, line=1):
    barrier = pltpu.get_barrier_semaphore()
    peers = [{"ctx": me ^ bit} for bit in bits]
    peers += [{"fsdp": lax.rem(line_index + step, line)} for step in line_steps]
    for peer in peers:
        pl.semaphore_signal(barrier, inc=1, device_id=peer, device_id_type=MESH_IDS)
    pl.semaphore_wait(barrier, len(peers))


def start_line_barrier(me, index, line):
    barrier = pltpu.get_barrier_semaphore()
    for bit in NEAR:
        pl.semaphore_signal(barrier, inc=1, device_id={"ctx": me ^ bit}, device_id_type=MESH_IDS)
    up, down = index < line - 1, index > 0
    for there, exists in ((index + 1, up), (index - 1, down)):

        @pl.when(exists)
        def _(there=there):
            peer = {"fsdp": jnp.clip(there, 0, line - 1)}
            pl.semaphore_signal(barrier, inc=1, device_id=peer, device_id_type=MESH_IDS)

    pl.semaphore_wait(barrier, len(NEAR) + up.astype(jnp.int32) + down.astype(jnp.int32))


class Copies:
    def __init__(self, send_sems, recv_sems, base=0):
        self.send_sems, self.recv_sems, self.next, self.sent = send_sems, recv_sems, base, []

    def number(self):
        self.next += 1
        return self.next - 1

    def make(self, number, source, target, peer, landing=None):
        return pltpu.make_async_remote_copy(
            src_ref=source,
            dst_ref=target,
            send_sem=self.send_sems.at[number],
            recv_sem=self.recv_sems.at[number if landing is None else landing],
            device_id=peer,
            device_id_type=MESH_IDS,
        )

    def send(self, number, source, target, peer):
        copy = self.make(number, source, target, peer)
        copy.start()
        self.sent.append(copy)

    def arrived(self, number, target):
        self.make(number, target, target, {"ctx": 0}).wait_recv()

    def finish(self):
        for copy in self.sent:
            copy.wait_send()


GATHER_COPIES = 14


class PlaneGather:
    def __init__(self, copies, me, own_half, part):
        self.copies, self.me, self.own_half, self.part = copies, me, own_half, part
        self.first = copies.next
        copies.next += GATHER_COPIES

    def copy(self, number):
        bit, half, receiver = (
            (0, 1, 2),
            (0, 0, 4),
            (0, 0, 2),
            (0, 1, 4),
            (0, 0, 1),
            (0, 1, 1),
            (2, 1, 4),
            (4, 0, 2),
            (2, 1, 1),
            (4, 0, 1),
            (2, 0, 1),
            (4, 1, 1),
            (6, 1, 1),
            (6, 0, 1),
        )[number]
        place = self.part(self.me ^ bit, half)
        source = self.own_half(half) if bit == 0 else place
        return self.copies.make(self.first + number, source, place, {"ctx": self.me ^ receiver})

    def send(self, *numbers):
        for number in numbers:
            self.copy(number).start()

    def hear(self, number, bit, half):
        self.copies.arrived(self.first + number, self.part(self.me ^ bit, half))

    def begin(self):
        self.send(0, 1, 2, 3, 4, 5)

    def first_hop(self):
        self.hear(0, 2, 1)
        self.send(6, 8)
        self.hear(1, 4, 0)
        self.send(7, 9)

    def second_hop(self):
        self.hear(2, 2, 0)
        self.send(10)
        self.hear(3, 4, 1)
        self.send(11)

    def third_hop(self):
        self.hear(6, 6, 1)
        self.send(12)
        self.hear(7, 6, 0)
        self.send(13)

    def shared(self, bit):
        for number, half in {1: (4, 0), 3: (8, 1), 5: (9, 0), 7: (12, 1)}[bit], {
            1: (5, 1),
            3: (10, 0),
            5: (11, 1),
            7: (13, 0),
        }[bit]:
            self.hear(number, bit, half)

    def last(self):
        for bit in (1, 3, 5, 7):
            self.shared(bit)

    def finish(self):
        for number in range(GATHER_COPIES):
            self.copy(number).wait_send()


def row_half(ref, rows):
    half = rows // 2

    def own(side):
        return ref.at[pl.ds(side * half, half), :]

    return own


def row_part(ref, rows):
    half = rows // 2

    def part(slot, side):
        if isinstance(side, slice):
            return ref.at[pl.ds(pl.multiple_of(slot * rows, rows), rows), :]
        return ref.at[pl.ds(pl.multiple_of(slot * rows + side * half, half), half), :]

    return part


class LineGather:
    def __init__(self, copies, index, line, own, place):
        self.copies, self.index, self.line = copies, index, line
        self.own, self.place = own, place
        self.first = copies.next
        copies.next += 2 * (line - 1)

    def move(self, step, upward, act):
        index, line = self.index, self.line
        if upward:
            slot, there = index - step, index + 1
            leaves = (slot >= 0) & (there < line)
        else:
            slot, there = index + step, index - 1
            leaves = (slot < line) & (there >= 0)
        number = self.first + step + (0 if upward else line - 1)

        @pl.when(leaves)
        def _():
            place = self.place(jnp.clip(slot, 0, line - 1))
            source = self.own if step == 0 else place
            act(self.copies.make(number, source, place, {"fsdp": jnp.clip(there, 0, line - 1)}))

    def hear(self, step, upward):
        index, line = self.index, self.line
        slot = index - 1 - step if upward else index + 1 + step
        comes = (slot >= 0) & (slot < line)
        number = self.first + step + (0 if upward else line - 1)

        @pl.when(comes)
        def _():
            place = self.place(jnp.clip(slot, 0, line - 1))
            self.copies.make(number, place, place, {"fsdp": 0}).wait_recv()

    def begin(self):
        for upward in (True, False):
            self.move(0, upward, lambda copy: copy.start())

    def hop(self, step):
        for upward in (True, False):
            self.hear(step - 1, upward)
            if step < self.line - 1:
                self.move(step, upward, lambda copy: copy.start())

    def finish(self):
        for step in range(self.line - 1):
            for upward in (True, False):
                self.move(step, upward, lambda copy: copy.wait_send())


def in_hbm(count):
    return [pl.BlockSpec(memory_space=pltpu.HBM)] * count


def anywhere(count):
    return [pl.BlockSpec(memory_space=pl.ANY)] * count


def local_copies(pairs, sems):
    copies = [
        pltpu.make_async_copy(source, target, sems.at[number])
        for number, (source, target) in enumerate(pairs)
    ]
    for copy in copies:
        copy.start()
    return copies


def remote_params(number, mebibytes=62):
    return pltpu.CompilerParams(
        collective_id=number, has_side_effects=True, vmem_limit_bytes=mebibytes << 20
    )


def first_kernel(
    line,
    x_ref,
    qkv_ref,
    wo_ref,
    gain_ref,
    gate_ref,
    up_ref,
    down_ref,
    xo_ref,
    qkvo_ref,
    woo_ref,
    gaino_ref,
    feedo_ref,
    feed,
    own,
    send,
    recv,
    here,
):
    me, index = lax.axis_index("ctx"), lax.axis_index("fsdp")
    plane = lax.axis_size("ctx")
    rows = x_ref.shape[0]
    part = row_part(xo_ref, rows)
    wo_rows = woo_ref.shape[1]
    wo_own = wo_ref.at[pl.ds(pl.multiple_of(me * wo_rows, wo_rows), wo_rows), :]
    local = local_copies(
        [
            (qkv_ref, qkvo_ref.at[index]),
            (wo_own, woo_ref.at[index]),
            (gain_ref, gaino_ref.at[index]),
            (x_ref, own),
        ],
        here.at[pl.ds(0, 4)],
    )
    start_line_barrier(me, index, line)
    copies = Copies(send, recv)
    gather = PlaneGather(copies, me, row_half(own, rows), part)
    lines = [
        LineGather(copies, index, line, own, lambda slot, ref=ref: ref.at[slot])
        for own, ref in ((qkv_ref, qkvo_ref), (gain_ref, gaino_ref), (wo_own, woo_ref))
    ]
    local.pop().wait()
    gather.begin()
    local += local_copies([(own, part(me, slice(None)))], here.at[pl.ds(3, 1)])
    for each in lines:
        each.begin()
    width = feed.shape[1] // 3
    unit = width // line
    pairs = []
    for side, ref in enumerate((gate_ref, up_ref)):
        for z in range(line):
            source = pl.ds(pl.multiple_of((z * plane + me) * unit, unit), unit)
            target = pl.ds(side * width + z * unit, unit)
            pairs.append((ref.at[:, source], feed.at[:, target]))
    for number in range(feed.shape[0] // unit):
        pairs.append(
            (
                down_ref.at[
                    pl.ds(pl.multiple_of(me * unit, unit), unit), pl.ds(number * width, width)
                ],
                feed.at[pl.ds(number * unit, unit), pl.ds(2 * width, width)],
            )
        )
    packed = local_copies(pairs, here.at[pl.ds(4, len(pairs))])
    gather.first_hop()
    for step in range(1, line):
        for each in lines:
            each.hop(step)
        if step == 1:
            gather.second_hop()
            for copy in packed:
                copy.wait()
            packed = local_copies([(feed, feedo_ref)], here.at[pl.ds(4 + len(pairs), 1)])
    gather.third_hop()
    gather.last()
    gather.finish()
    for each in lines:
        each.finish()
    for copy in local:
        copy.wait()
    packed[0].wait()


def first_exchange(line, x, qkv, wo, gains, gate, up, down):
    plane = lax.axis_size("ctx")
    count = GATHER_COPIES + 6 * (line - 1)
    model = x.shape[1]
    shard = model // line
    width = gate.shape[1] // plane
    own_rows = wo.shape[0] // plane
    feed = (shard, 3 * width)
    packing = 2 * line + shard * line // width + 1
    return pl.pallas_call(
        functools.partial(first_kernel, line),
        out_shape=(
            jax.ShapeDtypeStruct((plane * x.shape[0], model), x.dtype),
            jax.ShapeDtypeStruct((line, *qkv.shape), qkv.dtype),
            jax.ShapeDtypeStruct((line, own_rows, model), wo.dtype),
            jax.ShapeDtypeStruct((line, *gains.shape), gains.dtype),
            jax.ShapeDtypeStruct(feed, gate.dtype),
        ),
        in_specs=in_hbm(1) + anywhere(1) + in_hbm(1) + anywhere(1) + in_hbm(3),
        out_specs=tuple(anywhere(5)),
        scratch_shapes=[
            pltpu.VMEM(feed, gate.dtype),
            pltpu.VMEM(x.shape, x.dtype),
            pltpu.SemaphoreType.DMA((count,)),
            pltpu.SemaphoreType.DMA((count,)),
            pltpu.SemaphoreType.DMA((4 + packing,)),
        ],
        compiler_params=remote_params(1),
        name="first_exchange",
    )(x, qkv, wo, gains, gate, up, down)


def deal_rows(copies, me, pieces, wo_ref, place, recv_first, here):
    to_first = pieces * lax.rem(me, 2)
    line_slot = lax.div(me, 2)

    def copy(piece):
        return copies.make(
            recv_first + piece,
            wo_ref.at[piece],
            place(line_slot),
            {"ctx": to_first + piece},
            recv_first + line_slot,
        )

    for piece in range(pieces):

        @pl.when(to_first + piece != me)
        def _(piece=piece):
            copy(piece).start()

        @pl.when(to_first + piece == me)
        def _(piece=piece):
            pltpu.make_async_copy(wo_ref.at[piece], place(line_slot), here).start()

    def finish(line):
        for slot in range(line):

            @pl.when(2 * slot + lax.div(me, pieces) != me)
            def _(slot=slot):
                copies.make(
                    recv_first, wo_ref.at[0], place(slot), {"ctx": 0}, recv_first + slot
                ).wait_recv()

        for piece in range(pieces):

            @pl.when(to_first + piece != me)
            def _(piece=piece):
                copy(piece).wait_send()

            @pl.when(to_first + piece == me)
            def _(piece=piece):
                pltpu.make_async_copy(wo_ref.at[piece], place(line_slot), here).wait()

    return finish


class NearShares:
    def __init__(self, copies, me, refs, place):
        self.copies, self.me, self.refs, self.place = copies, me, refs, place
        self.first = copies.next
        copies.next += 7

    def copy(self, number):
        me, (own, near_x, near_y) = self.me, self.refs
        half = own.shape[0] // 2
        partner = {"ctx": me ^ 1}
        source, target, peer = (
            lambda: (near_y.at[pl.ds(0, half)], self.place(me ^ 4, 0), {"ctx": me ^ 2}),
            lambda: (near_x.at[pl.ds(half, half)], self.place(me ^ 2, 1), {"ctx": me ^ 4}),
            lambda: (own, self.place(me, None), partner),
            lambda: (near_x, self.place(me ^ 2, None), partner),
            lambda: (near_y, self.place(me ^ 4, None), partner),
            lambda: (self.place(me ^ 6, 0), self.place(me ^ 6, 0), partner),
            lambda: (self.place(me ^ 6, 1), self.place(me ^ 6, 1), partner),
        )[number]()
        return self.copies.make(self.first + number, source, target, peer)

    def begin(self):
        for number in range(5):
            self.copy(number).start()

    def diagonal(self):
        for side in (0, 1):
            self.copies.arrived(self.first + side, self.place(self.me ^ 6, side))
            self.copy(5 + side).start()

    def shared(self, bit):
        if bit == 7:
            for side in (0, 1):
                self.copies.arrived(self.first + 5 + side, self.place(self.me ^ 7, side))
        else:
            self.copies.arrived(self.first + 2 + bit // 2, self.place(self.me ^ bit, None))

    def finish(self):
        for number in range(7):
            self.copy(number).wait_send()


def block_place(ref, rows):
    half = rows // 2

    def place(slot, side):
        if side is None:
            return ref.at[pl.ds(pl.multiple_of(slot * rows, rows), rows), :]
        return ref.at[pl.ds(pl.multiple_of(slot * rows + side * half, half), half), :]

    return place


def second_kernel(
    o_ref,
    wo0_hbm,
    wo2_hbm,
    wo4_hbm,
    dy2_hbm,
    dy4_hbm,
    x_hbm,
    gain_ref,
    own_hbm,
    dy6_hbm,
    residual_hbm,
    normed_hbm,
    scale_ref,
    gained_hbm,
    near_x_hbm,
    near_y_hbm,
    x_ref,
    residual_ref,
    normed_ref,
    gained_ref,
    att,
    wo,
    send,
    recv,
    here,
):
    me = lax.axis_index("ctx")
    rows = x_ref.shape[0]
    half = rows // 2
    middle = wo.shape[0] // 2

    def wo_place(slot, side):
        return wo.at[:, slot] if side is None else wo.at[pl.ds(side * middle, middle), slot]

    own_wo = (wo0_hbm, wo2_hbm, wo4_hbm)
    local = local_copies(
        [
            (o_ref.at[pl.ds(pl.multiple_of(me * rows, rows), rows), :], att.at[me]),
            (x_hbm, x_ref),
        ]
        + [(ref, wo_place(me ^ (2 * number), None)) for number, ref in enumerate(own_wo)],
        here.at[pl.ds(0, 5)],
    )
    start_barrier(me, ALL)
    copies = Copies(send, recv)

    def block(slot):
        return o_ref.at[pl.ds(pl.multiple_of(slot * rows, rows), rows), :]

    numbers = {}
    for bit in (6, 7, 4, 5, 2, 3, 1):
        numbers[bit] = copies.number()
        copies.send(numbers[bit], block(me ^ bit), att.at[me], {"ctx": me ^ bit})
    shares = NearShares(copies, me, own_wo, wo_place)
    shares.begin()
    dy_first = copies.next
    copies.next += 2
    upper, lower = pl.ds(0, half), pl.ds(half, half)
    copies.send(dy_first, dy4_hbm.at[upper, :], dy6_hbm.at[upper, :], {"ctx": me ^ 2})
    copies.send(dy_first + 1, dy2_hbm.at[lower, :], dy6_hbm.at[lower, :], {"ctx": me ^ 4})
    shares.diagonal()
    for bit in (1, 3, 5, 7):
        shares.shared(bit)
    for bit, number in numbers.items():
        copies.arrived(number, att.at[me ^ bit])
    for copy in local:
        copy.wait()
    per_head = 2 * GROUP
    own = wo.at[lax.div(me, 2), pl.ds(per_head * lax.rem(me, 2), per_head)]
    keep = local_copies([(own, own_hbm)], here.at[pl.ds(5, 1)])
    plane = att.shape[0]
    near = copies.next
    for side in (0, 1):
        at = pl.ds(side * half, half)
        total = x_ref[at, :].astype(jnp.float32)
        for slot in range(plane):
            first = per_head * (slot % 2)
            weight = jnp.concatenate(
                [wo[slot // 2, first + piece] for piece in range(per_head)], axis=0
            )
            total = total + contract(att[slot, at, :], weight, 1, 0)
        residual_ref[at, :] = total
        scale = lax.rsqrt(jnp.mean(total * total, axis=-1, keepdims=True) + norm_epsilon)
        normed = total * scale
        scale_ref[at, :] = scale
        normed_ref[at, :] = normed
        gained_ref[at, :] = (normed * gain_ref[...]).astype(jnp.bfloat16)
        for number, target, bit in ((0, near_x_hbm, 2), (1, near_y_hbm, 4)):
            copies.send(
                near + 2 * side + number,
                gained_ref.at[at, :],
                target.at[at, :],
                {"ctx": me ^ bit},
            )
    keep += local_copies(
        [(residual_ref, residual_hbm), (normed_ref, normed_hbm), (gained_ref, gained_hbm)],
        here.at[pl.ds(6, 3)],
    )
    for copy in keep:
        copy.wait()
    shares.finish()
    copies.arrived(dy_first, dy6_hbm.at[upper, :])
    copies.arrived(dy_first + 1, dy6_hbm.at[lower, :])
    for side in (0, 1):
        at = pl.ds(side * half, half)
        copies.arrived(near + 2 * side, near_x_hbm.at[at, :])
        copies.arrived(near + 2 * side + 1, near_y_hbm.at[at, :])
    copies.finish()


def second_exchange(o, own_wo, grads, x, gain):
    plane = lax.axis_size("ctx")
    rows = x.shape[0]
    line, part, model = own_wo[0].shape
    count = 7 + 7 + 2 + 4
    f32 = jnp.float32
    return pl.pallas_call(
        second_kernel,
        out_shape=(
            jax.ShapeDtypeStruct((2 * GROUP, part, model), own_wo[0].dtype),
            jax.ShapeDtypeStruct((rows, model), x.dtype),
            jax.ShapeDtypeStruct((rows, model), f32),
            jax.ShapeDtypeStruct((rows, model), f32),
            jax.ShapeDtypeStruct((rows, 1), f32),
            *[jax.ShapeDtypeStruct((rows, model), x.dtype)] * 3,
        ),
        in_specs=in_hbm(7) + in_vmem(1),
        out_specs=(*anywhere(4), *in_vmem(1), *anywhere(3)),
        scratch_shapes=[
            pltpu.VMEM(x.shape, x.dtype),
            pltpu.VMEM(x.shape, f32),
            pltpu.VMEM(x.shape, f32),
            pltpu.VMEM(x.shape, x.dtype),
            pltpu.VMEM((plane, rows, o.shape[1]), o.dtype),
            pltpu.VMEM((line, plane, part, model), x.dtype),
            pltpu.SemaphoreType.DMA((count,)),
            pltpu.SemaphoreType.DMA((count,)),
            pltpu.SemaphoreType.DMA((9,)),
        ],
        compiler_params=remote_params(2),
        name="second_exchange",
    )(o, *own_wo, *grads, x, gain)


def near_kernel(own_hbm, near_x_hbm, near_y_hbm, whole_ref, send, recv, here):
    me = lax.axis_index("ctx")
    refs = (own_hbm, near_x_hbm, near_y_hbm)
    place = block_place(whole_ref, own_hbm.shape[0])
    local = local_copies(
        [(ref, place(me ^ (2 * number), None)) for number, ref in enumerate(refs)], here
    )
    start_barrier(me, NEAR)
    copies = Copies(send, recv)
    shares = NearShares(copies, me, refs, place)
    shares.begin()
    shares.diagonal()
    for bit in (1, 3, 5, 7):
        shares.shared(bit)
    for copy in local:
        copy.wait()
    shares.finish()


def near_gather(refs, number):
    plane = lax.axis_size("ctx")
    rows, columns = refs[0].shape
    return pl.pallas_call(
        near_kernel,
        out_shape=jax.ShapeDtypeStruct((plane * rows, columns), refs[0].dtype),
        in_specs=anywhere(3),
        out_specs=in_vmem(1)[0],
        scratch_shapes=[
            pltpu.SemaphoreType.DMA((7,)),
            pltpu.SemaphoreType.DMA((7,)),
            pltpu.SemaphoreType.DMA((3,)),
        ],
        compiler_params=remote_params(number, 24),
    )(*refs)


def third_kernel(
    g0_hbm, g2_hbm, g4_hbm, ot_hbm, wo_hbm, do_ref, dwo_ref, ot_ref, wo_ref, all_grads, dwo, send, recv, here
):
    me = lax.axis_index("ctx")
    rows = g0_hbm.shape[0]
    place = block_place(all_grads, rows)
    own_rows = (g0_hbm, g2_hbm, g4_hbm)
    fetch = local_copies(
        [(ref, place(me ^ (2 * number), None)) for number, ref in enumerate(own_rows)]
        + [(ot_hbm, ot_ref), (wo_hbm, wo_ref)],
        here,
    )
    start_barrier(me, NEAR)
    copies = Copies(send, recv)
    shares = NearShares(copies, me, own_rows, place)
    shares.begin()
    dwo[...] = jnp.zeros_like(dwo)
    for copy in fetch:
        copy.wait()

    def step(order, carry):
        @pl.when(order == 5)
        def _():
            shares.diagonal()

        for bit in (1, 3, 5, 7):

            @pl.when(order == bit)
            def _(bit=bit):
                shares.shared(bit)

        here_rows = pl.ds(pl.multiple_of((me ^ order) * rows, rows), rows)
        grads = all_grads[here_rows, :]
        do_ref[here_rows, :] = contract(grads, wo_ref[...], 1, 1).astype(jnp.bfloat16)
        dwo[...] += contract(ot_ref[:, here_rows], grads, 1, 0)
        return carry

    lax.fori_loop(0, 8, step, 0)
    line, _, across = dwo_ref.shape
    for slot in range(line):
        rows_at = slice(slot * HALF, (slot + 1) * HALF)
        for number in range(dwo.shape[1] // across):
            columns = slice(number * across, (number + 1) * across)
            dwo_ref[slot, number * HALF : (number + 1) * HALF, :] = dwo[rows_at, columns].astype(
                jnp.bfloat16
            )
    shares.finish()


def third_exchange(line, own_rows, ot, wo, across):
    plane = lax.axis_size("ctx")
    rows, model = own_rows[0].shape
    half_type, f32 = jnp.bfloat16, jnp.float32
    return pl.pallas_call(
        third_kernel,
        out_shape=(
            jax.ShapeDtypeStruct((plane * rows, wo.shape[0]), half_type),
            jax.ShapeDtypeStruct((line, HALF * model // across, across), half_type),
        ),
        in_specs=anywhere(5),
        out_specs=tuple(in_vmem(2)),
        scratch_shapes=[
            pltpu.VMEM(ot.shape, ot.dtype),
            pltpu.VMEM(wo.shape, wo.dtype),
            pltpu.VMEM((plane * rows, model), half_type),
            pltpu.VMEM((line * HALF, model), f32),
            pltpu.SemaphoreType.DMA((7,)),
            pltpu.SemaphoreType.DMA((7,)),
            pltpu.SemaphoreType.DMA((5,)),
        ],
        compiler_params=remote_params(6),
        name="third_exchange",
    )(*own_rows, ot, wo)


REDUCE_COPIES = 10


class PlaneReduce:
    def __init__(self, copies, me, block, heard, held, landed):
        self.copies, self.me, self.block = copies, me, block
        self.heard, self.held, self.landed = heard, held, landed
        self.first = copies.next
        copies.next += REDUCE_COPIES
        self.half = heard.shape[1] // 2
        self.x, self.y = {"ctx": me ^ 2}, {"ctx": me ^ 4}

    def side(self, ref, slot, half):
        return ref.at[slot, pl.ds(half * self.half, self.half), :]

    def share(self, order):
        self.shared(order).start()

    def shared(self, order):
        partner = self.me ^ 1
        source = self.block(partner ^ (6, 2, 4, 0)[order])
        return self.copies.make(
            self.first + order, source, self.heard.at[order], {"ctx": partner}
        )

    def combine(self, order, rows, extra=None):
        bit = (6, 2, 4)[order]
        total = self.block(self.me ^ bit)[rows, :].astype(jnp.float32) + self.heard[
            order, rows, :
        ].astype(jnp.float32)
        if extra is not None:
            total = total + extra
        self.held[order, rows, :] = total.astype(self.held.dtype)

    def onward(self, number):
        order, half, peer = {
            4: (0, 0, self.x),
            5: (0, 1, self.y),
            6: (1, 0, self.x),
            7: (2, 1, self.y),
            8: (1, 1, self.x),
            9: (2, 0, self.y),
        }[number]
        held, landed = self.side(self.held, order, half), self.side(self.landed, order, half)
        return self.copies.make(self.first + number, held, landed, peer)

    def finish(self):
        for order in range(4):
            self.shared(order).wait_send()
        for number in range(4, REDUCE_COPIES):
            self.onward(number).wait_send()

    def diagonal_sends(self):
        first, half = self.first, self.half
        self.copies.arrived(first + 0, self.heard.at[0])
        self.combine(0, pl.ds(0, 2 * half))
        self.onward(4).start()
        self.onward(5).start()

    def neighbour_send(self, order):
        first, half = self.first, self.half
        self.copies.arrived(first + order, self.heard.at[order])
        self.combine(order, pl.ds((order - 1) * half, half))
        self.onward(5 + order).start()

    def neighbour_sends(self):
        self.neighbour_send(1)
        self.neighbour_send(2)

    def second_sends(self):
        first, half = self.first, self.half
        upper, lower = pl.ds(0, half), pl.ds(half, half)
        landed, side, arrived = self.landed, self.side, self.copies.arrived
        arrived(first + 5, side(landed, 0, 1))
        self.combine(1, lower, landed[0, lower, :].astype(jnp.float32))
        self.onward(8).start()
        arrived(first + 4, side(landed, 0, 0))
        self.combine(2, upper, landed[0, upper, :].astype(jnp.float32))
        self.onward(9).start()

    def own_share(self):
        self.copies.arrived(self.first + 3, self.heard.at[3])

    def sum_half(self, which):
        first, half = self.first, self.half
        rows = pl.ds(which * half, half)
        self.copies.arrived(first + (6, 8)[which], self.side(self.landed, 1, which))
        self.copies.arrived(first + (9, 7)[which], self.side(self.landed, 2, which))
        return (
            self.block(self.me)[rows, :].astype(jnp.float32)
            + self.heard[3, rows, :].astype(jnp.float32)
            + self.landed[1, rows, :].astype(jnp.float32)
            + self.landed[2, rows, :].astype(jnp.float32)
        )


def feed_kernel(
    line,
    g0_hbm,
    g2_hbm,
    g4_hbm,
    dy0_hbm,
    dy2_hbm,
    dy4_hbm,
    dy6_hbm,
    w_hbm,
    ot_hbm,
    normed_hbm,
    scale_ref,
    gain_ref,
    residual_ref,
    term_ref,
    own_ref,
    near_x_ref,
    near_y_ref,
    dealt_hbm,
    out6_hbm,
    out2_hbm,
    out4_hbm,
    out0_hbm,
    dw_hbm,
    normed_ref,
    w_ref,
    dw_ref,
    down_ref,
    dy_ref,
    all_g,
    hid,
    hid_t,
    gate_t,
    up_t,
    part,
    heard,
    held,
    landed,
    out_mine,
    out_heard,
    send,
    recv,
    here,
):
    me = lax.axis_index("ctx")
    rows = residual_ref.shape[0]
    half = rows // 2
    width, model = down_ref.shape
    blocks = model // width
    unit = width // line
    partner = {"ctx": me ^ 1}

    def at(slot):
        return pl.ds(pl.multiple_of(slot * rows, rows), rows)

    own_grads = (dy0_hbm, dy2_hbm, dy4_hbm, dy6_hbm)
    own_rows = (g0_hbm, g2_hbm, g4_hbm)
    place = block_place(all_g, rows)
    dy_place = block_place(dy_ref, rows)
    local = local_copies(
        [(w_hbm, w_ref)]
        + [(ref, place(me ^ (2 * number), None)) for number, ref in enumerate(own_rows)]
        + [(ref, dy_place(me ^ (2 * number), None)) for number, ref in enumerate(own_grads)]
        + [(normed_hbm, normed_ref)],
        here.at[pl.ds(0, 9)],
    )
    start_barrier(me, ALL)
    copies = Copies(send, recv)
    shares = NearShares(copies, me, own_rows, place)
    shares.begin()
    dy_first = copies.next
    copies.next += 4
    for number, ref in enumerate(own_grads):
        copies.send(dy_first + number, ref, dy_place(me ^ (2 * number), None), partner)
    deal_first = copies.next
    copies.next += ot_hbm.shape[0]
    dealt = deal_rows(
        copies,
        me,
        ot_hbm.shape[0],
        ot_hbm,
        lambda slot: dealt_hbm.at[slot],
        deal_first,
        here.at[9],
    )
    local[0].wait()
    gate_ref, up_ref = w_ref.at[:, :width], w_ref.at[:, width : 2 * width]
    for z in range(line):
        for number in range(blocks):
            source = pl.ds((z * blocks + number) * unit, unit)
            down_ref[pl.ds(z * unit, unit), number * width : (number + 1) * width] = w_ref[
                source, 2 * width :
            ]
    for copy in local[1:]:
        copy.wait()
    gain = gain_ref[...]

    def block(slot):
        return part.at[at(slot), :]

    reduce = PlaneReduce(copies, me, block, heard, held, landed)

    def chunk(order):
        place = at(me ^ order)
        g = all_g[place, :]
        dy = dy_ref[place, :]
        gate_values = contract(g, gate_ref[...], 1, 0)
        up_values = contract(g, up_ref[...], 1, 0)
        sigmoid_gate = 1.0 / (1.0 + jnp.exp(-gate_values))
        activated = gate_values * sigmoid_gate
        hidden_act = (activated * up_values).astype(jnp.bfloat16)
        hid[place, :] = hidden_act
        hid_t[:, place] = hidden_act.T
        grad_hidden = contract(dy, down_ref[...], 1, 1)
        grad_gate = (
            grad_hidden * up_values * sigmoid_gate * (1.0 + gate_values * (1.0 - sigmoid_gate))
        ).astype(jnp.bfloat16)
        grad_up = (grad_hidden * activated).astype(jnp.bfloat16)
        gate_t[:, place] = grad_gate.T
        up_t[:, place] = grad_up.T
        part[place, :] = (
            contract(grad_gate, gate_ref[...], 1, 1) + contract(grad_up, up_ref[...], 1, 1)
        ).astype(jnp.bfloat16)

    def step(number, carry):
        @pl.when(number == 1)
        def _():
            shares.shared(3)
            copies.arrived(dy_first + 1, dy_place(me ^ 3, None))

        @pl.when(number == 2)
        def _():
            reduce.share(1)
            shares.diagonal()

        @pl.when(number == 3)
        def _():
            reduce.neighbour_send(1)
            shares.shared(7)
            copies.arrived(dy_first + 3, dy_place(me ^ 7, None))

        @pl.when(number == 4)
        def _():
            reduce.share(0)
            reduce.diagonal_sends()

        @pl.when(number == 5)
        def _():
            shares.shared(5)
            copies.arrived(dy_first + 2, dy_place(me ^ 5, None))

        @pl.when(number == 6)
        def _():
            reduce.share(2)
            reduce.neighbour_send(2)

        @pl.when(number == 7)
        def _():
            reduce.second_sends()
            shares.shared(1)
            copies.arrived(dy_first, dy_place(me ^ 1, None))

        pair = lax.div(number, 2)
        chunk(
            lax.rem(number, 2)
            + jnp.where(pair == 0, 2, jnp.where(pair == 1, 6, jnp.where(pair == 2, 4, 0)))
        )
        return carry

    lax.fori_loop(0, 8, step, 0)
    reduce.share(3)
    out_first = copies.next
    copies.next += 4

    def bit_of(number):
        return jnp.where(number == 0, 6, jnp.where(number == 3, 0, 2 * number))

    def out_copy(number):
        return copies.make(out_first + number, out_mine.at[number], out_heard.at[number], partner)

    def out_of(slot):
        return contract(hid[at(slot), :], down_ref[...], 1, 0)

    def give(number, carry):
        out_mine[number] = out_of(me ^ 1 ^ bit_of(number)).astype(jnp.bfloat16)
        out_copy(number).start()
        return carry

    def keep(number, carry):
        total = out_of(me ^ bit_of(number))
        out_copy(number).wait_recv()
        out_heard[number] = (total + out_heard[number].astype(jnp.float32)).astype(jnp.bfloat16)
        return carry

    def weights(number, carry):
        columns = pl.ds(pl.multiple_of(number * width, width), width)
        total = contract(hid_t[...], dy_ref[:, columns], 1, 0).astype(jnp.bfloat16)
        for z in range(line):
            target = pl.ds(pl.multiple_of((z * blocks + number) * unit, unit), unit)
            dw_ref[target, 2 * width :] = total[z * unit : (z + 1) * unit, :]
        for side, left in enumerate((gate_t, up_t)):
            total = contract(left[...], all_g[:, columns], 1, 0).astype(jnp.bfloat16)
            dw_ref[columns, side * width : (side + 1) * width] = total.T
        return carry

    reduce.own_share()
    lax.fori_loop(0, 4, give, 0)
    near = copies.next
    copies.next += 4
    total = jnp.zeros_like(gain)
    for which in (1, 0):
        rows_at = pl.ds(which * half, half)
        grad_normed, normed = reduce.sum_half(which), normed_ref[rows_at, :]
        scaled = grad_normed * gain
        mean = jnp.mean(scaled * normed, axis=-1, keepdims=True)
        total = total + jnp.sum(grad_normed * normed, axis=0, keepdims=True)
        dy = dy_ref[pl.ds(pl.multiple_of(me * rows + which * half, half), half), :]
        residual = dy.astype(jnp.float32) + scale_ref[rows_at, :] * (scaled - normed * mean)
        residual_ref[rows_at, :] = residual
        own_ref[rows_at, :] = residual.astype(jnp.bfloat16)
        for number, target, bit in ((0, near_x_ref, 2), (1, near_y_ref, 4)):
            copies.send(
                near + 2 * which + number,
                own_ref.at[rows_at, :],
                target.at[rows_at, :],
                {"ctx": me ^ bit},
            )
    term_ref[...] = total
    lax.fori_loop(0, 4, keep, 0)
    outputs = local_copies(
        [
            (out_heard.at[number], ref)
            for number, ref in enumerate((out6_hbm, out2_hbm, out4_hbm, out0_hbm))
        ],
        here.at[pl.ds(0, 4)],
    )
    lax.fori_loop(0, blocks, weights, 0)
    outputs += local_copies([(dw_ref, dw_hbm)], here.at[pl.ds(4, 1)])
    for number in range(4):
        out_copy(number).wait_send()
    for copy in outputs:
        copy.wait()
    dealt(dealt_hbm.shape[0])
    shares.finish()
    reduce.finish()
    for which in (1, 0):
        rows_at = pl.ds(which * half, half)
        copies.arrived(near + 2 * which, near_x_ref.at[rows_at, :])
        copies.arrived(near + 2 * which + 1, near_y_ref.at[rows_at, :])
    copies.finish()


def feed(own_rows, grads, w, ot, normed, scale, gain):
    plane, line = lax.axis_size("ctx"), lax.axis_size("fsdp")
    rows, model = own_rows[0].shape
    tokens = plane * rows
    width = w.shape[1] // 3
    pieces = 2 * GROUP
    ot = ot.reshape(pieces, -1, ot.shape[1])
    count = 7 + 4 + pieces + REDUCE_COPIES + 4 + 4
    half_type = jnp.bfloat16
    return pl.pallas_call(
        functools.partial(feed_kernel, line),
        out_shape=(
            jax.ShapeDtypeStruct((rows, model), jnp.float32),
            jax.ShapeDtypeStruct((1, model), jnp.float32),
            *[jax.ShapeDtypeStruct((rows, model), half_type)] * 3,
            jax.ShapeDtypeStruct((line, *ot.shape[1:]), ot.dtype),
            *[jax.ShapeDtypeStruct((rows, model), half_type)] * 4,
            jax.ShapeDtypeStruct(w.shape, half_type),
        ),
        in_specs=anywhere(10) + in_vmem(2),
        out_specs=(*in_vmem(3), *anywhere(8)),
        scratch_shapes=[
            pltpu.VMEM((rows, model), jnp.float32),
            pltpu.VMEM(w.shape, half_type),
            pltpu.VMEM(w.shape, half_type),
            pltpu.VMEM((width, model), half_type),
            pltpu.VMEM((tokens, model), half_type),
            pltpu.VMEM((tokens, model), half_type),
            pltpu.VMEM((tokens, width), half_type),
            pltpu.VMEM((width, tokens), half_type),
            pltpu.VMEM((width, tokens), half_type),
            pltpu.VMEM((width, tokens), half_type),
            pltpu.VMEM((tokens, model), half_type),
            pltpu.VMEM((4, rows, model), half_type),
            pltpu.VMEM((3, rows, model), half_type),
            pltpu.VMEM((3, rows, model), half_type),
            pltpu.VMEM((4, rows, model), half_type),
            pltpu.VMEM((4, rows, model), half_type),
            pltpu.SemaphoreType.DMA((count,)),
            pltpu.SemaphoreType.DMA((count,)),
            pltpu.SemaphoreType.DMA((10,)),
        ],
        compiler_params=pltpu.CompilerParams(
            collective_id=3, has_side_effects=True, vmem_limit_bytes=62 << 20
        ),
        name="feed",
    )(*own_rows, *grads, w, ot, normed, scale, gain)


def input_kernel(
    dqkv_ref,
    wp_hbm,
    x_hbm,
    residual_hbm,
    dwo_hbm,
    term_ref,
    gain_ref,
    pad_ref,
    input_ref,
    grads_ref,
    wp_ref,
    all_x,
    residual_ref,
    dwo_ref,
    part,
    dw,
    heard,
    held,
    landed,
    send,
    recv,
    here,
):
    me = lax.axis_index("ctx")
    rows = residual_ref.shape[0]
    fetch = local_copies(
        [(wp_hbm, wp_ref), (x_hbm, all_x), (residual_hbm, residual_ref), (dwo_hbm, dwo_ref)], here
    )
    start_barrier(me, NEAR)
    copies = Copies(send, recv)

    def at(slot):
        return pl.ds(pl.multiple_of(slot * rows, rows), rows)

    def compute(slot):
        place = at(slot)
        part[place, :] = contract(dqkv_ref[place, :], wp_ref[...], 1, 1).astype(jnp.bfloat16)

    reduce = PlaneReduce(copies, me, lambda slot: part.at[at(slot), :], heard, held, landed)
    fetch[0].wait()
    compute(me ^ 7)
    reduce.share(0)
    compute(me ^ 6)
    compute(me ^ 3)
    reduce.share(1)
    reduce.diagonal_sends()
    compute(me ^ 2)
    compute(me ^ 5)
    reduce.share(2)
    compute(me ^ 4)
    reduce.neighbour_sends()
    compute(me ^ 1)
    reduce.share(3)
    compute(me)
    gain = gain_ref[...]
    dw[...] = jnp.zeros_like(dw)
    for copy in fetch[1:]:
        copy.wait()

    def weights(slot, carry):
        place = at(slot)
        x = all_x[place, :].astype(jnp.float32)
        normed = x * lax.rsqrt(jnp.mean(x * x, axis=-1, keepdims=True) + norm_epsilon)
        gained = (normed * gain).astype(jnp.bfloat16)
        dw[...] += contract(dqkv_ref[place, :], gained, 0, 0)
        return carry

    plane = part.shape[0] // rows
    lax.fori_loop(0, plane // 2, weights, 0)
    reduce.second_sends()
    reduce.own_share()
    lax.fori_loop(plane // 2, plane, weights, 0)
    packed = contract(pad_ref[...], dw[...].astype(jnp.bfloat16), 1, 0)
    packed = packed.astype(jnp.bfloat16).T
    line = dwo_ref.shape[0]
    shard = packed.shape[0] // line
    for slot in range(line):
        grads_ref[slot, :shard, :] = packed[slot * shard : (slot + 1) * shard, :]
        grads_ref[slot, shard : shard + dwo_ref.shape[1], :] = dwo_ref[slot]
    half = rows // 2
    total = jnp.zeros_like(gain)
    for which in (1, 0):
        here_rows = pl.ds(which * half, half)
        grad = reduce.sum_half(which)
        own_rows = pl.ds(pl.multiple_of(me * rows + which * half, half), half)
        x = all_x[own_rows, :].astype(jnp.float32)
        scale = lax.rsqrt(jnp.mean(x * x, axis=-1, keepdims=True) + norm_epsilon)
        normed = x * scale
        total = total + jnp.sum(grad * normed, axis=0, keepdims=True)
        scaled = grad * gain
        mean = jnp.mean(scaled * normed, axis=-1, keepdims=True)
        input_ref[0, here_rows, :] = residual_ref[here_rows, :] + scale * (scaled - normed * mean)
    blank = jnp.zeros((GAIN_ROWS - 2, grads_ref.shape[2]), jnp.float32)
    for slot in range(line):
        columns = slice(slot * shard, (slot + 1) * shard)
        rows_of = jnp.concatenate([total[:, columns], term_ref[:, columns], blank], axis=0)
        grads_ref[slot, grads_ref.shape[1] - GAIN_ROWS :, :] = rows_of.astype(grads_ref.dtype)
    reduce.finish()
    copies.finish()


GAIN_ROWS = 32


def input_exchange(dqkv, wp, x, residual, dwo, term, gain, pad):
    rows, model = residual.shape
    line, dealt, across = dwo.shape
    f32 = jnp.float32
    return pl.pallas_call(
        input_kernel,
        out_shape=(
            jax.ShapeDtypeStruct((1, rows, model), f32),
            jax.ShapeDtypeStruct((line, model // line + dealt + GAIN_ROWS, across), dwo.dtype),
        ),
        in_specs=in_vmem(1) + in_hbm(4) + in_vmem(3),
        out_specs=tuple(in_vmem(2)),
        scratch_shapes=[
            pltpu.VMEM(wp.shape, wp.dtype),
            pltpu.VMEM(x.shape, x.dtype),
            pltpu.VMEM(residual.shape, residual.dtype),
            pltpu.VMEM(dwo.shape, dwo.dtype),
            pltpu.VMEM(x.shape, x.dtype),
            pltpu.VMEM((dqkv.shape[1], model), f32),
            pltpu.VMEM((4, rows, model), x.dtype),
            pltpu.VMEM((3, rows, model), x.dtype),
            pltpu.VMEM((3, rows, model), x.dtype),
            pltpu.SemaphoreType.DMA((REDUCE_COPIES,)),
            pltpu.SemaphoreType.DMA((REDUCE_COPIES,)),
            pltpu.SemaphoreType.DMA((4,)),
        ],
        compiler_params=remote_params(7),
        name="input_exchange",
    )(dqkv, wp, x, residual, dwo, term, gain, pad)


def pieces_kernel(
    piece_ref,
    residual_hbm,
    out0_hbm,
    out2_hbm,
    out4_hbm,
    out6_hbm,
    whole_ref,
    output_ref,
    own,
    residual_ref,
    outs_ref,
    send,
    recv,
    here,
):
    me = lax.axis_index("ctx")
    outs = (out0_hbm, out2_hbm, out4_hbm, out6_hbm)
    fetch = local_copies(
        [(piece_ref, own), (residual_hbm, residual_ref)]
        + [(ref, outs_ref.at[number]) for number, ref in enumerate(outs)],
        here.at[pl.ds(0, 6)],
    )
    start_barrier(me, NEAR)
    copies = Copies(send, recv)
    rows = piece_ref.shape[0]
    part = row_part(whole_ref, rows)
    gather = PlaneGather(copies, me, row_half(own, rows), part)
    fetch[0].wait()
    gather.begin()
    local = local_copies([(own, part(me, slice(None)))], here.at[pl.ds(6, 1)])
    for copy in fetch[1:]:
        copy.wait()
    total = residual_ref[...]
    for number in range(4):
        total = total + outs_ref[number].astype(jnp.float32)
    output_ref[0] = total.astype(output_ref.dtype)
    gather.first_hop()
    gather.second_hop()
    gather.third_hop()
    gather.last()
    gather.finish()
    local[0].wait()


def pieces_exchange(piece, residual, outs):
    plane = lax.axis_size("ctx")
    rows, model = residual.shape
    return pl.pallas_call(
        pieces_kernel,
        out_shape=(
            jax.ShapeDtypeStruct((plane * piece.shape[0], piece.shape[1]), piece.dtype),
            jax.ShapeDtypeStruct((1, rows, model), jnp.bfloat16),
        ),
        in_specs=anywhere(6),
        out_specs=(*anywhere(1), *in_vmem(1)),
        scratch_shapes=[
            pltpu.VMEM(piece.shape, piece.dtype),
            pltpu.VMEM((rows, model), jnp.float32),
            pltpu.VMEM((4, rows, model), outs[0].dtype),
            pltpu.SemaphoreType.DMA((GATHER_COPIES,)),
            pltpu.SemaphoreType.DMA((GATHER_COPIES,)),
            pltpu.SemaphoreType.DMA((7,)),
        ],
        compiler_params=remote_params(8),
        name="pieces_exchange",
    )(piece, residual, *outs)


def spread_kernel(gate_in, up_in, down_in, gate_ref, up_ref, down_ref):
    plane, shard, unit = gate_in.shape
    for source, target in ((gate_in, gate_ref), (up_in, up_ref)):
        for slot in range(plane):
            target[:, slot * unit : (slot + 1) * unit] = source[slot].astype(jnp.float32)
    width = down_in.shape[2]
    blocks = shard // unit
    for slot in range(down_in.shape[0]):
        for number in range(blocks):
            down_ref[slot * unit : (slot + 1) * unit, number * width : (number + 1) * width] = (
                down_in[slot, number * unit : (number + 1) * unit, :].astype(jnp.float32)
            )


def spread_feed(pieces, shard, line, unit):
    plane = lax.axis_size("ctx")
    width = line * unit
    model = line * shard
    pieces = pieces.reshape(plane, shard, 3 * width)
    each = plane // line
    return pl.pallas_call(
        spread_kernel,
        grid=(line,),
        in_specs=[
            pl.BlockSpec((plane, shard, unit), lambda z: (0, 0, z)),
            pl.BlockSpec((plane, shard, unit), lambda z: (0, 0, line + z)),
            pl.BlockSpec((each, shard, width), lambda z: (z, 0, 2)),
        ],
        out_specs=(
            pl.BlockSpec((shard, plane * unit), lambda z: (0, z)),
            pl.BlockSpec((shard, plane * unit), lambda z: (0, z)),
            pl.BlockSpec((each * unit, model), lambda z: (z, 0)),
        ),
        out_shape=(
            jax.ShapeDtypeStruct((shard, plane * width), jnp.float32),
            jax.ShapeDtypeStruct((shard, plane * width), jnp.float32),
            jax.ShapeDtypeStruct((plane * unit, model), jnp.float32),
        ),
        compiler_params=pltpu.CompilerParams(vmem_limit_bytes=62 << 20),
        name="spread_feed",
    )(pieces, pieces, pieces)


def spread_attention_kernel(in_ref, q_ref, k_ref, v_ref, wo_ref, gains_ref):
    plane, _, across = in_ref.shape
    shard = q_ref.shape[0]
    key_width = k_ref.shape[1] // plane
    query_width = q_ref.shape[1] // plane
    first = 0
    for target, width in ((q_ref, query_width), (k_ref, key_width), (v_ref, key_width)):
        target[...] = jnp.concatenate(
            [
                in_ref[slot, :shard, first : first + width].astype(jnp.float32)
                for slot in range(plane)
            ],
            axis=1,
        )
        first += width
    for slot in range(plane):
        for number in range(wo_ref.shape[1] // across):
            source = slice(shard + number * HALF, shard + (number + 1) * HALF)
            wo_ref[slot * HALF : (slot + 1) * HALF, number * across : (number + 1) * across] = (
                in_ref[slot, source, :].astype(jnp.float32)
            )
    terms = [in_ref[slot, in_ref.shape[1] - GAIN_ROWS :, :] for slot in range(plane)]
    gains_ref[...] = sum(term.astype(jnp.float32) for term in terms)[: gains_ref.shape[0], :]


def spread_attention(pieces, shard, model, query_width, key_width):
    plane = lax.axis_size("ctx")
    pieces = pieces.reshape(plane, -1, pieces.shape[1])
    f32 = jnp.float32
    return pl.pallas_call(
        spread_attention_kernel,
        in_specs=in_vmem(1),
        out_specs=tuple(in_vmem(5)),
        out_shape=(
            jax.ShapeDtypeStruct((shard, plane * query_width), f32),
            jax.ShapeDtypeStruct((shard, plane * key_width), f32),
            jax.ShapeDtypeStruct((shard, plane * key_width), f32),
            jax.ShapeDtypeStruct((plane * HALF, model), f32),
            jax.ShapeDtypeStruct((8, shard), f32),
        ),
        compiler_params=pltpu.CompilerParams(vmem_limit_bytes=40 << 20),
        name="spread_attention",
    )(pieces)


def head_local(
    block_input,
    block_table,
    output_grad,
    attention_gain,
    query_weight,
    key_weight,
    value_projection,
    output_weight,
    feedforward_gain,
    gate_weight,
    up_weight,
    down_weight,
):
    me = lax.axis_index("ctx")
    plane = lax.axis_size("ctx")
    line = lax.axis_size("fsdp")
    rows, model = block_input.shape[1:]
    shard = model // line
    hidden = gate_weight.shape[1]
    unit = hidden // (line * plane)
    table_row = block_table[0]
    slot_count = table_row.shape[0]
    block = rows * plane // slot_count
    places = jnp.arange(slot_count, dtype=jnp.int32)
    slots = jnp.sum(jnp.where(table_row[None, :] == places[:, None], places[None, :], 0), axis=1)

    def mine(array, width):
        return lax.dynamic_slice_in_dim(array, me * width, width, 1)

    query_width = query_weight.shape[1] // plane
    key_width = key_weight.shape[1] // plane
    qkv_mine = jnp.concatenate(
        [
            mine(query_weight, query_width),
            mine(key_weight, key_width),
            mine(value_projection, key_width),
        ],
        axis=1,
    )
    gains_mine = jnp.stack([attention_gain, feedforward_gain])
    x_all, qkv_w, wo_line, gains, feed_mine = first_exchange(
        line,
        block_input[0],
        qkv_mine,
        output_weight,
        gains_mine,
        gate_weight,
        up_weight,
        down_weight,
    )
    feed_w = lax.all_gather(feed_mine, "fsdp", axis=0, tiled=True)

    inner = angle_table(np.arange(block))
    outer = angle_table(np.arange(slot_count) * block)
    pad = padding(GROUP + 2)

    gains = jnp.transpose(gains, (1, 0, 2)).reshape(2, model).astype(jnp.float32)
    qkv_w = qkv_w.reshape(model, -1)
    grad_rows, wo_line, x_all = lax.optimization_barrier((output_grad[0], wo_line, x_all))
    grad_parts, wo_parts = [grad_rows], [wo_line]
    for bit in (2, 4):
        pairs = [(device, device ^ bit) for device in range(plane)]
        grad_parts.append(lax.ppermute(grad_rows, "ctx", pairs))
        wo_parts.append(lax.ppermute(wo_line, "ctx", pairs))
    qkv, o, o_columns, lse, qkv_pad = attend(
        slots, x_all, gains[:1], qkv_w, pad, inner, outer
    )
    wo_mine, far_grads, residual, normed_two, scale_two, *gained_two = second_exchange(
        o, wo_parts, grad_parts[1:], block_input[0], gains[1:]
    )
    grad_residual, feedforward_term, *rest = feed(
        gained_two,
        [*grad_parts, far_grads],
        feed_w,
        o_columns,
        normed_two,
        scale_two,
        gains[1:],
    )
    grad_attn, columns_mine, out_parts, feed_grads = rest[:3], rest[3], rest[4:8], rest[8]
    feed_grads = lax.psum_scatter(feed_grads, "fsdp", scatter_dimension=0, tiled=True)
    grad_o, wo_term = third_exchange(
        line,
        grad_attn,
        columns_mine.reshape(-1, columns_mine.shape[2]),
        wo_mine.reshape(-1, model),
        qkv_w.shape[1],
    )
    *out_parts, grad_o = lax.optimization_barrier((*out_parts, grad_o))
    outs = [out_parts[3]]
    for part, bit in enumerate((6, 2, 4)):
        pairs = [(device, device ^ bit) for device in range(plane)]
        outs.append(lax.ppermute(out_parts[part], "ctx", pairs))
    grads = attend_back(slots, qkv, o, grad_o, lse, pad, inner, outer)
    input_grad, attention_grads = input_exchange(
        grads, qkv_pad, x_all, grad_residual, wo_term, feedforward_term, gains[:1], pad
    )
    attention_grads, feed_grads = lax.optimization_barrier((attention_grads, feed_grads))
    attention_grads = lax.psum_scatter(
        attention_grads.reshape(-1, attention_grads.shape[2]),
        "fsdp",
        scatter_dimension=0,
        tiled=True,
    )
    feed_pieces, layer_output = pieces_exchange(feed_grads, residual, outs)
    attention_grads, layer_output = lax.optimization_barrier((attention_grads, layer_output))
    near_grads = []
    for bit in (2, 4):
        pairs = [(device, device ^ bit) for device in range(plane)]
        near_grads.append(lax.ppermute(attention_grads, "ctx", pairs))
    gate_grad, up_grad, down_grad = spread_feed(feed_pieces, shard, line, unit)
    attention_pieces = near_gather([attention_grads, *near_grads], 9)
    query_grad, key_grad, value_grad, out_grad, gain_terms = spread_attention(
        attention_pieces, shard, model, query_width, key_width
    )
    return (
        layer_output,
        input_grad,
        gain_terms[0],
        query_grad,
        key_grad,
        value_grad,
        out_grad,
        gain_terms[1],
        gate_grad,
        up_grad,
        down_grad,
    )


def solution(mesh):
    plane, line = mesh.shape["ctx"], mesh.shape["fsdp"]
    fits = plane == KEY_VALUE_HEADS == 8 and plane * line * HALF == QUERY_HEADS * HEAD_SIZE
    if fits:
        return placed(mesh, head_local)
    return placed(mesh, local)


def placed(mesh, plan):
    return jax.shard_map(
        plan,
        mesh=mesh,
        in_specs=(
            P("fsdp", "ctx", None),
            P("fsdp", None),
            P("fsdp", "ctx", None),
            P("fsdp"),
            P("fsdp", None),
            P("fsdp", None),
            P("fsdp", None),
            P("fsdp", None),
            P("fsdp"),
            P("fsdp", None),
            P("fsdp", None),
            P("fsdp", None),
        ),
        out_specs=(
            P("fsdp", "ctx", None),
            P("fsdp", "ctx", None),
            P("fsdp"),
            P("fsdp", None),
            P("fsdp", None),
            P("fsdp", None),
            P("fsdp", None),
            P("fsdp"),
            P("fsdp", None),
            P("fsdp", None),
            P("fsdp", None),
        ),
        check_vma=False,
    )
```

```python
import functools
import math

import jax
import jax.numpy as jnp
import numpy as np
from jax import lax
from jax.experimental import pallas as pl
from jax.experimental.pallas import tpu as pltpu
from jax.sharding import PartitionSpec as P


QUERY_HEADS = 16
KEY_VALUE_HEADS = 8
HEAD_SIZE = 96


norm_epsilon = 1e-05
rotary_base = 100000.0
score_with_mask = -1e30


def rope_tables(positions):
    half_width = HEAD_SIZE // 2
    steps_index = jnp.arange(half_width, dtype=jnp.float32)
    inverse = jnp.exp(steps_index * jnp.float32(-2.0 * math.log(rotary_base) / HEAD_SIZE))
    angles = positions.astype(jnp.float32)[:, None] * inverse[None, :]
    return (jnp.cos(angles), jnp.sin(angles))


def rotate(value_rows, cosine, sine_values, direction):
    count_of_rows = value_rows.shape[0]
    head_count = value_rows.shape[1] // HEAD_SIZE
    half_width = HEAD_SIZE // 2
    shaped = value_rows.reshape(count_of_rows, head_count, HEAD_SIZE)
    first_half = shaped[:, :, :half_width]
    second_half = shaped[:, :, half_width:]
    cos_part = cosine[:, None, :]
    sin_part = sine_values[:, None, :] * direction
    turned = jnp.concatenate(
        [
            first_half * cos_part - second_half * sin_part,
            second_half * cos_part + first_half * sin_part,
        ],
        axis=2,
    )
    return turned.reshape(count_of_rows, head_count * HEAD_SIZE)


def norm_scale(value_rows):
    return lax.rsqrt(jnp.mean(value_rows * value_rows, axis=-1, keepdims=True) + norm_epsilon)


def product(matrix, operand):
    return jnp.dot(matrix, operand, preferred_element_type=jnp.float32)


def cross_rows(matrix, operand):
    return lax.dot_general(
        matrix, operand, (((0,), (0,)), ((), ())), preferred_element_type=jnp.float32
    )


def back_product(matrix, operand):
    return lax.dot_general(
        matrix, operand, (((1,), (1,)), ((), ())), preferred_element_type=jnp.float32
    )


def block_scores(query_rank_four, block_of_keys, query_positions, key_positions):
    keys_rank_three = block_of_keys.reshape(block_of_keys.shape[0], KEY_VALUE_HEADS, HEAD_SIZE)
    scores = jnp.einsum(
        "rgjd,kgd->gjrk", query_rank_four, keys_rank_three, preferred_element_type=jnp.float32
    ) * HEAD_SIZE ** (-0.5)
    allowed = (key_positions[None, :] <= query_positions[:, None])[None, None]
    return (jnp.where(allowed, scores, score_with_mask), allowed)


def local(
    block_input,
    block_table,
    output_grad,
    attention_gain,
    query_weight,
    key_weight,
    value_projection,
    output_weight,
    feedforward_gain,
    gate_weight,
    up_weight,
    down_weight,
):
    query_group_width = QUERY_HEADS // KEY_VALUE_HEADS
    score_scale = HEAD_SIZE ** (-0.5)
    inputs = block_input[0].astype(jnp.float32)
    count_of_rows = inputs.shape[0]
    block_rows = count_of_rows // 2
    ctx_index = lax.axis_index("ctx")
    table_row = block_table[0]
    offsets = jnp.arange(block_rows, dtype=jnp.int32)
    query_blocks = lax.dynamic_slice_in_dim(table_row, 2 * ctx_index, 2)
    query_positions = (query_blocks[:, None] * block_rows + offsets[None, :]).reshape(count_of_rows)
    key_positions = (table_row[:, None] * block_rows + offsets[None, :]).reshape(-1)
    cosine, sine_values = rope_tables(query_positions)
    gain_one, query_full, key_full, value_full, out_full = (
        lax.all_gather(attention_gain, "fsdp", axis=0, tiled=True),
        lax.all_gather(query_weight, "fsdp", axis=0, tiled=True),
        lax.all_gather(key_weight, "fsdp", axis=0, tiled=True),
        lax.all_gather(value_projection, "fsdp", axis=0, tiled=True),
        lax.all_gather(output_weight, "fsdp", axis=0, tiled=True),
    )
    scale_one = norm_scale(inputs)
    normed_one = inputs * scale_one
    gained_one = (normed_one * gain_one.astype(jnp.float32)).astype(jnp.bfloat16)
    query_rows = rotate(product(gained_one, query_full), cosine, sine_values, 1.0).astype(
        jnp.bfloat16
    )
    keys_local = rotate(product(gained_one, key_full), cosine, sine_values, 1.0).astype(
        jnp.bfloat16
    )
    values_local = product(gained_one, value_full).astype(jnp.bfloat16)
    keys_all, values_all = (
        lax.all_gather(keys_local, "ctx", axis=0, tiled=True),
        lax.all_gather(values_local, "ctx", axis=0, tiled=True),
    )
    key_total_count = keys_all.shape[0]
    key_block_pass = 1024
    block_count = key_total_count // key_block_pass
    query_rank_four = query_rows.reshape(
        count_of_rows, KEY_VALUE_HEADS, query_group_width, HEAD_SIZE
    )
    key_places = key_positions.reshape(block_count, key_block_pass)

    def split_keys(array_in):
        return array_in.reshape(block_count, key_block_pass, array_in.shape[-1])

    def statistics_step(state_now, block_data):
        running_max, running_sum = state_now
        block_of_keys, key_place = block_data
        masked, allowed = block_scores(query_rank_four, block_of_keys, query_positions, key_place)
        new_max = jnp.maximum(running_max, jnp.max(masked, axis=-1))
        block_sum = jnp.sum(jnp.where(allowed, jnp.exp(masked - new_max[..., None]), 0.0), axis=-1)
        return ((new_max, running_sum * jnp.exp(running_max - new_max) + block_sum), None)

    initial_maximum = jnp.full(
        (KEY_VALUE_HEADS, query_group_width, count_of_rows), score_with_mask, jnp.float32
    )
    initial_sum = jnp.zeros((KEY_VALUE_HEADS, query_group_width, count_of_rows), jnp.float32)
    (final_max, final_sum), unused = lax.scan(
        statistics_step, (initial_maximum, initial_sum), (split_keys(keys_all), key_places)
    )
    log_total = final_max + jnp.log(final_sum)

    def output_step(state_now, block_data):
        block_of_keys, block_of_values, key_place = block_data
        masked, allowed = block_scores(query_rank_four, block_of_keys, query_positions, key_place)
        weights_half = jnp.where(allowed, jnp.exp(masked - log_total[..., None]), 0.0).astype(
            jnp.bfloat16
        )
        values_rank_three = block_of_values.reshape(key_block_pass, KEY_VALUE_HEADS, HEAD_SIZE)
        return (
            state_now
            + jnp.einsum(
                "gjrk,kgd->rgjd",
                weights_half,
                values_rank_three,
                preferred_element_type=jnp.float32,
            ),
            None,
        )

    initial_output = jnp.zeros(
        (count_of_rows, KEY_VALUE_HEADS, query_group_width, HEAD_SIZE), jnp.float32
    )
    summed_out, unused = lax.scan(
        output_step, initial_output, (split_keys(keys_all), split_keys(values_all), key_places)
    )
    attended_rows = summed_out.reshape(count_of_rows, QUERY_HEADS * HEAD_SIZE).astype(jnp.bfloat16)
    residual = inputs + product(attended_rows, out_full)
    scale_two = norm_scale(residual)
    normed_two = residual * scale_two
    gain_two, gate_full, up_full, down_full = (
        lax.all_gather(feedforward_gain, "fsdp", axis=0, tiled=True),
        lax.all_gather(gate_weight, "fsdp", axis=0, tiled=True),
        lax.all_gather(up_weight, "fsdp", axis=0, tiled=True),
        lax.all_gather(down_weight, "fsdp", axis=0, tiled=True),
    )
    gained_two = (normed_two * gain_two.astype(jnp.float32)).astype(jnp.bfloat16)
    gate_values = product(gained_two, gate_full)
    up_values = product(gained_two, up_full)
    sigmoid_gate = jax.nn.sigmoid(gate_values)
    activated = gate_values * sigmoid_gate
    hidden_act = (activated * up_values).astype(jnp.bfloat16)
    layer_output = (residual + product(hidden_act, down_full)).astype(jnp.bfloat16)
    gain_two_again, gate_back, up_back, down_back = (
        lax.all_gather(feedforward_gain, "fsdp", axis=0, tiled=True),
        lax.all_gather(gate_weight, "fsdp", axis=0, tiled=True),
        lax.all_gather(up_weight, "fsdp", axis=0, tiled=True),
        lax.all_gather(down_weight, "fsdp", axis=0, tiled=True),
    )
    grad_rows = output_grad[0]
    grad_hidden = back_product(grad_rows, down_back)
    down_term = cross_rows(hidden_act, grad_rows)
    grad_gate = (
        grad_hidden * up_values * sigmoid_gate * (1.0 + gate_values * (1.0 - sigmoid_gate))
    ).astype(jnp.bfloat16)
    grad_up = (grad_hidden * activated).astype(jnp.bfloat16)
    gate_term = cross_rows(gained_two, grad_gate)
    up_term = cross_rows(gained_two, grad_up)
    grad_normed_two = back_product(grad_gate, gate_back) + back_product(grad_up, up_back)
    feedforward_term = jnp.sum(grad_normed_two * normed_two, axis=0)
    grad_scaled_two = grad_normed_two * gain_two_again.astype(jnp.float32)
    grad_residual = grad_rows.astype(jnp.float32) + scale_two * (
        grad_scaled_two
        - normed_two * jnp.mean(grad_scaled_two * normed_two, axis=-1, keepdims=True)
    )
    gain_one_again, query_back, key_back, value_back, out_back = (
        lax.all_gather(attention_gain, "fsdp", axis=0, tiled=True),
        lax.all_gather(query_weight, "fsdp", axis=0, tiled=True),
        lax.all_gather(key_weight, "fsdp", axis=0, tiled=True),
        lax.all_gather(value_projection, "fsdp", axis=0, tiled=True),
        lax.all_gather(output_weight, "fsdp", axis=0, tiled=True),
    )
    grad_attn = grad_residual.astype(jnp.bfloat16)
    output_term = cross_rows(attended_rows, grad_attn)
    attended_gradient = back_product(grad_attn, out_back).astype(jnp.bfloat16)
    gradient_rank_four = attended_gradient.reshape(
        count_of_rows, KEY_VALUE_HEADS, query_group_width, HEAD_SIZE
    )
    attended_rank_four = attended_rows.reshape(
        count_of_rows, KEY_VALUE_HEADS, query_group_width, HEAD_SIZE
    )
    row_delta = jnp.transpose(
        jnp.sum(
            gradient_rank_four.astype(jnp.float32) * attended_rank_four.astype(jnp.float32), axis=-1
        ),
        (1, 2, 0),
    )
    keys_again, values_again = (
        lax.all_gather(keys_local, "ctx", axis=0, tiled=True),
        lax.all_gather(values_local, "ctx", axis=0, tiled=True),
    )

    def back_step(state_now, block_data):
        block_of_keys, block_of_values, key_place = block_data
        masked, allowed = block_scores(query_rank_four, block_of_keys, query_positions, key_place)
        weights_half = jnp.where(allowed, jnp.exp(masked - log_total[..., None]), 0.0).astype(
            jnp.bfloat16
        )
        values_rank_three = block_of_values.reshape(key_block_pass, KEY_VALUE_HEADS, HEAD_SIZE)
        keys_rank_three = block_of_keys.reshape(key_block_pass, KEY_VALUE_HEADS, HEAD_SIZE)
        grad_weights = jnp.einsum(
            "rgjd,kgd->gjrk",
            gradient_rank_four,
            values_rank_three,
            preferred_element_type=jnp.float32,
        )
        grad_scores = (
            weights_half.astype(jnp.float32) * (grad_weights - row_delta[..., None]) * score_scale
        ).astype(jnp.bfloat16)
        state_now = state_now + jnp.einsum(
            "gjrk,kgd->rgjd", grad_scores, keys_rank_three, preferred_element_type=jnp.float32
        )
        key_gradient = jnp.einsum(
            "gjrk,rgjd->kgd", grad_scores, query_rank_four, preferred_element_type=jnp.float32
        )
        value_gradient = jnp.einsum(
            "gjrk,rgjd->kgd", weights_half, gradient_rank_four, preferred_element_type=jnp.float32
        )
        return (
            state_now,
            (
                key_gradient.reshape(key_block_pass, KEY_VALUE_HEADS * HEAD_SIZE).astype(
                    jnp.bfloat16
                ),
                value_gradient.reshape(key_block_pass, KEY_VALUE_HEADS * HEAD_SIZE).astype(
                    jnp.bfloat16
                ),
            ),
        )

    first_query_index = jnp.zeros(
        (count_of_rows, KEY_VALUE_HEADS, query_group_width, HEAD_SIZE), jnp.float32
    )
    query_sum, (key_gradients, value_gradients) = lax.scan(
        back_step, first_query_index, (split_keys(keys_again), split_keys(values_again), key_places)
    )
    key_gradients = key_gradients.reshape(key_total_count, KEY_VALUE_HEADS * HEAD_SIZE)
    value_gradients = value_gradients.reshape(key_total_count, KEY_VALUE_HEADS * HEAD_SIZE)
    key_sums, value_sums = (
        lax.psum_scatter(key_gradients, "ctx", scatter_dimension=0, tiled=True).astype(jnp.float32),
        lax.psum_scatter(value_gradients, "ctx", scatter_dimension=0, tiled=True).astype(
            jnp.float32
        ),
    )
    query_gradients = rotate(
        query_sum.reshape(count_of_rows, QUERY_HEADS * HEAD_SIZE), cosine, sine_values, -1.0
    ).astype(jnp.bfloat16)
    grad_keys = rotate(key_sums, cosine, sine_values, -1.0).astype(jnp.bfloat16)
    grad_values = value_sums.astype(jnp.bfloat16)
    query_term = cross_rows(gained_one, query_gradients)
    key_term = cross_rows(gained_one, grad_keys)
    value_term = cross_rows(gained_one, grad_values)
    grad_normed_one = (
        back_product(query_gradients, query_back)
        + back_product(grad_keys, key_back)
        + back_product(grad_values, value_back)
    )
    attention_term = jnp.sum(grad_normed_one * normed_one, axis=0)
    grad_scaled_one = grad_normed_one * gain_one_again.astype(jnp.float32)
    input_grad = grad_residual + scale_one * (
        grad_scaled_one
        - normed_one * jnp.mean(grad_scaled_one * normed_one, axis=-1, keepdims=True)
    )
    shares = (
        lax.psum_scatter(
            attention_term.astype(jnp.bfloat16), "fsdp", scatter_dimension=0, tiled=True
        ).astype(jnp.float32),
        lax.psum_scatter(
            query_term.astype(jnp.bfloat16), "fsdp", scatter_dimension=0, tiled=True
        ).astype(jnp.float32),
        lax.psum_scatter(
            key_term.astype(jnp.bfloat16), "fsdp", scatter_dimension=0, tiled=True
        ).astype(jnp.float32),
        lax.psum_scatter(
            value_term.astype(jnp.bfloat16), "fsdp", scatter_dimension=0, tiled=True
        ).astype(jnp.float32),
        lax.psum_scatter(
            output_term.astype(jnp.bfloat16), "fsdp", scatter_dimension=0, tiled=True
        ).astype(jnp.float32),
        lax.psum_scatter(
            feedforward_term.astype(jnp.bfloat16), "fsdp", scatter_dimension=0, tiled=True
        ).astype(jnp.float32),
        lax.psum_scatter(
            gate_term.astype(jnp.bfloat16), "fsdp", scatter_dimension=0, tiled=True
        ).astype(jnp.float32),
        lax.psum_scatter(
            up_term.astype(jnp.bfloat16), "fsdp", scatter_dimension=0, tiled=True
        ).astype(jnp.float32),
        lax.psum_scatter(
            down_term.astype(jnp.bfloat16), "fsdp", scatter_dimension=0, tiled=True
        ).astype(jnp.float32),
    )
    totals = (
        lax.psum(shares[0].astype(jnp.bfloat16), "ctx").astype(jnp.float32),
        lax.psum(shares[1].astype(jnp.bfloat16), "ctx").astype(jnp.float32),
        lax.psum(shares[2].astype(jnp.bfloat16), "ctx").astype(jnp.float32),
        lax.psum(shares[3].astype(jnp.bfloat16), "ctx").astype(jnp.float32),
        lax.psum(shares[4].astype(jnp.bfloat16), "ctx").astype(jnp.float32),
        lax.psum(shares[5].astype(jnp.bfloat16), "ctx").astype(jnp.float32),
        lax.psum(shares[6].astype(jnp.bfloat16), "ctx").astype(jnp.float32),
        lax.psum(shares[7].astype(jnp.bfloat16), "ctx").astype(jnp.float32),
        lax.psum(shares[8].astype(jnp.bfloat16), "ctx").astype(jnp.float32),
    )
    return (
        layer_output[None],
        input_grad[None],
        totals[0],
        totals[1],
        totals[2],
        totals[3],
        totals[4],
        totals[5],
        totals[6],
        totals[7],
        totals[8],
    )


LANES = 128
HALF = HEAD_SIZE // 2
GROUP = QUERY_HEADS // KEY_VALUE_HEADS
score_scale = HEAD_SIZE ** (-0.5)
binary_scale = score_scale * math.log2(math.e)


def contract(left, right, left_dim, right_dim):
    return lax.dot_general(
        left, right, (((left_dim,), (right_dim,)), ((), ())), preferred_element_type=jnp.float32
    )


def in_vmem(count):
    return [pl.BlockSpec(memory_space=pltpu.VMEM)] * count


def padding(heads):
    column = np.arange(heads * HEAD_SIZE)
    target = column // HALF * (LANES // 2) + column % HALF
    lanes = np.arange(heads * LANES)
    return jnp.asarray((target[:, None] == lanes[None, :]).astype(np.float32), jnp.bfloat16)


def angle_table(positions):
    inverse = rotary_base ** (-2.0 * np.arange(HALF) / HEAD_SIZE)
    angles = positions[:, None] * inverse[None, :]
    both = np.stack([np.cos(angles), np.sin(angles)])
    both = np.pad(both, ((0, 0), (0, 0), (0, LANES // 2 - HALF)))
    return jnp.asarray(np.concatenate([both, both], axis=2), jnp.float32)


def turn(part, cosine, sine):
    return part * cosine + pltpu.roll(part, LANES // 2, 1) * sine


def tables(inner_ref, outer_ref, index, per_tile):
    inner_cos, inner_sin = inner_ref[0], inner_ref[1]
    sign = jnp.where(
        lax.broadcasted_iota(jnp.int32, inner_cos.shape, 1) < LANES // 2, -1.0, 1.0
    )
    cosines, sines = [], []
    for part in range(per_tile):
        at = pl.ds(index * per_tile + part, 1)
        outer_cos, outer_sin = outer_ref[0, at, :], outer_ref[1, at, :]
        cosines.append(inner_cos * outer_cos - inner_sin * outer_sin)
        sines.append(sign * (inner_sin * outer_cos + inner_cos * outer_sin))
    return jnp.concatenate(cosines, axis=0), jnp.concatenate(sines, axis=0)


def forward_kernel(
    slot_ref,
    xa_ref,
    xb_ref,
    gain_ref,
    w_ref,
    pad_ref,
    inner_ref,
    outer_ref,
    qkv_hbm,
    o_ref,
    ot_ref,
    lse_ref,
    wp_hbm,
    qkv_ref,
    wp,
    qs,
    vt,
    s_ref,
    here,
):
    index = pl.program_id(0)
    block = xa_ref.shape[0]
    tile = 2 * block
    width = GROUP * tile
    heads = GROUP + 2

    @pl.when(index == 0)
    def _():
        wp[...] = contract(w_ref[...], pad_ref[...], 1, 0).astype(jnp.bfloat16)
        pltpu.make_async_copy(wp, wp_hbm, here.at[1]).start()

    x = jnp.concatenate([xa_ref[...], xb_ref[...]], axis=0).astype(jnp.float32)
    normed = x * lax.rsqrt(jnp.mean(x * x, axis=-1, keepdims=True) + norm_epsilon)
    gained = (normed * gain_ref[...]).astype(jnp.bfloat16)
    raw = contract(gained, wp[...], 1, 0)
    cosine, sine = tables(inner_ref, outer_ref, index, 2)
    here_rows = pl.ds(pl.multiple_of(index * tile, tile), tile)
    for head in range(heads):
        lanes = slice(head * LANES, (head + 1) * LANES)
        part = raw[:, lanes]
        if head <= GROUP:
            part = turn(part, cosine, sine)
        part = part.astype(jnp.bfloat16)
        qkv_ref[here_rows, lanes] = part
        if head < GROUP:
            qs[head * tile : (head + 1) * tile, :] = part
        if head == heads - 1:
            vt[:, here_rows] = part.T

    def save(number):
        place = pl.ds(pl.multiple_of(number * tile, tile), tile)
        return pltpu.make_async_copy(qkv_ref.at[place, :], qkv_hbm.at[place, :], here.at[0])

    save(index).start()
    queries = qs[...]
    key_at = lax.broadcasted_iota(jnp.int32, (tile, width), 0)
    query_at = lax.rem(lax.broadcasted_iota(jnp.int32, (tile, width), 1), tile)
    diagonal = key_at <= query_at

    def scores_of(step):
        at = pl.ds(pl.multiple_of(step * tile, tile), tile)
        keys = qkv_ref[at, GROUP * LANES : (GROUP + 1) * LANES]
        return contract(keys, queries, 1, 1) * binary_scale

    last = jnp.where(diagonal, scores_of(index), score_with_mask)
    s_ref[here_rows, :] = last
    peak = jnp.max(last, axis=0, keepdims=True)

    def in_pairs(one, state):
        state = lax.fori_loop(
            0, lax.div(index, 2), lambda pair, state: one((2 * pair, 2 * pair + 1), state), state
        )
        return lax.fori_loop(0, lax.rem(index, 2), lambda _, state: one((index - 1,), state), state)

    def first_pass(steps, peak):
        found = [scores_of(step) for step in steps]
        for step, scores in zip(steps, found):
            s_ref[pl.ds(pl.multiple_of(step * tile, tile), tile), :] = scores
            peak = jnp.maximum(peak, jnp.max(scores, axis=0, keepdims=True))
        return peak

    peak = in_pairs(first_pass, peak)

    def second_pass(steps, state):
        total, out = state
        for step in steps:
            at = pl.ds(pl.multiple_of(step * tile, tile), tile)
            probs = jnp.exp2(s_ref[at, :] - peak)
            total = total + jnp.sum(probs, axis=0, keepdims=True)
            out = out + contract(vt[:, at], probs.astype(jnp.bfloat16), 1, 0)
        return (total, out)

    total, out = in_pairs(
        second_pass,
        second_pass(
            (index,), (jnp.zeros((1, width), jnp.float32), jnp.zeros((LANES, width), jnp.float32))
        ),
    )
    lse_ref[pl.ds(index, 1), :] = peak + jnp.log2(total)
    out = (out * (1.0 / total)).T.astype(jnp.bfloat16)
    out = jnp.concatenate([out[head * tile : (head + 1) * tile, :] for head in range(GROUP)], axis=1)
    out = contract(out, pad_ref[: GROUP * HEAD_SIZE, : GROUP * LANES], 1, 1).astype(jnp.bfloat16)
    for part in range(2):
        target = pl.ds(pl.multiple_of(slot_ref[index * 2 + part] * block, block), block)
        rows_at = slice(part * block, (part + 1) * block)
        o_ref[target, :] = out[rows_at, :]
        ot_ref[:, target] = out[rows_at, :].T

    save(index).wait()

    @pl.when(index == pl.num_programs(0) - 1)
    def _():
        pltpu.make_async_copy(wp, wp_hbm, here.at[1]).wait()


def attend(slots, x, gain, w, pad, inner, outer):
    rows, model = x.shape
    block = rows // slots.shape[0]
    tile = 2 * block
    width = GROUP * tile
    columns = pad.shape[1]
    whole = lambda *shape: pl.BlockSpec(shape, lambda i, s: (0,) * len(shape))
    return pl.pallas_call(
        forward_kernel,
        grid_spec=pltpu.PrefetchScalarGridSpec(
            num_scalar_prefetch=1,
            grid=(rows // tile,),
            in_specs=[
                pl.BlockSpec((block, model), lambda i, s: (s[2 * i], 0)),
                pl.BlockSpec((block, model), lambda i, s: (s[2 * i + 1], 0)),
                whole(1, model),
                whole(*w.shape),
                whole(*pad.shape),
                whole(*inner.shape),
                whole(*outer.shape),
            ],
            out_specs=(
                pl.BlockSpec(memory_space=pl.ANY),
                whole(rows, GROUP * HEAD_SIZE),
                whole(GROUP * HEAD_SIZE, rows),
                whole(rows // tile, width),
                pl.BlockSpec(memory_space=pl.ANY),
            ),
            scratch_shapes=[
                pltpu.VMEM((rows, columns), jnp.bfloat16),
                pltpu.VMEM((model, columns), jnp.bfloat16),
                pltpu.VMEM((width, LANES), jnp.bfloat16),
                pltpu.VMEM((LANES, rows), jnp.bfloat16),
                pltpu.VMEM((rows, width), jnp.float32),
                pltpu.SemaphoreType.DMA((2,)),
            ],
        ),
        out_shape=(
            jax.ShapeDtypeStruct((rows, columns), jnp.bfloat16),
            jax.ShapeDtypeStruct((rows, GROUP * HEAD_SIZE), jnp.bfloat16),
            jax.ShapeDtypeStruct((GROUP * HEAD_SIZE, rows), jnp.bfloat16),
            jax.ShapeDtypeStruct((rows // tile, width), jnp.float32),
            jax.ShapeDtypeStruct((model, columns), jnp.bfloat16),
        ),
        compiler_params=pltpu.CompilerParams(vmem_limit_bytes=62 << 20),
        cost_estimate=pl.CostEstimate(
            flops=4 * GROUP * rows * rows * LANES // 2 + 2 * rows * model * columns,
            bytes_accessed=4 * rows * model,
            transcendentals=GROUP * rows * rows // 2,
        ),
        name="attend",
    )(slots, x, x, gain, w, pad, inner, outer)


def backward_kernel(
    slot_ref,
    qkv_ref,
    o_ref,
    do_ref,
    lse_ref,
    pad_ref,
    inner_ref,
    outer_ref,
    dqkv_ref,
    qs,
    gs,
    kt,
    dk,
    dv,
):
    step_at = pl.program_id(0)
    tiles = pl.num_programs(0)
    index = tiles - 1 - step_at
    block = qkv_ref.shape[0] // slot_ref.shape[0]
    tile = 2 * block
    width = GROUP * tile
    first_key, first_value = GROUP * LANES, (GROUP + 1) * LANES

    @pl.when(step_at == 0)
    def _():
        kt[...] = qkv_ref[:, first_key:first_value].T
        dk[...] = jnp.zeros_like(dk)
        dv[...] = jnp.zeros_like(dv)

    here = pl.ds(pl.multiple_of(index * tile, tile), tile)
    sources = [
        pl.ds(pl.multiple_of(slot_ref[index * 2 + part] * block, block), block) for part in (0, 1)
    ]
    o = jnp.concatenate([o_ref[source, :] for source in sources], axis=0)
    grads = jnp.concatenate([do_ref[source, :] for source in sources], axis=0)
    products = (grads.astype(jnp.float32) * o.astype(jnp.float32)).T
    grads = contract(grads, pad_ref[: GROUP * HEAD_SIZE, : GROUP * LANES], 1, 0).astype(jnp.bfloat16)
    deltas = []
    for head in range(GROUP):
        lanes = slice(head * LANES, (head + 1) * LANES)
        at = slice(head * tile, (head + 1) * tile)
        qs[at, :] = qkv_ref[here, lanes]
        gs[at, :] = grads[:, lanes]
        features = slice(head * HEAD_SIZE, (head + 1) * HEAD_SIZE)
        deltas.append(jnp.sum(products[features, :], axis=0, keepdims=True))
    delta = jnp.concatenate(deltas, axis=1)
    lse = lse_ref[pl.ds(index, 1), :]
    key_at = lax.broadcasted_iota(jnp.int32, (tile, width), 0)
    query_at = lax.rem(lax.broadcasted_iota(jnp.int32, (tile, width), 1), tile)
    diagonal = key_at <= query_at

    def pieces(steps, masked=False):
        queries, grads = qs[...], gs[...]
        places = [pl.ds(pl.multiple_of(step * tile, tile), tile) for step in steps]
        scores = [contract(qkv_ref[at, first_key:first_value], queries, 1, 1) for at in places]
        grad_probs = [contract(qkv_ref[at, first_value:], grads, 1, 1) for at in places]
        total = None
        for at, score, grad_prob in zip(places, scores, grad_probs):
            probs = jnp.exp2(score * binary_scale - lse)
            if masked:
                probs = jnp.where(diagonal, probs, 0.0)
            dv[at, :] += contract(probs.astype(jnp.bfloat16), grads, 1, 0)
            grad_scores = (probs * (grad_prob - delta)).astype(jnp.bfloat16)
            dk[at, :] += contract(grad_scores, queries, 1, 0)
            part = contract(kt[:, at], grad_scores, 1, 0)
            total = part if total is None else total + part
        return total

    dq = pieces((index,), True)
    dq = lax.fori_loop(
        0, lax.div(index, 2), lambda pair, total: total + pieces((2 * pair, 2 * pair + 1)), dq
    )
    dq = lax.fori_loop(0, lax.rem(index, 2), lambda _, total: total + pieces((index - 1,)), dq)
    dq = dq.T * score_scale
    cosine, sine = tables(inner_ref, outer_ref, index, 2)
    parts = [turn(dq[head * tile : (head + 1) * tile, :], cosine, -sine) for head in range(GROUP)]
    parts.append(turn(dk[here, :] * score_scale, cosine, -sine))
    parts.append(dv[here, :])
    dqkv = jnp.concatenate([part.astype(jnp.bfloat16) for part in parts], axis=1)
    for part in (0, 1):
        dqkv_ref[sources[part], :] = dqkv[part * block : (part + 1) * block, :]


def attend_back(slots, qkv, o, do, lse, pad, inner, outer):
    rows, columns = qkv.shape
    block = rows // slots.shape[0]
    tile = 2 * block
    width = GROUP * tile
    tiles = rows // tile
    operands = (qkv, o, do, lse, pad, inner, outer)
    whole = lambda *shape: pl.BlockSpec(shape, lambda i, s: (0,) * len(shape))
    return pl.pallas_call(
        backward_kernel,
        grid_spec=pltpu.PrefetchScalarGridSpec(
            num_scalar_prefetch=1,
            grid=(tiles,),
            in_specs=[whole(*operand.shape) for operand in operands],
            out_specs=whole(rows, columns),
            scratch_shapes=[
                pltpu.VMEM((width, LANES), jnp.bfloat16),
                pltpu.VMEM((width, LANES), jnp.bfloat16),
                pltpu.VMEM((LANES, rows), jnp.bfloat16),
                pltpu.VMEM((rows, LANES), jnp.float32),
                pltpu.VMEM((rows, LANES), jnp.float32),
            ],
        ),
        out_shape=jax.ShapeDtypeStruct((rows, columns), jnp.bfloat16),
        compiler_params=pltpu.CompilerParams(vmem_limit_bytes=40 << 20),
        cost_estimate=pl.CostEstimate(
            flops=10 * GROUP * rows * rows * LANES // 2,
            bytes_accessed=8 * rows * columns,
            transcendentals=GROUP * rows * rows // 2,
        ),
        name="attend_back",
    )(slots, *operands)


MESH_IDS = pl.DeviceIdType.MESH


NEAR = (1, 2, 4)
ALL = (1, 2, 3, 4, 5, 6, 7)


def start_barrier(me, bits, line_steps=(), line_index=None, line=1):
    barrier = pltpu.get_barrier_semaphore()
    peers = [{"ctx": me ^ bit} for bit in bits]
    peers += [{"fsdp": lax.rem(line_index + step, line)} for step in line_steps]
    for peer in peers:
        pl.semaphore_signal(barrier, inc=1, device_id=peer, device_id_type=MESH_IDS)
    pl.semaphore_wait(barrier, len(peers))


def start_line_barrier(me, index, line):
    barrier = pltpu.get_barrier_semaphore()
    for bit in NEAR:
        pl.semaphore_signal(barrier, inc=1, device_id={"ctx": me ^ bit}, device_id_type=MESH_IDS)
    up, down = index < line - 1, index > 0
    for there, exists in ((index + 1, up), (index - 1, down)):

        @pl.when(exists)
        def _(there=there):
            peer = {"fsdp": jnp.clip(there, 0, line - 1)}
            pl.semaphore_signal(barrier, inc=1, device_id=peer, device_id_type=MESH_IDS)

    pl.semaphore_wait(barrier, len(NEAR) + up.astype(jnp.int32) + down.astype(jnp.int32))


class Copies:
    def __init__(self, send_sems, recv_sems, base=0):
        self.send_sems, self.recv_sems, self.next, self.sent = send_sems, recv_sems, base, []

    def number(self):
        self.next += 1
        return self.next - 1

    def make(self, number, source, target, peer, landing=None):
        return pltpu.make_async_remote_copy(
            src_ref=source,
            dst_ref=target,
            send_sem=self.send_sems.at[number],
            recv_sem=self.recv_sems.at[number if landing is None else landing],
            device_id=peer,
            device_id_type=MESH_IDS,
        )

    def send(self, number, source, target, peer):
        copy = self.make(number, source, target, peer)
        copy.start()
        self.sent.append(copy)

    def arrived(self, number, target):
        self.make(number, target, target, {"ctx": 0}).wait_recv()

    def finish(self):
        for copy in self.sent:
            copy.wait_send()


GATHER_COPIES = 14


class PlaneGather:
    def __init__(self, copies, me, own_half, part):
        self.copies, self.me, self.own_half, self.part = copies, me, own_half, part
        self.first = copies.next
        copies.next += GATHER_COPIES

    def copy(self, number):
        bit, half, receiver = (
            (0, 1, 2),
            (0, 0, 4),
            (0, 0, 2),
            (0, 1, 4),
            (0, 0, 1),
            (0, 1, 1),
            (2, 1, 4),
            (4, 0, 2),
            (2, 1, 1),
            (4, 0, 1),
            (2, 0, 1),
            (4, 1, 1),
            (6, 1, 1),
            (6, 0, 1),
        )[number]
        place = self.part(self.me ^ bit, half)
        source = self.own_half(half) if bit == 0 else place
        return self.copies.make(self.first + number, source, place, {"ctx": self.me ^ receiver})

    def send(self, *numbers):
        for number in numbers:
            self.copy(number).start()

    def hear(self, number, bit, half):
        self.copies.arrived(self.first + number, self.part(self.me ^ bit, half))

    def begin(self):
        self.send(0, 1, 2, 3, 4, 5)

    def first_hop(self):
        self.hear(0, 2, 1)
        self.send(6, 8)
        self.hear(1, 4, 0)
        self.send(7, 9)

    def second_hop(self):
        self.hear(2, 2, 0)
        self.send(10)
        self.hear(3, 4, 1)
        self.send(11)

    def third_hop(self):
        self.hear(6, 6, 1)
        self.send(12)
        self.hear(7, 6, 0)
        self.send(13)

    def shared(self, bit):
        for number, half in {1: (4, 0), 3: (8, 1), 5: (9, 0), 7: (12, 1)}[bit], {
            1: (5, 1),
            3: (10, 0),
            5: (11, 1),
            7: (13, 0),
        }[bit]:
            self.hear(number, bit, half)

    def last(self):
        for bit in (1, 3, 5, 7):
            self.shared(bit)

    def finish(self):
        for number in range(GATHER_COPIES):
            self.copy(number).wait_send()


def row_half(ref, rows):
    half = rows // 2

    def own(side):
        return ref.at[pl.ds(side * half, half), :]

    return own


def row_part(ref, rows):
    half = rows // 2

    def part(slot, side):
        if isinstance(side, slice):
            return ref.at[pl.ds(pl.multiple_of(slot * rows, rows), rows), :]
        return ref.at[pl.ds(pl.multiple_of(slot * rows + side * half, half), half), :]

    return part


class LineGather:
    def __init__(self, copies, index, line, own, place):
        self.copies, self.index, self.line = copies, index, line
        self.own, self.place = own, place
        self.first = copies.next
        copies.next += 2 * (line - 1)

    def move(self, step, upward, act):
        index, line = self.index, self.line
        if upward:
            slot, there = index - step, index + 1
            leaves = (slot >= 0) & (there < line)
        else:
            slot, there = index + step, index - 1
            leaves = (slot < line) & (there >= 0)
        number = self.first + step + (0 if upward else line - 1)

        @pl.when(leaves)
        def _():
            place = self.place(jnp.clip(slot, 0, line - 1))
            source = self.own if step == 0 else place
            act(self.copies.make(number, source, place, {"fsdp": jnp.clip(there, 0, line - 1)}))

    def hear(self, step, upward):
        index, line = self.index, self.line
        slot = index - 1 - step if upward else index + 1 + step
        comes = (slot >= 0) & (slot < line)
        number = self.first + step + (0 if upward else line - 1)

        @pl.when(comes)
        def _():
            place = self.place(jnp.clip(slot, 0, line - 1))
            self.copies.make(number, place, place, {"fsdp": 0}).wait_recv()

    def begin(self):
        for upward in (True, False):
            self.move(0, upward, lambda copy: copy.start())

    def hop(self, step):
        for upward in (True, False):
            self.hear(step - 1, upward)
            if step < self.line - 1:
                self.move(step, upward, lambda copy: copy.start())

    def finish(self):
        for step in range(self.line - 1):
            for upward in (True, False):
                self.move(step, upward, lambda copy: copy.wait_send())


def in_hbm(count):
    return [pl.BlockSpec(memory_space=pltpu.HBM)] * count


def anywhere(count):
    return [pl.BlockSpec(memory_space=pl.ANY)] * count


def local_copies(pairs, sems):
    copies = [
        pltpu.make_async_copy(source, target, sems.at[number])
        for number, (source, target) in enumerate(pairs)
    ]
    for copy in copies:
        copy.start()
    return copies


def remote_params(number, mebibytes=62):
    return pltpu.CompilerParams(
        collective_id=number, has_side_effects=True, vmem_limit_bytes=mebibytes << 20
    )


def first_kernel(
    line,
    x_ref,
    q_hbm,
    k_hbm,
    v_hbm,
    wo_ref,
    gain_ref,
    gate_ref,
    up_ref,
    down_ref,
    xo_ref,
    qkvo_ref,
    woo_ref,
    gaino_ref,
    feedo_ref,
    feed,
    own,
    windows,
    qkv_ref,
    send,
    recv,
    here,
):
    me, index = lax.axis_index("ctx"), lax.axis_index("fsdp")
    plane = lax.axis_size("ctx")
    rows = x_ref.shape[0]
    part = row_part(xo_ref, rows)
    wo_rows = woo_ref.shape[1]
    wo_own = wo_ref.at[pl.ds(pl.multiple_of(me * wo_rows, wo_rows), wo_rows), :]
    local = local_copies(
        [
            (wo_own, woo_ref.at[index]),
            (gain_ref, gaino_ref.at[index]),
            (x_ref, own),
        ],
        here.at[pl.ds(1, 3)],
    )
    wide = windows.shape[2]
    sources = (q_hbm, k_hbm, v_hbm)
    widths = [ref.shape[1] // plane for ref in sources]

    def first_lane(slot, number):
        last = sources[number].shape[1] - wide
        if isinstance(slot, int):
            return min(slot * widths[number] // LANES * LANES, last)
        return jnp.minimum(lax.div(slot * widths[number], LANES) * LANES, last)

    fetch = local_copies(
        [
            (
                ref.at[:, pl.ds(pl.multiple_of(first_lane(me, number), LANES), wide)],
                windows.at[number],
            )
            for number, ref in enumerate(sources)
        ],
        here.at[pl.ds(4, 3)],
    )
    start_line_barrier(me, index, line)
    for copy in fetch:
        copy.wait()
    for slot in range(plane):

        @pl.when(me == slot)
        def _(slot=slot):
            parts = []
            for number, width in enumerate(widths):
                at = slot * width - first_lane(slot, number)
                parts.append(windows[number].astype(jnp.float32)[:, at : at + width])
            qkv_ref[...] = jnp.concatenate(parts, axis=1).astype(qkv_ref.dtype)

    copies = Copies(send, recv)
    gather = PlaneGather(copies, me, row_half(own, rows), part)
    lines = [
        LineGather(copies, index, line, own, lambda slot, ref=ref: ref.at[slot])
        for own, ref in ((qkv_ref, qkvo_ref), (gain_ref, gaino_ref), (wo_own, woo_ref))
    ]
    local.pop().wait()
    gather.begin()
    local += local_copies(
        [(own, part(me, slice(None))), (qkv_ref, qkvo_ref.at[index])], here.at[pl.ds(3, 2)]
    )
    for each in lines:
        each.begin()
    width = feed.shape[1] // 3
    unit = width // line
    pairs = []
    for side, ref in enumerate((gate_ref, up_ref)):
        for z in range(line):
            source = pl.ds(pl.multiple_of((z * plane + me) * unit, unit), unit)
            target = pl.ds(side * width + z * unit, unit)
            pairs.append((ref.at[:, source], feed.at[:, target]))
    for number in range(feed.shape[0] // unit):
        pairs.append(
            (
                down_ref.at[
                    pl.ds(pl.multiple_of(me * unit, unit), unit), pl.ds(number * width, width)
                ],
                feed.at[pl.ds(number * unit, unit), pl.ds(2 * width, width)],
            )
        )
    packed = local_copies(pairs, here.at[pl.ds(7, len(pairs))])
    gather.first_hop()
    for step in range(1, line):
        for each in lines:
            each.hop(step)
        if step == 1:
            gather.second_hop()
            for copy in packed:
                copy.wait()
            packed = local_copies([(feed, feedo_ref)], here.at[pl.ds(7 + len(pairs), 1)])
    gather.third_hop()
    gather.last()
    gather.finish()
    for each in lines:
        each.finish()
    for copy in local:
        copy.wait()
    packed[0].wait()


def first_exchange(line, x, projections, wo, gains, gate, up, down):
    plane = lax.axis_size("ctx")
    count = GATHER_COPIES + 6 * (line - 1)
    model = x.shape[1]
    shard = model // line
    width = gate.shape[1] // plane
    own_rows = wo.shape[0] // plane
    across = sum(array.shape[1] for array in projections) // plane
    feed = (shard, 3 * width)
    packing = 2 * line + shard * line // width + 1
    return pl.pallas_call(
        functools.partial(first_kernel, line),
        out_shape=(
            jax.ShapeDtypeStruct((plane * x.shape[0], model), x.dtype),
            jax.ShapeDtypeStruct((line, shard, across), x.dtype),
            jax.ShapeDtypeStruct((line, own_rows, model), wo.dtype),
            jax.ShapeDtypeStruct((line, *gains.shape), gains.dtype),
            jax.ShapeDtypeStruct(feed, gate.dtype),
        ),
        in_specs=in_hbm(5) + anywhere(1) + in_hbm(3),
        out_specs=tuple(anywhere(5)),
        scratch_shapes=[
            pltpu.VMEM(feed, gate.dtype),
            pltpu.VMEM(x.shape, x.dtype),
            pltpu.VMEM((3, shard, 2 * LANES), x.dtype),
            pltpu.VMEM((shard, across), x.dtype),
            pltpu.SemaphoreType.DMA((count,)),
            pltpu.SemaphoreType.DMA((count,)),
            pltpu.SemaphoreType.DMA((7 + packing,)),
        ],
        compiler_params=remote_params(1),
        name="first_exchange",
    )(x, *projections, wo, gains, gate, up, down)


def deal_rows(copies, me, pieces, wo_ref, place, recv_first, here):
    to_first = pieces * lax.rem(me, 2)
    line_slot = lax.div(me, 2)

    def copy(piece):
        return copies.make(
            recv_first + piece,
            wo_ref.at[piece],
            place(line_slot),
            {"ctx": to_first + piece},
            recv_first + line_slot,
        )

    for piece in range(pieces):

        @pl.when(to_first + piece != me)
        def _(piece=piece):
            copy(piece).start()

        @pl.when(to_first + piece == me)
        def _(piece=piece):
            pltpu.make_async_copy(wo_ref.at[piece], place(line_slot), here).start()

    def finish(line):
        for slot in range(line):

            @pl.when(2 * slot + lax.div(me, pieces) != me)
            def _(slot=slot):
                copies.make(
                    recv_first, wo_ref.at[0], place(slot), {"ctx": 0}, recv_first + slot
                ).wait_recv()

        for piece in range(pieces):

            @pl.when(to_first + piece != me)
            def _(piece=piece):
                copy(piece).wait_send()

            @pl.when(to_first + piece == me)
            def _(piece=piece):
                pltpu.make_async_copy(wo_ref.at[piece], place(line_slot), here).wait()

    return finish


class NearShares:
    def __init__(self, copies, me, refs, place):
        self.copies, self.me, self.refs, self.place = copies, me, refs, place
        self.first = copies.next
        copies.next += 7

    def copy(self, number):
        me, (own, near_x, near_y) = self.me, self.refs
        half = own.shape[0] // 2
        partner = {"ctx": me ^ 1}
        source, target, peer = (
            lambda: (near_y.at[pl.ds(0, half)], self.place(me ^ 4, 0), {"ctx": me ^ 2}),
            lambda: (near_x.at[pl.ds(half, half)], self.place(me ^ 2, 1), {"ctx": me ^ 4}),
            lambda: (own, self.place(me, None), partner),
            lambda: (near_x, self.place(me ^ 2, None), partner),
            lambda: (near_y, self.place(me ^ 4, None), partner),
            lambda: (self.place(me ^ 6, 0), self.place(me ^ 6, 0), partner),
            lambda: (self.place(me ^ 6, 1), self.place(me ^ 6, 1), partner),
        )[number]()
        return self.copies.make(self.first + number, source, target, peer)

    def begin(self):
        for number in range(5):
            self.copy(number).start()

    def diagonal(self):
        for side in (0, 1):
            self.copies.arrived(self.first + side, self.place(self.me ^ 6, side))
            self.copy(5 + side).start()

    def shared(self, bit):
        if bit == 7:
            for side in (0, 1):
                self.copies.arrived(self.first + 5 + side, self.place(self.me ^ 7, side))
        else:
            self.copies.arrived(self.first + 2 + bit // 2, self.place(self.me ^ bit, None))

    def finish(self):
        for number in range(7):
            self.copy(number).wait_send()


def block_place(ref, rows):
    half = rows // 2

    def place(slot, side):
        if side is None:
            return ref.at[pl.ds(pl.multiple_of(slot * rows, rows), rows), :]
        return ref.at[pl.ds(pl.multiple_of(slot * rows + side * half, half), half), :]

    return place


def second_kernel(
    o_ref,
    wo0_hbm,
    wo2_hbm,
    wo4_hbm,
    dy2_hbm,
    dy4_hbm,
    x_hbm,
    gain_ref,
    own_hbm,
    dy6_hbm,
    residual_hbm,
    normed_hbm,
    scale_ref,
    gained_hbm,
    near_x_hbm,
    near_y_hbm,
    x_ref,
    residual_ref,
    normed_ref,
    gained_ref,
    att,
    wo,
    send,
    recv,
    here,
):
    me = lax.axis_index("ctx")
    rows = x_ref.shape[0]
    half = rows // 2
    middle = wo.shape[0] // 2

    def wo_place(slot, side):
        return wo.at[:, slot] if side is None else wo.at[pl.ds(side * middle, middle), slot]

    own_wo = (wo0_hbm, wo2_hbm, wo4_hbm)
    local = local_copies(
        [
            (o_ref.at[pl.ds(pl.multiple_of(me * rows, rows), rows), :], att.at[me]),
            (x_hbm, x_ref),
        ]
        + [(ref, wo_place(me ^ (2 * number), None)) for number, ref in enumerate(own_wo)],
        here.at[pl.ds(0, 5)],
    )
    start_barrier(me, ALL)
    copies = Copies(send, recv)

    def block(slot):
        return o_ref.at[pl.ds(pl.multiple_of(slot * rows, rows), rows), :]

    numbers = {}
    for bit in (6, 7, 4, 5, 2, 3, 1):
        numbers[bit] = copies.number()
        copies.send(numbers[bit], block(me ^ bit), att.at[me], {"ctx": me ^ bit})
    shares = NearShares(copies, me, own_wo, wo_place)
    shares.begin()
    dy_first = copies.next
    copies.next += 2
    upper, lower = pl.ds(0, half), pl.ds(half, half)
    copies.send(dy_first, dy4_hbm.at[upper, :], dy6_hbm.at[upper, :], {"ctx": me ^ 2})
    copies.send(dy_first + 1, dy2_hbm.at[lower, :], dy6_hbm.at[lower, :], {"ctx": me ^ 4})
    shares.diagonal()
    for bit in (1, 3, 5, 7):
        shares.shared(bit)
    for bit, number in numbers.items():
        copies.arrived(number, att.at[me ^ bit])
    for copy in local:
        copy.wait()
    per_head = 2 * GROUP
    own = wo.at[lax.div(me, 2), pl.ds(per_head * lax.rem(me, 2), per_head)]
    keep = local_copies([(own, own_hbm)], here.at[pl.ds(5, 1)])
    plane = att.shape[0]
    near = copies.next
    for side in (0, 1):
        at = pl.ds(side * half, half)
        total = x_ref[at, :].astype(jnp.float32)
        for slot in range(plane):
            first = per_head * (slot % 2)
            weight = jnp.concatenate(
                [wo[slot // 2, first + piece] for piece in range(per_head)], axis=0
            )
            total = total + contract(att[slot, at, :], weight, 1, 0)
        residual_ref[at, :] = total
        scale = lax.rsqrt(jnp.mean(total * total, axis=-1, keepdims=True) + norm_epsilon)
        normed = total * scale
        scale_ref[at, :] = scale
        normed_ref[at, :] = normed
        gained_ref[at, :] = (normed * gain_ref[...]).astype(jnp.bfloat16)
        for number, target, bit in ((0, near_x_hbm, 2), (1, near_y_hbm, 4)):
            copies.send(
                near + 2 * side + number,
                gained_ref.at[at, :],
                target.at[at, :],
                {"ctx": me ^ bit},
            )
    keep += local_copies(
        [(residual_ref, residual_hbm), (normed_ref, normed_hbm), (gained_ref, gained_hbm)],
        here.at[pl.ds(6, 3)],
    )
    for copy in keep:
        copy.wait()
    shares.finish()
    copies.arrived(dy_first, dy6_hbm.at[upper, :])
    copies.arrived(dy_first + 1, dy6_hbm.at[lower, :])
    for side in (0, 1):
        at = pl.ds(side * half, half)
        copies.arrived(near + 2 * side, near_x_hbm.at[at, :])
        copies.arrived(near + 2 * side + 1, near_y_hbm.at[at, :])
    copies.finish()


def second_exchange(o, own_wo, grads, x, gain):
    plane = lax.axis_size("ctx")
    rows = x.shape[0]
    line, part, model = own_wo[0].shape
    count = 7 + 7 + 2 + 4
    f32 = jnp.float32
    return pl.pallas_call(
        second_kernel,
        out_shape=(
            jax.ShapeDtypeStruct((2 * GROUP, part, model), own_wo[0].dtype),
            jax.ShapeDtypeStruct((rows, model), x.dtype),
            jax.ShapeDtypeStruct((rows, model), f32),
            jax.ShapeDtypeStruct((rows, model), f32),
            jax.ShapeDtypeStruct((rows, 1), f32),
            *[jax.ShapeDtypeStruct((rows, model), x.dtype)] * 3,
        ),
        in_specs=in_hbm(7) + in_vmem(1),
        out_specs=(*anywhere(4), *in_vmem(1), *anywhere(3)),
        scratch_shapes=[
            pltpu.VMEM(x.shape, x.dtype),
            pltpu.VMEM(x.shape, f32),
            pltpu.VMEM(x.shape, f32),
            pltpu.VMEM(x.shape, x.dtype),
            pltpu.VMEM((plane, rows, o.shape[1]), o.dtype),
            pltpu.VMEM((line, plane, part, model), x.dtype),
            pltpu.SemaphoreType.DMA((count,)),
            pltpu.SemaphoreType.DMA((count,)),
            pltpu.SemaphoreType.DMA((9,)),
        ],
        compiler_params=remote_params(2),
        name="second_exchange",
    )(o, *own_wo, *grads, x, gain)


def near_kernel(own_hbm, near_x_hbm, near_y_hbm, whole_ref, send, recv, here):
    me = lax.axis_index("ctx")
    refs = (own_hbm, near_x_hbm, near_y_hbm)
    place = block_place(whole_ref, own_hbm.shape[0])
    local = local_copies(
        [(ref, place(me ^ (2 * number), None)) for number, ref in enumerate(refs)], here
    )
    start_barrier(me, NEAR)
    copies = Copies(send, recv)
    shares = NearShares(copies, me, refs, place)
    shares.begin()
    shares.diagonal()
    for bit in (1, 3, 5, 7):
        shares.shared(bit)
    for copy in local:
        copy.wait()
    shares.finish()


def near_gather(refs, number):
    plane = lax.axis_size("ctx")
    rows, columns = refs[0].shape
    return pl.pallas_call(
        near_kernel,
        out_shape=jax.ShapeDtypeStruct((plane * rows, columns), refs[0].dtype),
        in_specs=anywhere(3),
        out_specs=in_vmem(1)[0],
        scratch_shapes=[
            pltpu.SemaphoreType.DMA((7,)),
            pltpu.SemaphoreType.DMA((7,)),
            pltpu.SemaphoreType.DMA((3,)),
        ],
        compiler_params=remote_params(number, 24),
    )(*refs)


def third_kernel(
    g0_hbm, g2_hbm, g4_hbm, ot_hbm, wo_hbm, do_ref, dwo_ref, ot_ref, wo_ref, all_grads, dwo, send, recv, here
):
    me = lax.axis_index("ctx")
    rows = g0_hbm.shape[0]
    place = block_place(all_grads, rows)
    own_rows = (g0_hbm, g2_hbm, g4_hbm)
    fetch = local_copies(
        [(ref, place(me ^ (2 * number), None)) for number, ref in enumerate(own_rows)]
        + [(ot_hbm, ot_ref), (wo_hbm, wo_ref)],
        here,
    )
    start_barrier(me, NEAR)
    copies = Copies(send, recv)
    shares = NearShares(copies, me, own_rows, place)
    shares.begin()
    dwo[...] = jnp.zeros_like(dwo)
    for copy in fetch:
        copy.wait()

    def step(order, carry):
        @pl.when(order == 5)
        def _():
            shares.diagonal()

        for bit in (1, 3, 5, 7):

            @pl.when(order == bit)
            def _(bit=bit):
                shares.shared(bit)

        here_rows = pl.ds(pl.multiple_of((me ^ order) * rows, rows), rows)
        grads = all_grads[here_rows, :]
        do_ref[here_rows, :] = contract(grads, wo_ref[...], 1, 1).astype(jnp.bfloat16)
        dwo[...] += contract(ot_ref[:, here_rows], grads, 1, 0)
        return carry

    lax.fori_loop(0, 8, step, 0)
    line, _, across = dwo_ref.shape
    for slot in range(line):
        rows_at = slice(slot * HALF, (slot + 1) * HALF)
        for number in range(dwo.shape[1] // across):
            columns = slice(number * across, (number + 1) * across)
            dwo_ref[slot, number * HALF : (number + 1) * HALF, :] = dwo[rows_at, columns].astype(
                jnp.bfloat16
            )
    shares.finish()


def third_exchange(line, own_rows, ot, wo, across):
    plane = lax.axis_size("ctx")
    rows, model = own_rows[0].shape
    half_type, f32 = jnp.bfloat16, jnp.float32
    return pl.pallas_call(
        third_kernel,
        out_shape=(
            jax.ShapeDtypeStruct((plane * rows, wo.shape[0]), half_type),
            jax.ShapeDtypeStruct((line, HALF * model // across, across), half_type),
        ),
        in_specs=anywhere(5),
        out_specs=tuple(in_vmem(2)),
        scratch_shapes=[
            pltpu.VMEM(ot.shape, ot.dtype),
            pltpu.VMEM(wo.shape, wo.dtype),
            pltpu.VMEM((plane * rows, model), half_type),
            pltpu.VMEM((line * HALF, model), f32),
            pltpu.SemaphoreType.DMA((7,)),
            pltpu.SemaphoreType.DMA((7,)),
            pltpu.SemaphoreType.DMA((5,)),
        ],
        compiler_params=remote_params(6),
        name="third_exchange",
    )(*own_rows, ot, wo)


REDUCE_COPIES = 10


class PlaneReduce:
    def __init__(self, copies, me, block, heard, held, landed):
        self.copies, self.me, self.block = copies, me, block
        self.heard, self.held, self.landed = heard, held, landed
        self.first = copies.next
        copies.next += REDUCE_COPIES
        self.half = heard.shape[1] // 2
        self.x, self.y = {"ctx": me ^ 2}, {"ctx": me ^ 4}

    def side(self, ref, slot, half):
        return ref.at[slot, pl.ds(half * self.half, self.half), :]

    def share(self, order):
        self.shared(order).start()

    def shared(self, order):
        partner = self.me ^ 1
        source = self.block(partner ^ (6, 2, 4, 0)[order])
        return self.copies.make(
            self.first + order, source, self.heard.at[order], {"ctx": partner}
        )

    def combine(self, order, rows, extra=None):
        bit = (6, 2, 4)[order]
        total = self.block(self.me ^ bit)[rows, :].astype(jnp.float32) + self.heard[
            order, rows, :
        ].astype(jnp.float32)
        if extra is not None:
            total = total + extra
        self.held[order, rows, :] = total.astype(self.held.dtype)

    def onward(self, number):
        order, half, peer = {
            4: (0, 0, self.x),
            5: (0, 1, self.y),
            6: (1, 0, self.x),
            7: (2, 1, self.y),
            8: (1, 1, self.x),
            9: (2, 0, self.y),
        }[number]
        held, landed = self.side(self.held, order, half), self.side(self.landed, order, half)
        return self.copies.make(self.first + number, held, landed, peer)

    def finish(self):
        for order in range(4):
            self.shared(order).wait_send()
        for number in range(4, REDUCE_COPIES):
            self.onward(number).wait_send()

    def diagonal_sends(self):
        first, half = self.first, self.half
        self.copies.arrived(first + 0, self.heard.at[0])
        self.combine(0, pl.ds(0, 2 * half))
        self.onward(4).start()
        self.onward(5).start()

    def neighbour_send(self, order):
        first, half = self.first, self.half
        self.copies.arrived(first + order, self.heard.at[order])
        self.combine(order, pl.ds((order - 1) * half, half))
        self.onward(5 + order).start()

    def neighbour_sends(self):
        self.neighbour_send(1)
        self.neighbour_send(2)

    def second_sends(self):
        first, half = self.first, self.half
        upper, lower = pl.ds(0, half), pl.ds(half, half)
        landed, side, arrived = self.landed, self.side, self.copies.arrived
        arrived(first + 5, side(landed, 0, 1))
        self.combine(1, lower, landed[0, lower, :].astype(jnp.float32))
        self.onward(8).start()
        arrived(first + 4, side(landed, 0, 0))
        self.combine(2, upper, landed[0, upper, :].astype(jnp.float32))
        self.onward(9).start()

    def own_share(self):
        self.copies.arrived(self.first + 3, self.heard.at[3])

    def sum_half(self, which):
        first, half = self.first, self.half
        rows = pl.ds(which * half, half)
        self.copies.arrived(first + (6, 8)[which], self.side(self.landed, 1, which))
        self.copies.arrived(first + (9, 7)[which], self.side(self.landed, 2, which))
        return (
            self.block(self.me)[rows, :].astype(jnp.float32)
            + self.heard[3, rows, :].astype(jnp.float32)
            + self.landed[1, rows, :].astype(jnp.float32)
            + self.landed[2, rows, :].astype(jnp.float32)
        )


def feed_kernel(
    line,
    g0_hbm,
    g2_hbm,
    g4_hbm,
    dy0_hbm,
    dy2_hbm,
    dy4_hbm,
    dy6_hbm,
    w_hbm,
    ot_hbm,
    normed_hbm,
    scale_ref,
    gain_ref,
    residual_ref,
    term_ref,
    own_ref,
    near_x_ref,
    near_y_ref,
    dealt_hbm,
    out6_hbm,
    out2_hbm,
    out4_hbm,
    out0_hbm,
    dw_hbm,
    normed_ref,
    w_ref,
    dw_ref,
    down_ref,
    dy_ref,
    all_g,
    hid,
    hid_t,
    gate_t,
    up_t,
    part,
    heard,
    held,
    landed,
    out_mine,
    out_heard,
    send,
    recv,
    here,
):
    me = lax.axis_index("ctx")
    rows = residual_ref.shape[0]
    half = rows // 2
    width, model = down_ref.shape
    blocks = model // width
    unit = width // line
    partner = {"ctx": me ^ 1}

    def at(slot):
        return pl.ds(pl.multiple_of(slot * rows, rows), rows)

    own_grads = (dy0_hbm, dy2_hbm, dy4_hbm, dy6_hbm)
    own_rows = (g0_hbm, g2_hbm, g4_hbm)
    place = block_place(all_g, rows)
    dy_place = block_place(dy_ref, rows)
    local = local_copies(
        [(w_hbm, w_ref)]
        + [(ref, place(me ^ (2 * number), None)) for number, ref in enumerate(own_rows)]
        + [(ref, dy_place(me ^ (2 * number), None)) for number, ref in enumerate(own_grads)]
        + [(normed_hbm, normed_ref)],
        here.at[pl.ds(0, 9)],
    )
    start_barrier(me, ALL)
    copies = Copies(send, recv)
    shares = NearShares(copies, me, own_rows, place)
    shares.begin()
    dy_first = copies.next
    copies.next += 4
    for number, ref in enumerate(own_grads):
        copies.send(dy_first + number, ref, dy_place(me ^ (2 * number), None), partner)
    deal_first = copies.next
    copies.next += ot_hbm.shape[0]
    dealt = deal_rows(
        copies,
        me,
        ot_hbm.shape[0],
        ot_hbm,
        lambda slot: dealt_hbm.at[slot],
        deal_first,
        here.at[9],
    )
    local[0].wait()
    gate_ref, up_ref = w_ref.at[:, :width], w_ref.at[:, width : 2 * width]
    for z in range(line):
        for number in range(blocks):
            source = pl.ds((z * blocks + number) * unit, unit)
            down_ref[pl.ds(z * unit, unit), number * width : (number + 1) * width] = w_ref[
                source, 2 * width :
            ]
    for copy in local[1:]:
        copy.wait()
    gain = gain_ref[...]

    def block(slot):
        return part.at[at(slot), :]

    reduce = PlaneReduce(copies, me, block, heard, held, landed)

    def chunk(order):
        place = at(me ^ order)
        g = all_g[place, :]
        dy = dy_ref[place, :]
        gate_values = contract(g, gate_ref[...], 1, 0)
        up_values = contract(g, up_ref[...], 1, 0)
        sigmoid_gate = 1.0 / (1.0 + jnp.exp(-gate_values))
        activated = gate_values * sigmoid_gate
        hidden_act = (activated * up_values).astype(jnp.bfloat16)
        hid[place, :] = hidden_act
        hid_t[:, place] = hidden_act.T
        grad_hidden = contract(dy, down_ref[...], 1, 1)
        grad_gate = (
            grad_hidden * up_values * sigmoid_gate * (1.0 + gate_values * (1.0 - sigmoid_gate))
        ).astype(jnp.bfloat16)
        grad_up = (grad_hidden * activated).astype(jnp.bfloat16)
        gate_t[:, place] = grad_gate.T
        up_t[:, place] = grad_up.T
        part[place, :] = (
            contract(grad_gate, gate_ref[...], 1, 1) + contract(grad_up, up_ref[...], 1, 1)
        ).astype(jnp.bfloat16)

    def step(number, carry):
        @pl.when(number == 1)
        def _():
            shares.shared(3)
            copies.arrived(dy_first + 1, dy_place(me ^ 3, None))

        @pl.when(number == 2)
        def _():
            reduce.share(1)
            shares.diagonal()

        @pl.when(number == 3)
        def _():
            reduce.neighbour_send(1)
            shares.shared(7)
            copies.arrived(dy_first + 3, dy_place(me ^ 7, None))

        @pl.when(number == 4)
        def _():
            reduce.share(0)
            reduce.diagonal_sends()

        @pl.when(number == 5)
        def _():
            shares.shared(5)
            copies.arrived(dy_first + 2, dy_place(me ^ 5, None))

        @pl.when(number == 6)
        def _():
            reduce.share(2)
            reduce.neighbour_send(2)

        @pl.when(number == 7)
        def _():
            reduce.second_sends()
            shares.shared(1)
            copies.arrived(dy_first, dy_place(me ^ 1, None))

        pair = lax.div(number, 2)
        chunk(
            lax.rem(number, 2)
            + jnp.where(pair == 0, 2, jnp.where(pair == 1, 6, jnp.where(pair == 2, 4, 0)))
        )
        return carry

    lax.fori_loop(0, 8, step, 0)
    reduce.share(3)
    out_first = copies.next
    copies.next += 4

    def bit_of(number):
        return jnp.where(number == 0, 6, jnp.where(number == 3, 0, 2 * number))

    def out_copy(number):
        return copies.make(out_first + number, out_mine.at[number], out_heard.at[number], partner)

    def out_of(slot):
        return contract(hid[at(slot), :], down_ref[...], 1, 0)

    def give(number, carry):
        out_mine[number] = out_of(me ^ 1 ^ bit_of(number)).astype(jnp.bfloat16)
        out_copy(number).start()
        return carry

    def keep(number, carry):
        total = out_of(me ^ bit_of(number))
        out_copy(number).wait_recv()
        out_heard[number] = (total + out_heard[number].astype(jnp.float32)).astype(jnp.bfloat16)
        return carry

    def weights(number, carry):
        columns = pl.ds(pl.multiple_of(number * width, width), width)
        total = contract(hid_t[...], dy_ref[:, columns], 1, 0).astype(jnp.bfloat16)
        for z in range(line):
            target = pl.ds(pl.multiple_of((z * blocks + number) * unit, unit), unit)
            dw_ref[target, 2 * width :] = total[z * unit : (z + 1) * unit, :]
        for side, left in enumerate((gate_t, up_t)):
            total = contract(left[...], all_g[:, columns], 1, 0).astype(jnp.bfloat16)
            dw_ref[columns, side * width : (side + 1) * width] = total.T
        return carry

    reduce.own_share()
    lax.fori_loop(0, 4, give, 0)
    near = copies.next
    copies.next += 4
    total = jnp.zeros_like(gain)
    for which in (1, 0):
        rows_at = pl.ds(which * half, half)
        grad_normed, normed = reduce.sum_half(which), normed_ref[rows_at, :]
        scaled = grad_normed * gain
        mean = jnp.mean(scaled * normed, axis=-1, keepdims=True)
        total = total + jnp.sum(grad_normed * normed, axis=0, keepdims=True)
        dy = dy_ref[pl.ds(pl.multiple_of(me * rows + which * half, half), half), :]
        residual = dy.astype(jnp.float32) + scale_ref[rows_at, :] * (scaled - normed * mean)
        residual_ref[rows_at, :] = residual
        own_ref[rows_at, :] = residual.astype(jnp.bfloat16)
        for number, target, bit in ((0, near_x_ref, 2), (1, near_y_ref, 4)):
            copies.send(
                near + 2 * which + number,
                own_ref.at[rows_at, :],
                target.at[rows_at, :],
                {"ctx": me ^ bit},
            )
    term_ref[...] = total
    lax.fori_loop(0, 4, keep, 0)
    outputs = local_copies(
        [
            (out_heard.at[number], ref)
            for number, ref in enumerate((out6_hbm, out2_hbm, out4_hbm, out0_hbm))
        ],
        here.at[pl.ds(0, 4)],
    )
    lax.fori_loop(0, blocks, weights, 0)
    outputs += local_copies([(dw_ref, dw_hbm)], here.at[pl.ds(4, 1)])
    for number in range(4):
        out_copy(number).wait_send()
    for copy in outputs:
        copy.wait()
    dealt(dealt_hbm.shape[0])
    shares.finish()
    reduce.finish()
    for which in (1, 0):
        rows_at = pl.ds(which * half, half)
        copies.arrived(near + 2 * which, near_x_ref.at[rows_at, :])
        copies.arrived(near + 2 * which + 1, near_y_ref.at[rows_at, :])
    copies.finish()


def feed(own_rows, grads, w, ot, normed, scale, gain):
    plane, line = lax.axis_size("ctx"), lax.axis_size("fsdp")
    rows, model = own_rows[0].shape
    tokens = plane * rows
    width = w.shape[1] // 3
    pieces = 2 * GROUP
    ot = ot.reshape(pieces, -1, ot.shape[1])
    count = 7 + 4 + pieces + REDUCE_COPIES + 4 + 4
    half_type = jnp.bfloat16
    return pl.pallas_call(
        functools.partial(feed_kernel, line),
        out_shape=(
            jax.ShapeDtypeStruct((rows, model), jnp.float32),
            jax.ShapeDtypeStruct((1, model), jnp.float32),
            *[jax.ShapeDtypeStruct((rows, model), half_type)] * 3,
            jax.ShapeDtypeStruct((line, *ot.shape[1:]), ot.dtype),
            *[jax.ShapeDtypeStruct((rows, model), half_type)] * 4,
            jax.ShapeDtypeStruct(w.shape, half_type),
        ),
        in_specs=anywhere(10) + in_vmem(2),
        out_specs=(*in_vmem(3), *anywhere(8)),
        scratch_shapes=[
            pltpu.VMEM((rows, model), jnp.float32),
            pltpu.VMEM(w.shape, half_type),
            pltpu.VMEM(w.shape, half_type),
            pltpu.VMEM((width, model), half_type),
            pltpu.VMEM((tokens, model), half_type),
            pltpu.VMEM((tokens, model), half_type),
            pltpu.VMEM((tokens, width), half_type),
            pltpu.VMEM((width, tokens), half_type),
            pltpu.VMEM((width, tokens), half_type),
            pltpu.VMEM((width, tokens), half_type),
            pltpu.VMEM((tokens, model), half_type),
            pltpu.VMEM((4, rows, model), half_type),
            pltpu.VMEM((3, rows, model), half_type),
            pltpu.VMEM((3, rows, model), half_type),
            pltpu.VMEM((4, rows, model), half_type),
            pltpu.VMEM((4, rows, model), half_type),
            pltpu.SemaphoreType.DMA((count,)),
            pltpu.SemaphoreType.DMA((count,)),
            pltpu.SemaphoreType.DMA((10,)),
        ],
        compiler_params=pltpu.CompilerParams(
            collective_id=3, has_side_effects=True, vmem_limit_bytes=62 << 20
        ),
        name="feed",
    )(*own_rows, *grads, w, ot, normed, scale, gain)


def input_kernel(
    dqkv_ref,
    wp_hbm,
    x_hbm,
    residual_hbm,
    dwo_hbm,
    term_ref,
    gain_ref,
    pad_ref,
    input_ref,
    grads_ref,
    wp_ref,
    all_x,
    residual_ref,
    dwo_ref,
    part,
    dw,
    heard,
    held,
    landed,
    send,
    recv,
    here,
):
    me = lax.axis_index("ctx")
    rows = residual_ref.shape[0]
    fetch = local_copies(
        [(wp_hbm, wp_ref), (x_hbm, all_x), (residual_hbm, residual_ref), (dwo_hbm, dwo_ref)], here
    )
    start_barrier(me, NEAR)
    copies = Copies(send, recv)

    def at(slot):
        return pl.ds(pl.multiple_of(slot * rows, rows), rows)

    def compute(slot):
        place = at(slot)
        part[place, :] = contract(dqkv_ref[place, :], wp_ref[...], 1, 1).astype(jnp.bfloat16)

    reduce = PlaneReduce(copies, me, lambda slot: part.at[at(slot), :], heard, held, landed)
    fetch[0].wait()
    compute(me ^ 7)
    reduce.share(0)
    compute(me ^ 6)
    compute(me ^ 3)
    reduce.share(1)
    reduce.diagonal_sends()
    compute(me ^ 2)
    compute(me ^ 5)
    reduce.share(2)
    compute(me ^ 4)
    reduce.neighbour_sends()
    compute(me ^ 1)
    reduce.share(3)
    compute(me)
    gain = gain_ref[...]
    dw[...] = jnp.zeros_like(dw)
    for copy in fetch[1:]:
        copy.wait()

    def weights(slot, carry):
        place = at(slot)
        x = all_x[place, :].astype(jnp.float32)
        normed = x * lax.rsqrt(jnp.mean(x * x, axis=-1, keepdims=True) + norm_epsilon)
        gained = (normed * gain).astype(jnp.bfloat16)
        dw[...] += contract(dqkv_ref[place, :], gained, 0, 0)
        return carry

    plane = part.shape[0] // rows
    lax.fori_loop(0, plane // 2, weights, 0)
    reduce.second_sends()
    reduce.own_share()
    lax.fori_loop(plane // 2, plane, weights, 0)
    packed = contract(pad_ref[...], dw[...].astype(jnp.bfloat16), 1, 0)
    packed = packed.astype(jnp.bfloat16).T
    line = dwo_ref.shape[0]
    shard = packed.shape[0] // line
    for slot in range(line):
        grads_ref[slot, :shard, :] = packed[slot * shard : (slot + 1) * shard, :]
        grads_ref[slot, shard : shard + dwo_ref.shape[1], :] = dwo_ref[slot]
    half = rows // 2
    total = jnp.zeros_like(gain)
    for which in (1, 0):
        here_rows = pl.ds(which * half, half)
        grad = reduce.sum_half(which)
        own_rows = pl.ds(pl.multiple_of(me * rows + which * half, half), half)
        x = all_x[own_rows, :].astype(jnp.float32)
        scale = lax.rsqrt(jnp.mean(x * x, axis=-1, keepdims=True) + norm_epsilon)
        normed = x * scale
        total = total + jnp.sum(grad * normed, axis=0, keepdims=True)
        scaled = grad * gain
        mean = jnp.mean(scaled * normed, axis=-1, keepdims=True)
        input_ref[0, here_rows, :] = residual_ref[here_rows, :] + scale * (scaled - normed * mean)
    blank = jnp.zeros((GAIN_ROWS - 2, grads_ref.shape[2]), jnp.float32)
    for slot in range(line):
        columns = slice(slot * shard, (slot + 1) * shard)
        rows_of = jnp.concatenate([total[:, columns], term_ref[:, columns], blank], axis=0)
        grads_ref[slot, grads_ref.shape[1] - GAIN_ROWS :, :] = rows_of.astype(grads_ref.dtype)
    reduce.finish()
    copies.finish()


GAIN_ROWS = 32


def input_exchange(dqkv, wp, x, residual, dwo, term, gain, pad):
    rows, model = residual.shape
    line, dealt, across = dwo.shape
    f32 = jnp.float32
    return pl.pallas_call(
        input_kernel,
        out_shape=(
            jax.ShapeDtypeStruct((1, rows, model), f32),
            jax.ShapeDtypeStruct((line, model // line + dealt + GAIN_ROWS, across), dwo.dtype),
        ),
        in_specs=in_vmem(1) + in_hbm(4) + in_vmem(3),
        out_specs=tuple(in_vmem(2)),
        scratch_shapes=[
            pltpu.VMEM(wp.shape, wp.dtype),
            pltpu.VMEM(x.shape, x.dtype),
            pltpu.VMEM(residual.shape, residual.dtype),
            pltpu.VMEM(dwo.shape, dwo.dtype),
            pltpu.VMEM(x.shape, x.dtype),
            pltpu.VMEM((dqkv.shape[1], model), f32),
            pltpu.VMEM((4, rows, model), x.dtype),
            pltpu.VMEM((3, rows, model), x.dtype),
            pltpu.VMEM((3, rows, model), x.dtype),
            pltpu.SemaphoreType.DMA((REDUCE_COPIES,)),
            pltpu.SemaphoreType.DMA((REDUCE_COPIES,)),
            pltpu.SemaphoreType.DMA((4,)),
        ],
        compiler_params=remote_params(7),
        name="input_exchange",
    )(dqkv, wp, x, residual, dwo, term, gain, pad)


def pieces_kernel(
    piece_ref,
    residual_hbm,
    out0_hbm,
    out2_hbm,
    out4_hbm,
    out6_hbm,
    whole_ref,
    output_ref,
    own,
    residual_ref,
    outs_ref,
    send,
    recv,
    here,
):
    me = lax.axis_index("ctx")
    outs = (out0_hbm, out2_hbm, out4_hbm, out6_hbm)
    fetch = local_copies(
        [(piece_ref, own), (residual_hbm, residual_ref)]
        + [(ref, outs_ref.at[number]) for number, ref in enumerate(outs)],
        here.at[pl.ds(0, 6)],
    )
    start_barrier(me, NEAR)
    copies = Copies(send, recv)
    rows = piece_ref.shape[0]
    part = row_part(whole_ref, rows)
    gather = PlaneGather(copies, me, row_half(own, rows), part)
    fetch[0].wait()
    gather.begin()
    local = local_copies([(own, part(me, slice(None)))], here.at[pl.ds(6, 1)])
    for copy in fetch[1:]:
        copy.wait()
    total = residual_ref[...]
    for number in range(4):
        total = total + outs_ref[number].astype(jnp.float32)
    output_ref[0] = total.astype(output_ref.dtype)
    gather.first_hop()
    gather.second_hop()
    gather.third_hop()
    gather.last()
    gather.finish()
    local[0].wait()


def pieces_exchange(piece, residual, outs):
    plane = lax.axis_size("ctx")
    rows, model = residual.shape
    return pl.pallas_call(
        pieces_kernel,
        out_shape=(
            jax.ShapeDtypeStruct((plane * piece.shape[0], piece.shape[1]), piece.dtype),
            jax.ShapeDtypeStruct((1, rows, model), jnp.bfloat16),
        ),
        in_specs=anywhere(6),
        out_specs=(*anywhere(1), *in_vmem(1)),
        scratch_shapes=[
            pltpu.VMEM(piece.shape, piece.dtype),
            pltpu.VMEM((rows, model), jnp.float32),
            pltpu.VMEM((4, rows, model), outs[0].dtype),
            pltpu.SemaphoreType.DMA((GATHER_COPIES,)),
            pltpu.SemaphoreType.DMA((GATHER_COPIES,)),
            pltpu.SemaphoreType.DMA((7,)),
        ],
        compiler_params=remote_params(8),
        name="pieces_exchange",
    )(piece, residual, *outs)


def spread_kernel(gate_in, up_in, down_in, gate_ref, up_ref, down_ref):
    plane, shard, unit = gate_in.shape
    for source, target in ((gate_in, gate_ref), (up_in, up_ref)):
        for slot in range(plane):
            target[:, slot * unit : (slot + 1) * unit] = source[slot].astype(jnp.float32)
    width = down_in.shape[2]
    blocks = shard // unit
    for slot in range(down_in.shape[0]):
        for number in range(blocks):
            down_ref[slot * unit : (slot + 1) * unit, number * width : (number + 1) * width] = (
                down_in[slot, number * unit : (number + 1) * unit, :].astype(jnp.float32)
            )


def spread_feed(pieces, shard, line, unit):
    plane = lax.axis_size("ctx")
    width = line * unit
    model = line * shard
    pieces = pieces.reshape(plane, shard, 3 * width)
    each = plane // line
    return pl.pallas_call(
        spread_kernel,
        grid=(line,),
        in_specs=[
            pl.BlockSpec((plane, shard, unit), lambda z: (0, 0, z)),
            pl.BlockSpec((plane, shard, unit), lambda z: (0, 0, line + z)),
            pl.BlockSpec((each, shard, width), lambda z: (z, 0, 2)),
        ],
        out_specs=(
            pl.BlockSpec((shard, plane * unit), lambda z: (0, z)),
            pl.BlockSpec((shard, plane * unit), lambda z: (0, z)),
            pl.BlockSpec((each * unit, model), lambda z: (z, 0)),
        ),
        out_shape=(
            jax.ShapeDtypeStruct((shard, plane * width), jnp.float32),
            jax.ShapeDtypeStruct((shard, plane * width), jnp.float32),
            jax.ShapeDtypeStruct((plane * unit, model), jnp.float32),
        ),
        compiler_params=pltpu.CompilerParams(vmem_limit_bytes=62 << 20),
        name="spread_feed",
    )(pieces, pieces, pieces)


def spread_attention_kernel(in_ref, q_ref, k_ref, v_ref, wo_ref, gains_ref):
    plane, _, across = in_ref.shape
    shard = q_ref.shape[0]
    key_width = k_ref.shape[1] // plane
    query_width = q_ref.shape[1] // plane
    first = 0
    for target, width in ((q_ref, query_width), (k_ref, key_width), (v_ref, key_width)):
        target[...] = jnp.concatenate(
            [
                in_ref[slot, :shard, first : first + width].astype(jnp.float32)
                for slot in range(plane)
            ],
            axis=1,
        )
        first += width
    for slot in range(plane):
        for number in range(wo_ref.shape[1] // across):
            source = slice(shard + number * HALF, shard + (number + 1) * HALF)
            wo_ref[slot * HALF : (slot + 1) * HALF, number * across : (number + 1) * across] = (
                in_ref[slot, source, :].astype(jnp.float32)
            )
    terms = [in_ref[slot, in_ref.shape[1] - GAIN_ROWS :, :] for slot in range(plane)]
    gains_ref[...] = sum(term.astype(jnp.float32) for term in terms)[: gains_ref.shape[0], :]


def spread_attention(pieces, shard, model, query_width, key_width):
    plane = lax.axis_size("ctx")
    pieces = pieces.reshape(plane, -1, pieces.shape[1])
    f32 = jnp.float32
    return pl.pallas_call(
        spread_attention_kernel,
        in_specs=in_vmem(1),
        out_specs=tuple(in_vmem(5)),
        out_shape=(
            jax.ShapeDtypeStruct((shard, plane * query_width), f32),
            jax.ShapeDtypeStruct((shard, plane * key_width), f32),
            jax.ShapeDtypeStruct((shard, plane * key_width), f32),
            jax.ShapeDtypeStruct((plane * HALF, model), f32),
            jax.ShapeDtypeStruct((8, shard), f32),
        ),
        compiler_params=pltpu.CompilerParams(vmem_limit_bytes=40 << 20),
        name="spread_attention",
    )(pieces)


def head_local(
    block_input,
    block_table,
    output_grad,
    attention_gain,
    query_weight,
    key_weight,
    value_projection,
    output_weight,
    feedforward_gain,
    gate_weight,
    up_weight,
    down_weight,
):
    plane = lax.axis_size("ctx")
    line = lax.axis_size("fsdp")
    rows, model = block_input.shape[1:]
    shard = model // line
    hidden = gate_weight.shape[1]
    unit = hidden // (line * plane)
    table_row = block_table[0]
    slot_count = table_row.shape[0]
    block = rows * plane // slot_count
    places = jnp.arange(slot_count, dtype=jnp.int32)
    slots = jnp.sum(jnp.where(table_row[None, :] == places[:, None], places[None, :], 0), axis=1)

    query_width = query_weight.shape[1] // plane
    key_width = key_weight.shape[1] // plane
    gains_mine = jnp.stack([attention_gain, feedforward_gain])
    x_all, qkv_w, wo_line, gains, feed_mine = first_exchange(
        line,
        block_input[0],
        (query_weight, key_weight, value_projection),
        output_weight,
        gains_mine,
        gate_weight,
        up_weight,
        down_weight,
    )
    feed_w = lax.all_gather(feed_mine, "fsdp", axis=0, tiled=True)

    inner = angle_table(np.arange(block))
    outer = angle_table(np.arange(slot_count) * block)
    pad = padding(GROUP + 2)

    gains = jnp.transpose(gains, (1, 0, 2)).reshape(2, model).astype(jnp.float32)
    qkv_w = qkv_w.reshape(model, -1)
    grad_rows, wo_line, x_all = lax.optimization_barrier((output_grad[0], wo_line, x_all))
    grad_parts, wo_parts = [grad_rows], [wo_line]
    for bit in (2, 4):
        pairs = [(device, device ^ bit) for device in range(plane)]
        grad_parts.append(lax.ppermute(grad_rows, "ctx", pairs))
        wo_parts.append(lax.ppermute(wo_line, "ctx", pairs))
    qkv, o, o_columns, lse, qkv_pad = attend(
        slots, x_all, gains[:1], qkv_w, pad, inner, outer
    )
    wo_mine, far_grads, residual, normed_two, scale_two, *gained_two = second_exchange(
        o, wo_parts, grad_parts[1:], block_input[0], gains[1:]
    )
    grad_residual, feedforward_term, *rest = feed(
        gained_two,
        [*grad_parts, far_grads],
        feed_w,
        o_columns,
        normed_two,
        scale_two,
        gains[1:],
    )
    grad_attn, columns_mine, out_parts, feed_grads = rest[:3], rest[3], rest[4:8], rest[8]
    feed_grads = lax.psum_scatter(feed_grads, "fsdp", scatter_dimension=0, tiled=True)
    grad_o, wo_term = third_exchange(
        line,
        grad_attn,
        columns_mine.reshape(-1, columns_mine.shape[2]),
        wo_mine.reshape(-1, model),
        qkv_w.shape[1],
    )
    *out_parts, grad_o = lax.optimization_barrier((*out_parts, grad_o))
    outs = [out_parts[3]]
    for part, bit in enumerate((6, 2, 4)):
        pairs = [(device, device ^ bit) for device in range(plane)]
        outs.append(lax.ppermute(out_parts[part], "ctx", pairs))
    grads = attend_back(slots, qkv, o, grad_o, lse, pad, inner, outer)
    input_grad, attention_grads = input_exchange(
        grads, qkv_pad, x_all, grad_residual, wo_term, feedforward_term, gains[:1], pad
    )
    attention_grads, feed_grads = lax.optimization_barrier((attention_grads, feed_grads))
    attention_grads = lax.psum_scatter(
        attention_grads.reshape(-1, attention_grads.shape[2]),
        "fsdp",
        scatter_dimension=0,
        tiled=True,
    )
    feed_pieces, layer_output = pieces_exchange(feed_grads, residual, outs)
    attention_grads, layer_output = lax.optimization_barrier((attention_grads, layer_output))
    near_grads = []
    for bit in (2, 4):
        pairs = [(device, device ^ bit) for device in range(plane)]
        near_grads.append(lax.ppermute(attention_grads, "ctx", pairs))
    gate_grad, up_grad, down_grad = spread_feed(feed_pieces, shard, line, unit)
    attention_pieces = near_gather([attention_grads, *near_grads], 9)
    query_grad, key_grad, value_grad, out_grad, gain_terms = spread_attention(
        attention_pieces, shard, model, query_width, key_width
    )
    return (
        layer_output,
        input_grad,
        gain_terms[0],
        query_grad,
        key_grad,
        value_grad,
        out_grad,
        gain_terms[1],
        gate_grad,
        up_grad,
        down_grad,
    )


def solution(mesh):
    plane, line = mesh.shape["ctx"], mesh.shape["fsdp"]
    fits = plane == KEY_VALUE_HEADS == 8 and plane * line * HALF == QUERY_HEADS * HEAD_SIZE
    if fits:
        return placed(mesh, head_local)
    return placed(mesh, local)


def placed(mesh, plan):
    return jax.shard_map(
        plan,
        mesh=mesh,
        in_specs=(
            P("fsdp", "ctx", None),
            P("fsdp", None),
            P("fsdp", "ctx", None),
            P("fsdp"),
            P("fsdp", None),
            P("fsdp", None),
            P("fsdp", None),
            P("fsdp", None),
            P("fsdp"),
            P("fsdp", None),
            P("fsdp", None),
            P("fsdp", None),
        ),
        out_specs=(
            P("fsdp", "ctx", None),
            P("fsdp", "ctx", None),
            P("fsdp"),
            P("fsdp", None),
            P("fsdp", None),
            P("fsdp", None),
            P("fsdp", None),
            P("fsdp"),
            P("fsdp", None),
            P("fsdp", None),
            P("fsdp", None),
        ),
        check_vma=False,
    )
```
